32 devices in a mesh: col: 4 (over z), row: 8 (over y, x, core).
Axes of the slice: x: 2, y: 2, z: 4, core: 2. Of those that a mesh axis runs over, the one named last changes fastest.
Arguments:
- vel_x: float32 [75, 2, 128, 768], P(None, None, 'row', 'col')
- vel_y: float32 [75, 2, 128, 768], P(None, None, 'row', 'col')
- pot_temp: float32 [75, 2, 128, 768], P(None, None, 'row', 'col')
- salinity: float32 [75, 2, 128, 768], P(None, None, 'row', 'col')
- surf_eta: float32 [2, 128, 768], P(None, 'row', 'col')
- trans_x: float32 [2, 128, 768], P(None, 'row', 'col')
- trans_y: float32 [2, 128, 768], P(None, 'row', 'col')
- col_depth: float32 [128, 768], P('row', 'col')
- wet_levels: int32 [128, 768], P('row', 'col')
- avg_weights: float32 [30], replicated
Outputs:
- output 1: float32 [2, 128, 768], P(None, 'row', 'col')
- output 2: float32 [2, 128, 768], P(None, 'row', 'col')
- output 3: float32 [2, 128, 768], P(None, 'row', 'col')
- output 4: float32 [75, 2, 128, 768], P(None, None, 'row', 'col')
- output 5: float32 [75, 2, 128, 768], P(None, None, 'row', 'col')
- output 6: float32 [75, 2, 128, 768], P(None, None, 'row', 'col')
- output 7: float32 [75, 2, 128, 768], P(None, None, 'row', 'col')
All inputs are finite; a program needn't handle non-finite values.
Results may differ from the reference program's by a relative error of at most 0.001.
Values sent between devices are 32-bit elements.
A program may use at most 1 GiB of HBM per device.

```python
import jax
import jax.numpy as jnp
from jax import lax

MEMBERS = 2
LEVELS = 75
SUBCYCLES = 30
GRID_Y = 128
GRID_X = 768

WAVE_COURANT = 0.4
THERM_EXP = 0.2
HALINE_CON = 0.15
PRESS_SCALE = 0.5
VISC_NUMBER = 1.0
DIFF_NUMBER = 0.5


def east_of(field_in):
    return jnp.roll(field_in, -1, axis=-1)


def west_of(field_in):
    return jnp.roll(field_in, 1, axis=-1)


def north_of(field_in):
    return jnp.concatenate([field_in[..., 1:, :], jnp.zeros_like(field_in[..., :1, :])], axis=-2)


def south_of(field_in):
    return jnp.concatenate([jnp.zeros_like(field_in[..., :1, :]), field_in[..., :-1, :]], axis=-2)


def wet_masks(wet_levels, level_total):
    levels = jnp.arange(level_total).reshape(level_total, 1, 1, 1)
    cell_mask = (levels < wet_levels).astype(jnp.float32)
    xface_mask = cell_mask * (levels < east_of(wet_levels)).astype(jnp.float32)
    yface_mask = cell_mask * (levels < north_of(wet_levels)).astype(jnp.float32)
    return cell_mask, xface_mask, yface_mask


def setup_inputs(seed: int = 0) -> dict:
    key_list = jax.random.split(jax.random.key(seed), 12)
    shape_3d = (LEVELS, MEMBERS, GRID_Y, GRID_X)
    shape_2d = (MEMBERS, GRID_Y, GRID_X)
    land_draw = jax.random.randint(key_list[0], (GRID_Y, GRID_X), 0, 10)
    depth_draw = jax.random.randint(key_list[1], (GRID_Y, GRID_X), 1, LEVELS + 1)
    wet_levels = jnp.where(land_draw == 0, 0, jnp.where(land_draw < 5, LEVELS, depth_draw)).astype(jnp.int32)
    cell_mask, xface_mask, yface_mask = wet_masks(wet_levels, LEVELS)
    profile = jnp.cos(jnp.pi * (jnp.arange(LEVELS) + 0.5) / LEVELS).reshape(LEVELS, 1, 1, 1)

    def tracer_field(key_pair):
        key_a, key_b, key_c = jax.random.split(key_pair, 3)
        base_field = jax.random.normal(key_a, shape_2d, jnp.float32)
        mode_field = jax.random.normal(key_b, shape_2d, jnp.float32)
        noise_3d = jax.random.normal(key_c, shape_3d, jnp.float32)
        return cell_mask * (base_field + mode_field * profile + 0.3 * noise_3d)

    vel_x = xface_mask * 0.3 * jax.random.normal(key_list[2], shape_3d, jnp.float32)
    vel_y = yface_mask * 0.3 * jax.random.normal(key_list[3], shape_3d, jnp.float32)
    pot_temp = tracer_field(key_list[4])
    salinity = tracer_field(key_list[5])
    surf_eta = cell_mask[0] * 0.3 * jax.random.normal(key_list[6], shape_2d, jnp.float32)
    trans_x = xface_mask[0] * 0.3 * jax.random.normal(key_list[7], shape_2d, jnp.float32)
    trans_y = yface_mask[0] * 0.3 * jax.random.normal(key_list[8], shape_2d, jnp.float32)
    col_depth = 0.5 + 1.5 * jax.random.uniform(key_list[9], (GRID_Y, GRID_X), jnp.float32)
    step_frac = (jnp.arange(SUBCYCLES) + 1.0) / SUBCYCLES
    raw_weights = step_frac * step_frac * (2.0 - step_frac * step_frac) * (0.3 + 1.4 * jax.random.uniform(key_list[10], (SUBCYCLES,), jnp.float32))
    avg_weights = raw_weights / jnp.sum(raw_weights)
    return {"vel_x": vel_x, "vel_y": vel_y, "pot_temp": pot_temp, "salinity": salinity, "surf_eta": surf_eta, "trans_x": trans_x, "trans_y": trans_y, "col_depth": col_depth, "wet_levels": wet_levels, "avg_weights": avg_weights}


def vertical_solve(right_side, face_mask, strength):
    mask_below = jnp.concatenate([face_mask[1:], jnp.zeros_like(face_mask[:1])], axis=0)
    face_up = face_mask * mask_below
    face_down = jnp.concatenate([jnp.zeros_like(face_up[:1]), face_up[:-1]], axis=0)
    lower_diag = -strength * face_down
    upper_diag = -strength * face_up
    main_diag = 1.0 + strength * (face_down + face_up)

    def forward(state_prev, level_row):
        upper_prev, side_prev = state_prev
        low_k, diag_k, up_k, side_k = level_row
        divisor = diag_k - low_k * upper_prev
        upper_new = up_k / divisor
        side_new = (side_k - low_k * side_prev) / divisor
        return (upper_new, side_new), (upper_new, side_new)

    zero_level = jnp.zeros_like(right_side[0])
    upper_all, side_all = lax.scan(forward, (zero_level, zero_level), (lower_diag, main_diag, upper_diag, right_side))[1]

    def backward(sol_next, level_row):
        up_k, side_k = level_row
        sol_k = side_k - up_k * sol_next
        return sol_k, sol_k

    return lax.scan(backward, zero_level, (upper_all, side_all), reverse=True)[1]


def tracer_step(tracer, vel_x, vel_y, cell_mask):
    flux_x = vel_x * 0.5 * (tracer + east_of(tracer))
    flux_y = vel_y * 0.5 * (tracer + north_of(tracer))
    advected = cell_mask * (tracer - (flux_x - west_of(flux_x) + flux_y - south_of(flux_y)))
    return vertical_solve(advected, cell_mask, DIFF_NUMBER)


def barotropic(surf_eta, trans_x, trans_y, force_x, force_y, depth_x, depth_y, wet_top, xface_top, yface_top, avg_weights):
    sub_count = avg_weights.shape[0]
    step_x = force_x / sub_count
    step_y = force_y / sub_count

    def subcycle(sub_state, weight):
        eta_now, tx_now, ty_now, eta_avg, tx_avg, ty_avg = sub_state
        eta_now = wet_top * (eta_now - WAVE_COURANT * (tx_now - west_of(tx_now) + ty_now - south_of(ty_now)))
        tx_now = xface_top * (tx_now + step_x - WAVE_COURANT * depth_x * (east_of(eta_now) - eta_now))
        ty_now = yface_top * (ty_now + step_y - WAVE_COURANT * depth_y * (north_of(eta_now) - eta_now))
        return (eta_now, tx_now, ty_now, eta_avg + weight * eta_now, tx_avg + weight * tx_now, ty_avg + weight * ty_now), None

    zero_field = jnp.zeros_like(surf_eta)
    end_state = lax.scan(subcycle, (surf_eta, trans_x, trans_y, zero_field, zero_field, zero_field), avg_weights)[0]
    return end_state[3], end_state[4], end_state[5]


def reference(vel_x, vel_y, pot_temp, salinity, surf_eta, trans_x, trans_y, col_depth, wet_levels, avg_weights):
    level_count = vel_x.shape[0]
    cell_mask, xface_mask, yface_mask = wet_masks(wet_levels, level_count)
    density = HALINE_CON * salinity - THERM_EXP * pot_temp
    pressure = (PRESS_SCALE / level_count) * (jnp.cumsum(density, axis=0) - 0.5 * density)
    vy_south = south_of(vel_y)
    vx_north = north_of(vel_x)
    vy_at_x = 0.25 * (vel_y + vy_south + east_of(vel_y) + east_of(vy_south))
    vx_at_y = 0.25 * (vel_x + west_of(vel_x) + vx_north + west_of(vx_north))
    tend_x = xface_mask * (pressure - east_of(pressure) - 0.5 * vel_x * (east_of(vel_x) - west_of(vel_x)) - 0.5 * vy_at_x * (vx_north - south_of(vel_x)))
    tend_y = yface_mask * (pressure - north_of(pressure) - 0.5 * vx_at_y * (east_of(vel_y) - west_of(vel_y)) - 0.5 * vel_y * (north_of(vel_y) - vy_south))
    count_x = jnp.maximum(jnp.sum(xface_mask, axis=0), 1.0)
    count_y = jnp.maximum(jnp.sum(yface_mask, axis=0), 1.0)
    depth_x = 0.5 * (col_depth + east_of(col_depth)) * xface_mask[0]
    depth_y = 0.5 * (col_depth + north_of(col_depth)) * yface_mask[0]
    force_x = depth_x * jnp.sum(tend_x, axis=0) / count_x
    force_y = depth_y * jnp.sum(tend_y, axis=0) / count_y
    pred_x = vertical_solve(vel_x + tend_x, xface_mask, VISC_NUMBER)
    pred_y = vertical_solve(vel_y + tend_y, yface_mask, VISC_NUMBER)
    temp_new = tracer_step(pot_temp, vel_x, vel_y, cell_mask)
    salt_new = tracer_step(salinity, vel_x, vel_y, cell_mask)
    eta_new, trans_x_new, trans_y_new = barotropic(surf_eta, trans_x, trans_y, force_x, force_y, depth_x, depth_y, cell_mask[0], xface_mask[0], yface_mask[0], avg_weights)
    vel_x_new = xface_mask * (pred_x - jnp.sum(pred_x, axis=0) / count_x + trans_x_new / (depth_x + 1.0 - xface_mask[0]))
    vel_y_new = yface_mask * (pred_y - jnp.sum(pred_y, axis=0) / count_y + trans_y_new / (depth_y + 1.0 - yface_mask[0]))
    return eta_new, trans_x_new, trans_y_new, vel_x_new, vel_y_new, temp_new, salt_new
```

```python
import functools
import numpy as np
import jax
import jax.numpy as jnp
from jax import lax
from jax.experimental import pallas as pl
from jax.experimental.pallas import tpu as pltpu
from jax.sharding import PartitionSpec as P

WAVE_COURANT = 0.4
THERM_EXP = 0.2
HALINE_CON = 0.15
PRESS_SCALE = 0.5
VISC_NUMBER = 1.0
DIFF_NUMBER = 0.5
SUBCYCLES = 30
HALO = 32
ROWS, WIDTH, PADDED, LANES = 16, 192, 256, 128
MESH = pl.DeviceIdType.MESH
F32 = jnp.float32


def solve_tables(level_count):
    rows = []
    for strength in (VISC_NUMBER, DIFF_NUMBER):
        inner, last = np.zeros(level_count), np.zeros(level_count)
        inner[0], last[0] = 1.0 + strength, 1.0
        for k in range(1, level_count):
            inner[k] = 1.0 + 2.0 * strength - strength * strength / inner[k - 1]
            last[k] = 1.0 + strength - strength * strength / inner[k - 1]
        rows += [1.0 / inner, 1.0 / last, strength / inner]
    return np.concatenate(rows).astype(np.float32)


def level_chunk(level_count):
    for size in (15, 5, 4, 3, 2):
        if level_count % size == 0:
            return size
    return 1


def step_kernel(
    row_count, col_count, level_count,
    table, weights, kmt_in, depth_in, eta_in, tx_in, ty_in, u_hbm, v_hbm, t_hbm, s_hbm,
    pu, pv, pt, ps, corr, faces, avg,
    ub, vb, tb, sb, rows_n, rows_s, kmt_n, pack_w, pack_e, col_e, col_w, corner_se, corner_nw,
    edge_e, edge_w, wide, fedge_e, fedge_w, wide_f, coef,
    load_sem, row_send, row_recv, misc_send, misc_recv, wide_send, wide_recv,
):
    K = level_count
    size = level_chunk(K)
    chunks = K // size
    r = lax.axis_index("row")
    c = lax.axis_index("col")
    east = lax.rem(c + 1, col_count)
    west = lax.rem(c + col_count - 1, col_count)
    has_n, has_s = r < row_count - 1, r > 0
    has_nn, has_ss = r < row_count - 2, r > 1
    fields_hbm = (u_hbm, v_hbm, t_hbm, s_hbm)
    fields = (ub, vb, tb, sb)

    loads = [pltpu.make_async_copy(src, dst, load_sem.at[i]) for i, (src, dst) in enumerate(zip(fields_hbm, fields))]
    for copy in loads:
        copy.start()

    wide[...] = jnp.zeros_like(wide)
    wide_f[...] = jnp.zeros_like(wide_f)

    @pl.when(jnp.logical_not(has_n))
    def _():
        rows_n[...] = jnp.zeros_like(rows_n)
        kmt_n[...] = jnp.zeros_like(kmt_n)
        corner_nw[...] = jnp.zeros_like(corner_nw)

    @pl.when(jnp.logical_not(has_s))
    def _():
        rows_s[...] = jnp.zeros_like(rows_s)
        corner_se[...] = jnp.zeros_like(corner_se)

    barrier = pltpu.get_barrier_semaphore()

    def signal(**where):
        pl.semaphore_signal(barrier, inc=1, device_id=where, device_id_type=MESH)

    signal(col=east)
    signal(col=west)

    @pl.when(has_n)
    def _():
        signal(row=r + 1)
        signal(row=r + 1, col=west)

    @pl.when(has_s)
    def _():
        signal(row=r - 1)
        signal(row=r - 1, col=east)

    @pl.when(has_nn)
    def _():
        signal(row=r + 2)

    @pl.when(has_ss)
    def _():
        signal(row=r - 2)

    def one(flag):
        return flag.astype(jnp.int32)

    pl.semaphore_wait(barrier, 2 + 2 * one(has_n) + 2 * one(has_s) + one(has_nn) + one(has_ss))

    def remote(src, dst, ssem, rsem, **where):
        return pltpu.make_async_remote_copy(src_ref=src, dst_ref=dst, send_sem=ssem, recv_sem=rsem, device_id=where, device_id_type=MESH)

    kmt_copy = remote(kmt_in.at[0:1, :], kmt_n, misc_send.at[4], misc_recv.at[4], row=r - 1)

    def row_copy(side, i, f):
        levels = pl.ds(i * size, size)
        if side == 0:
            return remote(fields_hbm[f].at[levels, :, 0, :], rows_n.at[levels, 2 * f:2 * f + 2, :], row_send.at[0, i, f], row_recv.at[0, i, f], row=r - 1)
        return remote(fields_hbm[f].at[levels, :, 15, :], rows_s.at[levels, 2 * f:2 * f + 2, :], row_send.at[1, i, f], row_recv.at[1, i, f], row=r + 1)

    @pl.when(has_s)
    def _():
        kmt_copy.start()

    for i in range(chunks):
        @pl.when(has_s)
        def _():
            for f in range(4):
                row_copy(0, i, f).start()

        @pl.when(has_n)
        def _():
            for f in range(2):
                row_copy(1, i, f).start()

    @pl.when(has_n)
    def _():
        for i in range(chunks):
            for f in (2, 3):
                row_copy(1, i, f).start()

    lane = lax.broadcasted_iota(jnp.int32, (ROWS, LANES), 1)
    lane1 = lax.broadcasted_iota(jnp.int32, (1, LANES), 1)
    lane_all = lax.broadcasted_iota(jnp.int32, (ROWS, PADDED), 1)
    row_id = lax.broadcasted_iota(jnp.int32, (ROWS, PADDED), 0)

    def padded(x):
        return jnp.concatenate([x, jnp.zeros((x.shape[0], 64), x.dtype)], axis=1)

    kmt = padded(kmt_in[...]).astype(F32)
    own = pl.ds(HALO, ROWS)
    wide[0, own, :] = jnp.where(kmt > 0.5, padded(depth_in[...]), 0.0)
    for m in range(2):
        wide[1 + m, own, :] = padded(eta_in[m])
        wide[3 + m, own, :] = padded(tx_in[m])
        wide[5 + m, own, :] = padded(ty_in[m])

    edge_copies = [
        remote(wide.at[:, own, 0:LANES], edge_e, misc_send.at[5], misc_recv.at[5], col=west),
        remote(wide.at[:, own, LANES:PADDED], edge_w, misc_send.at[6], misc_recv.at[6], col=east),
    ]

    for copy in loads:
        copy.wait()
    for copy in edge_copies:
        copy.start()

    for f in range(4):
        def gather(k, acc):
            out = []
            for m in range(2):
                a = fields[f][k, m, :, 0:LANES]
                b = padded(fields[f][k, m, :, LANES:WIDTH])
                out.append(jnp.where(lane == k, pltpu.roll(a, k, 1), acc[2 * m]))
                out.append(jnp.where(lane == k, pltpu.roll(b, lax.rem(k + 65, LANES), 1), acc[2 * m + 1]))
            return tuple(out)

        zero = jnp.zeros((ROWS, LANES), F32)
        acc = lax.fori_loop(0, K, gather, (zero,) * 4, unroll=5)
        for m in range(2):
            pack_w[f, m] = acc[2 * m] if (f, m) != (0, 0) else jnp.where(lane == 127, pltpu.roll(kmt[:, 0:LANES], 127, 1), acc[0])
            pack_e[f, m] = acc[2 * m + 1]

    pack_copies = [
        remote(pack_w, col_e, misc_send.at[0], misc_recv.at[0], col=west),
        remote(pack_e, col_w, misc_send.at[1], misc_recv.at[1], col=east),
    ]
    for copy in pack_copies:
        copy.start()
    corner_v = remote(pack_w.at[1, :, 8:ROWS, :], corner_se, misc_send.at[2], misc_recv.at[2], row=r + 1, col=west)
    corner_u = remote(pack_e.at[0, :, 0:8, :], corner_nw, misc_send.at[3], misc_recv.at[3], row=r - 1, col=east)

    @pl.when(has_n)
    def _():
        corner_v.start()

    @pl.when(has_s)
    def _():
        corner_u.start()

    def with_edges(x, from_east, from_west):
        b = jnp.where(lane < 64, x[:, LANES:PADDED], jnp.where(lane < 96, pltpu.roll(from_east, 64, 1), pltpu.roll(from_west, 64, 1)))
        return jnp.concatenate([x[:, 0:LANES], b], axis=1)

    def spread(buf, first_sem):
        src = buf.at[:, own, :]
        return (
            (has_n, remote(src, buf.at[:, pl.ds(ROWS, ROWS), :], wide_send.at[first_sem], wide_recv.at[first_sem], row=r + 1)),
            (has_s, remote(src, buf.at[:, pl.ds(48, ROWS), :], wide_send.at[first_sem + 1], wide_recv.at[first_sem + 1], row=r - 1)),
            (has_nn, remote(src, buf.at[:, pl.ds(0, ROWS), :], wide_send.at[first_sem + 2], wide_recv.at[first_sem + 2], row=r + 2)),
            (has_ss, remote(src, buf.at[:, pl.ds(64, ROWS), :], wide_send.at[first_sem + 3], wide_recv.at[first_sem + 3], row=r - 2)),
        )

    def start_spread(copies):
        for there, copy in copies:
            @pl.when(there)
            def _():
                copy.start()

    def finish_spread(copies):
        arrives = (has_s, has_n, has_ss, has_nn)
        for (there, copy), here in zip(copies, arrives):
            @pl.when(there)
            def _():
                copy.wait_send()

            @pl.when(here)
            def _():
                copy.wait_recv()

    for copy in edge_copies:
        copy.wait()
    for p in range(7):
        wide[p, own, :] = with_edges(wide[p, own, :], edge_e[p], edge_w[p])
    static_copies = spread(wide, 0)
    start_spread(static_copies)

    for copy in pack_copies:
        copy.wait()

    @pl.when(has_n)
    def _():
        corner_v.wait_send()
        kmt_copy.wait_recv()
        corner_u.wait_recv()

    @pl.when(has_s)
    def _():
        corner_u.wait_send()
        kmt_copy.wait_send()
        corner_v.wait_recv()

    def roll_e(x):
        return pltpu.roll(x, 255, 1)

    def roll_w(x):
        return pltpu.roll(x, 1, 1)

    def from_north(x, edge):
        return jnp.where(row_id == 15, edge, pltpu.roll(x, 15, 0))

    def from_south(x, edge):
        return jnp.where(row_id == 0, edge, pltpu.roll(x, 1, 0))

    kmt_east = jnp.where(lane_all == 191, jnp.concatenate([lane.astype(F32), pltpu.roll(col_e[0, 0], 64, 1)], axis=1), roll_e(kmt))
    kmt_north = from_north(kmt, padded(kmt_n[...]).astype(F32))
    in_block = lane_all < WIDTH
    kmt_cell = jnp.where(in_block, kmt, 0.0)
    mu = jnp.where(in_block, jnp.minimum(kmt, kmt_east), 0.0)
    mv = jnp.where(in_block, jnp.minimum(kmt, kmt_north), 0.0)
    faces[0] = mu
    faces[1] = mv
    faces[2] = kmt_cell

    def extended(f, k, m):
        b = padded(fields[f][k, m, :, LANES:WIDTH])
        to_east = pltpu.roll(col_e[f, m], lax.rem(WIDTH - k, LANES), 1)
        to_west = pltpu.roll(col_w[f, m], lax.rem(255 - k, LANES), 1)
        b = jnp.where(lane < 64, b, jnp.where(lane == 64, to_east, to_west))
        return jnp.concatenate([fields[f][k, m, :, 0:LANES], b], axis=1)

    def edge_row(rows, f, k, m):
        return padded(rows[k, pl.ds(2 * f + m, 1), :])

    def solve_factor(depth, k, first):
        inner, last = table[first * K + k], table[(first + 1) * K + k]
        kf = k.astype(F32)
        return jnp.where(depth > kf + 1.0, inner, jnp.where(depth > kf, last, 0.0))

    scale = PRESS_SCALE / K

    def momentum(k, carry):
        out = []
        kf = k.astype(F32)
        for m in range(2):
            total, total_n, gu_sum, gv_sum, side_u, side_v = carry[m]
            u, v = extended(0, k, m), extended(1, k, m)
            t, s = extended(2, k, m), extended(3, k, m)
            density = HALINE_CON * s - THERM_EXP * t
            total = total + density
            pressure = scale * (total - 0.5 * density)
            density_n = HALINE_CON * edge_row(rows_n, 3, k, m) - THERM_EXP * edge_row(rows_n, 2, k, m)
            total_n = total_n + density_n
            pressure_n = scale * (total_n - 0.5 * density_n)
            un_edge = edge_row(rows_n, 0, k, m)
            nw = pltpu.roll(corner_nw[m], lax.rem(255 - k, LANES), 1)[0:1, :]
            un_edge = jnp.concatenate([un_edge[:, 0:LANES], jnp.where(lane1 == 127, nw, un_edge[:, LANES:PADDED])], axis=1)
            vs_edge = edge_row(rows_s, 1, k, m)
            se = pltpu.roll(corner_se[m], lax.rem(WIDTH - k, LANES), 1)[7:8, :]
            vs_edge = jnp.concatenate([vs_edge[:, 0:LANES], jnp.where(lane1 == 64, se, vs_edge[:, LANES:PADDED])], axis=1)
            u_n, u_s = from_north(u, un_edge), from_south(u, edge_row(rows_s, 0, k, m))
            v_n, v_s = from_north(v, edge_row(rows_n, 1, k, m)), from_south(v, vs_edge)
            p_n = from_north(pressure, pressure_n)
            v_pair = v + v_s
            u_pair = u + u_n
            vu = 0.125 * (v_pair + roll_e(v_pair))
            uv = 0.125 * (u_pair + roll_w(u_pair))
            gu = pressure - roll_e(pressure) - 0.5 * u * (roll_e(u) - roll_w(u)) - vu * (u_n - u_s)
            gv = pressure - p_n - uv * (roll_e(v) - roll_w(v)) - 0.5 * v * (v_n - v_s)
            gu = jnp.where(mu > kf, gu, 0.0)
            gv = jnp.where(mv > kf, gv, 0.0)
            side_u = (u + gu + VISC_NUMBER * side_u) * solve_factor(mu, k, 0)
            side_v = (v + gv + VISC_NUMBER * side_v) * solve_factor(mv, k, 0)
            pu[k, m] = side_u[:, 0:WIDTH]
            pv[k, m] = side_v[:, 0:WIDTH]
            out.append((total, total_n, gu_sum + gu, gv_sum + gv, side_u, side_v))
        return tuple(out)

    zero = jnp.zeros((ROWS, PADDED), F32)
    zero_row = jnp.zeros((1, PADDED), F32)
    carry = ((zero, zero_row, zero, zero, zero, zero),) * 2
    for i in range(chunks):
        @pl.when(has_n)
        def _():
            for f in range(4):
                row_copy(0, i, f).wait_recv()

        @pl.when(has_s)
        def _():
            for f in range(2):
                row_copy(1, i, f).wait_recv()

        carry = lax.fori_loop(i * size, (i + 1) * size, momentum, carry)

    count_u = jnp.maximum(mu, 1.0)
    count_v = jnp.maximum(mv, 1.0)
    for m in range(2):
        wide_f[m, own, :] = carry[m][2] / count_u
        wide_f[2 + m, own, :] = carry[m][3] / count_v
    force_edges = [
        remote(wide_f.at[:, own, 0:LANES], fedge_e, misc_send.at[7], misc_recv.at[7], col=west),
        remote(wide_f.at[:, own, LANES:PADDED], fedge_w, misc_send.at[8], misc_recv.at[8], col=east),
    ]
    for copy in force_edges:
        copy.start()

    @pl.when(has_s)
    def _():
        for i in range(chunks):
            for f in (2, 3):
                row_copy(1, i, f).wait_recv()

    def tracer(f, dest):
        def level(k, carry):
            out = []
            kf = k.astype(F32)
            factor = solve_factor(kmt_cell, k, 3)
            for m in range(2):
                u, v, t = extended(0, k, m), extended(1, k, m), extended(f, k, m)
                t_n = from_north(t, edge_row(rows_n, f, k, m))
                flux_x = 0.5 * u * (t + roll_e(t))
                flux_y = 0.5 * v * (t + t_n)
                flux_s = 0.5 * edge_row(rows_s, 1, k, m) * (edge_row(rows_s, f, k, m) + t[0:1, :])
                moved = t - (flux_x - roll_w(flux_x) + flux_y - from_south(flux_y, flux_s))
                side = (moved + DIFF_NUMBER * carry[m]) * factor
                dest[k, m] = side[:, 0:WIDTH]
                out.append(side)
            return tuple(out)

        last = lax.fori_loop(0, K, level, (zero, zero))

        def back(j, carry):
            k = K - 2 - j
            ratio = table[5 * K + k]
            out = []
            for m in range(2):
                x = dest[k, m] + ratio * carry[m]
                dest[k, m] = x
                out.append(x)
            return tuple(out)

        lax.fori_loop(0, K - 1, back, tuple(x[:, 0:WIDTH] for x in last))

    tracer(2, pt)

    for copy in force_edges:
        copy.wait()
    for p in range(4):
        wide_f[p, own, :] = with_edges(wide_f[p, own, :], fedge_e[p], fedge_w[p])
    force_copies = spread(wide_f, 4)
    start_spread(force_copies)

    tracer(3, ps)

    def back(j, carry):
        k = K - 2 - j
        ratio = table[2 * K + k]
        out = []
        for m in range(2):
            xu, xv, su, sv = carry[m]
            xu = pu[k, m] + ratio * xu
            xv = pv[k, m] + ratio * xv
            pu[k, m] = xu
            pv[k, m] = xv
            out.append((xu, xv, su + xu, sv + xv))
        return tuple(out)

    start = tuple(tuple(carry[m][i][:, 0:WIDTH] for i in (4, 5, 4, 5)) for m in range(2))
    ends = lax.fori_loop(0, K - 1, back, start)

    finish_spread(static_copies)
    finish_spread(force_copies)

    depth = wide[0]
    depth_e = pltpu.roll(depth, 255, 1)
    depth_n = pltpu.roll(depth, 79, 0)
    hu = jnp.where((depth > 0.0) & (depth_e > 0.0), 0.5 * (depth + depth_e), 0.0)
    hv = jnp.where((depth > 0.0) & (depth_n > 0.0), 0.5 * (depth + depth_n), 0.0)
    coef[0] = WAVE_COURANT * hu
    coef[1] = WAVE_COURANT * hv
    for m in range(2):
        wide_f[m] = hu * wide_f[m] * (1.0 / SUBCYCLES)
        wide_f[2 + m] = hv * wide_f[2 + m] * (1.0 / SUBCYCLES)
        for p in range(3):
            avg[2 * p + m] = zero

    def subcycle(n, _):
        weight = weights[n]
        for m in range(2):
            eta, tx, ty = wide[1 + m], wide[3 + m], wide[5 + m]
            eta = eta - WAVE_COURANT * (tx - pltpu.roll(tx, 1, 1) + ty - pltpu.roll(ty, 1, 0))
            tx = tx + wide_f[m] - coef[0] * (pltpu.roll(eta, 255, 1) - eta)
            ty = ty + wide_f[2 + m] - coef[1] * (pltpu.roll(eta, 79, 0) - eta)
            wide[1 + m] = eta
            wide[3 + m] = tx
            wide[5 + m] = ty
            mine = slice(HALO, HALO + ROWS)
            avg[m] = avg[m] + weight * eta[mine]
            avg[2 + m] = avg[2 + m] + weight * tx[mine]
            avg[4 + m] = avg[4 + m] + weight * ty[mine]
        return 0

    lax.fori_loop(0, SUBCYCLES, subcycle, 0)

    mine = slice(HALO, HALO + ROWS)
    for m in range(2):
        corr[m] = avg[2 + m] / jnp.where(mu > 0.5, hu[mine], 1.0) - padded(ends[m][2]) / count_u
        corr[2 + m] = avg[4 + m] / jnp.where(mv > 0.5, hv[mine], 1.0) - padded(ends[m][3]) / count_v

    @pl.when(has_s)
    def _():
        for i in range(chunks):
            for f in range(4):
                row_copy(0, i, f).wait_send()

    @pl.when(has_n)
    def _():
        for i in range(chunks):
            for f in range(4):
                row_copy(1, i, f).wait_send()


def finish_kernel(size, pu, pv, pt, ps, corr, faces, avg, eta_o, tx_o, ty_o, u_o, v_o, t_o, s_o, sems):
    first = pl.program_id(0) * size
    through = [pltpu.make_async_copy(src, dst, sems.at[i]) for i, (src, dst) in enumerate(((pt, t_o), (ps, s_o)))]

    @pl.when(first == 0)
    def _():
        for copy in through:
            copy.start()
        for m in range(2):
            eta_o[m] = avg[m][:, 0:WIDTH]
            tx_o[m] = avg[2 + m][:, 0:WIDTH]
            ty_o[m] = avg[4 + m][:, 0:WIDTH]

    for j in range(size):
        level = (first + j).astype(F32)
        for m in range(2):
            for face, (src, dst) in enumerate(((pu, u_o), (pv, v_o))):
                wet = faces[face][:, 0:WIDTH] > level
                dst[j, m] = jnp.where(wet, src[first + j, m] + corr[2 * face + m][:, 0:WIDTH], 0.0)

    @pl.when(pl.program_id(0) == pl.num_programs(0) - 1)
    def _():
        for copy in through:
            copy.wait()


def solution(mesh):
    col_count, row_count = mesh.shape["col"], mesh.shape["row"]

    def local_step(vel_x, vel_y, pot_temp, salinity, surf_eta, trans_x, trans_y, col_depth, wet_levels, avg_weights):
        K = vel_x.shape[0]
        size = level_chunk(K)
        chunks = K // size
        table = jnp.asarray(solve_tables(K))
        smem = pl.BlockSpec(memory_space=pltpu.SMEM)
        vmem = pl.BlockSpec(memory_space=pltpu.VMEM)
        hbm = pl.BlockSpec(memory_space=pl.ANY)
        full = jax.ShapeDtypeStruct((K, 2, ROWS, WIDTH), F32)
        held = pltpu.VMEM((K, 2, ROWS, WIDTH), F32)
        dma = pltpu.SemaphoreType.DMA
        outs = pl.pallas_call(
            functools.partial(step_kernel, row_count, col_count, K),
            out_shape=(held,) * 4 + tuple(pltpu.VMEM((n, ROWS, PADDED), F32) for n in (4, 3, 6)),
            in_specs=[smem, smem] + [vmem] * 5 + [hbm] * 4,
            out_specs=(vmem,) * 7,
            scratch_shapes=[
                *[pltpu.VMEM((K, 2, ROWS, WIDTH), F32)] * 4,
                *[pltpu.VMEM((K, 8, WIDTH), F32)] * 2,
                pltpu.VMEM((1, WIDTH), jnp.int32),
                *[pltpu.VMEM((4, 2, ROWS, LANES), F32)] * 4,
                *[pltpu.VMEM((2, 8, LANES), F32)] * 2,
                *[pltpu.VMEM((7, ROWS, LANES), F32)] * 2,
                pltpu.VMEM((7, 80, PADDED), F32),
                *[pltpu.VMEM((4, ROWS, LANES), F32)] * 2,
                pltpu.VMEM((4, 80, PADDED), F32),
                pltpu.VMEM((2, 80, PADDED), F32),
                dma((4,)), dma((2, chunks, 4)), dma((2, chunks, 4)), dma((9,)), dma((9,)), dma((8,)), dma((8,)),
            ],
            compiler_params=pltpu.CompilerParams(collective_id=0, has_side_effects=True, vmem_limit_bytes=53 << 20),
            name="ocean_step",
        )(table, avg_weights, wet_levels, col_depth, surf_eta, trans_x, trans_y, vel_x, vel_y, pot_temp, salinity)

        small = jax.ShapeDtypeStruct((2, ROWS, WIDTH), F32)
        deep_out = pl.BlockSpec((size, 2, ROWS, WIDTH), lambda i: (i, 0, 0, 0))
        small_out = pl.BlockSpec((2, ROWS, WIDTH), lambda i: (0, 0, 0))
        return pl.pallas_call(
            functools.partial(finish_kernel, size),
            grid=(chunks,),
            out_shape=(small,) * 3 + (full,) * 4,
            in_specs=[vmem] * 7,
            out_specs=(small_out,) * 3 + (deep_out,) * 2 + (hbm,) * 2,
            scratch_shapes=[dma((2,))],
            compiler_params=pltpu.CompilerParams(vmem_limit_bytes=20 << 20),
            name="ocean_finish",
        )(*outs)

    spec_3d = P(None, None, "row", "col")
    spec_2d = P(None, "row", "col")
    spec_map = P("row", "col")
    return jax.shard_map(local_step, mesh=mesh, in_specs=(spec_3d,) * 4 + (spec_2d,) * 3 + (spec_map,) * 2 + (P(),), out_specs=(spec_2d,) * 3 + (spec_3d,) * 4, check_vma=False)
```

```python
import functools
import numpy as np
import jax
import jax.numpy as jnp
from jax import lax
from jax.experimental import pallas as pl
from jax.experimental.pallas import tpu as pltpu
from jax.sharding import PartitionSpec as P

WAVE_COURANT = 0.4
THERM_EXP = 0.2
HALINE_CON = 0.15
PRESS_SCALE = 0.5
VISC_NUMBER = 1.0
DIFF_NUMBER = 0.5
SUBCYCLES = 30
HALO = 32
ROWS, WIDTH, PADDED, LANES = 16, 192, 256, 128
MESH = pl.DeviceIdType.MESH
F32 = jnp.float32


def solve_tables(level_count):
    rows = []
    for strength in (VISC_NUMBER, DIFF_NUMBER):
        inner, last = np.zeros(level_count), np.zeros(level_count)
        inner[0], last[0] = 1.0 + strength, 1.0
        for k in range(1, level_count):
            inner[k] = 1.0 + 2.0 * strength - strength * strength / inner[k - 1]
            last[k] = 1.0 + strength - strength * strength / inner[k - 1]
        rows += [1.0 / inner, 1.0 / last, strength / inner]
    return np.concatenate(rows).astype(np.float32)


def level_chunk(level_count):
    for size in (15, 5, 4, 3, 2):
        if level_count % size == 0:
            return size
    return 1


def step_kernel(
    row_count, col_count, level_count,
    table, weights, kmt_in, depth_in, eta_in, tx_in, ty_in, u_hbm, v_hbm, t_hbm, s_hbm,
    pu, pv, pt, ps, corr, faces, avg,
    ub, vb, tb, sb, rows_n, rows_s, send_n, send_s, kmt_n, pack_w, pack_e, col_e, col_w, corner_se, corner_nw,
    edge_e, edge_w, wide, fedge_e, fedge_w, wide_f, coef,
    load_sem, row_send, row_recv, misc_send, misc_recv, wide_send, wide_recv,
):
    K = level_count
    size = level_chunk(K)
    chunks = K // size
    half = (size + 1) // 2
    tile_count = size + half
    r = lax.axis_index("row")
    c = lax.axis_index("col")
    east = lax.rem(c + 1, col_count)
    west = lax.rem(c + col_count - 1, col_count)
    has_n, has_s = r < row_count - 1, r > 0
    has_nn, has_ss = r < row_count - 2, r > 1
    fields_hbm = (u_hbm, v_hbm, t_hbm, s_hbm)
    fields = (ub, vb, tb, sb)

    loads = [
        [pltpu.make_async_copy(src.at[pl.ds(i * size, size)], dst.at[pl.ds(i * size, size)], load_sem.at[i, f]) for f, (src, dst) in enumerate(zip(fields_hbm, fields))]
        for i in range(chunks)
    ]
    for group in loads:
        for copy in group:
            copy.start()

    wide[...] = jnp.zeros_like(wide)
    wide_f[...] = jnp.zeros_like(wide_f)

    @pl.when(jnp.logical_not(has_n))
    def _():
        rows_n[...] = jnp.zeros_like(rows_n)
        kmt_n[...] = jnp.zeros_like(kmt_n)
        corner_nw[...] = jnp.zeros_like(corner_nw)

    @pl.when(jnp.logical_not(has_s))
    def _():
        rows_s[...] = jnp.zeros_like(rows_s)
        corner_se[...] = jnp.zeros_like(corner_se)

    barrier = pltpu.get_barrier_semaphore()

    def signal(**where):
        pl.semaphore_signal(barrier, inc=1, device_id=where, device_id_type=MESH)

    signal(col=east)
    signal(col=west)

    @pl.when(has_n)
    def _():
        signal(row=r + 1)
        signal(row=r + 1, col=west)

    @pl.when(has_s)
    def _():
        signal(row=r - 1)
        signal(row=r - 1, col=east)

    @pl.when(has_nn)
    def _():
        signal(row=r + 2)

    @pl.when(has_ss)
    def _():
        signal(row=r - 2)

    def one(flag):
        return flag.astype(jnp.int32)

    pl.semaphore_wait(barrier, 2 + 2 * one(has_n) + 2 * one(has_s) + one(has_nn) + one(has_ss))

    def remote(src, dst, ssem, rsem, **where):
        return pltpu.make_async_remote_copy(src_ref=src, dst_ref=dst, send_sem=ssem, recv_sem=rsem, device_id=where, device_id_type=MESH)

    kmt_copy = remote(kmt_in.at[0:1, :], kmt_n, misc_send.at[4], misc_recv.at[4], row=r - 1)

    @pl.when(has_s)
    def _():
        kmt_copy.start()

    def row_copy(side, i):
        tiles = pl.ds(i * tile_count, tile_count)
        if side == 0:
            return remote(send_s.at[tiles], rows_n.at[tiles], row_send.at[0, i], row_recv.at[0, i], row=r - 1)
        return remote(send_n.at[tiles], rows_s.at[tiles], row_send.at[1, i], row_recv.at[1, i], row=r + 1)

    lane = lax.broadcasted_iota(jnp.int32, (ROWS, LANES), 1)
    lane1 = lax.broadcasted_iota(jnp.int32, (1, LANES), 1)
    lane_all = lax.broadcasted_iota(jnp.int32, (ROWS, PADDED), 1)
    row_id = lax.broadcasted_iota(jnp.int32, (ROWS, PADDED), 0)

    def padded(x):
        return jnp.concatenate([x, jnp.zeros((x.shape[0], 64), x.dtype)], axis=1)

    kmt = padded(kmt_in[...]).astype(F32)
    own = pl.ds(HALO, ROWS)
    wide[0, own, :] = jnp.where(kmt > 0.5, padded(depth_in[...]), 0.0)
    for m in range(2):
        wide[1 + m, own, :] = padded(eta_in[m])
        wide[3 + m, own, :] = padded(tx_in[m])
        wide[5 + m, own, :] = padded(ty_in[m])

    edge_copies = [
        remote(wide.at[:, own, 0:LANES], edge_e, misc_send.at[5], misc_recv.at[5], col=west),
        remote(wide.at[:, own, LANES:PADDED], edge_w, misc_send.at[6], misc_recv.at[6], col=east),
    ]

    for copy in edge_copies:
        copy.start()

    sub = lax.broadcasted_iota(jnp.int32, (8, LANES), 0)

    def pack_level(k, acc):
        out, tiles = [], [[None, None], [None, None]]
        for f in range(4):
            for m in range(2):
                halves = (fields[f][k, m, :, 0:LANES], padded(fields[f][k, m, :, LANES:WIDTH]))
                for h in range(2):
                    turned = pltpu.roll(halves[h], k if h == 0 else lax.rem(k + 65, LANES), 1)
                    out.append(jnp.where(lane == k, turned, acc[len(out)]))
                    for side in range(2):
                        spot = 2 * f + m
                        row = pltpu.roll(halves[h][8 * side:8 * side + 8], spot if side == 0 else (spot + 1) % 8, 0)
                        old = tiles[side][h]
                        tiles[side][h] = row if old is None else jnp.where(sub == spot, row, old)
        return tuple(out), tiles

    acc = (jnp.zeros((ROWS, LANES), F32),) * 16
    lower = lax.broadcasted_iota(jnp.int32, (8, LANES), 1) < 64
    for i in range(chunks):
        def pack_pair(j, acc):
            j2 = jnp.minimum(j + half, size - 1)
            acc, one_level = pack_level(i * size + j, acc)
            acc, other = pack_level(i * size + j2, acc)
            for side, dest in enumerate((send_s, send_n)):
                dest[i * tile_count + j] = one_level[side][0]
                dest[i * tile_count + j2] = other[side][0]
                dest[i * tile_count + size + j] = jnp.where(lower, one_level[side][1], pltpu.roll(other[side][1], 64, 1))
            return acc

        for copy in loads[i]:
            copy.wait()
        acc = lax.fori_loop(0, half, pack_pair, acc, unroll=2)

        @pl.when(has_s)
        def _():
            row_copy(0, i).start()

        @pl.when(has_n)
        def _():
            row_copy(1, i).start()

    for f in range(4):
        for m in range(2):
            west_edge = acc[4 * f + 2 * m]
            pack_w[f, m] = west_edge if f + m > 0 else jnp.where(lane == 127, pltpu.roll(kmt[:, 0:LANES], 127, 1), west_edge)
            pack_e[f, m] = acc[4 * f + 2 * m + 1]

    pack_copies = [
        remote(pack_w, col_e, misc_send.at[0], misc_recv.at[0], col=west),
        remote(pack_e, col_w, misc_send.at[1], misc_recv.at[1], col=east),
    ]
    for copy in pack_copies:
        copy.start()
    corner_v = remote(pack_w.at[1, :, 8:ROWS, :], corner_se, misc_send.at[2], misc_recv.at[2], row=r + 1, col=west)
    corner_u = remote(pack_e.at[0, :, 0:8, :], corner_nw, misc_send.at[3], misc_recv.at[3], row=r - 1, col=east)

    @pl.when(has_n)
    def _():
        corner_v.start()

    @pl.when(has_s)
    def _():
        corner_u.start()

    def with_edges(x, from_east, from_west):
        b = jnp.where(lane < 64, x[:, LANES:PADDED], jnp.where(lane < 96, pltpu.roll(from_east, 64, 1), pltpu.roll(from_west, 64, 1)))
        return jnp.concatenate([x[:, 0:LANES], b], axis=1)

    def spread(buf, first_sem):
        src = buf.at[:, own, :]
        return (
            (has_n, remote(src, buf.at[:, pl.ds(ROWS, ROWS), :], wide_send.at[first_sem], wide_recv.at[first_sem], row=r + 1)),
            (has_s, remote(src, buf.at[:, pl.ds(48, ROWS), :], wide_send.at[first_sem + 1], wide_recv.at[first_sem + 1], row=r - 1)),
            (has_nn, remote(src, buf.at[:, pl.ds(0, ROWS), :], wide_send.at[first_sem + 2], wide_recv.at[first_sem + 2], row=r + 2)),
            (has_ss, remote(src, buf.at[:, pl.ds(64, ROWS), :], wide_send.at[first_sem + 3], wide_recv.at[first_sem + 3], row=r - 2)),
        )

    def start_spread(copies):
        for there, copy in copies:
            @pl.when(there)
            def _():
                copy.start()

    def finish_spread(copies):
        arrives = (has_s, has_n, has_ss, has_nn)
        for (there, copy), here in zip(copies, arrives):
            @pl.when(there)
            def _():
                copy.wait_send()

            @pl.when(here)
            def _():
                copy.wait_recv()

    for copy in edge_copies:
        copy.wait()
    for p in range(7):
        wide[p, own, :] = with_edges(wide[p, own, :], edge_e[p], edge_w[p])
    static_copies = spread(wide, 0)
    start_spread(static_copies)

    for copy in pack_copies:
        copy.wait()

    @pl.when(has_n)
    def _():
        corner_v.wait_send()
        kmt_copy.wait_recv()
        corner_u.wait_recv()

    @pl.when(has_s)
    def _():
        corner_u.wait_send()
        kmt_copy.wait_send()
        corner_v.wait_recv()

    def roll_e(x):
        return pltpu.roll(x, 255, 1)

    def roll_w(x):
        return pltpu.roll(x, 1, 1)

    def from_north(x, edge):
        return jnp.where(row_id == 15, edge, pltpu.roll(x, 15, 0))

    def from_south(x, edge):
        return jnp.where(row_id == 0, edge, pltpu.roll(x, 1, 0))

    kmt_east = jnp.where(lane_all == 191, jnp.concatenate([lane.astype(F32), pltpu.roll(col_e[0, 0], 64, 1)], axis=1), roll_e(kmt))
    kmt_north = from_north(kmt, padded(kmt_n[...]).astype(F32))
    in_block = lane_all < WIDTH
    kmt_cell = jnp.where(in_block, kmt, 0.0)
    mu = jnp.where(in_block, jnp.minimum(kmt, kmt_east), 0.0)
    mv = jnp.where(in_block, jnp.minimum(kmt, kmt_north), 0.0)
    faces[0] = mu
    faces[1] = mv
    faces[2] = kmt_cell

    def extended(f, k, m):
        b = padded(fields[f][k, m, :, LANES:WIDTH])
        to_east = pltpu.roll(col_e[f, m], lax.rem(WIDTH - k, LANES), 1)
        to_west = pltpu.roll(col_w[f, m], lax.rem(255 - k, LANES), 1)
        b = jnp.where(lane < 64, b, jnp.where(lane == 64, to_east, to_west))
        return jnp.concatenate([fields[f][k, m, :, 0:LANES], b], axis=1)

    def edge_row(rows, f, k, m):
        chunk = lax.div(k, size)
        j = k - chunk * size
        first, spot = chunk * tile_count, 2 * f + m
        tail = pltpu.roll(rows[first + size + lax.rem(j, half)], 64 * one(j >= half), 1)
        return jnp.concatenate([rows[first + j][spot:spot + 1], tail[spot:spot + 1]], axis=1)

    def solve_factor(depth, k, first):
        inner, last = table[first * K + k], table[(first + 1) * K + k]
        kf = k.astype(F32)
        return jnp.where(depth > kf + 1.0, inner, jnp.where(depth > kf, last, 0.0))

    scale = PRESS_SCALE / K

    def momentum(k, carry):
        out = []
        kf = k.astype(F32)
        for m in range(2):
            total, total_n, gu_sum, gv_sum, side_u, side_v = carry[m]
            u, v = extended(0, k, m), extended(1, k, m)
            t, s = extended(2, k, m), extended(3, k, m)
            density = HALINE_CON * s - THERM_EXP * t
            total = total + density
            pressure = scale * (total - 0.5 * density)
            density_n = HALINE_CON * edge_row(rows_n, 3, k, m) - THERM_EXP * edge_row(rows_n, 2, k, m)
            total_n = total_n + density_n
            pressure_n = scale * (total_n - 0.5 * density_n)
            un_edge = edge_row(rows_n, 0, k, m)
            nw = pltpu.roll(corner_nw[m], lax.rem(255 - k, LANES), 1)[0:1, :]
            un_edge = jnp.concatenate([un_edge[:, 0:LANES], jnp.where(lane1 == 127, nw, un_edge[:, LANES:PADDED])], axis=1)
            vs_edge = edge_row(rows_s, 1, k, m)
            se = pltpu.roll(corner_se[m], lax.rem(WIDTH - k, LANES), 1)[7:8, :]
            vs_edge = jnp.concatenate([vs_edge[:, 0:LANES], jnp.where(lane1 == 64, se, vs_edge[:, LANES:PADDED])], axis=1)
            u_n, u_s = from_north(u, un_edge), from_south(u, edge_row(rows_s, 0, k, m))
            v_n, v_s = from_north(v, edge_row(rows_n, 1, k, m)), from_south(v, vs_edge)
            p_n = from_north(pressure, pressure_n)
            v_pair = v + v_s
            u_pair = u + u_n
            vu = 0.125 * (v_pair + roll_e(v_pair))
            uv = 0.125 * (u_pair + roll_w(u_pair))
            gu = pressure - roll_e(pressure) - 0.5 * u * (roll_e(u) - roll_w(u)) - vu * (u_n - u_s)
            gv = pressure - p_n - uv * (roll_e(v) - roll_w(v)) - 0.5 * v * (v_n - v_s)
            gu = jnp.where(mu > kf, gu, 0.0)
            gv = jnp.where(mv > kf, gv, 0.0)
            side_u = (u + gu + VISC_NUMBER * side_u) * solve_factor(mu, k, 0)
            side_v = (v + gv + VISC_NUMBER * side_v) * solve_factor(mv, k, 0)
            pu[k, m] = side_u[:, 0:WIDTH]
            pv[k, m] = side_v[:, 0:WIDTH]
            out.append((total, total_n, gu_sum + gu, gv_sum + gv, side_u, side_v))
        return tuple(out)

    zero = jnp.zeros((ROWS, PADDED), F32)
    zero_row = jnp.zeros((1, PADDED), F32)
    carry = ((zero, zero_row, zero, zero, zero, zero),) * 2
    for i in range(chunks):
        @pl.when(has_n)
        def _():
            row_copy(0, i).wait_recv()

        @pl.when(has_s)
        def _():
            row_copy(1, i).wait_recv()

        carry = lax.fori_loop(i * size, (i + 1) * size, momentum, carry)

    count_u = jnp.maximum(mu, 1.0)
    count_v = jnp.maximum(mv, 1.0)
    for m in range(2):
        wide_f[m, own, :] = carry[m][2] / count_u
        wide_f[2 + m, own, :] = carry[m][3] / count_v
    force_edges = [
        remote(wide_f.at[:, own, 0:LANES], fedge_e, misc_send.at[7], misc_recv.at[7], col=west),
        remote(wide_f.at[:, own, LANES:PADDED], fedge_w, misc_send.at[8], misc_recv.at[8], col=east),
    ]
    for copy in force_edges:
        copy.start()

    def tracer(f, dest):
        def level(k, carry):
            out = []
            kf = k.astype(F32)
            factor = solve_factor(kmt_cell, k, 3)
            for m in range(2):
                u, v, t = extended(0, k, m), extended(1, k, m), extended(f, k, m)
                t_n = from_north(t, edge_row(rows_n, f, k, m))
                flux_x = 0.5 * u * (t + roll_e(t))
                flux_y = 0.5 * v * (t + t_n)
                flux_s = 0.5 * edge_row(rows_s, 1, k, m) * (edge_row(rows_s, f, k, m) + t[0:1, :])
                moved = t - (flux_x - roll_w(flux_x) + flux_y - from_south(flux_y, flux_s))
                side = (moved + DIFF_NUMBER * carry[m]) * factor
                dest[k, m] = side[:, 0:WIDTH]
                out.append(side)
            return tuple(out)

        last = lax.fori_loop(0, K, level, (zero, zero))

        def back(j, carry):
            k = K - 2 - j
            ratio = table[5 * K + k]
            out = []
            for m in range(2):
                x = dest[k, m] + ratio * carry[m]
                dest[k, m] = x
                out.append(x)
            return tuple(out)

        lax.fori_loop(0, K - 1, back, tuple(x[:, 0:WIDTH] for x in last))

    tracer(2, pt)

    for copy in force_edges:
        copy.wait()
    for p in range(4):
        wide_f[p, own, :] = with_edges(wide_f[p, own, :], fedge_e[p], fedge_w[p])
    force_copies = spread(wide_f, 4)
    start_spread(force_copies)

    tracer(3, ps)

    def back(j, carry):
        k = K - 2 - j
        ratio = table[2 * K + k]
        out = []
        for m in range(2):
            xu, xv, su, sv = carry[m]
            xu = pu[k, m] + ratio * xu
            xv = pv[k, m] + ratio * xv
            pu[k, m] = xu
            pv[k, m] = xv
            out.append((xu, xv, su + xu, sv + xv))
        return tuple(out)

    start = tuple(tuple(carry[m][i][:, 0:WIDTH] for i in (4, 5, 4, 5)) for m in range(2))
    ends = lax.fori_loop(0, K - 1, back, start)

    finish_spread(static_copies)
    finish_spread(force_copies)

    depth = wide[0]
    depth_e = pltpu.roll(depth, 255, 1)
    depth_n = pltpu.roll(depth, 79, 0)
    hu = jnp.where((depth > 0.0) & (depth_e > 0.0), 0.5 * (depth + depth_e), 0.0)
    hv = jnp.where((depth > 0.0) & (depth_n > 0.0), 0.5 * (depth + depth_n), 0.0)
    coef[0] = WAVE_COURANT * hu
    coef[1] = WAVE_COURANT * hv
    for m in range(2):
        wide_f[m] = hu * wide_f[m] * (1.0 / SUBCYCLES)
        wide_f[2 + m] = hv * wide_f[2 + m] * (1.0 / SUBCYCLES)
        for p in range(3):
            avg[2 * p + m] = zero

    def subcycle(n, _):
        weight = weights[n]
        for m in range(2):
            eta, tx, ty = wide[1 + m], wide[3 + m], wide[5 + m]
            eta = eta - WAVE_COURANT * (tx - pltpu.roll(tx, 1, 1) + ty - pltpu.roll(ty, 1, 0))
            tx = tx + wide_f[m] - coef[0] * (pltpu.roll(eta, 255, 1) - eta)
            ty = ty + wide_f[2 + m] - coef[1] * (pltpu.roll(eta, 79, 0) - eta)
            wide[1 + m] = eta
            wide[3 + m] = tx
            wide[5 + m] = ty
            mine = slice(HALO, HALO + ROWS)
            avg[m] = avg[m] + weight * eta[mine]
            avg[2 + m] = avg[2 + m] + weight * tx[mine]
            avg[4 + m] = avg[4 + m] + weight * ty[mine]
        return 0

    lax.fori_loop(0, SUBCYCLES, subcycle, 0)

    mine = slice(HALO, HALO + ROWS)
    for m in range(2):
        corr[m] = avg[2 + m] / jnp.where(mu > 0.5, hu[mine], 1.0) - padded(ends[m][2]) / count_u
        corr[2 + m] = avg[4 + m] / jnp.where(mv > 0.5, hv[mine], 1.0) - padded(ends[m][3]) / count_v

    @pl.when(has_s)
    def _():
        for i in range(chunks):
            row_copy(0, i).wait_send()

    @pl.when(has_n)
    def _():
        for i in range(chunks):
            row_copy(1, i).wait_send()


def finish_kernel(size, pu, pv, pt, ps, corr, faces, avg, eta_o, tx_o, ty_o, u_o, v_o, t_o, s_o, sems):
    first = pl.program_id(0) * size
    through = [pltpu.make_async_copy(src, dst, sems.at[i]) for i, (src, dst) in enumerate(((pt, t_o), (ps, s_o)))]

    @pl.when(first == 0)
    def _():
        for copy in through:
            copy.start()
        for m in range(2):
            eta_o[m] = avg[m][:, 0:WIDTH]
            tx_o[m] = avg[2 + m][:, 0:WIDTH]
            ty_o[m] = avg[4 + m][:, 0:WIDTH]

    for j in range(size):
        level = (first + j).astype(F32)
        for m in range(2):
            for face, (src, dst) in enumerate(((pu, u_o), (pv, v_o))):
                wet = faces[face][:, 0:WIDTH] > level
                dst[j, m] = jnp.where(wet, src[first + j, m] + corr[2 * face + m][:, 0:WIDTH], 0.0)

    @pl.when(pl.program_id(0) == pl.num_programs(0) - 1)
    def _():
        for copy in through:
            copy.wait()


def solution(mesh):
    col_count, row_count = mesh.shape["col"], mesh.shape["row"]

    def local_step(vel_x, vel_y, pot_temp, salinity, surf_eta, trans_x, trans_y, col_depth, wet_levels, avg_weights):
        K = vel_x.shape[0]
        size = level_chunk(K)
        chunks = K // size
        table = jnp.asarray(solve_tables(K))
        smem = pl.BlockSpec(memory_space=pltpu.SMEM)
        vmem = pl.BlockSpec(memory_space=pltpu.VMEM)
        hbm = pl.BlockSpec(memory_space=pl.ANY)
        full = jax.ShapeDtypeStruct((K, 2, ROWS, WIDTH), F32)
        held = pltpu.VMEM((K, 2, ROWS, WIDTH), F32)
        dma = pltpu.SemaphoreType.DMA
        outs = pl.pallas_call(
            functools.partial(step_kernel, row_count, col_count, K),
            out_shape=(held,) * 4 + tuple(pltpu.VMEM((n, ROWS, PADDED), F32) for n in (4, 3, 6)),
            in_specs=[smem, smem] + [vmem] * 5 + [hbm] * 4,
            out_specs=(vmem,) * 7,
            scratch_shapes=[
                *[pltpu.VMEM((K, 2, ROWS, WIDTH), F32)] * 4,
                *[pltpu.VMEM((chunks * (size + (size + 1) // 2), 8, LANES), F32)] * 4,
                pltpu.VMEM((1, WIDTH), jnp.int32),
                *[pltpu.VMEM((4, 2, ROWS, LANES), F32)] * 4,
                *[pltpu.VMEM((2, 8, LANES), F32)] * 2,
                *[pltpu.VMEM((7, ROWS, LANES), F32)] * 2,
                pltpu.VMEM((7, 80, PADDED), F32),
                *[pltpu.VMEM((4, ROWS, LANES), F32)] * 2,
                pltpu.VMEM((4, 80, PADDED), F32),
                pltpu.VMEM((2, 80, PADDED), F32),
                dma((chunks, 4)), dma((2, chunks)), dma((2, chunks)), dma((9,)), dma((9,)), dma((8,)), dma((8,)),
            ],
            compiler_params=pltpu.CompilerParams(collective_id=0, has_side_effects=True, vmem_limit_bytes=53 << 20),
            name="ocean_step",
        )(table, avg_weights, wet_levels, col_depth, surf_eta, trans_x, trans_y, vel_x, vel_y, pot_temp, salinity)

        small = jax.ShapeDtypeStruct((2, ROWS, WIDTH), F32)
        deep_out = pl.BlockSpec((size, 2, ROWS, WIDTH), lambda i: (i, 0, 0, 0))
        small_out = pl.BlockSpec((2, ROWS, WIDTH), lambda i: (0, 0, 0))
        return pl.pallas_call(
            functools.partial(finish_kernel, size),
            grid=(chunks,),
            out_shape=(small,) * 3 + (full,) * 4,
            in_specs=[vmem] * 7,
            out_specs=(small_out,) * 3 + (deep_out,) * 2 + (hbm,) * 2,
            scratch_shapes=[dma((2,))],
            compiler_params=pltpu.CompilerParams(vmem_limit_bytes=20 << 20),
            name="ocean_finish",
        )(*outs)

    spec_3d = P(None, None, "row", "col")
    spec_2d = P(None, "row", "col")
    spec_map = P("row", "col")
    return jax.shard_map(local_step, mesh=mesh, in_specs=(spec_3d,) * 4 + (spec_2d,) * 3 + (spec_map,) * 2 + (P(),), out_specs=(spec_2d,) * 3 + (spec_3d,) * 4, check_vma=False)
```

```python
import functools
import numpy as np
import jax
import jax.numpy as jnp
from jax import lax
from jax.experimental import pallas as pl
from jax.experimental.pallas import tpu as pltpu
from jax.sharding import PartitionSpec as P

WAVE_COURANT = 0.4
THERM_EXP = 0.2
HALINE_CON = 0.15
PRESS_SCALE = 0.5
VISC_NUMBER = 1.0
DIFF_NUMBER = 0.5
SUBCYCLES = 30
HALO = 32
MOMENTUM_UNROLL = 3
TRACER_UNROLL = 3
ROWS, WIDTH, PADDED, LANES = 16, 192, 256, 128
MESH = pl.DeviceIdType.MESH
F32 = jnp.float32


def solve_tables(level_count):
    rows = []
    for strength in (VISC_NUMBER, DIFF_NUMBER):
        inner, last = np.zeros(level_count), np.zeros(level_count)
        inner[0], last[0] = 1.0 + strength, 1.0
        for k in range(1, level_count):
            inner[k] = 1.0 + 2.0 * strength - strength * strength / inner[k - 1]
            last[k] = 1.0 + strength - strength * strength / inner[k - 1]
        rows += [1.0 / inner, 1.0 / last, strength / inner]
    return np.concatenate(rows).astype(np.float32)


def level_chunk(level_count):
    for size in (15, 5, 4, 3, 2):
        if level_count % size == 0:
            return size
    return 1


def step_kernel(
    row_count, col_count, level_count,
    table, weights, kmt_in, depth_in, eta_in, tx_in, ty_in, u_hbm, v_hbm, t_hbm, s_hbm,
    pu, pv, pt, ps, corr, faces, avg,
    ub, vb, tb, sb, ue, ve, te, se, rows_n, rows_s, send_n, send_s, kmt_n, pack_w, pack_e, col_e, col_w, corner_se, corner_nw,
    edge_e, edge_w, wide, fedge_e, fedge_w, wide_f, coef,
    load_sem, row_send, row_recv, col_send, col_recv, misc_send, misc_recv, wide_send, wide_recv,
):
    K = level_count
    open_scope = []

    def mark(name):
        if open_scope:
            open_scope.pop().__exit__(None, None, None)
        if name:
            open_scope.append(jax.named_scope(name))
            open_scope[-1].__enter__()

    size = level_chunk(K)
    chunks = K // size
    half = (size + 1) // 2
    tile_count = size + half
    r = lax.axis_index("row")
    c = lax.axis_index("col")
    east = lax.rem(c + 1, col_count)
    west = lax.rem(c + col_count - 1, col_count)
    has_n, has_s = r < row_count - 1, r > 0
    has_nn, has_ss = r < row_count - 2, r > 1
    raw, ext = (ub, vb, tb, sb), (ue, ve, te, se)

    def one(flag):
        return flag.astype(jnp.int32)

    mark("init")
    loads = [
        [pltpu.make_async_copy(src.at[pl.ds(i * size, size)], dst.at[pl.ds(i * size, size)], load_sem.at[i, f]) for f, (src, dst) in enumerate(zip((u_hbm, v_hbm, t_hbm, s_hbm), raw))]
        for i in range(chunks)
    ]
    for group in loads:
        for copy in group:
            copy.start()

    wide[...] = jnp.zeros_like(wide)
    wide_f[...] = jnp.zeros_like(wide_f)

    @pl.when(jnp.logical_not(has_n))
    def _():
        rows_n[...] = jnp.zeros_like(rows_n)
        kmt_n[...] = jnp.zeros_like(kmt_n)
        corner_nw[...] = jnp.zeros_like(corner_nw)

    @pl.when(jnp.logical_not(has_s))
    def _():
        rows_s[...] = jnp.zeros_like(rows_s)
        corner_se[...] = jnp.zeros_like(corner_se)

    barrier = pltpu.get_barrier_semaphore()

    def signal(**where):
        pl.semaphore_signal(barrier, inc=1, device_id=where, device_id_type=MESH)

    signal(col=east)
    signal(col=west)

    @pl.when(has_n)
    def _():
        signal(row=r + 1)
        signal(row=r + 1, col=west)

    @pl.when(has_s)
    def _():
        signal(row=r - 1)
        signal(row=r - 1, col=east)

    @pl.when(has_nn)
    def _():
        signal(row=r + 2)

    @pl.when(has_ss)
    def _():
        signal(row=r - 2)

    def remote(src, dst, ssem, rsem, **where):
        return pltpu.make_async_remote_copy(src_ref=src, dst_ref=dst, send_sem=ssem, recv_sem=rsem, device_id=where, device_id_type=MESH)

    lane = lax.broadcasted_iota(jnp.int32, (ROWS, LANES), 1)
    lane8, lane1 = lane[0:8], lane[0:1]
    sub = lax.broadcasted_iota(jnp.int32, (8, LANES), 0)
    sub2 = lax.broadcasted_iota(jnp.int32, (8, PADDED), 0)

    def padded(x):
        return jnp.concatenate([x, jnp.zeros((x.shape[0], PADDED - WIDTH), x.dtype)], axis=1)

    def overlapped(x):
        a, b = x[:, 0:LANES], x[:, LANES:PADDED]
        return jnp.concatenate([a, jnp.where(lane < 64, b, a)], axis=1)

    def linear(x):
        a, b = x[:, 0:LANES], x[:, LANES:PADDED]
        return jnp.concatenate([jnp.where(lane < 96, a, b), b], axis=1)

    kmt = padded(kmt_in[...]).astype(F32)
    own = pl.ds(HALO, ROWS)
    wide[0, own, :] = jnp.where(kmt > 0.5, padded(depth_in[...]), 0.0)
    for m in range(2):
        wide[1 + m, own, :] = padded(eta_in[m])
        wide[3 + m, own, :] = padded(tx_in[m])
        wide[5 + m, own, :] = padded(ty_in[m])

    kmt_copy = remote(kmt_in.at[0:1, :], kmt_n, misc_send.at[0], misc_recv.at[0], row=r - 1)

    def south_copy(i):
        tiles = pl.ds(i * tile_count, tile_count)
        return remote(send_s.at[tiles], rows_n.at[tiles], row_send.at[0, i], row_recv.at[0, i], row=r - 1)

    def north_copy(i):
        tiles = pl.ds(i * tile_count, tile_count)
        return remote(send_n.at[tiles], rows_s.at[tiles], row_send.at[1, i], row_recv.at[1, i], row=r + 1)

    def west_copy(i):
        return remote(pack_w.at[i], col_e.at[i], col_send.at[0, i], col_recv.at[0, i], col=west)

    def east_copy(i):
        return remote(pack_e.at[i], col_w.at[i], col_send.at[1, i], col_recv.at[1, i], col=east)

    def corner_v(i):
        return remote(pack_w.at[i, 8:16, :], corner_se.at[i], col_send.at[2, i], col_recv.at[2, i], row=r + 1, col=west)

    def corner_u(i):
        return remote(pack_e.at[i, 0:8, :], corner_nw.at[i], col_send.at[3, i], col_recv.at[3, i], row=r - 1, col=east)

    def pack_level(k, j, acc):
        acc, tiles = list(acc), [[None, None], [None, None]]
        for f in range(4):
            for m in range(2):
                spot = 2 * f + m
                target = size * spot + j
                halves = (raw[f][k, m, :, 0:LANES], jnp.concatenate([raw[f][k, m, :, LANES:WIDTH]] * 2, axis=1))
                for h in range(2):
                    turned = pltpu.roll(halves[h], target if h == 0 else lax.rem(target + 1, LANES), 1)
                    acc[h] = jnp.where(lane == target, turned, acc[h])
                    for side in range(2):
                        row = pltpu.roll(halves[h][8 * side:8 * side + 8], spot if side == 0 else (spot + 1) % 8, 0)
                        old = tiles[side][h]
                        tiles[side][h] = row if old is None else jnp.where(sub == spot, row, old)
        return tuple(acc), tiles

    def pack_chunk(i):
        def pack_pair(j, acc):
            j2 = jnp.minimum(j + half, size - 1)
            acc, one_level = pack_level(i * size + j, j, acc)
            acc, other = pack_level(i * size + j2, j2, acc)
            for side, dest in enumerate((send_s, send_n)):
                dest[i * tile_count + j] = one_level[side][0]
                dest[i * tile_count + j2] = other[side][0]
                dest[i * tile_count + size + j] = jnp.where(lane8 < 64, one_level[side][1], other[side][1])
            return acc

        for copy in loads[i]:
            copy.wait()
        first = pltpu.roll(kmt[:, 0:LANES], LANES - 1, 1)
        acc = lax.fori_loop(0, half, pack_pair, (first, first), unroll=2)
        pack_w[i] = acc[0]
        pack_e[i] = acc[1]

    def start_chunk(i):
        west_copy(i).start()
        east_copy(i).start()

        @pl.when(has_s)
        def _():
            corner_u(i).start()
            south_copy(i).start()

        @pl.when(has_n)
        def _():
            corner_v(i).start()
            north_copy(i).start()

    mark("pack_early")
    early = min(2, chunks)
    for i in range(early):
        pack_chunk(i)
    mark("barrier_wait")
    pl.semaphore_wait(barrier, 2 + 2 * one(has_n) + 2 * one(has_s) + one(has_nn) + one(has_ss))

    @pl.when(has_s)
    def _():
        kmt_copy.start()

    for i in range(early):
        start_chunk(i)
    mark("pack_late")
    for i in range(early, chunks):
        pack_chunk(i)
        start_chunk(i)

    def edge_pair(buf, to_east, to_west, sem):
        return [
            remote(buf.at[:, own, 0:LANES], to_west, misc_send.at[sem], misc_recv.at[sem], col=west),
            remote(buf.at[:, own, LANES:PADDED], to_east, misc_send.at[sem + 1], misc_recv.at[sem + 1], col=east),
        ]

    def with_edges(x, from_east, from_west):
        b = jnp.where(lane < 64, x[:, LANES:PADDED], jnp.where(lane < 96, pltpu.roll(from_east, 64, 1), pltpu.roll(from_west, 64, 1)))
        return jnp.concatenate([x[:, 0:LANES], b], axis=1)

    def spread(buf, sem):
        src = buf.at[:, own, :]
        parts = ((has_n, has_s, 16, r + 1), (has_s, has_n, 48, r - 1), (has_nn, has_ss, 0, r + 2), (has_ss, has_nn, 64, r - 2))
        return [(there, here, remote(src, buf.at[:, pl.ds(at, ROWS), :], wide_send.at[sem + n], wide_recv.at[sem + n], row=row)) for n, (there, here, at, row) in enumerate(parts)]

    def start_spread(copies):
        for there, _, copy in copies:
            @pl.when(there)
            def _():
                copy.start()

    def finish_spread(copies):
        for there, here, copy in copies:
            @pl.when(there)
            def _():
                copy.wait_send()

            @pl.when(here)
            def _():
                copy.wait_recv()

    mark("edges")
    edge_copies = edge_pair(wide, edge_w, edge_e, 1)
    for copy in edge_copies:
        copy.start()

    def roll_e(x):
        return jnp.concatenate([pltpu.roll(x[:, 0:LANES], LANES - 1, 1), pltpu.roll(x[:, LANES:PADDED], LANES - 1, 1)], axis=1)

    def roll_w(x):
        return jnp.concatenate([pltpu.roll(x[:, 0:LANES], 1, 1), pltpu.roll(x[:, LANES:PADDED], 1, 1)], axis=1)

    def from_north(x, edge):
        low, high = pltpu.roll(x[0:8], 7, 0), pltpu.roll(x[8:16], 7, 0)
        return jnp.concatenate([jnp.where(sub2 == 7, high, low), jnp.where(sub2 == 7, edge, high)], axis=0)

    def from_south(x, edge):
        low, high = pltpu.roll(x[0:8], 1, 0), pltpu.roll(x[8:16], 1, 0)
        return jnp.concatenate([jnp.where(sub2 == 0, edge, low), jnp.where(sub2 == 0, low, high)], axis=0)

    def wait_columns(i):
        west_copy(i).wait_recv()
        east_copy(i).wait_recv()

    def insert_columns(i):
        def level(j, _):
            k = i * size + j
            for f in range(4):
                for m in range(2):
                    place = size * (2 * f + m) + j
                    to_east = pltpu.roll(col_e[i], lax.rem(LANES + 64 - place, LANES), 1)
                    to_west = pltpu.roll(col_w[i], LANES - 1 - place, 1)
                    a = raw[f][k, m, :, 0:LANES]
                    b = jnp.concatenate([raw[f][k, m, :, LANES:WIDTH]] * 2, axis=1)
                    ext[f][k, m, :, 0:LANES] = jnp.where(lane == LANES - 1, to_west, a)
                    ext[f][k, m, :, LANES:PADDED] = jnp.where(lane < 64, b, jnp.where(lane == 64, to_east, a))
            return 0

        lax.fori_loop(0, size, level, 0, unroll=5)

    mark("column_wait")
    wait_columns(0)

    @pl.when(has_n)
    def _():
        kmt_copy.wait_recv()

    @pl.when(has_s)
    def _():
        kmt_copy.wait_send()

    mark("masks")
    kmt2 = overlapped(kmt)
    kmt_edge = jnp.where(lane == 64, pltpu.roll(col_e[0], 65, 1), kmt2[:, LANES:PADDED])
    kmt_row = padded(kmt_n[...]).astype(F32)
    kmt_north = jnp.concatenate([kmt_row[:, 0:LANES], jnp.where(lane1 < 64, kmt_row[:, LANES:PADDED], kmt_row[:, 0:LANES])], axis=1)
    mu = jnp.minimum(kmt2, roll_e(jnp.concatenate([kmt2[:, 0:LANES], kmt_edge], axis=1)))
    mv = jnp.minimum(kmt2, from_north(kmt2, kmt_north))
    faces[0] = linear(mu)
    faces[1] = linear(mv)

    def solve_factor(depth, k, first):
        inner, last = table[first * K + k], table[(first + 1) * K + k]
        kf = k.astype(F32)
        return jnp.where(depth > kf + 1.0, inner, jnp.where(depth > kf, last, 0.0))

    def edge_tiles(rows, i, j, shifted):
        late = one(j >= half)
        first = i * tile_count
        a, b_raw = rows[first + j], rows[first + size + j - half * late]
        late = 64 * late
        b = jnp.where(lane8 < 64, pltpu.roll(b_raw, late, 1), a)
        if shifted == 0:
            return a, b
        if shifted == 1:
            a1 = pltpu.roll(a, 1, 1)
            return a, b, a1, jnp.where((lane8 >= 1) & (lane8 < 65), pltpu.roll(b_raw, late + 1, 1), a1)
        a1 = pltpu.roll(a, LANES - 1, 1)
        return a, b, a1, jnp.where((lane8 < 63) | (lane8 == LANES - 1), pltpu.roll(b_raw, lax.rem(late + LANES - 1, LANES), 1), a1)

    def join(a, b, spot):
        return jnp.concatenate([a[spot:spot + 1], b[spot:spot + 1]], axis=1)

    half_scale = 0.5 * PRESS_SCALE / K
    edge_weight = jnp.where(sub < 6, -half_scale * THERM_EXP, half_scale * HALINE_CON)

    def momentum(i):
        def level(j, carry):
            (na, nb), members = carry
            k = i * size + j
            kf = k.astype(F32)
            an, bn, wan, wbn = edge_tiles(rows_n, i, j, 1)
            as_, bs, eas, ebs = edge_tiles(rows_s, i, j, 2)
            xa, xb = an * edge_weight, bn * edge_weight
            ha, hb = xa + pltpu.roll(xa, 6, 0), xb + pltpu.roll(xb, 6, 0)
            pna, pnb = na + ha, nb + hb
            factor_u, factor_v = solve_factor(mu, k, 0), solve_factor(mv, k, 0)
            out = []
            for m in range(2):
                total, gu_sum, gv_sum, side_u, side_v = members[m]
                u, v = ue[k, m], ve[k, m]
                step = (half_scale * HALINE_CON) * se[k, m] - (half_scale * THERM_EXP) * te[k, m]
                pressure = total + step
                corner_n = pltpu.roll(corner_nw[i], LANES - (size * m + j), 1)[0:1]
                corner_s = pltpu.roll(corner_se[i], lax.rem(LANES + 63 - (size * (2 + m) + j), LANES), 1)[7:8]
                u_edge = join(an, bn, m)
                v_edge = join(as_, bs, 2 + m)
                u_edge_w = jnp.concatenate([jnp.where(lane1 == 0, corner_n, wan[m:m + 1]), wbn[m:m + 1]], axis=1)
                v_edge_e = jnp.concatenate([eas[2 + m:3 + m], jnp.where(lane1 == 63, corner_s, ebs[2 + m:3 + m])], axis=1)
                v_e, v_w, u_e, u_w = roll_e(v), roll_w(v), roll_e(u), roll_w(u)
                v_pair, u_pair = v + v_e, u + u_w
                vu = 0.125 * (v_pair + from_south(v_pair, v_edge + v_edge_e))
                uv = 0.125 * (u_pair + from_north(u_pair, u_edge + u_edge_w))
                u_n, u_s = from_north(u, u_edge), from_south(u, join(as_, bs, m))
                v_n, v_s = from_north(v, join(an, bn, 2 + m)), from_south(v, v_edge)
                p_n = from_north(pressure, join(pna, pnb, 4 + m))
                gu = pressure - roll_e(pressure) - 0.5 * u * (u_e - u_w) - vu * (u_n - u_s)
                gv = pressure - p_n - uv * (v_e - v_w) - 0.5 * v * (v_n - v_s)
                gu = jnp.where(mu > kf, gu, 0.0)
                gv = jnp.where(mv > kf, gv, 0.0)
                side_u = (u + gu + VISC_NUMBER * side_u) * factor_u
                side_v = (v + gv + VISC_NUMBER * side_v) * factor_v
                pu[k, m] = linear(side_u)[:, 0:WIDTH]
                pv[k, m] = linear(side_v)[:, 0:WIDTH]
                out.append((pressure + step, gu_sum + gu, gv_sum + gv, side_u, side_v))
            return (pna + ha, pnb + hb), tuple(out)

        return level

    zero = jnp.zeros((ROWS, PADDED), F32)
    zero_row = jnp.zeros((8, LANES), F32)
    carry = ((zero_row, zero_row), ((zero,) * 5,) * 2)
    for i in range(chunks):
        if i > 0:
            wait_columns(i)
        mark("insert")
        insert_columns(i)

        mark("row_wait")
        @pl.when(has_n)
        def _():
            south_copy(i).wait_recv()
            corner_u(i).wait_recv()

        @pl.when(has_s)
        def _():
            north_copy(i).wait_recv()
            corner_v(i).wait_recv()

        mark("momentum")
        carry = lax.fori_loop(0, size, momentum(i), carry, unroll=MOMENTUM_UNROLL)

        mark("next")
        if i == chunks // 2:
            for copy in edge_copies:
                copy.wait()
            for p in range(7):
                wide[p, own, :] = with_edges(wide[p, own, :], edge_e[p], edge_w[p])
            static_copies = spread(wide, 0)
            start_spread(static_copies)

    members = carry[1]
    mark("force")
    count_u = linear(jnp.maximum(mu, 1.0))
    count_v = linear(jnp.maximum(mv, 1.0))
    for m in range(2):
        wide_f[m, own, :] = linear(members[m][1]) / count_u
        wide_f[2 + m, own, :] = linear(members[m][2]) / count_v
    force_edges = edge_pair(wide_f, fedge_w, fedge_e, 3)
    for copy in force_edges:
        copy.start()

    def tracers(i, carry):
        def level(j, carry):
            k = i * size + j
            an, bn = edge_tiles(rows_n, i, j, 0)
            as_, bs = edge_tiles(rows_s, i, j, 0)
            factor = solve_factor(kmt2, k, 3)
            out = []
            for m in range(2):
                u, v = 0.5 * ue[k, m], 0.5 * ve[k, m]
                u_w = roll_w(u)
                v_edge = 0.5 * join(as_, bs, 2 + m)
                for f, dest in ((2, pt), (3, ps)):
                    t = ext[f][k, m]
                    flux_x = u * (t + roll_e(t)) - u_w * (t + roll_w(t))
                    flux_y = v * (t + from_north(t, join(an, bn, 2 * f + m)))
                    flux_s = v_edge * (join(as_, bs, 2 * f + m) + t[0:1])
                    moved = t - (flux_x + flux_y - from_south(flux_y, flux_s))
                    side = (moved + DIFF_NUMBER * carry[len(out)]) * factor
                    dest[k, m] = linear(side)[:, 0:WIDTH]
                    out.append(side)
            return tuple(out)

        return lax.fori_loop(0, size, level, carry, unroll=TRACER_UNROLL)

    mark("tracer_1")
    tail = (zero,) * 4
    split = (3 * chunks + 4) // 5
    tail = lax.fori_loop(0, split, tracers, tail)

    mark("force_edge_wait")
    for copy in force_edges:
        copy.wait()
    mark("force_spread")
    for p in range(4):
        wide_f[p, own, :] = with_edges(wide_f[p, own, :], fedge_e[p], fedge_w[p])
    force_copies = spread(wide_f, 4)
    start_spread(force_copies)

    mark("tracer_2")
    tail = lax.fori_loop(split, chunks, tracers, tail)

    def back_tracers(j, carry):
        k = K - 2 - j
        ratio = table[5 * K + k]
        out = []
        for m in range(2):
            for dest in (pt, ps):
                x = dest[k, m] + ratio * carry[len(out)]
                dest[k, m] = x
                out.append(x)
        return tuple(out)

    mark("back_tracers")
    lax.fori_loop(0, K - 1, back_tracers, tuple(linear(x)[:, 0:WIDTH] for x in tail), unroll=2)

    def back(j, carry):
        k = K - 2 - j
        ratio = table[2 * K + k]
        out = []
        for m in range(2):
            xu, xv, su, sv = carry[m]
            xu = pu[k, m] + ratio * xu
            xv = pv[k, m] + ratio * xv
            pu[k, m] = xu
            pv[k, m] = xv
            out.append((xu, xv, su + xu, sv + xv))
        return tuple(out)

    mark("back_uv")
    start = tuple(tuple(linear(members[m][n])[:, 0:WIDTH] for n in (3, 4, 3, 4)) for m in range(2))
    ends = lax.fori_loop(0, K - 1, back, start)

    mark("static_wait")
    finish_spread(static_copies)
    mark("force_wait")
    finish_spread(force_copies)

    mark("coef")
    depth = wide[0]
    depth_e = pltpu.roll(depth, PADDED - 1, 1)
    depth_n = pltpu.roll(depth, 79, 0)
    hu = jnp.where((depth > 0.0) & (depth_e > 0.0), 0.5 * (depth + depth_e), 0.0)
    hv = jnp.where((depth > 0.0) & (depth_n > 0.0), 0.5 * (depth + depth_n), 0.0)
    coef[0] = WAVE_COURANT * hu
    coef[1] = WAVE_COURANT * hv
    for m in range(2):
        wide_f[m] = hu * wide_f[m] * (1.0 / SUBCYCLES)
        wide_f[2 + m] = hv * wide_f[2 + m] * (1.0 / SUBCYCLES)
        for p in range(3):
            avg[2 * p + m] = zero

    def subcycles(first, last, margin):
        height = ROWS + 2 * margin
        rows = pl.ds(HALO - margin, height)
        mine = slice(margin, margin + ROWS)

        def subcycle(n, _):
            weight = weights[n]
            for m in range(2):
                eta, tx, ty = wide[1 + m, rows], wide[3 + m, rows], wide[5 + m, rows]
                eta = eta - WAVE_COURANT * (tx - pltpu.roll(tx, 1, 1) + ty - pltpu.roll(ty, 1, 0))
                tx = tx + wide_f[m, rows] - coef[0, rows] * (pltpu.roll(eta, PADDED - 1, 1) - eta)
                ty = ty + wide_f[2 + m, rows] - coef[1, rows] * (pltpu.roll(eta, height - 1, 0) - eta)
                wide[1 + m, rows] = eta
                wide[3 + m, rows] = tx
                wide[5 + m, rows] = ty
                avg[m] = avg[m] + weight * eta[mine]
                avg[2 + m] = avg[2 + m] + weight * tx[mine]
                avg[4 + m] = avg[4 + m] + weight * ty[mine]
            return 0

        lax.fori_loop(first, last, subcycle, 0)

    mark("subcycles")
    subcycles(0, SUBCYCLES - 16, HALO)
    subcycles(SUBCYCLES - 16, SUBCYCLES, 16)

    mark("corr")
    mine = slice(HALO, HALO + ROWS)
    for m in range(2):
        corr[m] = avg[2 + m] / jnp.where(hu[mine] > 0.0, hu[mine], 1.0) - padded(ends[m][2]) / count_u
        corr[2 + m] = avg[4 + m] / jnp.where(hv[mine] > 0.0, hv[mine], 1.0) - padded(ends[m][3]) / count_v

    mark("send_wait")
    for i in range(chunks):
        west_copy(i).wait_send()
        east_copy(i).wait_send()

    @pl.when(has_s)
    def _():
        for i in range(chunks):
            south_copy(i).wait_send()
            corner_u(i).wait_send()

    @pl.when(has_n)
    def _():
        for i in range(chunks):
            north_copy(i).wait_send()
            corner_v(i).wait_send()
    mark("")


def finish_kernel(size, pu, pv, pt, ps, corr, faces, avg, eta_o, tx_o, ty_o, u_o, v_o, t_o, s_o, sems):
    first = pl.program_id(0) * size
    through = [pltpu.make_async_copy(src, dst, sems.at[i]) for i, (src, dst) in enumerate(((pt, t_o), (ps, s_o)))]

    @pl.when(first == 0)
    def _():
        for copy in through:
            copy.start()
        for m in range(2):
            eta_o[m] = avg[m][:, 0:WIDTH]
            tx_o[m] = avg[2 + m][:, 0:WIDTH]
            ty_o[m] = avg[4 + m][:, 0:WIDTH]

    for j in range(size):
        level = (first + j).astype(F32)
        for m in range(2):
            for face, (src, dst) in enumerate(((pu, u_o), (pv, v_o))):
                wet = faces[face][:, 0:WIDTH] > level
                dst[j, m] = jnp.where(wet, src[first + j, m] + corr[2 * face + m][:, 0:WIDTH], 0.0)

    @pl.when(pl.program_id(0) == pl.num_programs(0) - 1)
    def _():
        for copy in through:
            copy.wait()


def solution(mesh):
    col_count, row_count = mesh.shape["col"], mesh.shape["row"]

    def local_step(vel_x, vel_y, pot_temp, salinity, surf_eta, trans_x, trans_y, col_depth, wet_levels, avg_weights):
        K = vel_x.shape[0]
        size = level_chunk(K)
        chunks = K // size
        table = jnp.asarray(solve_tables(K))
        smem = pl.BlockSpec(memory_space=pltpu.SMEM)
        vmem = pl.BlockSpec(memory_space=pltpu.VMEM)
        hbm = pl.BlockSpec(memory_space=pl.ANY)
        full = jax.ShapeDtypeStruct((K, 2, ROWS, WIDTH), F32)
        held = pltpu.VMEM((K, 2, ROWS, WIDTH), F32)
        dma = pltpu.SemaphoreType.DMA
        outs = pl.pallas_call(
            functools.partial(step_kernel, row_count, col_count, K),
            out_shape=(held,) * 4 + tuple(pltpu.VMEM((n, ROWS, PADDED), F32) for n in (4, 2, 6)),
            in_specs=[smem, smem] + [vmem] * 5 + [hbm] * 4,
            out_specs=(vmem,) * 7,
            scratch_shapes=[
                *[pltpu.VMEM((K, 2, ROWS, WIDTH), F32)] * 4,
                *[pltpu.VMEM((K, 2, ROWS, PADDED), F32)] * 4,
                *[pltpu.VMEM((chunks * (size + (size + 1) // 2), 8, LANES), F32)] * 4,
                pltpu.VMEM((1, WIDTH), jnp.int32),
                *[pltpu.VMEM((chunks, ROWS, LANES), F32)] * 4,
                *[pltpu.VMEM((chunks, 8, LANES), F32)] * 2,
                *[pltpu.VMEM((7, ROWS, LANES), F32)] * 2,
                pltpu.VMEM((7, 80, PADDED), F32),
                *[pltpu.VMEM((4, ROWS, LANES), F32)] * 2,
                pltpu.VMEM((4, 80, PADDED), F32),
                pltpu.VMEM((2, 80, PADDED), F32),
                dma((chunks, 4)), dma((2, chunks)), dma((2, chunks)), dma((4, chunks)), dma((4, chunks)), dma((5,)), dma((5,)), dma((8,)), dma((8,)),
            ],
            compiler_params=pltpu.CompilerParams(collective_id=0, has_side_effects=True, vmem_limit_bytes=53 << 20),
            name="ocean_step",
        )(table, avg_weights, wet_levels, col_depth, surf_eta, trans_x, trans_y, vel_x, vel_y, pot_temp, salinity)

        small = jax.ShapeDtypeStruct((2, ROWS, WIDTH), F32)
        deep_out = pl.BlockSpec((size, 2, ROWS, WIDTH), lambda i: (i, 0, 0, 0))
        small_out = pl.BlockSpec((2, ROWS, WIDTH), lambda i: (0, 0, 0))
        return pl.pallas_call(
            functools.partial(finish_kernel, size),
            grid=(chunks,),
            out_shape=(small,) * 3 + (full,) * 4,
            in_specs=[vmem] * 7,
            out_specs=(small_out,) * 3 + (deep_out,) * 2 + (hbm,) * 2,
            scratch_shapes=[dma((2,))],
            compiler_params=pltpu.CompilerParams(vmem_limit_bytes=20 << 20),
            name="ocean_finish",
        )(*outs)

    spec_3d = P(None, None, "row", "col")
    spec_2d = P(None, "row", "col")
    spec_map = P("row", "col")
    return jax.shard_map(local_step, mesh=mesh, in_specs=(spec_3d,) * 4 + (spec_2d,) * 3 + (spec_map,) * 2 + (P(),), out_specs=(spec_2d,) * 3 + (spec_3d,) * 4, check_vma=False)
```

```python
import functools
import numpy as np
import jax
import jax.numpy as jnp
from jax import lax
from jax.experimental import pallas as pl
from jax.experimental.pallas import tpu as pltpu
from jax.sharding import PartitionSpec as P

WAVE_COURANT = 0.4
THERM_EXP = 0.2
HALINE_CON = 0.15
PRESS_SCALE = 0.5
VISC_NUMBER = 1.0
DIFF_NUMBER = 0.5
SUBCYCLES = 30
HALO = 32
MOMENTUM_UNROLL = 3
TRACER_UNROLL = 3
ROWS, WIDTH, PADDED, LANES = 16, 192, 256, 128
MESH = pl.DeviceIdType.MESH
F32 = jnp.float32


def solve_tables(level_count):
    rows = []
    for strength in (VISC_NUMBER, DIFF_NUMBER):
        inner, last = np.zeros(level_count), np.zeros(level_count)
        inner[0], last[0] = 1.0 + strength, 1.0
        for k in range(1, level_count):
            inner[k] = 1.0 + 2.0 * strength - strength * strength / inner[k - 1]
            last[k] = 1.0 + strength - strength * strength / inner[k - 1]
        rows += [1.0 / inner, 1.0 / last, strength / inner]
    return np.concatenate(rows).astype(np.float32)


def level_chunk(level_count):
    for size in (15, 5, 4, 3, 2):
        if level_count % size == 0:
            return size
    return 1


def step_kernel(
    row_count, col_count, level_count,
    table, weights, kmt_in, depth_in, eta_in, tx_in, ty_in, u_hbm, v_hbm, t_hbm, s_hbm,
    pu, pv, pt, ps, corr, faces, avg,
    ub, vb, tb, sb, ue, ve, te, se, rows_n, rows_s, send_n, send_s, kmt_n, pack_w, pack_e, col_e, col_w, corner_se, corner_nw,
    edge_e, edge_w, wide, fedge_e, fedge_w, wide_f, coef,
    load_sem, row_send, row_recv, col_send, col_recv, misc_send, misc_recv, wide_send, wide_recv,
):
    K = level_count
    open_scope = []

    def mark(name):
        if open_scope:
            open_scope.pop().__exit__(None, None, None)
        if name:
            open_scope.append(jax.named_scope(name))
            open_scope[-1].__enter__()

    size = level_chunk(K)
    chunks = K // size
    half = (size + 1) // 2
    tile_count = size + half
    r = lax.axis_index("row")
    c = lax.axis_index("col")
    east = lax.rem(c + 1, col_count)
    west = lax.rem(c + col_count - 1, col_count)
    has_n, has_s = r < row_count - 1, r > 0
    has_nn, has_ss = r < row_count - 2, r > 1
    raw, ext = (ub, vb, tb, sb), (ue, ve, te, se)

    def one(flag):
        return flag.astype(jnp.int32)

    mark("init")
    loads = [
        [pltpu.make_async_copy(src.at[pl.ds(i * size, size)], dst.at[pl.ds(i * size, size)], load_sem.at[i, f]) for f, (src, dst) in enumerate(zip((u_hbm, v_hbm, t_hbm, s_hbm), raw))]
        for i in range(chunks)
    ]
    for group in loads:
        for copy in group:
            copy.start()

    wide[...] = jnp.zeros_like(wide)
    wide_f[...] = jnp.zeros_like(wide_f)

    @pl.when(jnp.logical_not(has_n))
    def _():
        rows_n[...] = jnp.zeros_like(rows_n)
        kmt_n[...] = jnp.zeros_like(kmt_n)
        corner_nw[...] = jnp.zeros_like(corner_nw)

    @pl.when(jnp.logical_not(has_s))
    def _():
        rows_s[...] = jnp.zeros_like(rows_s)
        corner_se[...] = jnp.zeros_like(corner_se)

    barrier = pltpu.get_barrier_semaphore()

    def signal(**where):
        pl.semaphore_signal(barrier, inc=1, device_id=where, device_id_type=MESH)

    signal(col=east)
    signal(col=west)

    @pl.when(has_n)
    def _():
        signal(row=r + 1)
        signal(row=r + 1, col=west)

    @pl.when(has_s)
    def _():
        signal(row=r - 1)
        signal(row=r - 1, col=east)

    @pl.when(has_nn)
    def _():
        signal(row=r + 2)

    @pl.when(has_ss)
    def _():
        signal(row=r - 2)

    def remote(src, dst, ssem, rsem, **where):
        return pltpu.make_async_remote_copy(src_ref=src, dst_ref=dst, send_sem=ssem, recv_sem=rsem, device_id=where, device_id_type=MESH)

    lane = lax.broadcasted_iota(jnp.int32, (ROWS, LANES), 1)
    lane8, lane1 = lane[0:8], lane[0:1]
    sub = lax.broadcasted_iota(jnp.int32, (8, LANES), 0)
    sub2 = lax.broadcasted_iota(jnp.int32, (8, PADDED), 0)

    def padded(x):
        return jnp.concatenate([x, jnp.zeros((x.shape[0], PADDED - WIDTH), x.dtype)], axis=1)

    def overlapped(x):
        a, b = x[:, 0:LANES], x[:, LANES:PADDED]
        return jnp.concatenate([a, jnp.where(lane < 64, b, a)], axis=1)

    def linear(x):
        a, b = x[:, 0:LANES], x[:, LANES:PADDED]
        return jnp.concatenate([jnp.where(lane < 96, a, b), b], axis=1)

    kmt = padded(kmt_in[...]).astype(F32)
    own = pl.ds(HALO, ROWS)
    wide[0, own, :] = jnp.where(kmt > 0.5, padded(depth_in[...]), 0.0)
    for m in range(2):
        wide[1 + m, own, :] = padded(eta_in[m])
        wide[3 + m, own, :] = padded(tx_in[m])
        wide[5 + m, own, :] = padded(ty_in[m])

    kmt_copy = remote(kmt_in.at[0:1, :], kmt_n, misc_send.at[0], misc_recv.at[0], row=r - 1)

    def south_copy(i):
        tiles = pl.ds(i * tile_count, tile_count)
        return remote(send_s.at[tiles], rows_n.at[tiles], row_send.at[0, i], row_recv.at[0, i], row=r - 1)

    def north_copy(i):
        tiles = pl.ds(i * tile_count, tile_count)
        return remote(send_n.at[tiles], rows_s.at[tiles], row_send.at[1, i], row_recv.at[1, i], row=r + 1)

    def west_copy(i):
        return remote(pack_w.at[i], col_e.at[i], col_send.at[0, i], col_recv.at[0, i], col=west)

    def east_copy(i):
        return remote(pack_e.at[i], col_w.at[i], col_send.at[1, i], col_recv.at[1, i], col=east)

    def corner_v(i):
        return remote(pack_w.at[i, 8:16, :], corner_se.at[i], col_send.at[2, i], col_recv.at[2, i], row=r + 1, col=west)

    def corner_u(i):
        return remote(pack_e.at[i, 0:8, :], corner_nw.at[i], col_send.at[3, i], col_recv.at[3, i], row=r - 1, col=east)

    def pack_level(h, k, j, acc):
        acc, tiles = list(acc), [None, None]
        for f in range(4):
            for m in range(2):
                spot = 2 * f + m
                x = raw[f][k, m, :, 0:LANES] if h == 0 else padded(raw[f][k, m, :, LANES:WIDTH])
                acc[spot] = jnp.where(lane == j, pltpu.roll(x, j if h == 0 else j + 65, 1), acc[spot])
                for side in range(2):
                    row = pltpu.roll(x[8 * side:8 * side + 8], (spot + side) % 8, 0)
                    tiles[side] = row if tiles[side] is None else jnp.where(sub == spot, row, tiles[side])
        return tuple(acc), tiles

    def pack_chunk(i):
        for copy in loads[i]:
            copy.wait()
        for h, pack in enumerate((pack_w, pack_e)):
            def pack_pair(j, acc):
                j2 = jnp.minimum(j + half, size - 1)
                acc, one_level = pack_level(h, i * size + j, j, acc)
                acc, other = pack_level(h, i * size + j2, j2, acc)
                for one_tile, other_tile, dest in zip(one_level, other, (send_s, send_n)):
                    if h == 0:
                        dest[i * tile_count + j] = one_tile
                        dest[i * tile_count + j2] = other_tile
                    else:
                        dest[i * tile_count + size + j] = jnp.where(lane8 < 64, one_tile, pltpu.roll(other_tile, 64, 1))
                return acc

            acc = lax.fori_loop(0, half, pack_pair, (jnp.zeros((ROWS, LANES), F32),) * 8, unroll=2)
            merged = pltpu.roll(kmt[:, 0:LANES], LANES - 1, 1)
            for spot in range(8):
                merged = jnp.where((lane >= size * spot) & (lane < size * spot + size), pltpu.roll(acc[spot], size * spot, 1), merged)
            pack[i] = merged

    def start_chunk(i):
        west_copy(i).start()
        east_copy(i).start()

        @pl.when(has_s)
        def _():
            corner_u(i).start()
            south_copy(i).start()

        @pl.when(has_n)
        def _():
            corner_v(i).start()
            north_copy(i).start()

    mark("pack_early")
    early = min(2, chunks)
    for i in range(early):
        pack_chunk(i)
    mark("barrier_wait")
    pl.semaphore_wait(barrier, 2 + 2 * one(has_n) + 2 * one(has_s) + one(has_nn) + one(has_ss))

    @pl.when(has_s)
    def _():
        kmt_copy.start()

    for i in range(early):
        start_chunk(i)
    mark("pack_late")
    for i in range(early, chunks):
        pack_chunk(i)
        start_chunk(i)

    def edge_pair(buf, to_east, to_west, sem):
        return [
            remote(buf.at[:, own, 0:LANES], to_west, misc_send.at[sem], misc_recv.at[sem], col=west),
            remote(buf.at[:, own, LANES:PADDED], to_east, misc_send.at[sem + 1], misc_recv.at[sem + 1], col=east),
        ]

    def with_edges(x, from_east, from_west):
        b = jnp.where(lane < 64, x[:, LANES:PADDED], jnp.where(lane < 96, pltpu.roll(from_east, 64, 1), pltpu.roll(from_west, 64, 1)))
        return jnp.concatenate([x[:, 0:LANES], b], axis=1)

    def spread(buf, sem):
        src = buf.at[:, own, :]
        parts = ((has_n, has_s, 16, r + 1), (has_s, has_n, 48, r - 1), (has_nn, has_ss, 0, r + 2), (has_ss, has_nn, 64, r - 2))
        return [(there, here, remote(src, buf.at[:, pl.ds(at, ROWS), :], wide_send.at[sem + n], wide_recv.at[sem + n], row=row)) for n, (there, here, at, row) in enumerate(parts)]

    def start_spread(copies):
        for there, _, copy in copies:
            @pl.when(there)
            def _():
                copy.start()

    def finish_spread(copies):
        for there, here, copy in copies:
            @pl.when(there)
            def _():
                copy.wait_send()

            @pl.when(here)
            def _():
                copy.wait_recv()

    mark("edges")
    edge_copies = edge_pair(wide, edge_w, edge_e, 1)
    for copy in edge_copies:
        copy.start()

    def roll_e(x):
        return jnp.concatenate([pltpu.roll(x[:, 0:LANES], LANES - 1, 1), pltpu.roll(x[:, LANES:PADDED], LANES - 1, 1)], axis=1)

    def roll_w(x):
        return jnp.concatenate([pltpu.roll(x[:, 0:LANES], 1, 1), pltpu.roll(x[:, LANES:PADDED], 1, 1)], axis=1)

    def from_north(x, edge):
        low, high = pltpu.roll(x[0:8], 7, 0), pltpu.roll(x[8:16], 7, 0)
        return jnp.concatenate([jnp.where(sub2 == 7, high, low), jnp.where(sub2 == 7, edge, high)], axis=0)

    def from_south(x, edge):
        low, high = pltpu.roll(x[0:8], 1, 0), pltpu.roll(x[8:16], 1, 0)
        return jnp.concatenate([jnp.where(sub2 == 0, edge, low), jnp.where(sub2 == 0, low, high)], axis=0)

    def wait_columns(i):
        west_copy(i).wait_recv()
        east_copy(i).wait_recv()

    def insert_columns(i):
        def level(j, _):
            k = i * size + j
            for f in range(4):
                for m in range(2):
                    place = size * (2 * f + m) + j
                    to_east = pltpu.roll(col_e[i], lax.rem(LANES + 64 - place, LANES), 1)
                    to_west = pltpu.roll(col_w[i], LANES - 1 - place, 1)
                    a = raw[f][k, m, :, 0:LANES]
                    b = padded(raw[f][k, m, :, LANES:WIDTH])
                    ext[f][k, m, :, 0:LANES] = jnp.where(lane == LANES - 1, to_west, a)
                    ext[f][k, m, :, LANES:PADDED] = jnp.where(lane < 64, b, jnp.where(lane == 64, to_east, a))
            return 0

        lax.fori_loop(0, size, level, 0, unroll=5)

    mark("column_wait")
    wait_columns(0)

    @pl.when(has_n)
    def _():
        kmt_copy.wait_recv()

    @pl.when(has_s)
    def _():
        kmt_copy.wait_send()

    mark("masks")
    kmt2 = overlapped(kmt)
    kmt_edge = jnp.where(lane == 64, pltpu.roll(col_e[0], 65, 1), kmt2[:, LANES:PADDED])
    kmt_row = padded(kmt_n[...]).astype(F32)
    kmt_north = jnp.concatenate([kmt_row[:, 0:LANES], jnp.where(lane1 < 64, kmt_row[:, LANES:PADDED], kmt_row[:, 0:LANES])], axis=1)
    mu = jnp.minimum(kmt2, roll_e(jnp.concatenate([kmt2[:, 0:LANES], kmt_edge], axis=1)))
    mv = jnp.minimum(kmt2, from_north(kmt2, kmt_north))
    faces[0] = linear(mu)
    faces[1] = linear(mv)

    def solve_factor(depth, k, first):
        inner, last = table[first * K + k], table[(first + 1) * K + k]
        kf = k.astype(F32)
        return jnp.where(depth > kf + 1.0, inner, jnp.where(depth > kf, last, 0.0))

    def edge_tiles(rows, i, j, shifted):
        late = one(j >= half)
        first = i * tile_count
        a, b_raw = rows[first + j], rows[first + size + j - half * late]
        late = 64 * late
        b = jnp.where(lane8 < 64, pltpu.roll(b_raw, late, 1), a)
        if shifted == 0:
            return a, b
        if shifted == 1:
            a1 = pltpu.roll(a, 1, 1)
            return a, b, a1, jnp.where((lane8 >= 1) & (lane8 < 65), pltpu.roll(b_raw, late + 1, 1), a1)
        a1 = pltpu.roll(a, LANES - 1, 1)
        return a, b, a1, jnp.where((lane8 < 63) | (lane8 == LANES - 1), pltpu.roll(b_raw, lax.rem(late + LANES - 1, LANES), 1), a1)

    def join(a, b, spot):
        return jnp.concatenate([a[spot:spot + 1], b[spot:spot + 1]], axis=1)

    half_scale = 0.5 * PRESS_SCALE / K
    edge_weight = jnp.where(sub < 6, -half_scale * THERM_EXP, half_scale * HALINE_CON)

    def momentum(i):
        def level(j, carry):
            (na, nb), members = carry
            k = i * size + j
            kf = k.astype(F32)
            an, bn, wan, wbn = edge_tiles(rows_n, i, j, 1)
            as_, bs, eas, ebs = edge_tiles(rows_s, i, j, 2)
            xa, xb = an * edge_weight, bn * edge_weight
            ha, hb = xa + pltpu.roll(xa, 6, 0), xb + pltpu.roll(xb, 6, 0)
            pna, pnb = na + ha, nb + hb
            factor_u, factor_v = solve_factor(mu, k, 0), solve_factor(mv, k, 0)
            out = []
            for m in range(2):
                total, gu_sum, gv_sum, side_u, side_v = members[m]
                u, v = ue[k, m], ve[k, m]
                step = (half_scale * HALINE_CON) * se[k, m] - (half_scale * THERM_EXP) * te[k, m]
                pressure = total + step
                corner_n = pltpu.roll(corner_nw[i], LANES - (size * m + j), 1)[0:1]
                corner_s = pltpu.roll(corner_se[i], lax.rem(LANES + 63 - (size * (2 + m) + j), LANES), 1)[7:8]
                u_edge = join(an, bn, m)
                v_edge = join(as_, bs, 2 + m)
                u_edge_w = jnp.concatenate([jnp.where(lane1 == 0, corner_n, wan[m:m + 1]), wbn[m:m + 1]], axis=1)
                v_edge_e = jnp.concatenate([eas[2 + m:3 + m], jnp.where(lane1 == 63, corner_s, ebs[2 + m:3 + m])], axis=1)
                v_e, v_w, u_e, u_w = roll_e(v), roll_w(v), roll_e(u), roll_w(u)
                v_pair, u_pair = v + v_e, u + u_w
                vu = 0.125 * (v_pair + from_south(v_pair, v_edge + v_edge_e))
                uv = 0.125 * (u_pair + from_north(u_pair, u_edge + u_edge_w))
                u_n, u_s = from_north(u, u_edge), from_south(u, join(as_, bs, m))
                v_n, v_s = from_north(v, join(an, bn, 2 + m)), from_south(v, v_edge)
                p_n = from_north(pressure, join(pna, pnb, 4 + m))
                gu = pressure - roll_e(pressure) - 0.5 * u * (u_e - u_w) - vu * (u_n - u_s)
                gv = pressure - p_n - uv * (v_e - v_w) - 0.5 * v * (v_n - v_s)
                gu = jnp.where(mu > kf, gu, 0.0)
                gv = jnp.where(mv > kf, gv, 0.0)
                side_u = (u + gu + VISC_NUMBER * side_u) * factor_u
                side_v = (v + gv + VISC_NUMBER * side_v) * factor_v
                pu[k, m] = linear(side_u)[:, 0:WIDTH]
                pv[k, m] = linear(side_v)[:, 0:WIDTH]
                out.append((pressure + step, gu_sum + gu, gv_sum + gv, side_u, side_v))
            return (pna + ha, pnb + hb), tuple(out)

        return level

    zero = jnp.zeros((ROWS, PADDED), F32)
    zero_row = jnp.zeros((8, LANES), F32)
    carry = ((zero_row, zero_row), ((zero,) * 5,) * 2)
    for i in range(chunks):
        if i > 0:
            wait_columns(i)
        mark("insert")
        insert_columns(i)

        mark("row_wait")
        @pl.when(has_n)
        def _():
            south_copy(i).wait_recv()
            corner_u(i).wait_recv()

        @pl.when(has_s)
        def _():
            north_copy(i).wait_recv()
            corner_v(i).wait_recv()

        mark("momentum")
        carry = lax.fori_loop(0, size, momentum(i), carry, unroll=MOMENTUM_UNROLL)

        mark("next")
        if i == chunks // 2:
            for copy in edge_copies:
                copy.wait()
            for p in range(7):
                wide[p, own, :] = with_edges(wide[p, own, :], edge_e[p], edge_w[p])
            static_copies = spread(wide, 0)
            start_spread(static_copies)

    members = carry[1]
    mark("force")
    count_u = linear(jnp.maximum(mu, 1.0))
    count_v = linear(jnp.maximum(mv, 1.0))
    for m in range(2):
        wide_f[m, own, :] = linear(members[m][1]) / count_u
        wide_f[2 + m, own, :] = linear(members[m][2]) / count_v
    force_edges = edge_pair(wide_f, fedge_w, fedge_e, 3)
    for copy in force_edges:
        copy.start()

    def tracers(i, carry):
        def level(j, carry):
            k = i * size + j
            an, bn = edge_tiles(rows_n, i, j, 0)
            as_, bs = edge_tiles(rows_s, i, j, 0)
            factor = solve_factor(kmt2, k, 3)
            out = []
            for m in range(2):
                u, v = 0.5 * ue[k, m], 0.5 * ve[k, m]
                u_w = roll_w(u)
                v_edge = 0.5 * join(as_, bs, 2 + m)
                for f, dest in ((2, pt), (3, ps)):
                    t = ext[f][k, m]
                    flux_x = u * (t + roll_e(t)) - u_w * (t + roll_w(t))
                    flux_y = v * (t + from_north(t, join(an, bn, 2 * f + m)))
                    flux_s = v_edge * (join(as_, bs, 2 * f + m) + t[0:1])
                    moved = t - (flux_x + flux_y - from_south(flux_y, flux_s))
                    side = (moved + DIFF_NUMBER * carry[len(out)]) * factor
                    dest[k, m] = linear(side)[:, 0:WIDTH]
                    out.append(side)
            return tuple(out)

        return lax.fori_loop(0, size, level, carry, unroll=TRACER_UNROLL)

    mark("tracer_1")
    tail = (zero,) * 4
    split = (3 * chunks + 4) // 5
    tail = lax.fori_loop(0, split, tracers, tail)

    mark("force_edge_wait")
    for copy in force_edges:
        copy.wait()
    mark("force_spread")
    for p in range(4):
        wide_f[p, own, :] = with_edges(wide_f[p, own, :], fedge_e[p], fedge_w[p])
    force_copies = spread(wide_f, 4)
    start_spread(force_copies)

    mark("tracer_2")
    tail = lax.fori_loop(split, chunks, tracers, tail)

    def back_tracers(j, carry):
        k = K - 2 - j
        ratio = table[5 * K + k]
        out = []
        for m in range(2):
            for dest in (pt, ps):
                x = dest[k, m] + ratio * carry[len(out)]
                dest[k, m] = x
                out.append(x)
        return tuple(out)

    mark("back_tracers")
    lax.fori_loop(0, K - 1, back_tracers, tuple(linear(x)[:, 0:WIDTH] for x in tail), unroll=2)

    def back(j, carry):
        k = K - 2 - j
        ratio = table[2 * K + k]
        out = []
        for m in range(2):
            xu, xv, su, sv = carry[m]
            xu = pu[k, m] + ratio * xu
            xv = pv[k, m] + ratio * xv
            pu[k, m] = xu
            pv[k, m] = xv
            out.append((xu, xv, su + xu, sv + xv))
        return tuple(out)

    mark("back_uv")
    start = tuple(tuple(linear(members[m][n])[:, 0:WIDTH] for n in (3, 4, 3, 4)) for m in range(2))
    ends = lax.fori_loop(0, K - 1, back, start)

    mark("static_wait")
    finish_spread(static_copies)
    mark("force_wait")
    finish_spread(force_copies)

    mark("coef")
    depth = wide[0]
    depth_e = pltpu.roll(depth, PADDED - 1, 1)
    depth_n = pltpu.roll(depth, 79, 0)
    hu = jnp.where((depth > 0.0) & (depth_e > 0.0), 0.5 * (depth + depth_e), 0.0)
    hv = jnp.where((depth > 0.0) & (depth_n > 0.0), 0.5 * (depth + depth_n), 0.0)
    coef[0] = WAVE_COURANT * hu
    coef[1] = WAVE_COURANT * hv
    for m in range(2):
        wide_f[m] = hu * wide_f[m] * (1.0 / SUBCYCLES)
        wide_f[2 + m] = hv * wide_f[2 + m] * (1.0 / SUBCYCLES)
        for p in range(3):
            avg[2 * p + m] = zero

    def subcycles(first, last, margin):
        height = ROWS + 2 * margin
        rows = pl.ds(HALO - margin, height)
        mine = slice(margin, margin + ROWS)

        def subcycle(n, _):
            weight = weights[n]
            for m in range(2):
                eta, tx, ty = wide[1 + m, rows], wide[3 + m, rows], wide[5 + m, rows]
                eta = eta - WAVE_COURANT * (tx - pltpu.roll(tx, 1, 1) + ty - pltpu.roll(ty, 1, 0))
                tx = tx + wide_f[m, rows] - coef[0, rows] * (pltpu.roll(eta, PADDED - 1, 1) - eta)
                ty = ty + wide_f[2 + m, rows] - coef[1, rows] * (pltpu.roll(eta, height - 1, 0) - eta)
                wide[1 + m, rows] = eta
                wide[3 + m, rows] = tx
                wide[5 + m, rows] = ty
                avg[m] = avg[m] + weight * eta[mine]
                avg[2 + m] = avg[2 + m] + weight * tx[mine]
                avg[4 + m] = avg[4 + m] + weight * ty[mine]
            return 0

        lax.fori_loop(first, last, subcycle, 0)

    mark("subcycles")
    subcycles(0, SUBCYCLES - 16, HALO)
    subcycles(SUBCYCLES - 16, SUBCYCLES, 16)

    mark("corr")
    mine = slice(HALO, HALO + ROWS)
    for m in range(2):
        corr[m] = avg[2 + m] / jnp.where(hu[mine] > 0.0, hu[mine], 1.0) - padded(ends[m][2]) / count_u
        corr[2 + m] = avg[4 + m] / jnp.where(hv[mine] > 0.0, hv[mine], 1.0) - padded(ends[m][3]) / count_v

    mark("send_wait")
    for i in range(chunks):
        west_copy(i).wait_send()
        east_copy(i).wait_send()

    @pl.when(has_s)
    def _():
        for i in range(chunks):
            south_copy(i).wait_send()
            corner_u(i).wait_send()

    @pl.when(has_n)
    def _():
        for i in range(chunks):
            north_copy(i).wait_send()
            corner_v(i).wait_send()
    mark("")


def finish_kernel(size, pu, pv, pt, ps, corr, faces, avg, eta_o, tx_o, ty_o, u_o, v_o, t_o, s_o, sems):
    first = pl.program_id(0) * size
    through = [pltpu.make_async_copy(src, dst, sems.at[i]) for i, (src, dst) in enumerate(((pt, t_o), (ps, s_o)))]

    @pl.when(first == 0)
    def _():
        for copy in through:
            copy.start()
        for m in range(2):
            eta_o[m] = avg[m][:, 0:WIDTH]
            tx_o[m] = avg[2 + m][:, 0:WIDTH]
            ty_o[m] = avg[4 + m][:, 0:WIDTH]

    for j in range(size):
        level = (first + j).astype(F32)
        for m in range(2):
            for face, (src, dst) in enumerate(((pu, u_o), (pv, v_o))):
                wet = faces[face][:, 0:WIDTH] > level
                dst[j, m] = jnp.where(wet, src[first + j, m] + corr[2 * face + m][:, 0:WIDTH], 0.0)

    @pl.when(pl.program_id(0) == pl.num_programs(0) - 1)
    def _():
        for copy in through:
            copy.wait()


def solution(mesh):
    col_count, row_count = mesh.shape["col"], mesh.shape["row"]

    def local_step(vel_x, vel_y, pot_temp, salinity, surf_eta, trans_x, trans_y, col_depth, wet_levels, avg_weights):
        K = vel_x.shape[0]
        size = level_chunk(K)
        chunks = K // size
        table = jnp.asarray(solve_tables(K))
        smem = pl.BlockSpec(memory_space=pltpu.SMEM)
        vmem = pl.BlockSpec(memory_space=pltpu.VMEM)
        hbm = pl.BlockSpec(memory_space=pl.ANY)
        full = jax.ShapeDtypeStruct((K, 2, ROWS, WIDTH), F32)
        held = pltpu.VMEM((K, 2, ROWS, WIDTH), F32)
        dma = pltpu.SemaphoreType.DMA
        outs = pl.pallas_call(
            functools.partial(step_kernel, row_count, col_count, K),
            out_shape=(held,) * 4 + tuple(pltpu.VMEM((n, ROWS, PADDED), F32) for n in (4, 2, 6)),
            in_specs=[smem, smem] + [vmem] * 5 + [hbm] * 4,
            out_specs=(vmem,) * 7,
            scratch_shapes=[
                *[pltpu.VMEM((K, 2, ROWS, WIDTH), F32)] * 4,
                *[pltpu.VMEM((K, 2, ROWS, PADDED), F32)] * 4,
                *[pltpu.VMEM((chunks * (size + (size + 1) // 2), 8, LANES), F32)] * 4,
                pltpu.VMEM((1, WIDTH), jnp.int32),
                *[pltpu.VMEM((chunks, ROWS, LANES), F32)] * 4,
                *[pltpu.VMEM((chunks, 8, LANES), F32)] * 2,
                *[pltpu.VMEM((7, ROWS, LANES), F32)] * 2,
                pltpu.VMEM((7, 80, PADDED), F32),
                *[pltpu.VMEM((4, ROWS, LANES), F32)] * 2,
                pltpu.VMEM((4, 80, PADDED), F32),
                pltpu.VMEM((2, 80, PADDED), F32),
                dma((chunks, 4)), dma((2, chunks)), dma((2, chunks)), dma((4, chunks)), dma((4, chunks)), dma((5,)), dma((5,)), dma((8,)), dma((8,)),
            ],
            compiler_params=pltpu.CompilerParams(collective_id=0, has_side_effects=True, vmem_limit_bytes=53 << 20),
            name="ocean_step",
        )(table, avg_weights, wet_levels, col_depth, surf_eta, trans_x, trans_y, vel_x, vel_y, pot_temp, salinity)

        small = jax.ShapeDtypeStruct((2, ROWS, WIDTH), F32)
        deep_out = pl.BlockSpec((size, 2, ROWS, WIDTH), lambda i: (i, 0, 0, 0))
        small_out = pl.BlockSpec((2, ROWS, WIDTH), lambda i: (0, 0, 0))
        return pl.pallas_call(
            functools.partial(finish_kernel, size),
            grid=(chunks,),
            out_shape=(small,) * 3 + (full,) * 4,
            in_specs=[vmem] * 7,
            out_specs=(small_out,) * 3 + (deep_out,) * 2 + (hbm,) * 2,
            scratch_shapes=[dma((2,))],
            compiler_params=pltpu.CompilerParams(vmem_limit_bytes=20 << 20),
            name="ocean_finish",
        )(*outs)

    spec_3d = P(None, None, "row", "col")
    spec_2d = P(None, "row", "col")
    spec_map = P("row", "col")
    return jax.shard_map(local_step, mesh=mesh, in_specs=(spec_3d,) * 4 + (spec_2d,) * 3 + (spec_map,) * 2 + (P(),), out_specs=(spec_2d,) * 3 + (spec_3d,) * 4, check_vma=False)
```

```python
import functools
import numpy as np
import jax
import jax.numpy as jnp
from jax import lax
from jax.experimental import pallas as pl
from jax.experimental.pallas import tpu as pltpu
from jax.sharding import PartitionSpec as P

WAVE_COURANT = 0.4
THERM_EXP = 0.2
HALINE_CON = 0.15
PRESS_SCALE = 0.5
VISC_NUMBER = 1.0
DIFF_NUMBER = 0.5
SUBCYCLES = 30
HALO = 32
MOMENTUM_UNROLL = 5
TRACER_UNROLL = 5
ROWS, WIDTH, PADDED, LANES = 16, 192, 256, 128
MESH = pl.DeviceIdType.MESH
F32 = jnp.float32


def solve_tables(level_count):
    rows = []
    for strength in (VISC_NUMBER, DIFF_NUMBER):
        inner, last = np.zeros(level_count), np.zeros(level_count)
        inner[0], last[0] = 1.0 + strength, 1.0
        for k in range(1, level_count):
            inner[k] = 1.0 + 2.0 * strength - strength * strength / inner[k - 1]
            last[k] = 1.0 + strength - strength * strength / inner[k - 1]
        rows += [1.0 / inner, 1.0 / last, strength / inner]
    return np.concatenate(rows).astype(np.float32)


def level_chunk(level_count):
    for size in (15, 5, 4, 3, 2):
        if level_count % size == 0:
            return size
    return 1


def step_kernel(
    row_count, col_count, level_count,
    table, weights, kmt_in, depth_in, eta_in, tx_in, ty_in, u_hbm, v_hbm, t_hbm, s_hbm,
    pu, pv, pt, ps, corr, faces, avg,
    ub, vb, tb, sb, ue, ve, te, se, rows_n, rows_s, send_n, send_s, kmt_n, pack_w, pack_e, col_e, col_w, corner_se, corner_nw,
    edge_e, edge_w, wide, fedge_e, fedge_w, wide_f, coef, east_eta,
    load_sem, row_send, row_recv, col_send, col_recv, misc_send, misc_recv, wide_send, wide_recv,
):
    K = level_count
    open_scope = []

    def mark(name):
        if open_scope:
            open_scope.pop().__exit__(None, None, None)
        if name:
            open_scope.append(jax.named_scope(name))
            open_scope[-1].__enter__()

    size = level_chunk(K)
    chunks = K // size
    half = (size + 1) // 2
    tile_count = size + half
    r = lax.axis_index("row")
    c = lax.axis_index("col")
    east = lax.rem(c + 1, col_count)
    west = lax.rem(c + col_count - 1, col_count)
    has_n, has_s = r < row_count - 1, r > 0
    has_nn, has_ss = r < row_count - 2, r > 1
    raw, ext = (ub, vb, tb, sb), (ue, ve, te, se)

    def one(flag):
        return flag.astype(jnp.int32)

    mark("init")
    loads = [
        [pltpu.make_async_copy(src.at[pl.ds(i * size, size)], dst.at[pl.ds(i * size, size)], load_sem.at[i, f]) for f, (src, dst) in enumerate(zip((u_hbm, v_hbm, t_hbm, s_hbm), raw))]
        for i in range(chunks)
    ]
    for group in loads:
        for copy in group:
            copy.start()

    wide[...] = jnp.zeros_like(wide)
    wide_f[...] = jnp.zeros_like(wide_f)

    @pl.when(jnp.logical_not(has_n))
    def _():
        rows_n[...] = jnp.zeros_like(rows_n)
        kmt_n[...] = jnp.zeros_like(kmt_n)
        corner_nw[...] = jnp.zeros_like(corner_nw)

    @pl.when(jnp.logical_not(has_s))
    def _():
        rows_s[...] = jnp.zeros_like(rows_s)
        corner_se[...] = jnp.zeros_like(corner_se)

    barrier = pltpu.get_barrier_semaphore()

    def signal(**where):
        pl.semaphore_signal(barrier, inc=1, device_id=where, device_id_type=MESH)

    signal(col=east)
    signal(col=west)

    @pl.when(has_n)
    def _():
        signal(row=r + 1)
        signal(row=r + 1, col=west)

    @pl.when(has_s)
    def _():
        signal(row=r - 1)
        signal(row=r - 1, col=east)

    @pl.when(has_nn)
    def _():
        signal(row=r + 2)

    @pl.when(has_ss)
    def _():
        signal(row=r - 2)

    def remote(src, dst, ssem, rsem, **where):
        return pltpu.make_async_remote_copy(src_ref=src, dst_ref=dst, send_sem=ssem, recv_sem=rsem, device_id=where, device_id_type=MESH)

    lane = lax.broadcasted_iota(jnp.int32, (ROWS, LANES), 1)
    lane8, lane1 = lane[0:8], lane[0:1]
    sub = lax.broadcasted_iota(jnp.int32, (8, LANES), 0)
    sub2 = lax.broadcasted_iota(jnp.int32, (8, PADDED), 0)

    def padded(x):
        return jnp.concatenate([x, jnp.zeros((x.shape[0], PADDED - WIDTH), x.dtype)], axis=1)

    def overlapped(x):
        a, b = x[:, 0:LANES], x[:, LANES:PADDED]
        return jnp.concatenate([a, jnp.where(lane < 64, b, a)], axis=1)

    def linear(x):
        a, b = x[:, 0:LANES], x[:, LANES:PADDED]
        return jnp.concatenate([jnp.where(lane < 96, a, b), b], axis=1)

    kmt = padded(kmt_in[...]).astype(F32)
    own = pl.ds(HALO, ROWS)
    wide[0, own, :] = jnp.where(kmt > 0.5, padded(depth_in[...]), 0.0)
    for m in range(2):
        wide[1 + m, own, :] = padded(eta_in[m])
        wide[3 + m, own, :] = padded(tx_in[m])
        wide[5 + m, own, :] = padded(ty_in[m])

    kmt_copy = remote(kmt_in.at[0:1, :], kmt_n, misc_send.at[0], misc_recv.at[0], row=r - 1)

    def south_copy(i):
        tiles = pl.ds(i * tile_count, tile_count)
        return remote(send_s.at[tiles], rows_n.at[tiles], row_send.at[0, i], row_recv.at[0, i], row=r - 1)

    def north_copy(i):
        tiles = pl.ds(i * tile_count, tile_count)
        return remote(send_n.at[tiles], rows_s.at[tiles], row_send.at[1, i], row_recv.at[1, i], row=r + 1)

    def west_copy(i):
        return remote(pack_w.at[i], col_e.at[i], col_send.at[0, i], col_recv.at[0, i], col=west)

    def east_copy(i):
        return remote(pack_e.at[i], col_w.at[i], col_send.at[1, i], col_recv.at[1, i], col=east)

    def corner_v(i):
        return remote(pack_w.at[i, 8:16, :], corner_se.at[i], col_send.at[2, i], col_recv.at[2, i], row=r + 1, col=west)

    def corner_u(i):
        return remote(pack_e.at[i, 0:8, :], corner_nw.at[i], col_send.at[3, i], col_recv.at[3, i], row=r - 1, col=east)

    def pack_level(h, k, j, acc):
        acc, tiles = list(acc), [None, None]
        for f in range(4):
            for m in range(2):
                spot = 2 * f + m
                x = raw[f][k, m, :, 0:LANES] if h == 0 else padded(raw[f][k, m, :, LANES:WIDTH])
                acc[spot] = jnp.where(lane == j, pltpu.roll(x, j if h == 0 else j + 65, 1), acc[spot])
                for side in range(2):
                    row = pltpu.roll(x[8 * side:8 * side + 8], (spot + side) % 8, 0)
                    tiles[side] = row if tiles[side] is None else jnp.where(sub == spot, row, tiles[side])
        return tuple(acc), tiles

    def pack_chunk(i):
        for copy in loads[i]:
            copy.wait()
        for h, pack in enumerate((pack_w, pack_e)):
            def pack_pair(j, acc):
                j2 = jnp.minimum(j + half, size - 1)
                acc, one_level = pack_level(h, i * size + j, j, acc)
                acc, other = pack_level(h, i * size + j2, j2, acc)
                for one_tile, other_tile, dest in zip(one_level, other, (send_s, send_n)):
                    if h == 0:
                        dest[i * tile_count + j] = one_tile
                        dest[i * tile_count + j2] = other_tile
                    else:
                        dest[i * tile_count + size + j] = jnp.where(lane8 < 64, one_tile, pltpu.roll(other_tile, 64, 1))
                return acc

            acc = lax.fori_loop(0, half, pack_pair, (jnp.zeros((ROWS, LANES), F32),) * 8, unroll=half)
            merged = pltpu.roll(kmt[:, 0:LANES], LANES - 1, 1)
            for spot in range(8):
                merged = jnp.where((lane >= size * spot) & (lane < size * spot + size), pltpu.roll(acc[spot], size * spot, 1), merged)
            pack[i] = merged

    def start_chunk(i):
        west_copy(i).start()
        east_copy(i).start()

        @pl.when(has_s)
        def _():
            corner_u(i).start()
            south_copy(i).start()

        @pl.when(has_n)
        def _():
            corner_v(i).start()
            north_copy(i).start()

    mark("pack_early")
    early = min(2, chunks)
    for i in range(early):
        pack_chunk(i)
    mark("barrier_wait")
    pl.semaphore_wait(barrier, 2 + 2 * one(has_n) + 2 * one(has_s) + one(has_nn) + one(has_ss))

    @pl.when(has_s)
    def _():
        kmt_copy.start()

    for i in range(early):
        start_chunk(i)
    mark("pack_late")
    for i in range(early, chunks):
        pack_chunk(i)
        start_chunk(i)

    def edge_pair(buf, to_east, to_west, sem):
        return [
            remote(buf.at[:, own, 0:LANES], to_west, misc_send.at[sem], misc_recv.at[sem], col=west),
            remote(buf.at[:, own, LANES:PADDED], to_east, misc_send.at[sem + 1], misc_recv.at[sem + 1], col=east),
        ]

    def with_edges(x, from_east, from_west):
        b = jnp.where(lane < 64, x[:, LANES:PADDED], jnp.where(lane < 96, pltpu.roll(from_east, 64, 1), pltpu.roll(from_west, 64, 1)))
        return jnp.concatenate([x[:, 0:LANES], b], axis=1)

    def spread(buf, sem):
        src = buf.at[:, own, :]
        parts = ((has_n, has_s, 16, r + 1), (has_s, has_n, 48, r - 1), (has_nn, has_ss, 0, r + 2), (has_ss, has_nn, 64, r - 2))
        return [(there, here, remote(src, buf.at[:, pl.ds(at, ROWS), :], wide_send.at[sem + n], wide_recv.at[sem + n], row=row)) for n, (there, here, at, row) in enumerate(parts)]

    def start_spread(copies):
        for there, _, copy in copies:
            @pl.when(there)
            def _():
                copy.start()

    def finish_spread(copies):
        for there, here, copy in copies:
            @pl.when(there)
            def _():
                copy.wait_send()

            @pl.when(here)
            def _():
                copy.wait_recv()

    mark("edges")
    edge_copies = edge_pair(wide, edge_w, edge_e, 1)
    for copy in edge_copies:
        copy.start()

    def roll_e(x):
        return jnp.concatenate([pltpu.roll(x[:, 0:LANES], LANES - 1, 1), pltpu.roll(x[:, LANES:PADDED], LANES - 1, 1)], axis=1)

    def roll_w(x):
        return jnp.concatenate([pltpu.roll(x[:, 0:LANES], 1, 1), pltpu.roll(x[:, LANES:PADDED], 1, 1)], axis=1)

    def from_north(x, edge):
        low, high = pltpu.roll(x[0:8], 7, 0), pltpu.roll(x[8:16], 7, 0)
        return jnp.concatenate([jnp.where(sub2 == 7, high, low), jnp.where(sub2 == 7, edge, high)], axis=0)

    def from_south(x, edge):
        low, high = pltpu.roll(x[0:8], 1, 0), pltpu.roll(x[8:16], 1, 0)
        return jnp.concatenate([jnp.where(sub2 == 0, edge, low), jnp.where(sub2 == 0, low, high)], axis=0)

    def wait_columns(i):
        west_copy(i).wait_recv()
        east_copy(i).wait_recv()

    def insert_columns(i):
        def level(j, _):
            k = i * size + j
            for f in range(4):
                for m in range(2):
                    place = size * (2 * f + m) + j
                    to_east = pltpu.roll(col_e[i], lax.rem(LANES + 64 - place, LANES), 1)
                    to_west = pltpu.roll(col_w[i], LANES - 1 - place, 1)
                    a = raw[f][k, m, :, 0:LANES]
                    b = padded(raw[f][k, m, :, LANES:WIDTH])
                    ext[f][k, m, :, 0:LANES] = jnp.where(lane == LANES - 1, to_west, a)
                    ext[f][k, m, :, LANES:PADDED] = jnp.where(lane < 64, b, jnp.where(lane == 64, to_east, a))
            return 0

        lax.fori_loop(0, size, level, 0, unroll=5)

    mark("column_wait")
    wait_columns(0)

    @pl.when(has_n)
    def _():
        kmt_copy.wait_recv()

    @pl.when(has_s)
    def _():
        kmt_copy.wait_send()

    mark("masks")
    kmt2 = overlapped(kmt)
    kmt_edge = jnp.where(lane == 64, pltpu.roll(col_e[0], 65, 1), kmt2[:, LANES:PADDED])
    kmt_row = padded(kmt_n[...]).astype(F32)
    kmt_north = jnp.concatenate([kmt_row[:, 0:LANES], jnp.where(lane1 < 64, kmt_row[:, LANES:PADDED], kmt_row[:, 0:LANES])], axis=1)
    mu = jnp.minimum(kmt2, roll_e(jnp.concatenate([kmt2[:, 0:LANES], kmt_edge], axis=1)))
    mv = jnp.minimum(kmt2, from_north(kmt2, kmt_north))
    faces[0] = linear(mu)
    faces[1] = linear(mv)

    def solve_factor(depth, k, first):
        inner, last = table[first * K + k], table[(first + 1) * K + k]
        kf = k.astype(F32)
        return jnp.where(depth > kf + 1.0, inner, jnp.where(depth > kf, last, 0.0))

    def edge_tiles(rows, i, j, shifted):
        late = one(j >= half)
        first = i * tile_count
        a, b_raw = rows[first + j], rows[first + size + j - half * late]
        late = 64 * late
        b = jnp.where(lane8 < 64, pltpu.roll(b_raw, late, 1), a)
        if shifted == 0:
            return a, b
        if shifted == 1:
            a1 = pltpu.roll(a, 1, 1)
            return a, b, a1, jnp.where((lane8 >= 1) & (lane8 < 65), pltpu.roll(b_raw, late + 1, 1), a1)
        a1 = pltpu.roll(a, LANES - 1, 1)
        return a, b, a1, jnp.where((lane8 < 63) | (lane8 == LANES - 1), pltpu.roll(b_raw, lax.rem(late + LANES - 1, LANES), 1), a1)

    def join(a, b, spot):
        return jnp.concatenate([a[spot:spot + 1], b[spot:spot + 1]], axis=1)

    half_scale = 0.5 * PRESS_SCALE / K
    edge_weight = jnp.where(sub < 6, -half_scale * THERM_EXP, half_scale * HALINE_CON)

    def momentum(i):
        def level(j, carry):
            (na, nb), members = carry
            k = i * size + j
            kf = k.astype(F32)
            an, bn, wan, wbn = edge_tiles(rows_n, i, j, 1)
            as_, bs, eas, ebs = edge_tiles(rows_s, i, j, 2)
            xa, xb = an * edge_weight, bn * edge_weight
            ha, hb = xa + pltpu.roll(xa, 6, 0), xb + pltpu.roll(xb, 6, 0)
            pna, pnb = na + ha, nb + hb
            factor_u, factor_v = solve_factor(mu, k, 0), solve_factor(mv, k, 0)
            out = []
            for m in range(2):
                total, gu_sum, gv_sum, side_u, side_v = members[m]
                u, v = ue[k, m], ve[k, m]
                step = (half_scale * HALINE_CON) * se[k, m] - (half_scale * THERM_EXP) * te[k, m]
                pressure = total + step
                corner_n = pltpu.roll(corner_nw[i], LANES - (size * m + j), 1)[0:1]
                corner_s = pltpu.roll(corner_se[i], lax.rem(LANES + 63 - (size * (2 + m) + j), LANES), 1)[7:8]
                u_edge = join(an, bn, m)
                v_edge = join(as_, bs, 2 + m)
                u_edge_w = jnp.concatenate([jnp.where(lane1 == 0, corner_n, wan[m:m + 1]), wbn[m:m + 1]], axis=1)
                v_edge_e = jnp.concatenate([eas[2 + m:3 + m], jnp.where(lane1 == 63, corner_s, ebs[2 + m:3 + m])], axis=1)
                v_e, v_w, u_e, u_w = roll_e(v), roll_w(v), roll_e(u), roll_w(u)
                v_pair, u_pair = v + v_e, u + u_w
                vu = 0.125 * (v_pair + from_south(v_pair, v_edge + v_edge_e))
                uv = 0.125 * (u_pair + from_north(u_pair, u_edge + u_edge_w))
                u_n, u_s = from_north(u, u_edge), from_south(u, join(as_, bs, m))
                v_n, v_s = from_north(v, join(an, bn, 2 + m)), from_south(v, v_edge)
                p_n = from_north(pressure, join(pna, pnb, 4 + m))
                gu = pressure - roll_e(pressure) - 0.5 * u * (u_e - u_w) - vu * (u_n - u_s)
                gv = pressure - p_n - uv * (v_e - v_w) - 0.5 * v * (v_n - v_s)
                gu = jnp.where(mu > kf, gu, 0.0)
                gv = jnp.where(mv > kf, gv, 0.0)
                side_u = (u + gu + VISC_NUMBER * side_u) * factor_u
                side_v = (v + gv + VISC_NUMBER * side_v) * factor_v
                pu[k, m] = linear(side_u)[:, 0:WIDTH]
                pv[k, m] = linear(side_v)[:, 0:WIDTH]
                out.append((pressure + step, gu_sum + gu, gv_sum + gv, side_u, side_v))
            return (pna + ha, pnb + hb), tuple(out)

        return level

    zero = jnp.zeros((ROWS, PADDED), F32)
    zero_row = jnp.zeros((8, LANES), F32)
    carry = ((zero_row, zero_row), ((zero,) * 5,) * 2)
    for i in range(chunks):
        if i > 0:
            wait_columns(i)
        mark("insert")
        insert_columns(i)

        mark("row_wait")
        @pl.when(has_n)
        def _():
            south_copy(i).wait_recv()
            corner_u(i).wait_recv()

        @pl.when(has_s)
        def _():
            north_copy(i).wait_recv()
            corner_v(i).wait_recv()

        mark("momentum")
        carry = lax.fori_loop(0, size, momentum(i), carry, unroll=MOMENTUM_UNROLL)

        mark("next")
        if i == chunks // 2:
            for copy in edge_copies:
                copy.wait()
            for p in range(7):
                wide[p, own, :] = with_edges(wide[p, own, :], edge_e[p], edge_w[p])
            static_copies = spread(wide, 0)
            start_spread(static_copies)

    members = carry[1]
    mark("force")
    count_u = linear(jnp.maximum(mu, 1.0))
    count_v = linear(jnp.maximum(mv, 1.0))
    for m in range(2):
        wide_f[m, own, :] = linear(members[m][1]) / count_u
        wide_f[2 + m, own, :] = linear(members[m][2]) / count_v
    force_edges = edge_pair(wide_f, fedge_w, fedge_e, 3)
    for copy in force_edges:
        copy.start()

    def tracers(i, carry):
        def level(j, carry):
            k = i * size + j
            an, bn = edge_tiles(rows_n, i, j, 0)
            as_, bs = edge_tiles(rows_s, i, j, 0)
            factor = solve_factor(kmt2, k, 3)
            out = []
            for m in range(2):
                u, v = 0.5 * ue[k, m], 0.5 * ve[k, m]
                u_w = roll_w(u)
                v_edge = 0.5 * join(as_, bs, 2 + m)
                for f, dest in ((2, pt), (3, ps)):
                    t = ext[f][k, m]
                    flux_x = u * (t + roll_e(t)) - u_w * (t + roll_w(t))
                    flux_y = v * (t + from_north(t, join(an, bn, 2 * f + m)))
                    flux_s = v_edge * (join(as_, bs, 2 * f + m) + t[0:1])
                    moved = t - (flux_x + flux_y - from_south(flux_y, flux_s))
                    side = (moved + DIFF_NUMBER * carry[len(out)]) * factor
                    dest[k, m] = linear(side)[:, 0:WIDTH]
                    out.append(side)
            return tuple(out)

        return lax.fori_loop(0, size, level, carry, unroll=TRACER_UNROLL)

    mark("tracer_1")
    tail = (zero,) * 4
    split = (3 * chunks + 4) // 5
    tail = lax.fori_loop(0, split, tracers, tail)

    mark("force_edge_wait")
    for copy in force_edges:
        copy.wait()
    mark("force_spread")
    for p in range(4):
        wide_f[p, own, :] = with_edges(wide_f[p, own, :], fedge_e[p], fedge_w[p])
    force_copies = spread(wide_f, 4)
    start_spread(force_copies)

    mark("tracer_2")
    tail = lax.fori_loop(split, chunks, tracers, tail)

    def back_tracers(j, carry):
        k = K - 2 - j
        ratio = table[5 * K + k]
        out = []
        for m in range(2):
            for dest in (pt, ps):
                x = dest[k, m] + ratio * carry[len(out)]
                dest[k, m] = x
                out.append(x)
        return tuple(out)

    mark("back_tracers")
    lax.fori_loop(0, K - 1, back_tracers, tuple(linear(x)[:, 0:WIDTH] for x in tail), unroll=2)

    def back(j, carry):
        k = K - 2 - j
        ratio = table[2 * K + k]
        out = []
        for m in range(2):
            xu, xv, su, sv = carry[m]
            xu = pu[k, m] + ratio * xu
            xv = pv[k, m] + ratio * xv
            pu[k, m] = xu
            pv[k, m] = xv
            out.append((xu, xv, su + xu, sv + xv))
        return tuple(out)

    mark("back_uv")
    start = tuple(tuple(linear(members[m][n])[:, 0:WIDTH] for n in (3, 4, 3, 4)) for m in range(2))
    ends = lax.fori_loop(0, K - 1, back, start)

    mark("static_wait")
    finish_spread(static_copies)
    mark("force_wait")
    finish_spread(force_copies)

    mark("coef")
    depth = wide[0]
    depth_e = pltpu.roll(depth, PADDED - 1, 1)
    depth_n = pltpu.roll(depth, 79, 0)
    hu = jnp.where((depth > 0.0) & (depth_e > 0.0), 0.5 * (depth + depth_e), 0.0)
    hv = jnp.where((depth > 0.0) & (depth_n > 0.0), 0.5 * (depth + depth_n), 0.0)
    coef[0] = WAVE_COURANT * hu
    coef[1] = WAVE_COURANT * hv
    for m in range(2):
        wide_f[m] = hu * wide_f[m] * (1.0 / SUBCYCLES)
        wide_f[2 + m] = hv * wide_f[2 + m] * (1.0 / SUBCYCLES)
        for p in range(3):
            avg[2 * p + m] = zero

    def subcycles(first, last, margin):
        height = ROWS + 2 * margin
        rows = pl.ds(HALO - margin, height)
        mine = slice(margin, margin + ROWS)

        def to_e(x):
            return pltpu.roll(x, PADDED - 1, 1)

        def subcycle(n, _):
            weight = weights[n]
            state = []
            for m in range(2):
                tx, ty = wide[3 + m, rows], wide[5 + m, rows]
                tx_e, ty_e = to_e(tx), to_e(ty)
                eta = wide[1 + m, rows] - WAVE_COURANT * (tx - pltpu.roll(tx, 1, 1) + ty - pltpu.roll(ty, 1, 0))
                eta_e = east_eta[m, rows] - WAVE_COURANT * (tx_e - tx + ty_e - pltpu.roll(ty_e, 1, 0))
                state.append((eta, eta_e, tx, ty))
            for m, (eta, eta_e, tx, ty) in enumerate(state):
                tx = tx + wide_f[m, rows] - coef[0, rows] * (eta_e - eta)
                ty = ty + wide_f[2 + m, rows] - coef[1, rows] * (pltpu.roll(eta, height - 1, 0) - eta)
                wide[1 + m, rows] = eta
                east_eta[m, rows] = eta_e
                wide[3 + m, rows] = tx
                wide[5 + m, rows] = ty
                avg[m] = avg[m] + weight * eta[mine]
                avg[2 + m] = avg[2 + m] + weight * tx[mine]
                avg[4 + m] = avg[4 + m] + weight * ty[mine]
            return 0

        lax.fori_loop(first, last, subcycle, 0)

    mark("subcycles")
    for m in range(2):
        east_eta[m] = pltpu.roll(wide[1 + m], PADDED - 1, 1)
    done = 0
    for margin in (32, 24, 16, 8):
        last = SUBCYCLES - (margin - 8)
        subcycles(done, last, margin)
        done = last

    mark("corr")
    mine = slice(HALO, HALO + ROWS)
    for m in range(2):
        corr[m] = avg[2 + m] / jnp.where(hu[mine] > 0.0, hu[mine], 1.0) - padded(ends[m][2]) / count_u
        corr[2 + m] = avg[4 + m] / jnp.where(hv[mine] > 0.0, hv[mine], 1.0) - padded(ends[m][3]) / count_v

    mark("send_wait")
    for i in range(chunks):
        west_copy(i).wait_send()
        east_copy(i).wait_send()

    @pl.when(has_s)
    def _():
        for i in range(chunks):
            south_copy(i).wait_send()
            corner_u(i).wait_send()

    @pl.when(has_n)
    def _():
        for i in range(chunks):
            north_copy(i).wait_send()
            corner_v(i).wait_send()
    mark("")


def finish_kernel(size, pu, pv, pt, ps, corr, faces, avg, eta_o, tx_o, ty_o, u_o, v_o, t_o, s_o, sems):
    first = pl.program_id(0) * size
    through = [pltpu.make_async_copy(src, dst, sems.at[i]) for i, (src, dst) in enumerate(((pt, t_o), (ps, s_o)))]

    @pl.when(first == 0)
    def _():
        for copy in through:
            copy.start()
        for m in range(2):
            eta_o[m] = avg[m][:, 0:WIDTH]
            tx_o[m] = avg[2 + m][:, 0:WIDTH]
            ty_o[m] = avg[4 + m][:, 0:WIDTH]

    for j in range(size):
        level = (first + j).astype(F32)
        for m in range(2):
            for face, (src, dst) in enumerate(((pu, u_o), (pv, v_o))):
                wet = faces[face][:, 0:WIDTH] > level
                dst[j, m] = jnp.where(wet, src[first + j, m] + corr[2 * face + m][:, 0:WIDTH], 0.0)

    @pl.when(pl.program_id(0) == pl.num_programs(0) - 1)
    def _():
        for copy in through:
            copy.wait()


def solution(mesh):
    col_count, row_count = mesh.shape["col"], mesh.shape["row"]

    def local_step(vel_x, vel_y, pot_temp, salinity, surf_eta, trans_x, trans_y, col_depth, wet_levels, avg_weights):
        K = vel_x.shape[0]
        size = level_chunk(K)
        chunks = K // size
        table = jnp.asarray(solve_tables(K))
        smem = pl.BlockSpec(memory_space=pltpu.SMEM)
        vmem = pl.BlockSpec(memory_space=pltpu.VMEM)
        hbm = pl.BlockSpec(memory_space=pl.ANY)
        full = jax.ShapeDtypeStruct((K, 2, ROWS, WIDTH), F32)
        held = pltpu.VMEM((K, 2, ROWS, WIDTH), F32)
        dma = pltpu.SemaphoreType.DMA
        outs = pl.pallas_call(
            functools.partial(step_kernel, row_count, col_count, K),
            out_shape=(held,) * 4 + tuple(pltpu.VMEM((n, ROWS, PADDED), F32) for n in (4, 2, 6)),
            in_specs=[smem, smem] + [vmem] * 5 + [hbm] * 4,
            out_specs=(vmem,) * 7,
            scratch_shapes=[
                *[pltpu.VMEM((K, 2, ROWS, WIDTH), F32)] * 4,
                *[pltpu.VMEM((K, 2, ROWS, PADDED), F32)] * 4,
                *[pltpu.VMEM((chunks * (size + (size + 1) // 2), 8, LANES), F32)] * 4,
                pltpu.VMEM((1, WIDTH), jnp.int32),
                *[pltpu.VMEM((chunks, ROWS, LANES), F32)] * 4,
                *[pltpu.VMEM((chunks, 8, LANES), F32)] * 2,
                *[pltpu.VMEM((7, ROWS, LANES), F32)] * 2,
                pltpu.VMEM((7, 80, PADDED), F32),
                *[pltpu.VMEM((4, ROWS, LANES), F32)] * 2,
                pltpu.VMEM((4, 80, PADDED), F32),
                *[pltpu.VMEM((2, 80, PADDED), F32)] * 2,
                dma((chunks, 4)), dma((2, chunks)), dma((2, chunks)), dma((4, chunks)), dma((4, chunks)), dma((5,)), dma((5,)), dma((8,)), dma((8,)),
            ],
            compiler_params=pltpu.CompilerParams(collective_id=0, has_side_effects=True, vmem_limit_bytes=53 << 20),
            name="ocean_step",
        )(table, avg_weights, wet_levels, col_depth, surf_eta, trans_x, trans_y, vel_x, vel_y, pot_temp, salinity)

        small = jax.ShapeDtypeStruct((2, ROWS, WIDTH), F32)
        deep_out = pl.BlockSpec((size, 2, ROWS, WIDTH), lambda i: (i, 0, 0, 0))
        small_out = pl.BlockSpec((2, ROWS, WIDTH), lambda i: (0, 0, 0))
        return pl.pallas_call(
            functools.partial(finish_kernel, size),
            grid=(chunks,),
            out_shape=(small,) * 3 + (full,) * 4,
            in_specs=[vmem] * 7,
            out_specs=(small_out,) * 3 + (deep_out,) * 2 + (hbm,) * 2,
            scratch_shapes=[dma((2,))],
            compiler_params=pltpu.CompilerParams(vmem_limit_bytes=20 << 20),
            name="ocean_finish",
        )(*outs)

    spec_3d = P(None, None, "row", "col")
    spec_2d = P(None, "row", "col")
    spec_map = P("row", "col")
    return jax.shard_map(local_step, mesh=mesh, in_specs=(spec_3d,) * 4 + (spec_2d,) * 3 + (spec_map,) * 2 + (P(),), out_specs=(spec_2d,) * 3 + (spec_3d,) * 4, check_vma=False)
```

```python
import functools
import numpy as np
import jax
import jax.numpy as jnp
from jax import lax
from jax.experimental import pallas as pl
from jax.experimental.pallas import tpu as pltpu
from jax.sharding import PartitionSpec as P

WAVE_COURANT = 0.4
THERM_EXP = 0.2
HALINE_CON = 0.15
PRESS_SCALE = 0.5
VISC_NUMBER = 1.0
DIFF_NUMBER = 0.5
SUBCYCLES = 30
HALO = 32
PAIR = (0, 1)
MOMENTUM_UNROLL = 5
TRACER_UNROLL = 5
ROWS, WIDTH, PADDED, LANES = 16, 192, 256, 128
MESH = pl.DeviceIdType.MESH
F32 = jnp.float32


def solve_tables(level_count):
    rows = []
    for strength in (VISC_NUMBER, DIFF_NUMBER):
        inner, last = np.zeros(level_count), np.zeros(level_count)
        inner[0], last[0] = 1.0 + strength, 1.0
        for k in range(1, level_count):
            inner[k] = 1.0 + 2.0 * strength - strength * strength / inner[k - 1]
            last[k] = 1.0 + strength - strength * strength / inner[k - 1]
        rows += [1.0 / inner, 1.0 / last, strength / inner]
    return np.concatenate(rows).astype(np.float32)


def level_chunk(level_count):
    for size in (15, 5, 4, 3, 2):
        if level_count % size == 0:
            return size
    return 1


def step_kernel(
    row_count, col_count, level_count,
    table, kmt_in, depth_in, eta_in, tx_in, ty_in, u_hbm, v_hbm, t_hbm, s_hbm,
    pu, pv, pt, ps, mean, faces, coef, force, state,
    ub, vb, tb, sb, ue, ve, te, se, rows_n, rows_s, send_n, send_s, kmt_n, pack_w, pack_e, col_e, col_w, corner_se, corner_nw,
    edge_e, edge_w, wide, fedge_e, fedge_w, wide_f,
    load_sem, row_send, row_recv, col_send, col_recv, misc_send, misc_recv, wide_send, wide_recv,
):
    K = level_count
    open_scope = []

    def mark(name):
        if open_scope:
            open_scope.pop().__exit__(None, None, None)
        if name:
            open_scope.append(jax.named_scope(name))
            open_scope[-1].__enter__()

    size = level_chunk(K)
    chunks = K // size
    half = (size + 1) // 2
    tile_count = size + half
    r = lax.axis_index("row")
    c = lax.axis_index("col")
    east = lax.rem(c + 1, col_count)
    west = lax.rem(c + col_count - 1, col_count)
    has_n, has_s = r < row_count - 1, r > 0
    has_nn, has_ss = r < row_count - 2, r > 1
    raw, ext = (ub, vb, tb, sb), (ue, ve, te, se)

    def one(flag):
        return flag.astype(jnp.int32)

    mark("init")
    loads = [
        [pltpu.make_async_copy(src.at[pl.ds(i * size, size)], dst.at[pl.ds(i * size, size)], load_sem.at[i, f]) for f, (src, dst) in enumerate(zip((u_hbm, v_hbm, t_hbm, s_hbm), raw))]
        for i in range(chunks)
    ]
    for group in loads:
        for copy in group:
            copy.start()

    wide[...] = jnp.zeros_like(wide)
    wide_f[...] = jnp.zeros_like(wide_f)

    @pl.when(jnp.logical_not(has_n))
    def _():
        rows_n[...] = jnp.zeros_like(rows_n)
        kmt_n[...] = jnp.zeros_like(kmt_n)
        corner_nw[...] = jnp.zeros_like(corner_nw)

    @pl.when(jnp.logical_not(has_s))
    def _():
        rows_s[...] = jnp.zeros_like(rows_s)
        corner_se[...] = jnp.zeros_like(corner_se)

    barrier = pltpu.get_barrier_semaphore()

    def signal(**where):
        pl.semaphore_signal(barrier, inc=1, device_id=where, device_id_type=MESH)

    signal(col=east)
    signal(col=west)

    @pl.when(has_n)
    def _():
        signal(row=r + 1)
        signal(row=r + 1, col=west)

    @pl.when(has_s)
    def _():
        signal(row=r - 1)
        signal(row=r - 1, col=east)

    @pl.when(has_nn)
    def _():
        signal(row=r + 2)

    @pl.when(has_ss)
    def _():
        signal(row=r - 2)

    def remote(src, dst, ssem, rsem, **where):
        return pltpu.make_async_remote_copy(src_ref=src, dst_ref=dst, send_sem=ssem, recv_sem=rsem, device_id=where, device_id_type=MESH)

    lane = lax.broadcasted_iota(jnp.int32, (ROWS, LANES), 1)
    lane8, lane1 = lane[0:8], lane[0:1]
    sub = lax.broadcasted_iota(jnp.int32, (8, LANES), 0)
    sub2 = lax.broadcasted_iota(jnp.int32, (8, PADDED), 0)

    def padded(x):
        return jnp.concatenate([x, jnp.zeros((x.shape[0], PADDED - WIDTH), x.dtype)], axis=1)

    def overlapped(x):
        a, b = x[:, 0:LANES], x[:, LANES:PADDED]
        return jnp.concatenate([a, jnp.where(lane < 64, b, a)], axis=1)

    def linear(x):
        a, b = x[:, 0:LANES], x[:, LANES:PADDED]
        return jnp.concatenate([jnp.where(lane < 96, a, b), b], axis=1)

    kmt = padded(kmt_in[...]).astype(F32)
    own = pl.ds(HALO, ROWS)
    wide[0, own, :] = jnp.where(kmt > 0.5, padded(depth_in[...]), 0.0)
    for m in PAIR:
        wide[1 + m, own, :] = padded(eta_in[m])
        wide[3 + m, own, :] = padded(tx_in[m])
        wide[5 + m, own, :] = padded(ty_in[m])

    kmt_copy = remote(kmt_in.at[0:1, :], kmt_n, misc_send.at[0], misc_recv.at[0], row=r - 1)

    def south_copy(i):
        tiles = pl.ds(i * tile_count, tile_count)
        return remote(send_s.at[tiles], rows_n.at[tiles], row_send.at[0, i], row_recv.at[0, i], row=r - 1)

    def north_copy(i):
        tiles = pl.ds(i * tile_count, tile_count)
        return remote(send_n.at[tiles], rows_s.at[tiles], row_send.at[1, i], row_recv.at[1, i], row=r + 1)

    def west_copy(i):
        return remote(pack_w.at[i], col_e.at[i], col_send.at[0, i], col_recv.at[0, i], col=west)

    def east_copy(i):
        return remote(pack_e.at[i], col_w.at[i], col_send.at[1, i], col_recv.at[1, i], col=east)

    def corner_v(i):
        return remote(pack_w.at[i, 8:16, :], corner_se.at[i], col_send.at[2, i], col_recv.at[2, i], row=r + 1, col=west)

    def corner_u(i):
        return remote(pack_e.at[i, 0:8, :], corner_nw.at[i], col_send.at[3, i], col_recv.at[3, i], row=r - 1, col=east)

    def pack_level(h, k, j, acc):
        acc, tiles = list(acc), [None, None]
        for f in range(4):
            for m in PAIR:
                spot = 2 * f + m
                x = raw[f][k, m, :, 0:LANES] if h == 0 else padded(raw[f][k, m, :, LANES:WIDTH])
                acc[spot] = jnp.where(lane == j, pltpu.roll(x, j if h == 0 else j + 65, 1), acc[spot])
                for side in PAIR:
                    row = pltpu.roll(x[8 * side:8 * side + 8], (spot + side) % 8, 0)
                    tiles[side] = row if tiles[side] is None else jnp.where(sub == spot, row, tiles[side])
        return tuple(acc), tiles

    def pack_chunk(i):
        for copy in loads[i]:
            copy.wait()
        for h, pack in enumerate((pack_w, pack_e)):
            def pack_pair(j, acc):
                j2 = jnp.minimum(j + half, size - 1)
                acc, one_level = pack_level(h, i * size + j, j, acc)
                acc, other = pack_level(h, i * size + j2, j2, acc)
                for one_tile, other_tile, dest in zip(one_level, other, (send_s, send_n)):
                    if h == 0:
                        dest[i * tile_count + j] = one_tile
                        dest[i * tile_count + j2] = other_tile
                    else:
                        dest[i * tile_count + size + j] = jnp.where(lane8 < 64, one_tile, pltpu.roll(other_tile, 64, 1))
                return acc

            acc = lax.fori_loop(0, half, pack_pair, (jnp.zeros((ROWS, LANES), F32),) * 8, unroll=half)
            merged = pltpu.roll(kmt[:, 0:LANES], LANES - 1, 1)
            for spot in range(8):
                merged = jnp.where((lane >= size * spot) & (lane < size * spot + size), pltpu.roll(acc[spot], size * spot, 1), merged)
            pack[i] = merged

    def start_chunk(i):
        west_copy(i).start()
        east_copy(i).start()

        @pl.when(has_s)
        def _():
            corner_u(i).start()
            south_copy(i).start()

        @pl.when(has_n)
        def _():
            corner_v(i).start()
            north_copy(i).start()

    mark("pack_early")
    early = min(2, chunks)
    for i in range(early):
        pack_chunk(i)
    mark("barrier_wait")
    pl.semaphore_wait(barrier, 2 + 2 * one(has_n) + 2 * one(has_s) + one(has_nn) + one(has_ss))

    @pl.when(has_s)
    def _():
        kmt_copy.start()

    for i in range(early):
        start_chunk(i)
    mark("pack_late")
    for i in range(early, chunks):
        pack_chunk(i)
        start_chunk(i)

    def edge_pair(buf, to_east, to_west, sem):
        return [
            remote(buf.at[:, own, 0:LANES], to_west, misc_send.at[sem], misc_recv.at[sem], col=west),
            remote(buf.at[:, own, LANES:PADDED], to_east, misc_send.at[sem + 1], misc_recv.at[sem + 1], col=east),
        ]

    def with_edges(x, from_east, from_west):
        b = jnp.where(lane < 64, x[:, LANES:PADDED], jnp.where(lane < 96, pltpu.roll(from_east, 64, 1), pltpu.roll(from_west, 64, 1)))
        return jnp.concatenate([x[:, 0:LANES], b], axis=1)

    def spread(buf, sem):
        src = buf.at[:, own, :]
        parts = ((has_n, has_s, 16, r + 1), (has_s, has_n, 48, r - 1), (has_nn, has_ss, 0, r + 2), (has_ss, has_nn, 64, r - 2))
        return [(there, here, remote(src, buf.at[:, pl.ds(at, ROWS), :], wide_send.at[sem + n], wide_recv.at[sem + n], row=row)) for n, (there, here, at, row) in enumerate(parts)]

    def start_spread(copies):
        for there, _, copy in copies:
            @pl.when(there)
            def _():
                copy.start()

    def finish_spread(copies):
        for there, here, copy in copies:
            @pl.when(there)
            def _():
                copy.wait_send()

            @pl.when(here)
            def _():
                copy.wait_recv()

    mark("edges")
    edge_copies = edge_pair(wide, edge_w, edge_e, 1)
    for copy in edge_copies:
        copy.start()

    def roll_e(x):
        return jnp.concatenate([pltpu.roll(x[:, 0:LANES], LANES - 1, 1), pltpu.roll(x[:, LANES:PADDED], LANES - 1, 1)], axis=1)

    def roll_w(x):
        return jnp.concatenate([pltpu.roll(x[:, 0:LANES], 1, 1), pltpu.roll(x[:, LANES:PADDED], 1, 1)], axis=1)

    def from_north(x, edge):
        low, high = pltpu.roll(x[0:8], 7, 0), pltpu.roll(x[8:16], 7, 0)
        return jnp.concatenate([jnp.where(sub2 == 7, high, low), jnp.where(sub2 == 7, edge, high)], axis=0)

    def from_south(x, edge):
        low, high = pltpu.roll(x[0:8], 1, 0), pltpu.roll(x[8:16], 1, 0)
        return jnp.concatenate([jnp.where(sub2 == 0, edge, low), jnp.where(sub2 == 0, low, high)], axis=0)

    def wait_columns(i):
        west_copy(i).wait_recv()
        east_copy(i).wait_recv()

    def insert_columns(i):
        def level(j, _):
            k = i * size + j
            for f in range(4):
                for m in PAIR:
                    place = size * (2 * f + m) + j
                    to_east = pltpu.roll(col_e[i], lax.rem(LANES + 64 - place, LANES), 1)
                    to_west = pltpu.roll(col_w[i], LANES - 1 - place, 1)
                    a = raw[f][k, m, :, 0:LANES]
                    b = padded(raw[f][k, m, :, LANES:WIDTH])
                    ext[f][k, m, :, 0:LANES] = jnp.where(lane == LANES - 1, to_west, a)
                    ext[f][k, m, :, LANES:PADDED] = jnp.where(lane < 64, b, jnp.where(lane == 64, to_east, a))
            return 0

        lax.fori_loop(0, size, level, 0, unroll=5)

    mark("column_wait")
    wait_columns(0)

    @pl.when(has_n)
    def _():
        kmt_copy.wait_recv()

    @pl.when(has_s)
    def _():
        kmt_copy.wait_send()

    mark("masks")
    kmt2 = overlapped(kmt)
    kmt_edge = jnp.where(lane == 64, pltpu.roll(col_e[0], 65, 1), kmt2[:, LANES:PADDED])
    kmt_row = padded(kmt_n[...]).astype(F32)
    kmt_north = jnp.concatenate([kmt_row[:, 0:LANES], jnp.where(lane1 < 64, kmt_row[:, LANES:PADDED], kmt_row[:, 0:LANES])], axis=1)
    mu = jnp.minimum(kmt2, roll_e(jnp.concatenate([kmt2[:, 0:LANES], kmt_edge], axis=1)))
    mv = jnp.minimum(kmt2, from_north(kmt2, kmt_north))
    faces[0] = linear(mu)
    faces[1] = linear(mv)

    def solve_factor(depth, k, first):
        inner, last = table[first * K + k], table[(first + 1) * K + k]
        kf = k.astype(F32)
        return jnp.where(depth > kf + 1.0, inner, jnp.where(depth > kf, last, 0.0))

    def edge_tiles(rows, i, j, shifted):
        late = one(j >= half)
        first = i * tile_count
        a, b_raw = rows[first + j], rows[first + size + j - half * late]
        late = 64 * late
        b = jnp.where(lane8 < 64, pltpu.roll(b_raw, late, 1), a)
        if shifted == 0:
            return a, b
        if shifted == 1:
            a1 = pltpu.roll(a, 1, 1)
            return a, b, a1, jnp.where((lane8 >= 1) & (lane8 < 65), pltpu.roll(b_raw, late + 1, 1), a1)
        a1 = pltpu.roll(a, LANES - 1, 1)
        return a, b, a1, jnp.where((lane8 < 63) | (lane8 == LANES - 1), pltpu.roll(b_raw, lax.rem(late + LANES - 1, LANES), 1), a1)

    def join(a, b, spot):
        return jnp.concatenate([a[spot:spot + 1], b[spot:spot + 1]], axis=1)

    half_scale = 0.5 * PRESS_SCALE / K
    edge_weight = jnp.where(sub < 6, -half_scale * THERM_EXP, half_scale * HALINE_CON)

    def momentum(i):
        def level(j, carry):
            (na, nb), members = carry
            k = i * size + j
            kf = k.astype(F32)
            an, bn, wan, wbn = edge_tiles(rows_n, i, j, 1)
            as_, bs, eas, ebs = edge_tiles(rows_s, i, j, 2)
            xa, xb = an * edge_weight, bn * edge_weight
            ha, hb = xa + pltpu.roll(xa, 6, 0), xb + pltpu.roll(xb, 6, 0)
            pna, pnb = na + ha, nb + hb
            factor_u, factor_v = solve_factor(mu, k, 0), solve_factor(mv, k, 0)
            out = []
            for m in PAIR:
                total, gu_sum, gv_sum, side_u, side_v = members[m]
                u, v = ue[k, m], ve[k, m]
                step = (half_scale * HALINE_CON) * se[k, m] - (half_scale * THERM_EXP) * te[k, m]
                pressure = total + step
                corner_n = pltpu.roll(corner_nw[i], LANES - (size * m + j), 1)[0:1]
                corner_s = pltpu.roll(corner_se[i], lax.rem(LANES + 63 - (size * (2 + m) + j), LANES), 1)[7:8]
                u_edge = join(an, bn, m)
                v_edge = join(as_, bs, 2 + m)
                u_edge_w = jnp.concatenate([jnp.where(lane1 == 0, corner_n, wan[m:m + 1]), wbn[m:m + 1]], axis=1)
                v_edge_e = jnp.concatenate([eas[2 + m:3 + m], jnp.where(lane1 == 63, corner_s, ebs[2 + m:3 + m])], axis=1)
                v_e, v_w, u_e, u_w = roll_e(v), roll_w(v), roll_e(u), roll_w(u)
                v_pair, u_pair = v + v_e, u + u_w
                vu = 0.125 * (v_pair + from_south(v_pair, v_edge + v_edge_e))
                uv = 0.125 * (u_pair + from_north(u_pair, u_edge + u_edge_w))
                u_n, u_s = from_north(u, u_edge), from_south(u, join(as_, bs, m))
                v_n, v_s = from_north(v, join(an, bn, 2 + m)), from_south(v, v_edge)
                p_n = from_north(pressure, join(pna, pnb, 4 + m))
                gu = pressure - roll_e(pressure) - 0.5 * u * (u_e - u_w) - vu * (u_n - u_s)
                gv = pressure - p_n - uv * (v_e - v_w) - 0.5 * v * (v_n - v_s)
                gu = jnp.where(mu > kf, gu, 0.0)
                gv = jnp.where(mv > kf, gv, 0.0)
                side_u = (u + gu + VISC_NUMBER * side_u) * factor_u
                side_v = (v + gv + VISC_NUMBER * side_v) * factor_v
                pu[k, m] = linear(side_u)[:, 0:WIDTH]
                pv[k, m] = linear(side_v)[:, 0:WIDTH]
                out.append((pressure + step, gu_sum + gu, gv_sum + gv, side_u, side_v))
            return (pna + ha, pnb + hb), tuple(out)

        return level

    zero = jnp.zeros((ROWS, PADDED), F32)
    zero_row = jnp.zeros((8, LANES), F32)
    carry = ((zero_row, zero_row), ((zero,) * 5,) * 2)
    for i in range(chunks):
        if i > 0:
            wait_columns(i)
        mark("insert")
        insert_columns(i)

        mark("row_wait")
        @pl.when(has_n)
        def _():
            south_copy(i).wait_recv()
            corner_u(i).wait_recv()

        @pl.when(has_s)
        def _():
            north_copy(i).wait_recv()
            corner_v(i).wait_recv()

        mark("momentum")
        carry = lax.fori_loop(0, size, momentum(i), carry, unroll=MOMENTUM_UNROLL)

        mark("next")
        if i == chunks // 2:
            for copy in edge_copies:
                copy.wait()
            for p in range(7):
                wide[p, own, :] = with_edges(wide[p, own, :], edge_e[p], edge_w[p])
            static_copies = spread(wide, 0)
            start_spread(static_copies)

    members = carry[1]
    mark("force")
    count_u = linear(jnp.maximum(mu, 1.0))
    count_v = linear(jnp.maximum(mv, 1.0))
    for m in PAIR:
        wide_f[m, own, :] = linear(members[m][1]) / count_u
        wide_f[2 + m, own, :] = linear(members[m][2]) / count_v
    force_edges = edge_pair(wide_f, fedge_w, fedge_e, 3)
    for copy in force_edges:
        copy.start()

    def tracers(i, carry):
        def level(j, carry):
            k = i * size + j
            an, bn = edge_tiles(rows_n, i, j, 0)
            as_, bs = edge_tiles(rows_s, i, j, 0)
            factor = solve_factor(kmt2, k, 3)
            out = []
            for m in PAIR:
                u, v = 0.5 * ue[k, m], 0.5 * ve[k, m]
                u_w = roll_w(u)
                v_edge = 0.5 * join(as_, bs, 2 + m)
                for f, dest in ((2, pt), (3, ps)):
                    t = ext[f][k, m]
                    flux_x = u * (t + roll_e(t)) - u_w * (t + roll_w(t))
                    flux_y = v * (t + from_north(t, join(an, bn, 2 * f + m)))
                    flux_s = v_edge * (join(as_, bs, 2 * f + m) + t[0:1])
                    moved = t - (flux_x + flux_y - from_south(flux_y, flux_s))
                    side = (moved + DIFF_NUMBER * carry[len(out)]) * factor
                    dest[k, m] = linear(side)[:, 0:WIDTH]
                    out.append(side)
            return tuple(out)

        return lax.fori_loop(0, size, level, carry, unroll=TRACER_UNROLL)

    mark("tracer_1")
    tail = (zero,) * 4
    split = (3 * chunks + 4) // 5
    tail = lax.fori_loop(0, split, tracers, tail)

    mark("force_edge_wait")
    for copy in force_edges:
        copy.wait()
    mark("force_spread")
    for p in range(4):
        wide_f[p, own, :] = with_edges(wide_f[p, own, :], fedge_e[p], fedge_w[p])
    force_copies = spread(wide_f, 4)
    start_spread(force_copies)

    mark("tracer_2")
    tail = lax.fori_loop(split, chunks, tracers, tail)

    def back_tracers(j, carry):
        k = K - 2 - j
        ratio = table[5 * K + k]
        out = []
        for m in PAIR:
            for dest in (pt, ps):
                x = dest[k, m] + ratio * carry[len(out)]
                dest[k, m] = x
                out.append(x)
        return tuple(out)

    mark("back_tracers")
    lax.fori_loop(0, K - 1, back_tracers, tuple(linear(x)[:, 0:WIDTH] for x in tail), unroll=2)

    def back(j, carry):
        k = K - 2 - j
        ratio = table[2 * K + k]
        out = []
        for m in PAIR:
            xu, xv, su, sv = carry[m]
            xu = pu[k, m] + ratio * xu
            xv = pv[k, m] + ratio * xv
            pu[k, m] = xu
            pv[k, m] = xv
            out.append((xu, xv, su + xu, sv + xv))
        return tuple(out)

    mark("back_uv")
    start = tuple(tuple(linear(members[m][n])[:, 0:WIDTH] for n in (3, 4, 3, 4)) for m in PAIR)
    ends = lax.fori_loop(0, K - 1, back, start)

    mark("static_wait")
    finish_spread(static_copies)
    mark("force_wait")
    finish_spread(force_copies)

    mark("coef")
    depth = wide[0]
    depth_e = pltpu.roll(depth, PADDED - 1, 1)
    depth_n = pltpu.roll(depth, 79, 0)
    hu = jnp.where((depth > 0.0) & (depth_e > 0.0), 0.5 * (depth + depth_e), 0.0)
    hv = jnp.where((depth > 0.0) & (depth_n > 0.0), 0.5 * (depth + depth_n), 0.0)
    coef[0] = WAVE_COURANT * WAVE_COURANT * hu
    coef[1] = WAVE_COURANT * WAVE_COURANT * hv
    for m in PAIR:
        force[m] = hu * wide_f[m] * (WAVE_COURANT / SUBCYCLES)
        force[2 + m] = hv * wide_f[2 + m] * (WAVE_COURANT / SUBCYCLES)
        state[m] = wide[1 + m]
        state[2 + m] = WAVE_COURANT * wide[3 + m]
        state[4 + m] = WAVE_COURANT * wide[5 + m]
        state[6 + m] = pltpu.roll(wide[1 + m], PADDED - 1, 1)
    mine = slice(HALO, HALO + ROWS)
    for p, (h, count) in enumerate(((hu[mine], count_u), (hv[mine], count_v))):
        faces[2 + p] = 1.0 / (WAVE_COURANT * jnp.where(h > 0.0, h, 1.0))
        for m in PAIR:
            mean[2 * p + m] = padded(ends[m][2 + p]) / count

    mark("send_wait")
    for i in range(chunks):
        west_copy(i).wait_send()
        east_copy(i).wait_send()

    @pl.when(has_s)
    def _():
        for i in range(chunks):
            south_copy(i).wait_send()
            corner_u(i).wait_send()

    @pl.when(has_n)
    def _():
        for i in range(chunks):
            north_copy(i).wait_send()
            corner_v(i).wait_send()
    mark("")


def finish_kernel(
    K, size,
    weights, pu, pv, pt, ps, mean, faces, coef, force, first_state,
    eta_o, tx_o, ty_o, u_o, v_o, t_o, s_o,
    state, avg, out_u, out_v, sems,
):
    chunks = K // size
    through = [pltpu.make_async_copy(src, dst, sems.at[i, 0]) for i, (src, dst) in enumerate(((pt, t_o), (ps, s_o)))]
    for copy in through:
        copy.start()
    state[...] = first_state[...]
    avg[...] = jnp.zeros_like(avg)

    def subcycles(first, last, margin):
        height = ROWS + 2 * margin
        rows = pl.ds(HALO - margin, height)
        mine = slice(margin, margin + ROWS)

        def to_e(x):
            return pltpu.roll(x, PADDED - 1, 1)

        def subcycle(n, _):
            weight = weights[n]
            for m in PAIR:
                tx, ty = state[2 + m, rows], state[4 + m, rows]
                tx_e, ty_e = to_e(tx), to_e(ty)
                eta = state[m, rows] - (tx - pltpu.roll(tx, 1, 1) + ty - pltpu.roll(ty, 1, 0))
                eta_e = state[6 + m, rows] - (tx_e - tx + ty_e - pltpu.roll(ty_e, 1, 0))
                tx = tx + force[m, rows] - coef[0, rows] * (eta_e - eta)
                ty = ty + force[2 + m, rows] - coef[1, rows] * (pltpu.roll(eta, height - 1, 0) - eta)
                for p, x in enumerate((eta, tx, ty)):
                    state[2 * p + m, rows] = x
                    avg[2 * p + m] = avg[2 * p + m] + weight * x[mine]
                state[6 + m, rows] = eta_e
            return 0

        lax.fori_loop(first, last, subcycle, 0)

    done = 0
    for margin in (32, 24, 16, 8):
        last = SUBCYCLES - (margin - 8)
        subcycles(done, last, margin)
        done = last

    corr = []
    for m in PAIR:
        eta_o[m] = avg[m][:, 0:WIDTH]
        for p, dest in enumerate((tx_o, ty_o)):
            transport = avg[2 + 2 * p + m]
            dest[m] = (transport * (1.0 / WAVE_COURANT))[:, 0:WIDTH]
            corr.append((transport * faces[2 + p] - mean[2 * p + m])[:, 0:WIDTH])
    depth_u, depth_v = faces[0][:, 0:WIDTH], faces[1][:, 0:WIDTH]

    def out_copies(i):
        levels = pl.ds(i * size, size)
        return [pltpu.make_async_copy(src.at[levels], dst.at[levels], sems.at[p, 1 + i]) for p, (src, dst) in enumerate(((out_u, u_o), (out_v, v_o)))]

    for i in range(chunks):
        def level(j, _):
            k = i * size + j
            kf = k.astype(F32)
            for m in PAIR:
                out_u[k, m] = jnp.where(depth_u > kf, pu[k, m] + corr[2 * m], 0.0)
                out_v[k, m] = jnp.where(depth_v > kf, pv[k, m] + corr[2 * m + 1], 0.0)
            return 0

        lax.fori_loop(0, size, level, 0, unroll=3 if size % 3 == 0 else 1)
        for copy in out_copies(i):
            copy.start()

    for copy in through + [copy for i in range(chunks) for copy in out_copies(i)]:
        copy.wait()


def solution(mesh):
    col_count, row_count = mesh.shape["col"], mesh.shape["row"]

    def local_step(vel_x, vel_y, pot_temp, salinity, surf_eta, trans_x, trans_y, col_depth, wet_levels, avg_weights):
        K = vel_x.shape[0]
        size = level_chunk(K)
        chunks = K // size
        table = jnp.asarray(solve_tables(K))
        smem = pl.BlockSpec(memory_space=pltpu.SMEM)
        vmem = pl.BlockSpec(memory_space=pltpu.VMEM)
        hbm = pl.BlockSpec(memory_space=pl.ANY)
        full = jax.ShapeDtypeStruct((K, 2, ROWS, WIDTH), F32)
        held = pltpu.VMEM((K, 2, ROWS, WIDTH), F32)
        dma = pltpu.SemaphoreType.DMA
        outs = pl.pallas_call(
            functools.partial(step_kernel, row_count, col_count, K),
            out_shape=(held,) * 4 + tuple(pltpu.VMEM((n, ROWS, PADDED), F32) for n in (4, 4)) + tuple(pltpu.VMEM((n, 80, PADDED), F32) for n in (2, 4, 8)),
            in_specs=[smem] + [vmem] * 5 + [hbm] * 4,
            out_specs=(vmem,) * 9,
            scratch_shapes=[
                *[pltpu.VMEM((K, 2, ROWS, WIDTH), F32)] * 4,
                *[pltpu.VMEM((K, 2, ROWS, PADDED), F32)] * 4,
                *[pltpu.VMEM((chunks * (size + (size + 1) // 2), 8, LANES), F32)] * 4,
                pltpu.VMEM((1, WIDTH), jnp.int32),
                *[pltpu.VMEM((chunks, ROWS, LANES), F32)] * 4,
                *[pltpu.VMEM((chunks, 8, LANES), F32)] * 2,
                *[pltpu.VMEM((7, ROWS, LANES), F32)] * 2,
                pltpu.VMEM((7, 80, PADDED), F32),
                *[pltpu.VMEM((4, ROWS, LANES), F32)] * 2,
                pltpu.VMEM((4, 80, PADDED), F32),
                dma((chunks, 4)), dma((2, chunks)), dma((2, chunks)), dma((4, chunks)), dma((4, chunks)), dma((5,)), dma((5,)), dma((8,)), dma((8,)),
            ],
            compiler_params=pltpu.CompilerParams(collective_id=0, has_side_effects=True, vmem_limit_bytes=52 << 20),
            name="ocean_step",
        )(table, wet_levels, col_depth, surf_eta, trans_x, trans_y, vel_x, vel_y, pot_temp, salinity)

        small = jax.ShapeDtypeStruct((2, ROWS, WIDTH), F32)
        return pl.pallas_call(
            functools.partial(finish_kernel, K, size),
            out_shape=(small,) * 3 + (full,) * 4,
            in_specs=[smem] + [vmem] * 9,
            out_specs=(vmem,) * 3 + (hbm,) * 4,
            scratch_shapes=[
                pltpu.VMEM((8, 80, PADDED), F32),
                pltpu.VMEM((6, ROWS, PADDED), F32),
                *[pltpu.VMEM((K, 2, ROWS, WIDTH), F32)] * 2,
                dma((2, 1 + chunks)),
            ],
            compiler_params=pltpu.CompilerParams(vmem_limit_bytes=20 << 20),
            name="ocean_finish",
        )(avg_weights, *outs)

    spec_3d = P(None, None, "row", "col")
    spec_2d = P(None, "row", "col")
    spec_map = P("row", "col")
    return jax.shard_map(local_step, mesh=mesh, in_specs=(spec_3d,) * 4 + (spec_2d,) * 3 + (spec_map,) * 2 + (P(),), out_specs=(spec_2d,) * 3 + (spec_3d,) * 4, check_vma=False)
```

```python
import functools
import numpy as np
import jax
import jax.numpy as jnp
from jax import lax
from jax.experimental import pallas as pl
from jax.experimental.pallas import tpu as pltpu
from jax.sharding import PartitionSpec as P

WAVE_COURANT = 0.4
THERM_EXP = 0.2
HALINE_CON = 0.15
PRESS_SCALE = 0.5
VISC_NUMBER = 1.0
DIFF_NUMBER = 0.5
SUBCYCLES = 30
HALO = 32
PAIR = (0, 1)
QUAD = (0, 1, 2, 3)
MOMENTUM_UNROLL = 5
TRACER_UNROLL = 5
PACK_UNROLL = 5
ROWS, WIDTH, PADDED, LANES = 16, 192, 256, 128
LAST, KEEP = LANES - 1, slice(0, WIDTH)
MESH = pl.DeviceIdType.MESH
F32 = jnp.float32


def solve_tables(level_count):
    rows = []
    for strength in (VISC_NUMBER, DIFF_NUMBER):
        inner, last = np.zeros(level_count), np.zeros(level_count)
        inner[0], last[0] = 1.0 + strength, 1.0
        for k in range(1, level_count):
            inner[k] = 1.0 + 2.0 * strength - strength * strength / inner[k - 1]
            last[k] = 1.0 + strength - strength * strength / inner[k - 1]
        rows += [1.0 / inner, 1.0 / last, strength / inner]
    return np.concatenate(rows).astype(np.float32)


def level_chunk(level_count):
    return next(size for size in (15, 5, 4) if level_count % size == 0)


def step_kernel(
    row_count, col_count, level_count,
    table, kmt_in, depth_in, eta_in, tx_in, ty_in, u_hbm, v_hbm, t_hbm, s_hbm,
    pu, pv, pt, ps, mean, faces, coef, force, state,
    raw_u, raw_v, raw_t, raw_s, ua, va, ta, sa, ub, vb, tb, sb, rows_n, rows_s, send_n, send_s, tail_n, tail_s, north_w, south_e, north_h, kmt_n, pack, col_e, col_w, corner_se, corner_nw,
    edge_e, edge_w, wide, fedge_e, fedge_w, wide_f,
    load_sem, row_send, row_recv, col_send, col_recv, misc_send, misc_recv, wide_send, wide_recv,
):
    K = level_count
    open_scope = []

    def mark(name):
        if open_scope:
            open_scope.pop().__exit__(None, None, None)
        if name:
            open_scope.append(jax.named_scope(name))
            open_scope[-1].__enter__()

    size = level_chunk(K)
    chunks = K // size
    r = lax.axis_index("row")
    c = lax.axis_index("col")
    east = lax.rem(c + 1, col_count)
    west = lax.rem(c + col_count - 1, col_count)
    has_n, has_s = r < row_count - 1, r > 0
    has_nn, has_ss = r < row_count - 2, r > 1
    raw, first, second = (raw_u, raw_v, raw_t, raw_s), (ua, va, ta, sa), (ub, vb, tb, sb)

    def one(flag):
        return flag.astype(jnp.int32)

    mark("init")
    def block(k, m):
        return pl.ds(pl.multiple_of((2 * k + m) * ROWS, ROWS), ROWS)

    loads = []
    for i in range(chunks):
        levels = pl.ds(i * size * 2 * ROWS, size * 2 * ROWS)
        group = []
        for f, src in enumerate((u_hbm, v_hbm, t_hbm, s_hbm)):
            group.append(pltpu.make_async_copy(src.at[levels, 0:LANES], first[f].at[levels], load_sem.at[i, f]))
            group.append(pltpu.make_async_copy(src.at[levels], raw[f].at[levels], load_sem.at[i, 4 + f]))
        loads.append(group)
    for group in loads:
        for copy in group:
            copy.start()

    wide[...] = jnp.zeros_like(wide)
    wide_f[...] = jnp.zeros_like(wide_f)

    @pl.when(jnp.logical_not(has_n))
    def _():
        rows_n[...] = jnp.zeros_like(rows_n)
        kmt_n[...] = jnp.zeros_like(kmt_n)
        corner_nw[...] = jnp.zeros_like(corner_nw)

    @pl.when(jnp.logical_not(has_s))
    def _():
        rows_s[...] = jnp.zeros_like(rows_s)
        corner_se[...] = jnp.zeros_like(corner_se)

    barrier = pltpu.get_barrier_semaphore()

    def signal(**where):
        pl.semaphore_signal(barrier, inc=1, device_id=where, device_id_type=MESH)

    signal(col=east)
    signal(col=west)

    @pl.when(has_n)
    def _():
        signal(row=r + 1)
        signal(row=r + 1, col=west)

    @pl.when(has_s)
    def _():
        signal(row=r - 1)
        signal(row=r - 1, col=east)

    @pl.when(has_nn)
    def _():
        signal(row=r + 2)

    @pl.when(has_ss)
    def _():
        signal(row=r - 2)

    def remote(src, dst, ssem, rsem, **where):
        return pltpu.make_async_remote_copy(src_ref=src, dst_ref=dst, send_sem=ssem, recv_sem=rsem, device_id=where, device_id_type=MESH)

    lane = lax.broadcasted_iota(jnp.int32, (ROWS, LANES), 1)
    lane8, lane1 = lane[0:8], lane[0:1]
    sub = lax.broadcasted_iota(jnp.int32, (8, LANES), 0)
    sub2 = lax.broadcasted_iota(jnp.int32, (8, PADDED), 0)

    def padded(x):
        return jnp.concatenate([x, jnp.zeros((x.shape[0], PADDED - WIDTH), x.dtype)], axis=1)

    def overlapped(x):
        a, b = x[:, 0:LANES], x[:, LANES:PADDED]
        return jnp.concatenate([a, jnp.where(lane < 64, b, a)], axis=1)

    def linear(x):
        a, b = x[:, 0:LANES], x[:, LANES:PADDED]
        return jnp.concatenate([jnp.where(lane < 96, a, b), b], axis=1)

    kmt = padded(kmt_in[...]).astype(F32)
    own = pl.ds(HALO, ROWS)
    wide[0, own, :] = jnp.where(kmt > 0.5, padded(depth_in[...]), 0.0)
    for m in PAIR:
        wide[1 + m, own, :] = padded(eta_in[m])
        wide[3 + m, own, :] = padded(tx_in[m])
        wide[5 + m, own, :] = padded(ty_in[m])

    kmt_copy = remote(kmt_in.at[0:1, :], kmt_n, misc_send.at[0], misc_recv.at[0], row=r - 1)

    def south_copy(i):
        return remote(send_s.at[i], rows_n.at[i], row_send.at[0, i], row_recv.at[0, i], row=r - 1)

    def north_copy(i):
        return remote(send_n.at[i], rows_s.at[i], row_send.at[1, i], row_recv.at[1, i], row=r + 1)

    def west_copy(i):
        return remote(pack.at[i], col_e.at[i], col_send.at[0, i], col_recv.at[0, i], col=west)

    def east_copy(i):
        return remote(pack.at[i], col_w.at[i], col_send.at[1, i], col_recv.at[1, i], col=east)

    def corner_v(i):
        return remote(pack.at[i, 0, 8:16, :], corner_se.at[i], col_send.at[2, i], col_recv.at[2, i], row=r + 1, col=west)

    def corner_u(i):
        return remote(pack.at[i, 0, 0:8, :], corner_nw.at[i], col_send.at[3, i], col_recv.at[3, i], row=r - 1, col=east)

    groups = [*range(0, size - 3, 4)] + [size - 4] * (size % 4 > 0)

    def pack_chunk(i):
        for copy in loads[i]:
            copy.wait()

        def collect(j, acc):
            out = []
            here = (lane == j) | (lane == j + 63)
            for f in QUAD:
                for m in PAIR:
                    at = block(i * size + j, m)
                    x = first[f][at, :]
                    y = jnp.where(lane < 64, padded(raw[f][at, LANES:WIDTH]), x)
                    second[f][at, :] = y
                    out.append(jnp.where(here, pltpu.roll(jnp.where(lane == 0, x, y), j, 1), acc[len(out)]))
            return tuple(out)

        acc = lax.fori_loop(0, size, collect, (jnp.zeros((ROWS, LANES), F32),) * 8, unroll=PACK_UNROLL)
        for g in PAIR:
            merged = pltpu.roll(kmt[:, 0:LANES], LAST, 1)
            for n in QUAD:
                low = size * n
                here = (lane >= low) & (lane < low + size) | (lane >= low + 63) & (lane < low + 63 + size)
                merged = jnp.where(here, pltpu.roll(acc[4 * g + n], low, 1), merged)
            pack[i, g] = merged
        for row, dest in ((0, send_s), (15, send_n)):
            for j in groups:
                at, spot = pl.ds((i * size + j) * 2 * ROWS + row, 8, stride=ROWS), pl.ds(2 * j, 8)
                tails = []
                for f in QUAD:
                    dest[i, f, spot, :] = first[f][at, :]
                    tails.append(second[f][at, :])
                for p in PAIR:
                    dest[i, 4 + p, spot, :] = jnp.where(lane8 < 64, tails[2 * p], pltpu.roll(tails[2 * p + 1], 64, 1))

    def start_chunk(i):
        west_copy(i).start()
        east_copy(i).start()

        @pl.when(has_s)
        def _():
            corner_u(i).start()
            south_copy(i).start()

        @pl.when(has_n)
        def _():
            corner_v(i).start()
            north_copy(i).start()

    mark("pack_early")
    early = min(2, chunks)
    for i in range(early):
        pack_chunk(i)
    mark("barrier_wait")
    pl.semaphore_wait(barrier, 2 + 2 * one(has_n) + 2 * one(has_s) + one(has_nn) + one(has_ss))

    @pl.when(has_s)
    def _():
        kmt_copy.start()

    for i in range(early):
        start_chunk(i)
    mark("pack_late")
    for i in range(early, chunks):
        pack_chunk(i)
        start_chunk(i)

    def edge_pair(buf, to_east, to_west, sem):
        return [
            remote(buf.at[:, own, 0:LANES], to_west, misc_send.at[sem], misc_recv.at[sem], col=west),
            remote(buf.at[:, own, LANES:PADDED], to_east, misc_send.at[sem + 1], misc_recv.at[sem + 1], col=east),
        ]

    def with_edges(x, from_east, from_west):
        b = jnp.where(lane < 64, x[:, LANES:PADDED], jnp.where(lane < 96, pltpu.roll(from_east, 64, 1), pltpu.roll(from_west, 64, 1)))
        return jnp.concatenate([x[:, 0:LANES], b], axis=1)

    def spread(buf, sem):
        src = buf.at[:, own, :]
        parts = ((has_n, has_s, 16, r + 1), (has_s, has_n, 48, r - 1), (has_nn, has_ss, 0, r + 2), (has_ss, has_nn, 64, r - 2))
        return [(there, here, remote(src, buf.at[:, pl.ds(at, ROWS), :], wide_send.at[sem + n], wide_recv.at[sem + n], row=row)) for n, (there, here, at, row) in enumerate(parts)]

    def start_spread(copies):
        for there, _, copy in copies:
            @pl.when(there)
            def _():
                copy.start()

    def finish_spread(copies):
        for there, here, copy in copies:
            @pl.when(there)
            def _():
                copy.wait_send()

            @pl.when(here)
            def _():
                copy.wait_recv()

    mark("edges")
    edge_copies = edge_pair(wide, edge_w, edge_e, 1)
    for copy in edge_copies:
        copy.start()

    def roll_e(x):
        return jnp.concatenate([pltpu.roll(x[:, 0:LANES], LAST, 1), pltpu.roll(x[:, LANES:PADDED], LAST, 1)], axis=1)

    def roll_w(x):
        return jnp.concatenate([pltpu.roll(x[:, 0:LANES], 1, 1), pltpu.roll(x[:, LANES:PADDED], 1, 1)], axis=1)

    def from_north(x, edge):
        low, high = pltpu.roll(x[0:8], 7, 0), pltpu.roll(x[8:16], 7, 0)
        return jnp.concatenate([jnp.where(sub2 == 7, high, low), jnp.where(sub2 == 7, edge, high)], axis=0)

    def from_south(x, edge):
        low, high = pltpu.roll(x[0:8], 1, 0), pltpu.roll(x[8:16], 1, 0)
        return jnp.concatenate([jnp.where(sub2 == 0, edge, low), jnp.where(sub2 == 0, low, high)], axis=0)

    def wait_columns(i):
        west_copy(i).wait_recv()
        east_copy(i).wait_recv()

    def insert_columns(i):
        columns = [jnp.where(lane < 62, col_e[i, g], col_w[i, g]) for g in PAIR]

        def level(j, _):
            k = i * size + j
            for f in QUAD:
                for m in PAIR:
                    place = size * (2 * (f % 2) + m) + j
                    turned = pltpu.roll(columns[f // 2], lax.rem(LANES + 64 - place, LANES), 1)
                    pltpu.store(first[f].at[block(k, m)], turned, mask=lane == LAST)
                    pltpu.store(second[f].at[block(k, m)], turned, mask=lane == 64)
            return 0

        lax.fori_loop(0, size, level, 0, unroll=5)

    edge_lane = lax.broadcasted_iota(jnp.int32, rows_n.shape[2:], 1)

    def unpack_rows(i):
        for rows, tails in ((rows_n, tail_n), (rows_s, tail_s)):
            for f in QUAD:
                packed = rows[i, 4 + f // 2]
                tails[i, f] = jnp.where(edge_lane < 64, packed if f % 2 == 0 else pltpu.roll(packed, 64, 1), rows[i, f])
        for h, (u, v, t, s) in enumerate(((rows_n.at[i, 0], rows_s.at[i, 1], rows_n.at[i, 2], rows_n.at[i, 3]), (tail_n.at[i, 0], tail_s.at[i, 1], tail_n.at[i, 2], tail_n.at[i, 3]))):
            north_w[i, h] = u[...] + pltpu.roll(u[...], 1, 1)
            south_e[i, h] = v[...] + pltpu.roll(v[...], LAST, 1)
            north_h[i, h] = (half_scale * HALINE_CON) * s[...] - (half_scale * THERM_EXP) * t[...]

    half_scale = 0.5 * PRESS_SCALE / K

    def both(tiles, k, m, f):
        return jnp.concatenate([tiles[0][f][block(k, m), :], tiles[1][f][block(k, m), :]], axis=1)

    def edge(rows, tails, f, i, at):
        return jnp.concatenate([rows[i, f, at, :], tails[i, f, at, :]], axis=1)

    mark("column_wait")
    wait_columns(0)

    @pl.when(has_n)
    def _():
        kmt_copy.wait_recv()

    @pl.when(has_s)
    def _():
        kmt_copy.wait_send()

    mark("masks")
    kmt2 = overlapped(kmt)
    kmt_edge = jnp.where(lane == 64, pltpu.roll(col_e[0, 0], 65, 1), kmt2[:, LANES:PADDED])
    kmt_row = padded(kmt_n[...]).astype(F32)
    kmt_north = jnp.concatenate([kmt_row[:, 0:LANES], jnp.where(lane1 < 64, kmt_row[:, LANES:PADDED], kmt_row[:, 0:LANES])], axis=1)
    mu = jnp.minimum(kmt2, roll_e(jnp.concatenate([kmt2[:, 0:LANES], kmt_edge], axis=1)))
    mv = jnp.minimum(kmt2, from_north(kmt2, kmt_north))
    faces[0] = linear(mu)
    faces[1] = linear(mv)

    def solve_factor(depth, k, first):
        inner, last = table[first * K + k], table[(first + 1) * K + k]
        kf = k.astype(F32)
        return jnp.where(depth > kf + 1.0, inner, jnp.where(depth > kf, last, 0.0))

    def momentum(i):
        def level(j, members):
            k = i * size + j
            kf = k.astype(F32)
            factor_u, factor_v = solve_factor(mu, k, 0), solve_factor(mv, k, 0)
            out = []
            for m in PAIR:
                total, total_n, gu_sum, gv_sum, side_u, side_v = members[m]
                at = pl.ds(2 * j + m, 1)
                u, v, t, s = (both((first, second), k, m, f) for f in QUAD)
                step = (half_scale * HALINE_CON) * s - (half_scale * THERM_EXP) * t
                pressure = total + step
                step_n = jnp.concatenate([north_h[i, 0, at, :], north_h[i, 1, at, :]], axis=1)
                pressure_n = total_n + step_n
                corner_n = pltpu.roll(corner_nw[i], 65 - (size * m + j), 1)[0:1]
                corner_s = pltpu.roll(corner_se[i], lax.rem(LANES + 63 - (size * (2 + m) + j), LANES), 1)[7:8]
                u_edge, v_edge = edge(rows_n, tail_n, 0, i, at), edge(rows_s, tail_s, 1, i, at)
                u_pair_n = jnp.concatenate([jnp.where(lane1 == 0, u_edge[:, 0:LANES] + corner_n, north_w[i, 0, at, :]), north_w[i, 1, at, :]], axis=1)
                v_pair_s = jnp.concatenate([south_e[i, 0, at, :], jnp.where(lane1 == 63, v_edge[:, LANES:PADDED] + corner_s, south_e[i, 1, at, :])], axis=1)
                v_e, v_w, u_e, u_w = roll_e(v), roll_w(v), roll_e(u), roll_w(u)
                v_pair, u_pair = v + v_e, u + u_w
                vu = 0.125 * (v_pair + from_south(v_pair, v_pair_s))
                uv = 0.125 * (u_pair + from_north(u_pair, u_pair_n))
                u_n, u_s = from_north(u, u_edge), from_south(u, edge(rows_s, tail_s, 0, i, at))
                v_n, v_s = from_north(v, edge(rows_n, tail_n, 1, i, at)), from_south(v, v_edge)
                p_n = from_north(pressure, pressure_n)
                gu = pressure - roll_e(pressure) - 0.5 * u * (u_e - u_w) - vu * (u_n - u_s)
                gv = pressure - p_n - uv * (v_e - v_w) - 0.5 * v * (v_n - v_s)
                gu = jnp.where(mu > kf, gu, 0.0)
                gv = jnp.where(mv > kf, gv, 0.0)
                side_u = (u + gu + VISC_NUMBER * side_u) * factor_u
                side_v = (v + gv + VISC_NUMBER * side_v) * factor_v
                pu[k, m] = linear(side_u)[:, KEEP]
                pv[k, m] = linear(side_v)[:, KEEP]
                out.append((pressure + step, pressure_n + step_n, gu_sum + gu, gv_sum + gv, side_u, side_v))
            return tuple(out)

        return level

    zero = jnp.zeros((ROWS, PADDED), F32)
    zero_row = jnp.zeros((1, PADDED), F32)
    members = ((zero, zero_row, zero, zero, zero, zero),) * 2
    for i in range(chunks):
        if i > 0:
            wait_columns(i)
        mark("insert")
        insert_columns(i)

        mark("row_wait")
        @pl.when(has_n)
        def _():
            south_copy(i).wait_recv()
            corner_u(i).wait_recv()

        @pl.when(has_s)
        def _():
            north_copy(i).wait_recv()
            corner_v(i).wait_recv()

        mark("momentum")
        unpack_rows(i)
        members = lax.fori_loop(0, size, momentum(i), members, unroll=MOMENTUM_UNROLL)

        mark("next")
        if i == chunks // 2:
            for copy in edge_copies:
                copy.wait()
            for p in range(7):
                wide[p, own, :] = with_edges(wide[p, own, :], edge_e[p], edge_w[p])
            static_copies = spread(wide, 0)
            start_spread(static_copies)

    mark("force")
    count_u = linear(jnp.maximum(mu, 1.0))
    count_v = linear(jnp.maximum(mv, 1.0))
    for m in PAIR:
        wide_f[m, own, :] = linear(members[m][2]) / count_u
        wide_f[2 + m, own, :] = linear(members[m][3]) / count_v
    force_edges = edge_pair(wide_f, fedge_w, fedge_e, 3)
    for copy in force_edges:
        copy.start()

    def tracers(i, carry):
        def level(j, carry):
            k = i * size + j
            factor = solve_factor(kmt2, k, 3)
            out = []
            for m in PAIR:
                at = pl.ds(2 * j + m, 1)
                u, v = (0.5 * both((first, second), k, m, f) for f in PAIR)
                u_w = roll_w(u)
                v_edge = 0.5 * edge(rows_s, tail_s, 1, i, at)
                for f, dest in ((2, pt), (3, ps)):
                    t = both((first, second), k, m, f)
                    flux_x = u * (t + roll_e(t)) - u_w * (t + roll_w(t))
                    flux_y = v * (t + from_north(t, edge(rows_n, tail_n, f, i, at)))
                    flux_s = v_edge * (edge(rows_s, tail_s, f, i, at) + t[0:1])
                    moved = t - (flux_x + flux_y - from_south(flux_y, flux_s))
                    side = (moved + DIFF_NUMBER * carry[len(out)]) * factor
                    dest[k, m] = linear(side)[:, KEEP]
                    out.append(side)
            return tuple(out)

        return lax.fori_loop(0, size, level, carry, unroll=TRACER_UNROLL)

    mark("tracer_1")
    tail = (zero,) * 4
    split = (3 * chunks + 4) // 5
    tail = lax.fori_loop(0, split, tracers, tail)

    mark("force_edge_wait")
    for copy in force_edges:
        copy.wait()
    mark("force_spread")
    for p in QUAD:
        wide_f[p, own, :] = with_edges(wide_f[p, own, :], fedge_e[p], fedge_w[p])
    force_copies = spread(wide_f, 4)
    start_spread(force_copies)

    mark("tracer_2")
    tail = lax.fori_loop(split, chunks, tracers, tail)

    def back_tracers(j, carry):
        k = K - 2 - j
        ratio = table[5 * K + k]
        out = []
        for m in PAIR:
            for dest in (pt, ps):
                x = dest[k, m] + ratio * carry[len(out)]
                dest[k, m] = x
                out.append(x)
        return tuple(out)

    mark("back_tracers")
    lax.fori_loop(0, K - 1, back_tracers, tuple(linear(x)[:, KEEP] for x in tail), unroll=2)

    def back(j, carry):
        k = K - 2 - j
        ratio = table[2 * K + k]
        out = []
        for m in PAIR:
            xu, xv, su, sv = carry[m]
            xu = pu[k, m] + ratio * xu
            xv = pv[k, m] + ratio * xv
            pu[k, m] = xu
            pv[k, m] = xv
            out.append((xu, xv, su + xu, sv + xv))
        return tuple(out)

    mark("back_uv")
    start = tuple(tuple(linear(members[m][n])[:, KEEP] for n in (4, 5, 4, 5)) for m in PAIR)
    ends = lax.fori_loop(0, K - 1, back, start)

    mark("static_wait")
    finish_spread(static_copies)
    mark("force_wait")
    finish_spread(force_copies)

    mark("coef")
    depth = wide[0]
    depth_e = pltpu.roll(depth, PADDED - 1, 1)
    depth_n = pltpu.roll(depth, 79, 0)
    hu = jnp.where((depth > 0.0) & (depth_e > 0.0), 0.5 * (depth + depth_e), 0.0)
    hv = jnp.where((depth > 0.0) & (depth_n > 0.0), 0.5 * (depth + depth_n), 0.0)
    coef[0] = WAVE_COURANT * WAVE_COURANT * hu
    coef[1] = WAVE_COURANT * WAVE_COURANT * hv
    for m in PAIR:
        force[m] = hu * wide_f[m] * (WAVE_COURANT / SUBCYCLES)
        force[2 + m] = hv * wide_f[2 + m] * (WAVE_COURANT / SUBCYCLES)
        state[m] = wide[1 + m]
        state[2 + m] = WAVE_COURANT * wide[3 + m]
        state[4 + m] = WAVE_COURANT * wide[5 + m]
        state[6 + m] = pltpu.roll(wide[1 + m], PADDED - 1, 1)
    mine = slice(HALO, HALO + ROWS)
    for p, (h, count) in enumerate(((hu[mine], count_u), (hv[mine], count_v))):
        faces[2 + p] = 1.0 / (WAVE_COURANT * jnp.where(h > 0.0, h, 1.0))
        for m in PAIR:
            mean[2 * p + m] = padded(ends[m][2 + p]) / count

    mark("send_wait")
    for i in range(chunks):
        west_copy(i).wait_send()
        east_copy(i).wait_send()

    @pl.when(has_s)
    def _():
        for i in range(chunks):
            south_copy(i).wait_send()
            corner_u(i).wait_send()

    @pl.when(has_n)
    def _():
        for i in range(chunks):
            north_copy(i).wait_send()
            corner_v(i).wait_send()
    mark("")


def finish_kernel(
    K, size,
    weights, pu, pv, pt, ps, mean, faces, coef, force, first_state,
    eta_o, tx_o, ty_o, u_o, v_o, t_o, s_o,
    state, avg, out_u, out_v, sems,
):
    chunks = K // size
    through = [pltpu.make_async_copy(src, dst, sems.at[i, 0]) for i, (src, dst) in enumerate(((pt, t_o), (ps, s_o)))]
    for copy in through:
        copy.start()
    state[...] = first_state[...]
    avg[...] = jnp.zeros_like(avg)

    def subcycles(first, last, margin):
        height = ROWS + 2 * margin
        rows = pl.ds(HALO - margin, height)
        mine = slice(margin, margin + ROWS)

        def to_e(x):
            return pltpu.roll(x, PADDED - 1, 1)

        def subcycle(n, _):
            weight = weights[n]
            for m in PAIR:
                tx, ty = state[2 + m, rows], state[4 + m, rows]
                tx_e, ty_e = to_e(tx), to_e(ty)
                eta = state[m, rows] - (tx - pltpu.roll(tx, 1, 1) + ty - pltpu.roll(ty, 1, 0))
                eta_e = state[6 + m, rows] - (tx_e - tx + ty_e - pltpu.roll(ty_e, 1, 0))
                tx = tx + force[m, rows] - coef[0, rows] * (eta_e - eta)
                ty = ty + force[2 + m, rows] - coef[1, rows] * (pltpu.roll(eta, height - 1, 0) - eta)
                for p, x in enumerate((eta, tx, ty)):
                    state[2 * p + m, rows] = x
                    avg[2 * p + m] = avg[2 * p + m] + weight * x[mine]
                state[6 + m, rows] = eta_e
            return 0

        lax.fori_loop(first, last, subcycle, 0)

    done = 0
    for margin in (32, 24, 16, 8):
        last = SUBCYCLES - (margin - 8)
        subcycles(done, last, margin)
        done = last

    corr = []
    for m in PAIR:
        eta_o[m] = avg[m][:, KEEP]
        for p, dest in enumerate((tx_o, ty_o)):
            transport = avg[2 + 2 * p + m]
            dest[m] = (transport * (1.0 / WAVE_COURANT))[:, KEEP]
            corr.append((transport * faces[2 + p] - mean[2 * p + m])[:, KEEP])
    depth_u, depth_v = faces[0][:, KEEP], faces[1][:, KEEP]

    def out_copies(i):
        levels = pl.ds(i * size, size)
        return [pltpu.make_async_copy(src.at[levels], dst.at[levels], sems.at[p, 1 + i]) for p, (src, dst) in enumerate(((out_u, u_o), (out_v, v_o)))]

    for i in range(chunks):
        def level(j, _):
            k = i * size + j
            kf = k.astype(F32)
            for m in PAIR:
                out_u[k, m] = jnp.where(depth_u > kf, pu[k, m] + corr[2 * m], 0.0)
                out_v[k, m] = jnp.where(depth_v > kf, pv[k, m] + corr[2 * m + 1], 0.0)
            return 0

        lax.fori_loop(0, size, level, 0, unroll=3 if size % 3 == 0 else 1)
        for copy in out_copies(i):
            copy.start()

    for copy in through + [copy for i in range(chunks) for copy in out_copies(i)]:
        copy.wait()


def solution(mesh):
    col_count, row_count = mesh.shape["col"], mesh.shape["row"]

    def local_step(vel_x, vel_y, pot_temp, salinity, surf_eta, trans_x, trans_y, col_depth, wet_levels, avg_weights):
        K = vel_x.shape[0]
        size = level_chunk(K)
        chunks = K // size
        edge_rows = (2 * size + 7) // 8 * 8
        table = jnp.asarray(solve_tables(K))
        smem = pl.BlockSpec(memory_space=pltpu.SMEM)
        vmem = pl.BlockSpec(memory_space=pltpu.VMEM)
        hbm = pl.BlockSpec(memory_space=pl.ANY)
        full = jax.ShapeDtypeStruct((K, 2, ROWS, WIDTH), F32)
        held = pltpu.VMEM((K, 2, ROWS, WIDTH), F32)
        dma = pltpu.SemaphoreType.DMA
        outs = pl.pallas_call(
            functools.partial(step_kernel, row_count, col_count, K),
            out_shape=(held,) * 4 + tuple(pltpu.VMEM((n, ROWS, PADDED), F32) for n in (4, 4)) + tuple(pltpu.VMEM((n, 80, PADDED), F32) for n in (2, 4, 8)),
            in_specs=[smem] + [vmem] * 5 + [hbm] * 4,
            out_specs=(vmem,) * 9,
            scratch_shapes=[
                *[pltpu.VMEM((K * 2 * ROWS, WIDTH), F32)] * 4,
                *[pltpu.VMEM((K * 2 * ROWS, LANES), F32)] * 8,
                *[pltpu.VMEM((chunks, 6, edge_rows, LANES), F32)] * 4,
                *[pltpu.VMEM((chunks, 4, edge_rows, LANES), F32)] * 2,
                *[pltpu.VMEM((chunks, 2, edge_rows, LANES), F32)] * 3,
                pltpu.VMEM((1, WIDTH), jnp.int32),
                *[pltpu.VMEM((chunks, 2, ROWS, LANES), F32)] * 3,
                *[pltpu.VMEM((chunks, 8, LANES), F32)] * 2,
                *[pltpu.VMEM((7, ROWS, LANES), F32)] * 2,
                pltpu.VMEM((7, 80, PADDED), F32),
                *[pltpu.VMEM((4, ROWS, LANES), F32)] * 2,
                pltpu.VMEM((4, 80, PADDED), F32),
                dma((chunks, 8)), dma((2, chunks)), dma((2, chunks)), dma((4, chunks)), dma((4, chunks)), dma((5,)), dma((5,)), dma((8,)), dma((8,)),
            ],
            compiler_params=pltpu.CompilerParams(collective_id=0, has_side_effects=True, vmem_limit_bytes=52 << 20),
            name="ocean_step",
        )(table, wet_levels, col_depth, surf_eta, trans_x, trans_y, *(x.reshape(-1, WIDTH) for x in (vel_x, vel_y, pot_temp, salinity)))

        small = jax.ShapeDtypeStruct((2, ROWS, WIDTH), F32)
        return pl.pallas_call(
            functools.partial(finish_kernel, K, size),
            out_shape=(small,) * 3 + (full,) * 4,
            in_specs=[smem] + [vmem] * 9,
            out_specs=(vmem,) * 3 + (hbm,) * 4,
            scratch_shapes=[
                pltpu.VMEM((8, 80, PADDED), F32),
                pltpu.VMEM((6, ROWS, PADDED), F32),
                *[pltpu.VMEM((K, 2, ROWS, WIDTH), F32)] * 2,
                dma((2, 1 + chunks)),
            ],
            compiler_params=pltpu.CompilerParams(vmem_limit_bytes=20 << 20),
            name="ocean_finish",
        )(avg_weights, *outs)

    spec_3d = P(None, None, "row", "col")
    spec_2d = P(None, "row", "col")
    spec_map = P("row", "col")
    return jax.shard_map(local_step, mesh=mesh, in_specs=(spec_3d,) * 4 + (spec_2d,) * 3 + (spec_map,) * 2 + (P(),), out_specs=(spec_2d,) * 3 + (spec_3d,) * 4, check_vma=False)
```

```python
import functools
import numpy as np
import jax
import jax.numpy as jnp
from jax import lax
from jax.experimental import pallas as pl
from jax.experimental.pallas import tpu as pltpu
from jax.sharding import PartitionSpec as P

WAVE_COURANT = 0.4
THERM_EXP = 0.2
HALINE_CON = 0.15
PRESS_SCALE = 0.5
VISC_NUMBER = 1.0
DIFF_NUMBER = 0.5
SUBCYCLES = 30
HALO = 32
PAIR = (0, 1)
QUAD = (0, 1, 2, 3)
ZERO, HALF = 0.0, 0.5
UNROLL = 5
ROWS, WIDTH, PADDED, LANES = 16, 192, 256, 128
LAST, KEEP = LANES - 1, slice(0, WIDTH)
MESH = pl.DeviceIdType.MESH
F32 = jnp.float32


def solve_tables(level_count):
    rows = []
    for strength in (VISC_NUMBER, DIFF_NUMBER):
        inner, last = np.zeros(level_count), np.zeros(level_count)
        inner[0], last[0] = 1.0 + strength, 1.0
        for k in range(1, level_count):
            inner[k] = 1.0 + 2.0 * strength - strength * strength / inner[k - 1]
            last[k] = 1.0 + strength - strength * strength / inner[k - 1]
        rows += [1.0 / inner, 1.0 / last, strength / inner]
    return np.concatenate(rows).astype(np.float32)


def level_chunk(level_count):
    return next(size for size in (15, 5, 4) if level_count % size == 0)


def step_kernel(
    row_count, col_count, level_count,
    table, kmt_in, depth_in, eta_in, tx_in, ty_in, u_hbm, v_hbm, t_hbm, s_hbm,
    pu, pv, pt, ps, mean, faces, coef, force, state,
    raw_u, raw_v, raw_t, raw_s, ua, va, ta, sa, ub, vb, tb, sb, rows_n, rows_s, send_n, send_s, tail_n, tail_s, north_w, south_e, north_h, kmt_n, pack, col_e, col_w, corner_se, corner_nw,
    edge_e, edge_w, wide, fedge_e, fedge_w, wide_f,
    load_sem, row_send, row_recv, col_send, col_recv, misc_send, misc_recv, wide_send, wide_recv,
):
    K = level_count
    open_scope = []

    def mark(name):
        if open_scope:
            open_scope.pop().__exit__(None, None, None)
        if name:
            open_scope.append(jax.named_scope(name))
            open_scope[-1].__enter__()

    size = level_chunk(K)
    chunks = K // size
    r = lax.axis_index("row")
    c = lax.axis_index("col")
    east = lax.rem(c + 1, col_count)
    west = lax.rem(c + col_count - 1, col_count)
    has_n, has_s = r < row_count - 1, r > 0
    has_nn, has_ss = r < row_count - 2, r > 1
    raw, first, second = (raw_u, raw_v, raw_t, raw_s), (ua, va, ta, sa), (ub, vb, tb, sb)

    def one(flag):
        return flag.astype(jnp.int32)

    mark("init")
    def block(k, m):
        return pl.ds(pl.multiple_of((2 * k + m) * ROWS, ROWS), ROWS)

    loads = []
    for i in range(chunks):
        levels = pl.ds(i * size * 2 * ROWS, size * 2 * ROWS)
        group = []
        for f, src in enumerate((u_hbm, v_hbm, t_hbm, s_hbm)):
            group.append(pltpu.make_async_copy(src.at[levels], raw[f].at[levels], load_sem.at[i, f]))
        loads.append(group)
    for group in loads:
        for copy in group:
            copy.start()

    wide[...] = jnp.zeros_like(wide)
    wide_f[...] = jnp.zeros_like(wide_f)

    @pl.when(jnp.logical_not(has_n))
    def _():
        rows_n[...] = jnp.zeros_like(rows_n)
        kmt_n[...] = jnp.zeros_like(kmt_n)
        corner_nw[...] = jnp.zeros_like(corner_nw)

    @pl.when(jnp.logical_not(has_s))
    def _():
        rows_s[...] = jnp.zeros_like(rows_s)
        corner_se[...] = jnp.zeros_like(corner_se)

    barrier = pltpu.get_barrier_semaphore()

    def signal(**where):
        pl.semaphore_signal(barrier, inc=1, device_id=where, device_id_type=MESH)

    signal(col=east)
    signal(col=west)

    @pl.when(has_n)
    def _():
        signal(row=r + 1)
        signal(row=r + 1, col=west)

    @pl.when(has_s)
    def _():
        signal(row=r - 1)
        signal(row=r - 1, col=east)

    @pl.when(has_nn)
    def _():
        signal(row=r + 2)

    @pl.when(has_ss)
    def _():
        signal(row=r - 2)

    def remote(src, dst, ssem, rsem, **where):
        return pltpu.make_async_remote_copy(src_ref=src, dst_ref=dst, send_sem=ssem, recv_sem=rsem, device_id=where, device_id_type=MESH)

    lane = lax.broadcasted_iota(jnp.int32, (ROWS, LANES), 1)
    lane8, lane1 = lane[0:8], lane[0:1]
    sub = lax.broadcasted_iota(jnp.int32, (8, LANES), 0)
    sub2 = lax.broadcasted_iota(jnp.int32, (8, PADDED), 0)

    def padded(x):
        return jnp.concatenate([x, jnp.zeros((x.shape[0], PADDED - WIDTH), x.dtype)], axis=1)

    def overlapped(x):
        a, b = x[:, 0:LANES], x[:, LANES:PADDED]
        return jnp.concatenate([a, jnp.where(lane < 64, b, a)], axis=1)

    def linear(x):
        a, b = x[:, 0:LANES], x[:, LANES:PADDED]
        return jnp.concatenate([jnp.where(lane < 96, a, b), b], axis=1)

    kmt = padded(kmt_in[...]).astype(F32)
    own = pl.ds(HALO, ROWS)
    wide[0, own, :] = jnp.where(kmt > 0.5, padded(depth_in[...]), ZERO)
    for m in PAIR:
        wide[1 + m, own, :] = padded(eta_in[m])
        wide[3 + m, own, :] = padded(tx_in[m])
        wide[5 + m, own, :] = padded(ty_in[m])

    kmt_copy = remote(kmt_in.at[0:1, :], kmt_n, misc_send.at[0], misc_recv.at[0], row=r - 1)

    def south_copy(i):
        return remote(send_s.at[i], rows_n.at[i], row_send.at[0, i], row_recv.at[0, i], row=r - 1)

    def north_copy(i):
        return remote(send_n.at[i], rows_s.at[i], row_send.at[1, i], row_recv.at[1, i], row=r + 1)

    def west_copy(i):
        return remote(pack.at[i], col_e.at[i], col_send.at[0, i], col_recv.at[0, i], col=west)

    def east_copy(i):
        return remote(pack.at[i], col_w.at[i], col_send.at[1, i], col_recv.at[1, i], col=east)

    def corner_v(i):
        return remote(pack.at[i, 0, 8:16, :], corner_se.at[i], col_send.at[2, i], col_recv.at[2, i], row=r + 1, col=west)

    def corner_u(i):
        return remote(pack.at[i, 0, 0:8, :], corner_nw.at[i], col_send.at[3, i], col_recv.at[3, i], row=r - 1, col=east)

    groups = [*range(0, size - 3, 4)] + [size - 4] * (size % 4 > 0)

    def pack_chunk(i):
        for copy in loads[i]:
            copy.wait()

        def collect(j, acc):
            out = []
            here = (lane == j) | (lane == j + 63)
            for f in QUAD:
                for m in PAIR:
                    at = block(i * size + j, m)
                    x = raw[f][at, 0:LANES]
                    first[f][at, :] = x
                    y = jnp.where(lane < 64, padded(raw[f][at, LANES:WIDTH]), x)
                    second[f][at, :] = y
                    out.append(jnp.where(here, pltpu.roll(jnp.where(lane == 0, x, y), j, 1), acc[len(out)]))
            return tuple(out)

        acc = lax.fori_loop(0, size, collect, (jnp.zeros((ROWS, LANES), F32),) * 8, unroll=UNROLL)
        for g in PAIR:
            merged = pltpu.roll(kmt[:, 0:LANES], LAST, 1)
            for n in QUAD:
                low = size * n
                here = (lane >= low) & (lane < low + size) | (lane >= low + 63) & (lane < low + 63 + size)
                merged = jnp.where(here, pltpu.roll(acc[4 * g + n], low, 1), merged)
            pack[i, g] = merged
        for row, dest in ((0, send_s), (15, send_n)):
            for j in groups:
                at, spot = pl.ds((i * size + j) * 2 * ROWS + row, 8, stride=ROWS), pl.ds(2 * j, 8)
                tails = []
                for f in QUAD:
                    dest[i, f, spot, :] = first[f][at, :]
                    tails.append(second[f][at, :])
                for p in PAIR:
                    dest[i, 4 + p, spot, :] = jnp.where(lane8 < 64, tails[2 * p], pltpu.roll(tails[2 * p + 1], 64, 1))

    def start_chunk(i):
        west_copy(i).start()
        east_copy(i).start()

        @pl.when(has_s)
        def _():
            corner_u(i).start()
            south_copy(i).start()

        @pl.when(has_n)
        def _():
            corner_v(i).start()
            north_copy(i).start()

    mark("pack_early")
    def edge_pair(buf, to_east, to_west, sem):
        return [
            remote(buf.at[:, own, 0:LANES], to_west, misc_send.at[sem], misc_recv.at[sem], col=west),
            remote(buf.at[:, own, LANES:PADDED], to_east, misc_send.at[sem + 1], misc_recv.at[sem + 1], col=east),
        ]

    edge_copies = edge_pair(wide, edge_w, edge_e, 1)
    early = 1
    for i in range(early):
        pack_chunk(i)
    mark("barrier_wait")
    pl.semaphore_wait(barrier, 2 + 2 * one(has_n) + 2 * one(has_s) + one(has_nn) + one(has_ss))

    @pl.when(has_s)
    def _():
        kmt_copy.start()

    for i in range(early):
        start_chunk(i)
    for copy in edge_copies:
        copy.start()
    mark("pack_late")
    for i in range(early, chunks):
        pack_chunk(i)
        start_chunk(i)

    def with_edges(x, from_east, from_west):
        b = jnp.where(lane < 64, x[:, LANES:PADDED], jnp.where(lane < 96, pltpu.roll(from_east, 64, 1), pltpu.roll(from_west, 64, 1)))
        return jnp.concatenate([x[:, 0:LANES], b], axis=1)

    def spread(buf, sem):
        even = lax.rem(r, 2) == 0
        odd = jnp.logical_not(even)

        def part(at, to, out, to_sem, row):
            return remote(buf.at[:, pl.ds(at, ROWS), :], buf.at[:, pl.ds(to, ROWS), :], wide_send.at[sem + out], wide_recv.at[sem + to_sem], row=row)

        direct = (
            (has_n, has_s, part(HALO, 16, 0, 0, r + 1)),
            (has_s, has_n, part(HALO, 48, 1, 1, r - 1)),
            (has_nn & even, has_ss, part(HALO, 0, 2, 2, r + 2)),
            (has_ss & odd, has_nn, part(HALO, 64, 3, 3, r - 2)),
        )
        relayed = ((has_s & even, part(16, 0, 4, 2, r + 1)), (has_n & odd, part(48, 64, 5, 3, r - 1)))
        return direct, relayed

    def start_spread(copies):
        for there, _, copy in copies[0]:
            @pl.when(there)
            def _():
                copy.start()

    def relay_spread(copies):
        for (_, here, copy), (there, again) in zip(copies[0], copies[1]):
            @pl.when(here)
            def _():
                copy.wait_recv()

            @pl.when(there)
            def _():
                again.start()

    def finish_spread(copies):
        for n, (there, here, copy) in enumerate(copies[0]):
            @pl.when(there)
            def _():
                copy.wait_send()

            if n > 1:
                @pl.when(here)
                def _():
                    copy.wait_recv()

        for there, again in copies[1]:
            @pl.when(there)
            def _():
                again.wait_send()


    def roll_e(x):
        return jnp.concatenate([pltpu.roll(x[:, 0:LANES], LAST, 1), pltpu.roll(x[:, LANES:PADDED], LAST, 1)], axis=1)

    def roll_w(x):
        return jnp.concatenate([pltpu.roll(x[:, 0:LANES], 1, 1), pltpu.roll(x[:, LANES:PADDED], 1, 1)], axis=1)

    def from_north(x, edge):
        low, high = pltpu.roll(x[0:8], 7, 0), pltpu.roll(x[8:16], 7, 0)
        return jnp.concatenate([jnp.where(sub2 == 7, high, low), jnp.where(sub2 == 7, edge, high)], axis=0)

    def from_south(x, edge):
        low, high = pltpu.roll(x[0:8], 1, 0), pltpu.roll(x[8:16], 1, 0)
        return jnp.concatenate([jnp.where(sub2 == 0, edge, low), jnp.where(sub2 == 0, low, high)], axis=0)

    def wait_columns(i):
        west_copy(i).wait_recv()
        east_copy(i).wait_recv()

    def insert_columns(i):
        columns = [jnp.where(lane < 62, col_e[i, g], col_w[i, g]) for g in PAIR]

        def level(j, _):
            k = i * size + j
            for f in QUAD:
                for m in PAIR:
                    place = size * (2 * (f % 2) + m) + j
                    turned = pltpu.roll(columns[f // 2], lax.rem(LANES + 64 - place, LANES), 1)
                    pltpu.store(first[f].at[block(k, m)], turned, mask=lane == LAST)
                    pltpu.store(second[f].at[block(k, m)], turned, mask=lane == 64)
            return 0

        lax.fori_loop(0, size, level, 0, unroll=UNROLL)

    edge_lane = lax.broadcasted_iota(jnp.int32, rows_n.shape[2:], 1)

    def unpack_rows(i):
        for rows, tails in ((rows_n, tail_n), (rows_s, tail_s)):
            for f in QUAD:
                packed = rows[i, 4 + f // 2]
                tails[i, f] = jnp.where(edge_lane < 64, packed if f % 2 == 0 else pltpu.roll(packed, 64, 1), rows[i, f])
        for h, (u, v, t, s) in enumerate(((rows_n.at[i, 0], rows_s.at[i, 1], rows_n.at[i, 2], rows_n.at[i, 3]), (tail_n.at[i, 0], tail_s.at[i, 1], tail_n.at[i, 2], tail_n.at[i, 3]))):
            u, v = u[...], v[...]
            north_w[i, h] = u + pltpu.roll(u, 1, 1)
            south_e[i, h] = v + pltpu.roll(v, LAST, 1)
            north_h[i, h] = (half_scale * HALINE_CON) * s[...] - (half_scale * THERM_EXP) * t[...]

    half_scale = HALF * PRESS_SCALE / K

    def both(tiles, k, m, f):
        return jnp.concatenate([tiles[0][f][block(k, m), :], tiles[1][f][block(k, m), :]], axis=1)

    def edge(rows, tails, f, i, at):
        return jnp.concatenate([rows[i, f, at, :], tails[i, f, at, :]], axis=1)

    mark("column_wait")
    wait_columns(0)

    @pl.when(has_n)
    def _():
        kmt_copy.wait_recv()

    @pl.when(has_s)
    def _():
        kmt_copy.wait_send()

    mark("masks")
    kmt2 = overlapped(kmt)
    kmt_edge = jnp.where(lane == 64, pltpu.roll(col_e[0, 0], 65, 1), kmt2[:, LANES:PADDED])
    kmt_row = padded(kmt_n[...]).astype(F32)
    kmt_north = jnp.concatenate([kmt_row[:, 0:LANES], jnp.where(lane1 < 64, kmt_row[:, LANES:PADDED], kmt_row[:, 0:LANES])], axis=1)
    mu = jnp.minimum(kmt2, roll_e(jnp.concatenate([kmt2[:, 0:LANES], kmt_edge], axis=1)))
    mv = jnp.minimum(kmt2, from_north(kmt2, kmt_north))
    faces[0] = linear(mu)
    faces[1] = linear(mv)

    def solve_factor(depth, k, first):
        inner, last = table[first * K + k], table[(first + 1) * K + k]
        kf = k.astype(F32)
        return jnp.where(depth > kf + 1.0, inner, jnp.where(depth > kf, last, ZERO))

    def momentum(i):
        def level(j, members):
            k = i * size + j
            kf = k.astype(F32)
            factor_u, factor_v = solve_factor(mu, k, 0), solve_factor(mv, k, 0)
            out = []
            for m in PAIR:
                total, total_n, gu_sum, gv_sum, side_u, side_v = members[m]
                at = pl.ds(2 * j + m, 1)
                u, v, t, s = (both((first, second), k, m, f) for f in QUAD)
                step = (half_scale * HALINE_CON) * s - (half_scale * THERM_EXP) * t
                pressure = total + step
                step_n = jnp.concatenate([north_h[i, 0, at, :], north_h[i, 1, at, :]], axis=1)
                pressure_n = total_n + step_n
                corner_n = pltpu.roll(corner_nw[i], 65 - (size * m + j), 1)[0:1]
                corner_s = pltpu.roll(corner_se[i], lax.rem(LANES + 63 - (size * (2 + m) + j), LANES), 1)[7:8]
                u_edge, v_edge = edge(rows_n, tail_n, 0, i, at), edge(rows_s, tail_s, 1, i, at)
                u_pair_n = jnp.concatenate([jnp.where(lane1 == 0, u_edge[:, 0:LANES] + corner_n, north_w[i, 0, at, :]), north_w[i, 1, at, :]], axis=1)
                v_pair_s = jnp.concatenate([south_e[i, 0, at, :], jnp.where(lane1 == 63, v_edge[:, LANES:PADDED] + corner_s, south_e[i, 1, at, :])], axis=1)
                v_e, v_w, u_e, u_w = roll_e(v), roll_w(v), roll_e(u), roll_w(u)
                v_pair, u_pair = v + v_e, u + u_w
                vu = 0.125 * (v_pair + from_south(v_pair, v_pair_s))
                uv = 0.125 * (u_pair + from_north(u_pair, u_pair_n))
                u_n, u_s = from_north(u, u_edge), from_south(u, edge(rows_s, tail_s, 0, i, at))
                v_n, v_s = from_north(v, edge(rows_n, tail_n, 1, i, at)), from_south(v, v_edge)
                p_n = from_north(pressure, pressure_n)
                gu = pressure - roll_e(pressure) - HALF * u * (u_e - u_w) - vu * (u_n - u_s)
                gv = pressure - p_n - uv * (v_e - v_w) - HALF * v * (v_n - v_s)
                gu = jnp.where(mu > kf, gu, ZERO)
                gv = jnp.where(mv > kf, gv, ZERO)
                side_u = (u + gu + VISC_NUMBER * side_u) * factor_u
                side_v = (v + gv + VISC_NUMBER * side_v) * factor_v
                pu[k, m] = linear(side_u)[:, KEEP]
                pv[k, m] = linear(side_v)[:, KEEP]
                out.append((pressure + step, pressure_n + step_n, gu_sum + gu, gv_sum + gv, side_u, side_v))
            return tuple(out)

        return level

    zero = jnp.zeros((ROWS, PADDED), F32)
    zero_row = jnp.zeros((1, PADDED), F32)
    members = ((zero, zero_row, zero, zero, zero, zero),) * 2
    for i in range(chunks):
        if i > 0:
            wait_columns(i)
        mark("insert")
        insert_columns(i)

        mark("row_wait")
        @pl.when(has_n)
        def _():
            south_copy(i).wait_recv()
            corner_u(i).wait_recv()

        @pl.when(has_s)
        def _():
            north_copy(i).wait_recv()
            corner_v(i).wait_recv()

        mark("momentum")
        unpack_rows(i)
        members = lax.fori_loop(0, size, momentum(i), members, unroll=UNROLL)

        mark("next")
        if i == 0:
            for copy in edge_copies:
                copy.wait()
            for p in range(7):
                wide[p, own, :] = with_edges(wide[p, own, :], edge_e[p], edge_w[p])
            static_copies = spread(wide, 0)
            start_spread(static_copies)

    mark("force")
    relay_spread(static_copies)
    count_u = linear(jnp.maximum(mu, 1.0))
    count_v = linear(jnp.maximum(mv, 1.0))
    for m in PAIR:
        wide_f[m, own, :] = linear(members[m][2]) / count_u
        wide_f[2 + m, own, :] = linear(members[m][3]) / count_v
    force_edges = edge_pair(wide_f, fedge_w, fedge_e, 3)
    for copy in force_edges:
        copy.start()

    def tracers(i, carry):
        def level(j, carry):
            k = i * size + j
            factor = solve_factor(kmt2, k, 3)
            out = []
            for m in PAIR:
                at = pl.ds(2 * j + m, 1)
                u, v = (HALF * both((first, second), k, m, f) for f in PAIR)
                u_w = roll_w(u)
                v_edge = HALF * edge(rows_s, tail_s, 1, i, at)
                for f, dest in ((2, pt), (3, ps)):
                    t = both((first, second), k, m, f)
                    flux_x = u * (t + roll_e(t)) - u_w * (t + roll_w(t))
                    flux_y = v * (t + from_north(t, edge(rows_n, tail_n, f, i, at)))
                    flux_s = v_edge * (edge(rows_s, tail_s, f, i, at) + t[0:1])
                    moved = t - (flux_x + flux_y - from_south(flux_y, flux_s))
                    side = (moved + DIFF_NUMBER * carry[len(out)]) * factor
                    dest[k, m] = linear(side)[:, KEEP]
                    out.append(side)
            return tuple(out)

        return lax.fori_loop(0, size, level, carry, unroll=UNROLL)

    mark("tracer_1")
    tail = (zero,) * 4
    split = (3 * chunks + 4) // 5
    tail = lax.fori_loop(0, split, tracers, tail)

    mark("force_edge_wait")
    for copy in force_edges:
        copy.wait()
    mark("force_spread")
    for p in QUAD:
        wide_f[p, own, :] = with_edges(wide_f[p, own, :], fedge_e[p], fedge_w[p])
    force_copies = spread(wide_f, 6)
    start_spread(force_copies)

    mark("tracer_2")
    tail = lax.fori_loop(split, chunks, tracers, tail)

    def back_tracers(j, carry):
        k = K - 2 - j
        ratio = table[5 * K + k]
        out = []
        for m in PAIR:
            for dest in (pt, ps):
                x = dest[k, m] + ratio * carry[len(out)]
                dest[k, m] = x
                out.append(x)
        return tuple(out)

    relay_spread(force_copies)
    mark("back_tracers")
    lax.fori_loop(0, K - 1, back_tracers, tuple(linear(x)[:, KEEP] for x in tail), unroll=2)

    def back(j, carry):
        k = K - 2 - j
        ratio = table[2 * K + k]
        out = []
        for m in PAIR:
            xu, xv, su, sv = carry[m]
            xu = pu[k, m] + ratio * xu
            xv = pv[k, m] + ratio * xv
            pu[k, m] = xu
            pv[k, m] = xv
            out.append((xu, xv, su + xu, sv + xv))
        return tuple(out)

    mark("back_uv")
    start = tuple(tuple(linear(members[m][n])[:, KEEP] for n in (4, 5, 4, 5)) for m in PAIR)
    ends = lax.fori_loop(0, K - 1, back, start)

    mark("static_wait")
    finish_spread(static_copies)
    mark("force_wait")
    finish_spread(force_copies)

    mark("coef")
    depth = wide[0]
    depth_e = pltpu.roll(depth, PADDED - 1, 1)
    depth_n = pltpu.roll(depth, 79, 0)
    hu = jnp.where((depth > ZERO) & (depth_e > ZERO), HALF * (depth + depth_e), ZERO)
    hv = jnp.where((depth > ZERO) & (depth_n > ZERO), HALF * (depth + depth_n), ZERO)
    coef[0] = WAVE_COURANT * WAVE_COURANT * hu
    coef[1] = WAVE_COURANT * WAVE_COURANT * hv
    for m in PAIR:
        force[m] = hu * wide_f[m] * (WAVE_COURANT / SUBCYCLES)
        force[2 + m] = hv * wide_f[2 + m] * (WAVE_COURANT / SUBCYCLES)
        state[m] = wide[1 + m]
        state[2 + m] = WAVE_COURANT * wide[3 + m]
        state[4 + m] = WAVE_COURANT * wide[5 + m]
        state[6 + m] = pltpu.roll(wide[1 + m], PADDED - 1, 1)
    mine = slice(HALO, HALO + ROWS)
    for p, (h, count) in enumerate(((hu[mine], count_u), (hv[mine], count_v))):
        faces[2 + p] = 1.0 / (WAVE_COURANT * jnp.where(h > ZERO, h, 1.0))
        for m in PAIR:
            mean[2 * p + m] = padded(ends[m][2 + p]) / count

    mark("send_wait")
    for i in range(chunks):
        west_copy(i).wait_send()
        east_copy(i).wait_send()

    @pl.when(has_s)
    def _():
        for i in range(chunks):
            south_copy(i).wait_send()
            corner_u(i).wait_send()

    @pl.when(has_n)
    def _():
        for i in range(chunks):
            north_copy(i).wait_send()
            corner_v(i).wait_send()
    mark("")


def finish_kernel(
    K, size,
    weights, pu, pv, pt, ps, mean, faces, coef, force, first_state,
    eta_o, tx_o, ty_o, u_o, v_o, t_o, s_o,
    state, avg, out_u, out_v, sems,
):
    chunks = K // size
    through = [pltpu.make_async_copy(src, dst, sems.at[i, 0]) for i, (src, dst) in enumerate(((pt, t_o), (ps, s_o)))]
    for copy in through:
        copy.start()
    state[...] = first_state[...]
    avg[...] = jnp.zeros_like(avg)

    def subcycles(first, last, margin):
        height = ROWS + 2 * margin
        rows = pl.ds(HALO - margin, height)
        mine = slice(margin, margin + ROWS)

        def to_e(x):
            return pltpu.roll(x, PADDED - 1, 1)

        def subcycle(n, _):
            weight = weights[n]
            for m in PAIR:
                tx, ty = state[2 + m, rows], state[4 + m, rows]
                tx_e, ty_e = to_e(tx), to_e(ty)
                eta = state[m, rows] - (tx - pltpu.roll(tx, 1, 1) + ty - pltpu.roll(ty, 1, 0))
                eta_e = state[6 + m, rows] - (tx_e - tx + ty_e - pltpu.roll(ty_e, 1, 0))
                tx = tx + force[m, rows] - coef[0, rows] * (eta_e - eta)
                ty = ty + force[2 + m, rows] - coef[1, rows] * (pltpu.roll(eta, height - 1, 0) - eta)
                for p, x in enumerate((eta, tx, ty)):
                    state[2 * p + m, rows] = x
                    avg[2 * p + m] = avg[2 * p + m] + weight * x[mine]
                state[6 + m, rows] = eta_e
            return 0

        lax.fori_loop(first, last, subcycle, 0)

    done = 0
    for margin in (32, 24, 16, 8):
        last = SUBCYCLES - (margin - 8)
        subcycles(done, last, margin)
        done = last

    corr = []
    for m in PAIR:
        eta_o[m] = avg[m][:, KEEP]
        for p, dest in enumerate((tx_o, ty_o)):
            transport = avg[2 + 2 * p + m]
            dest[m] = (transport * (1.0 / WAVE_COURANT))[:, KEEP]
            corr.append((transport * faces[2 + p] - mean[2 * p + m])[:, KEEP])
    depth_u, depth_v = faces[0][:, KEEP], faces[1][:, KEEP]

    def out_copies(i):
        levels = pl.ds(i * size, size)
        return [pltpu.make_async_copy(src.at[levels], dst.at[levels], sems.at[p, 1 + i]) for p, (src, dst) in enumerate(((out_u, u_o), (out_v, v_o)))]

    for i in range(chunks):
        def level(j, _):
            k = i * size + j
            kf = k.astype(F32)
            for m in PAIR:
                out_u[k, m] = jnp.where(depth_u > kf, pu[k, m] + corr[2 * m], ZERO)
                out_v[k, m] = jnp.where(depth_v > kf, pv[k, m] + corr[2 * m + 1], ZERO)
            return 0

        lax.fori_loop(0, size, level, 0, unroll=3 if size % 3 == 0 else 1)
        for copy in out_copies(i):
            copy.start()

    for copy in through + [copy for i in range(chunks) for copy in out_copies(i)]:
        copy.wait()


def solution(mesh):
    col_count, row_count = mesh.shape["col"], mesh.shape["row"]

    def local_step(vel_x, vel_y, pot_temp, salinity, surf_eta, trans_x, trans_y, col_depth, wet_levels, avg_weights):
        K = vel_x.shape[0]
        size = level_chunk(K)
        chunks = K // size
        edge_rows = (2 * size + 7) // 8 * 8
        table = jnp.asarray(solve_tables(K))
        smem = pl.BlockSpec(memory_space=pltpu.SMEM)
        vmem = pl.BlockSpec(memory_space=pltpu.VMEM)
        hbm = pl.BlockSpec(memory_space=pl.ANY)
        full = jax.ShapeDtypeStruct((K, 2, ROWS, WIDTH), F32)
        held = pltpu.VMEM((K, 2, ROWS, WIDTH), F32)
        dma = pltpu.SemaphoreType.DMA
        outs = pl.pallas_call(
            functools.partial(step_kernel, row_count, col_count, K),
            out_shape=(held,) * 4 + tuple(pltpu.VMEM((n, ROWS, PADDED), F32) for n in (4, 4)) + tuple(pltpu.VMEM((n, 80, PADDED), F32) for n in (2, 4, 8)),
            in_specs=[smem] + [vmem] * 5 + [hbm] * 4,
            out_specs=(vmem,) * 9,
            scratch_shapes=[
                *[pltpu.VMEM((K * 2 * ROWS, WIDTH), F32)] * 4,
                *[pltpu.VMEM((K * 2 * ROWS, LANES), F32)] * 8,
                *[pltpu.VMEM((chunks, 6, edge_rows, LANES), F32)] * 4,
                *[pltpu.VMEM((chunks, 4, edge_rows, LANES), F32)] * 2,
                *[pltpu.VMEM((chunks, 2, edge_rows, LANES), F32)] * 3,
                pltpu.VMEM((1, WIDTH), jnp.int32),
                *[pltpu.VMEM((chunks, 2, ROWS, LANES), F32)] * 3,
                *[pltpu.VMEM((chunks, 8, LANES), F32)] * 2,
                *[pltpu.VMEM((7, ROWS, LANES), F32)] * 2,
                pltpu.VMEM((7, 80, PADDED), F32),
                *[pltpu.VMEM((4, ROWS, LANES), F32)] * 2,
                pltpu.VMEM((4, 80, PADDED), F32),
                dma((chunks, 4)), dma((2, chunks)), dma((2, chunks)), dma((4, chunks)), dma((4, chunks)), dma((5,)), dma((5,)), dma((12,)), dma((12,)),
            ],
            compiler_params=pltpu.CompilerParams(collective_id=0, has_side_effects=True, vmem_limit_bytes=52 << 20),
            name="ocean_step",
        )(table, wet_levels, col_depth, surf_eta, trans_x, trans_y, *(x.reshape(-1, WIDTH) for x in (vel_x, vel_y, pot_temp, salinity)))

        small = jax.ShapeDtypeStruct((2, ROWS, WIDTH), F32)
        return pl.pallas_call(
            functools.partial(finish_kernel, K, size),
            out_shape=(small,) * 3 + (full,) * 4,
            in_specs=[smem] + [vmem] * 9,
            out_specs=(vmem,) * 3 + (hbm,) * 4,
            scratch_shapes=[
                pltpu.VMEM((8, 80, PADDED), F32),
                pltpu.VMEM((6, ROWS, PADDED), F32),
                *[pltpu.VMEM((K, 2, ROWS, WIDTH), F32)] * 2,
                dma((2, 1 + chunks)),
            ],
            compiler_params=pltpu.CompilerParams(vmem_limit_bytes=20 << 20),
            name="ocean_finish",
        )(avg_weights, *outs)

    spec_3d = P(None, None, "row", "col")
    spec_2d = P(None, "row", "col")
    spec_map = P("row", "col")
    return jax.shard_map(local_step, mesh=mesh, in_specs=(spec_3d,) * 4 + (spec_2d,) * 3 + (spec_map,) * 2 + (P(),), out_specs=(spec_2d,) * 3 + (spec_3d,) * 4, check_vma=False)
```

```python
import functools
import numpy as np
import jax
import jax.numpy as jnp
from jax import lax
from jax.experimental import pallas as pl
from jax.experimental.pallas import tpu as pltpu
from jax.sharding import PartitionSpec as P

WAVE_COURANT = 0.4
THERM_EXP = 0.2
HALINE_CON = 0.15
PRESS_SCALE = 0.5
VISC_NUMBER = 1.0
DIFF_NUMBER = 0.5
SUBCYCLES = 30
HALO = 32
PAIR = (0, 1)
QUAD = (0, 1, 2, 3)
ZERO, HALF = 0.0, 0.5
UNROLL = 5
ROWS, WIDTH, PADDED, LANES = 16, 192, 256, 128
LAST, KEEP = LANES - 1, slice(0, WIDTH)
MESH = pl.DeviceIdType.MESH
F32 = jnp.float32


def solve_tables(level_count):
    rows = []
    for strength in (VISC_NUMBER, DIFF_NUMBER):
        inner, last = np.zeros(level_count), np.zeros(level_count)
        inner[0], last[0] = 1.0 + strength, 1.0
        for k in range(1, level_count):
            inner[k] = 1.0 + 2.0 * strength - strength * strength / inner[k - 1]
            last[k] = 1.0 + strength - strength * strength / inner[k - 1]
        rows += [1.0 / inner, 1.0 / last, strength / inner]
    return np.concatenate(rows).astype(np.float32)


def level_chunk(level_count):
    return next(size for size in (15, 5, 4) if level_count % size == 0)


def step_kernel(
    row_count, col_count, level_count,
    table, kmt_in, depth_in, eta_in, tx_in, ty_in, u_hbm, v_hbm, t_hbm, s_hbm,
    pu, pv, pt, ps, mean, faces, coef, force, state,
    raw_u, raw_v, raw_t, raw_s, ua, va, ta, sa, ub, vb, tb, sb, rows_n, rows_s, send_n, send_s, tail_n, tail_s, north_w, south_e, north_h, kmt_n, pack, col_e, col_w, corner_se, corner_nw,
    edge_e, edge_w, wide, fedge_e, fedge_w, wide_f,
    load_sem, row_send, row_recv, col_send, col_recv, misc_send, misc_recv, wide_send, wide_recv,
):
    K = level_count
    open_scope = []

    def mark(name):
        if open_scope:
            open_scope.pop().__exit__(None, None, None)
        if name:
            open_scope.append(jax.named_scope(name))
            open_scope[-1].__enter__()

    size = level_chunk(K)
    chunks = K // size
    r = lax.axis_index("row")
    c = lax.axis_index("col")
    east = lax.rem(c + 1, col_count)
    west = lax.rem(c + col_count - 1, col_count)
    has_n, has_s = r < row_count - 1, r > 0
    has_nn, has_ss = r < row_count - 2, r > 1
    raw, first, second = (raw_u, raw_v, raw_t, raw_s), (ua, va, ta, sa), (ub, vb, tb, sb)

    def one(flag):
        return flag.astype(jnp.int32)

    mark("init")
    def block(k, m):
        return pl.ds(pl.multiple_of((2 * k + m) * ROWS, ROWS), ROWS)

    loads = []
    for i in range(chunks):
        levels = pl.ds(i * size * 2 * ROWS, size * 2 * ROWS)
        group = []
        for f, src in enumerate((u_hbm, v_hbm, t_hbm, s_hbm)):
            group.append(pltpu.make_async_copy(src.at[levels], raw[f].at[levels], load_sem.at[i, f]))
        loads.append(group)
    for group in loads:
        for copy in group:
            copy.start()

    wide[...] = jnp.zeros_like(wide)
    wide_f[...] = jnp.zeros_like(wide_f)

    @pl.when(jnp.logical_not(has_n))
    def _():
        rows_n[...] = jnp.zeros_like(rows_n)
        kmt_n[...] = jnp.zeros_like(kmt_n)
        corner_nw[...] = jnp.zeros_like(corner_nw)

    @pl.when(jnp.logical_not(has_s))
    def _():
        rows_s[...] = jnp.zeros_like(rows_s)
        corner_se[...] = jnp.zeros_like(corner_se)

    barrier = pltpu.get_barrier_semaphore()

    def signal(**where):
        pl.semaphore_signal(barrier, inc=1, device_id=where, device_id_type=MESH)

    signal(col=east)
    signal(col=west)

    @pl.when(has_n)
    def _():
        signal(row=r + 1)
        signal(row=r + 1, col=west)

    @pl.when(has_s)
    def _():
        signal(row=r - 1)
        signal(row=r - 1, col=east)

    @pl.when(has_nn)
    def _():
        signal(row=r + 2)

    @pl.when(has_ss)
    def _():
        signal(row=r - 2)

    def remote(src, dst, ssem, rsem, **where):
        return pltpu.make_async_remote_copy(src_ref=src, dst_ref=dst, send_sem=ssem, recv_sem=rsem, device_id=where, device_id_type=MESH)

    lane = lax.broadcasted_iota(jnp.int32, (ROWS, LANES), 1)
    lane8, lane1 = lane[0:8], lane[0:1]
    sub = lax.broadcasted_iota(jnp.int32, (8, LANES), 0)
    sub2 = lax.broadcasted_iota(jnp.int32, (8, PADDED), 0)

    def padded(x):
        return jnp.concatenate([x, jnp.zeros((x.shape[0], PADDED - WIDTH), x.dtype)], axis=1)

    def overlapped(x):
        a, b = x[:, 0:LANES], x[:, LANES:PADDED]
        return jnp.concatenate([a, jnp.where(lane < 64, b, a)], axis=1)

    def linear(x):
        a, b = x[:, 0:LANES], x[:, LANES:PADDED]
        return jnp.concatenate([jnp.where(lane < 96, a, b), b], axis=1)

    kmt = padded(kmt_in[...]).astype(F32)
    own = pl.ds(HALO, ROWS)
    wide[0, own, :] = jnp.where(kmt > 0.5, padded(depth_in[...]), ZERO)
    for m in PAIR:
        wide[1 + m, own, :] = padded(eta_in[m])
        wide[3 + m, own, :] = padded(tx_in[m])
        wide[5 + m, own, :] = padded(ty_in[m])

    kmt_copy = remote(kmt_in.at[0:1, :], kmt_n, misc_send.at[0], misc_recv.at[0], row=r - 1)

    def south_copy(i):
        return remote(send_s.at[i], rows_n.at[i], row_send.at[0, i], row_recv.at[0, i], row=r - 1)

    def north_copy(i):
        return remote(send_n.at[i], rows_s.at[i], row_send.at[1, i], row_recv.at[1, i], row=r + 1)

    def west_copy(i):
        return remote(pack.at[i], col_e.at[i], col_send.at[0, i], col_recv.at[0, i], col=west)

    def east_copy(i):
        return remote(pack.at[i], col_w.at[i], col_send.at[1, i], col_recv.at[1, i], col=east)

    def corner_v(i):
        return remote(pack.at[i, 0, 8:16, :], corner_se.at[i], col_send.at[2, i], col_recv.at[2, i], row=r + 1, col=west)

    def corner_u(i):
        return remote(pack.at[i, 0, 0:8, :], corner_nw.at[i], col_send.at[3, i], col_recv.at[3, i], row=r - 1, col=east)

    groups = [*range(0, size - 3, 4)] + [size - 4] * (size % 4 > 0)

    def pack_chunk(i):
        for copy in loads[i]:
            copy.wait()

        def collect(j, acc):
            out = []
            here = (lane == j) | (lane == j + 63)
            for f in QUAD:
                for m in PAIR:
                    at = block(i * size + j, m)
                    x = raw[f][at, 0:LANES]
                    first[f][at, :] = x
                    y = jnp.where(lane < 64, padded(raw[f][at, LANES:WIDTH]), x)
                    second[f][at, :] = y
                    out.append(jnp.where(here, pltpu.roll(jnp.where(lane == 0, x, y), j, 1), acc[len(out)]))
            return tuple(out)

        acc = lax.fori_loop(0, size, collect, (jnp.zeros((ROWS, LANES), F32),) * 8, unroll=UNROLL)
        for g in PAIR:
            merged = pltpu.roll(kmt[:, 0:LANES], LAST, 1)
            for n in QUAD:
                low = size * n
                here = (lane >= low) & (lane < low + size) | (lane >= low + 63) & (lane < low + 63 + size)
                merged = jnp.where(here, pltpu.roll(acc[4 * g + n], low, 1), merged)
            pack[i, g] = merged
        for row, dest in ((0, send_s), (15, send_n)):
            for j in groups:
                at, spot = pl.ds((i * size + j) * 2 * ROWS + row, 8, stride=ROWS), pl.ds(2 * j, 8)
                tails = []
                for f in QUAD:
                    dest[i, f, spot, :] = first[f][at, :]
                    tails.append(second[f][at, :])
                for p in PAIR:
                    dest[i, 4 + p, spot, :] = jnp.where(lane8 < 64, tails[2 * p], pltpu.roll(tails[2 * p + 1], 64, 1))

    def start_chunk(i):
        west_copy(i).start()
        east_copy(i).start()

        @pl.when(has_s)
        def _():
            corner_u(i).start()
            south_copy(i).start()

        @pl.when(has_n)
        def _():
            corner_v(i).start()
            north_copy(i).start()

    mark("pack_early")
    def edge_pair(buf, to_east, to_west, sem):
        return [
            remote(buf.at[:, own, 0:LANES], to_west, misc_send.at[sem], misc_recv.at[sem], col=west),
            remote(buf.at[:, own, LANES:PADDED], to_east, misc_send.at[sem + 1], misc_recv.at[sem + 1], col=east),
        ]

    edge_copies = edge_pair(wide, edge_w, edge_e, 1)
    early = 1
    for i in range(early):
        pack_chunk(i)
    mark("barrier_wait")
    pl.semaphore_wait(barrier, 2 + 2 * one(has_n) + 2 * one(has_s) + one(has_nn) + one(has_ss))

    @pl.when(has_s)
    def _():
        kmt_copy.start()

    for i in range(early):
        start_chunk(i)
    for copy in edge_copies:
        copy.start()
    mark("pack_late")
    for i in range(early, chunks):
        pack_chunk(i)
        start_chunk(i)

    def with_edges(x, from_east, from_west):
        b = jnp.where(lane < 64, x[:, LANES:PADDED], jnp.where(lane < 96, pltpu.roll(from_east, 64, 1), pltpu.roll(from_west, 64, 1)))
        return jnp.concatenate([x[:, 0:LANES], b], axis=1)

    def spread(buf, sem):
        even = lax.rem(r, 2) == 0
        odd = jnp.logical_not(even)

        def part(at, to, out, to_sem, row):
            return remote(buf.at[:, pl.ds(at, ROWS), :], buf.at[:, pl.ds(to, ROWS), :], wide_send.at[sem + out], wide_recv.at[sem + to_sem], row=row)

        direct = (
            (has_n, has_s, part(HALO, 16, 0, 0, r + 1)),
            (has_s, has_n, part(HALO, 48, 1, 1, r - 1)),
            (has_nn & even, has_ss, part(HALO, 0, 2, 2, r + 2)),
            (has_ss & odd, has_nn, part(HALO, 64, 3, 3, r - 2)),
        )
        relayed = ((has_s & even, part(16, 0, 4, 2, r + 1)), (has_n & odd, part(48, 64, 5, 3, r - 1)))
        return direct, relayed

    def start_spread(copies):
        for there, _, copy in copies[0]:
            @pl.when(there)
            def _():
                copy.start()

    def relay_spread(copies):
        for (_, here, copy), (there, again) in zip(copies[0], copies[1]):
            @pl.when(here)
            def _():
                copy.wait_recv()

            @pl.when(there)
            def _():
                again.start()

    def finish_spread(copies):
        for n, (there, here, copy) in enumerate(copies[0]):
            @pl.when(there)
            def _():
                copy.wait_send()

            if n > 1:
                @pl.when(here)
                def _():
                    copy.wait_recv()

        for there, again in copies[1]:
            @pl.when(there)
            def _():
                again.wait_send()


    def roll_e(x):
        return jnp.concatenate([pltpu.roll(x[:, 0:LANES], LAST, 1), pltpu.roll(x[:, LANES:PADDED], LAST, 1)], axis=1)

    def roll_w(x):
        return jnp.concatenate([pltpu.roll(x[:, 0:LANES], 1, 1), pltpu.roll(x[:, LANES:PADDED], 1, 1)], axis=1)

    def from_north(x, edge):
        low, high = pltpu.roll(x[0:8], 7, 0), pltpu.roll(x[8:16], 7, 0)
        return jnp.concatenate([jnp.where(sub2 == 7, high, low), jnp.where(sub2 == 7, edge, high)], axis=0)

    def from_south(x, edge):
        low, high = pltpu.roll(x[0:8], 1, 0), pltpu.roll(x[8:16], 1, 0)
        return jnp.concatenate([jnp.where(sub2 == 0, edge, low), jnp.where(sub2 == 0, low, high)], axis=0)

    def wait_columns(i):
        west_copy(i).wait_recv()
        east_copy(i).wait_recv()

    def insert_columns(i):
        columns = [jnp.where(lane < 62, col_e[i, g], col_w[i, g]) for g in PAIR]

        def level(j, _):
            k = i * size + j
            for f in QUAD:
                for m in PAIR:
                    place = size * (2 * (f % 2) + m) + j
                    turned = pltpu.roll(columns[f // 2], lax.rem(LANES + 64 - place, LANES), 1)
                    pltpu.store(first[f].at[block(k, m)], turned, mask=lane == LAST)
                    pltpu.store(second[f].at[block(k, m)], turned, mask=lane == 64)
            return 0

        lax.fori_loop(0, size, level, 0, unroll=UNROLL)

    edge_lane = lax.broadcasted_iota(jnp.int32, rows_n.shape[2:], 1)

    def unpack_rows(i):
        for rows, tails in ((rows_n, tail_n), (rows_s, tail_s)):
            for f in QUAD:
                packed = rows[i, 4 + f // 2]
                tails[i, f] = jnp.where(edge_lane < 64, packed if f % 2 == 0 else pltpu.roll(packed, 64, 1), rows[i, f])
        for h, (u, v, t, s) in enumerate(((rows_n.at[i, 0], rows_s.at[i, 1], rows_n.at[i, 2], rows_n.at[i, 3]), (tail_n.at[i, 0], tail_s.at[i, 1], tail_n.at[i, 2], tail_n.at[i, 3]))):
            u, v = u[...], v[...]
            north_w[i, h] = u + pltpu.roll(u, 1, 1)
            south_e[i, h] = v + pltpu.roll(v, LAST, 1)
            north_h[i, h] = (half_scale * HALINE_CON) * s[...] - (half_scale * THERM_EXP) * t[...]

    half_scale = HALF * PRESS_SCALE / K

    def both(tiles, k, m, f):
        return jnp.concatenate([tiles[0][f][block(k, m), :], tiles[1][f][block(k, m), :]], axis=1)

    def edge(rows, tails, f, i, at):
        return jnp.concatenate([rows[i, f, at, :], tails[i, f, at, :]], axis=1)

    mark("column_wait")
    wait_columns(0)

    @pl.when(has_n)
    def _():
        kmt_copy.wait_recv()

    @pl.when(has_s)
    def _():
        kmt_copy.wait_send()

    mark("masks")
    kmt2 = overlapped(kmt)
    kmt_edge = jnp.where(lane == 64, pltpu.roll(col_e[0, 0], 65, 1), kmt2[:, LANES:PADDED])
    kmt_row = padded(kmt_n[...]).astype(F32)
    kmt_north = jnp.concatenate([kmt_row[:, 0:LANES], jnp.where(lane1 < 64, kmt_row[:, LANES:PADDED], kmt_row[:, 0:LANES])], axis=1)
    mu = jnp.minimum(kmt2, roll_e(jnp.concatenate([kmt2[:, 0:LANES], kmt_edge], axis=1)))
    mv = jnp.minimum(kmt2, from_north(kmt2, kmt_north))
    faces[0] = linear(mu)
    faces[1] = linear(mv)

    def solve_factor(depth, k, first):
        inner, last = table[first * K + k], table[(first + 1) * K + k]
        kf = k.astype(F32)
        return jnp.where(depth > kf + 1.0, inner, jnp.where(depth > kf, last, ZERO))

    def momentum(i):
        def level(j, members):
            k = i * size + j
            kf = k.astype(F32)
            out = []
            for m in PAIR:
                total, total_n, gu_sum, gv_sum = members[m]
                at = pl.ds(2 * j + m, 1)
                u, v, t, s = (both((first, second), k, m, f) for f in QUAD)
                step = (half_scale * HALINE_CON) * s - (half_scale * THERM_EXP) * t
                pressure = total + step
                step_n = jnp.concatenate([north_h[i, 0, at, :], north_h[i, 1, at, :]], axis=1)
                pressure_n = total_n + step_n
                corner_n = pltpu.roll(corner_nw[i], 65 - (size * m + j), 1)[0:1]
                corner_s = pltpu.roll(corner_se[i], lax.rem(LANES + 63 - (size * (2 + m) + j), LANES), 1)[7:8]
                u_edge, v_edge = edge(rows_n, tail_n, 0, i, at), edge(rows_s, tail_s, 1, i, at)
                u_pair_n = jnp.concatenate([jnp.where(lane1 == 0, u_edge[:, 0:LANES] + corner_n, north_w[i, 0, at, :]), north_w[i, 1, at, :]], axis=1)
                v_pair_s = jnp.concatenate([south_e[i, 0, at, :], jnp.where(lane1 == 63, v_edge[:, LANES:PADDED] + corner_s, south_e[i, 1, at, :])], axis=1)
                v_e, v_w, u_e, u_w = roll_e(v), roll_w(v), roll_e(u), roll_w(u)
                v_pair, u_pair = v + v_e, u + u_w
                vu = 0.125 * (v_pair + from_south(v_pair, v_pair_s))
                uv = 0.125 * (u_pair + from_north(u_pair, u_pair_n))
                u_n, u_s = from_north(u, u_edge), from_south(u, edge(rows_s, tail_s, 0, i, at))
                v_n, v_s = from_north(v, edge(rows_n, tail_n, 1, i, at)), from_south(v, v_edge)
                p_n = from_north(pressure, pressure_n)
                gu = pressure - roll_e(pressure) - HALF * u * (u_e - u_w) - vu * (u_n - u_s)
                gv = pressure - p_n - uv * (v_e - v_w) - HALF * v * (v_n - v_s)
                gu = jnp.where(mu > kf, gu, ZERO)
                gv = jnp.where(mv > kf, gv, ZERO)
                pu[k, m] = linear(u + gu)[:, KEEP]
                pv[k, m] = linear(v + gv)[:, KEEP]
                out.append((pressure + step, pressure_n + step_n, gu_sum + gu, gv_sum + gv))
            return tuple(out)

        return level

    zero = jnp.zeros((ROWS, PADDED), F32)
    zero_row = jnp.zeros((1, PADDED), F32)
    members = ((zero, zero_row, zero, zero),) * 2
    for i in range(chunks):
        if i > 0:
            wait_columns(i)
        mark("insert")
        insert_columns(i)

        mark("row_wait")
        @pl.when(has_n)
        def _():
            south_copy(i).wait_recv()
            corner_u(i).wait_recv()

        @pl.when(has_s)
        def _():
            north_copy(i).wait_recv()
            corner_v(i).wait_recv()

        mark("momentum")
        unpack_rows(i)
        members = lax.fori_loop(0, size, momentum(i), members, unroll=UNROLL)

        mark("next")
        if i == 0:
            for copy in edge_copies:
                copy.wait()
            for p in range(7):
                wide[p, own, :] = with_edges(wide[p, own, :], edge_e[p], edge_w[p])
            static_copies = spread(wide, 0)
            start_spread(static_copies)

    mark("force")
    relay_spread(static_copies)
    count_u = linear(jnp.maximum(mu, 1.0))
    count_v = linear(jnp.maximum(mv, 1.0))
    for m in PAIR:
        wide_f[m, own, :] = linear(members[m][2]) / count_u
        wide_f[2 + m, own, :] = linear(members[m][3]) / count_v
    force_edges = edge_pair(wide_f, fedge_w, fedge_e, 3)
    for copy in force_edges:
        copy.start()

    def tracers(i, carry):
        def level(j, carry):
            k = i * size + j
            factor = solve_factor(kmt2, k, 3)
            out = []
            for m in PAIR:
                at = pl.ds(2 * j + m, 1)
                u, v = (HALF * both((first, second), k, m, f) for f in PAIR)
                u_w = roll_w(u)
                v_edge = HALF * edge(rows_s, tail_s, 1, i, at)
                for f, dest in ((2, pt), (3, ps)):
                    t = both((first, second), k, m, f)
                    flux_x = u * (t + roll_e(t)) - u_w * (t + roll_w(t))
                    flux_y = v * (t + from_north(t, edge(rows_n, tail_n, f, i, at)))
                    flux_s = v_edge * (edge(rows_s, tail_s, f, i, at) + t[0:1])
                    moved = t - (flux_x + flux_y - from_south(flux_y, flux_s))
                    side = (moved + DIFF_NUMBER * carry[len(out)]) * factor
                    dest[k, m] = linear(side)[:, KEEP]
                    out.append(side)
            return tuple(out)

        return lax.fori_loop(0, size, level, carry, unroll=UNROLL)

    mark("tracer_1")
    tail = (zero,) * 4
    split = (3 * chunks + 4) // 5
    tail = lax.fori_loop(0, split, tracers, tail)

    mark("forward_uv")
    depth_u, depth_v = faces[0][:, KEEP], faces[1][:, KEEP]

    def forward(k, carry):
        out = []
        for field, depth in ((pu, depth_u), (pv, depth_v)):
            factor = solve_factor(depth, k, 0)
            for m in PAIR:
                x = (field[k, m] + VISC_NUMBER * carry[len(out)]) * factor
                field[k, m] = x
                out.append(x)
        return tuple(out)

    sides = lax.fori_loop(0, K, forward, (zero[:, KEEP],) * 4, unroll=UNROLL)

    mark("force_edge_wait")
    for copy in force_edges:
        copy.wait()
    mark("force_spread")
    for p in QUAD:
        wide_f[p, own, :] = with_edges(wide_f[p, own, :], fedge_e[p], fedge_w[p])
    force_copies = spread(wide_f, 6)
    start_spread(force_copies)

    mark("tracer_2")
    tail = lax.fori_loop(split, chunks, tracers, tail)

    def back_tracers(j, carry):
        k = K - 2 - j
        ratio = table[5 * K + k]
        out = []
        for m in PAIR:
            for dest in (pt, ps):
                x = dest[k, m] + ratio * carry[len(out)]
                dest[k, m] = x
                out.append(x)
        return tuple(out)

    relay_spread(force_copies)
    mark("back_tracers")
    lax.fori_loop(0, K - 1, back_tracers, tuple(linear(x)[:, KEEP] for x in tail), unroll=2)

    def back(j, carry):
        k = K - 2 - j
        ratio = table[2 * K + k]
        out = []
        for m in PAIR:
            xu, xv, su, sv = carry[m]
            xu = pu[k, m] + ratio * xu
            xv = pv[k, m] + ratio * xv
            pu[k, m] = xu
            pv[k, m] = xv
            out.append((xu, xv, su + xu, sv + xv))
        return tuple(out)

    mark("back_uv")
    start = tuple((sides[m], sides[2 + m], sides[m], sides[2 + m]) for m in PAIR)
    ends = lax.fori_loop(0, K - 1, back, start)

    mark("static_wait")
    finish_spread(static_copies)
    mark("force_wait")
    finish_spread(force_copies)

    mark("coef")
    depth = wide[0]
    depth_e = pltpu.roll(depth, PADDED - 1, 1)
    depth_n = pltpu.roll(depth, 79, 0)
    hu = jnp.where((depth > ZERO) & (depth_e > ZERO), HALF * (depth + depth_e), ZERO)
    hv = jnp.where((depth > ZERO) & (depth_n > ZERO), HALF * (depth + depth_n), ZERO)
    coef[0] = WAVE_COURANT * WAVE_COURANT * hu
    coef[1] = WAVE_COURANT * WAVE_COURANT * hv
    for m in PAIR:
        force[m] = hu * wide_f[m] * (WAVE_COURANT / SUBCYCLES)
        force[2 + m] = hv * wide_f[2 + m] * (WAVE_COURANT / SUBCYCLES)
        state[m] = wide[1 + m]
        state[2 + m] = WAVE_COURANT * wide[3 + m]
        state[4 + m] = WAVE_COURANT * wide[5 + m]
        state[6 + m] = pltpu.roll(wide[1 + m], PADDED - 1, 1)
    mine = slice(HALO, HALO + ROWS)
    for p, (h, count) in enumerate(((hu[mine], count_u), (hv[mine], count_v))):
        faces[2 + p] = 1.0 / (WAVE_COURANT * jnp.where(h > ZERO, h, 1.0))
        for m in PAIR:
            mean[2 * p + m] = padded(ends[m][2 + p]) / count

    mark("send_wait")
    for i in range(chunks):
        west_copy(i).wait_send()
        east_copy(i).wait_send()

    @pl.when(has_s)
    def _():
        for i in range(chunks):
            south_copy(i).wait_send()
            corner_u(i).wait_send()

    @pl.when(has_n)
    def _():
        for i in range(chunks):
            north_copy(i).wait_send()
            corner_v(i).wait_send()
    mark("")


def finish_kernel(
    K, size,
    weights, pu, pv, pt, ps, mean, faces, coef, force, first_state,
    eta_o, tx_o, ty_o, u_o, v_o, t_o, s_o,
    state, avg, out_u, out_v, sems,
):
    chunks = K // size
    through = [pltpu.make_async_copy(src, dst, sems.at[i, 0]) for i, (src, dst) in enumerate(((pt, t_o), (ps, s_o)))]
    for copy in through:
        copy.start()
    state[...] = first_state[...]
    avg[...] = jnp.zeros_like(avg)

    def subcycles(first, last, margin):
        height = ROWS + 2 * margin
        rows = pl.ds(HALO - margin, height)
        mine = slice(margin, margin + ROWS)

        def to_e(x):
            return pltpu.roll(x, PADDED - 1, 1)

        def subcycle(n, _):
            weight = weights[n]
            for m in PAIR:
                tx, ty = state[2 + m, rows], state[4 + m, rows]
                tx_e, ty_e = to_e(tx), to_e(ty)
                eta = state[m, rows] - (tx - pltpu.roll(tx, 1, 1) + ty - pltpu.roll(ty, 1, 0))
                eta_e = state[6 + m, rows] - (tx_e - tx + ty_e - pltpu.roll(ty_e, 1, 0))
                tx = tx + force[m, rows] - coef[0, rows] * (eta_e - eta)
                ty = ty + force[2 + m, rows] - coef[1, rows] * (pltpu.roll(eta, height - 1, 0) - eta)
                for p, x in enumerate((eta, tx, ty)):
                    state[2 * p + m, rows] = x
                    avg[2 * p + m] = avg[2 * p + m] + weight * x[mine]
                state[6 + m, rows] = eta_e
            return 0

        lax.fori_loop(first, last, subcycle, 0)

    done = 0
    for margin in (32, 24, 16, 8):
        last = SUBCYCLES - (margin - 8)
        subcycles(done, last, margin)
        done = last

    corr = []
    for m in PAIR:
        eta_o[m] = avg[m][:, KEEP]
        for p, dest in enumerate((tx_o, ty_o)):
            transport = avg[2 + 2 * p + m]
            dest[m] = (transport * (1.0 / WAVE_COURANT))[:, KEEP]
            corr.append((transport * faces[2 + p] - mean[2 * p + m])[:, KEEP])
    depth_u, depth_v = faces[0][:, KEEP], faces[1][:, KEEP]

    def out_copies(i):
        levels = pl.ds(i * size, size)
        return [pltpu.make_async_copy(src.at[levels], dst.at[levels], sems.at[p, 1 + i]) for p, (src, dst) in enumerate(((out_u, u_o), (out_v, v_o)))]

    for i in range(chunks):
        def level(j, _):
            k = i * size + j
            kf = k.astype(F32)
            for m in PAIR:
                out_u[k, m] = jnp.where(depth_u > kf, pu[k, m] + corr[2 * m], ZERO)
                out_v[k, m] = jnp.where(depth_v > kf, pv[k, m] + corr[2 * m + 1], ZERO)
            return 0

        lax.fori_loop(0, size, level, 0, unroll=3 if size % 3 == 0 else 1)
        for copy in out_copies(i):
            copy.start()

    for copy in through + [copy for i in range(chunks) for copy in out_copies(i)]:
        copy.wait()


def solution(mesh):
    col_count, row_count = mesh.shape["col"], mesh.shape["row"]

    def local_step(vel_x, vel_y, pot_temp, salinity, surf_eta, trans_x, trans_y, col_depth, wet_levels, avg_weights):
        K = vel_x.shape[0]
        size = level_chunk(K)
        chunks = K // size
        edge_rows = (2 * size + 7) // 8 * 8
        table = jnp.asarray(solve_tables(K))
        smem = pl.BlockSpec(memory_space=pltpu.SMEM)
        vmem = pl.BlockSpec(memory_space=pltpu.VMEM)
        hbm = pl.BlockSpec(memory_space=pl.ANY)
        full = jax.ShapeDtypeStruct((K, 2, ROWS, WIDTH), F32)
        held = pltpu.VMEM((K, 2, ROWS, WIDTH), F32)
        dma = pltpu.SemaphoreType.DMA
        outs = pl.pallas_call(
            functools.partial(step_kernel, row_count, col_count, K),
            out_shape=(held,) * 4 + tuple(pltpu.VMEM((n, ROWS, PADDED), F32) for n in (4, 4)) + tuple(pltpu.VMEM((n, 80, PADDED), F32) for n in (2, 4, 8)),
            in_specs=[smem] + [vmem] * 5 + [hbm] * 4,
            out_specs=(vmem,) * 9,
            scratch_shapes=[
                *[pltpu.VMEM((K * 2 * ROWS, WIDTH), F32)] * 4,
                *[pltpu.VMEM((K * 2 * ROWS, LANES), F32)] * 8,
                *[pltpu.VMEM((chunks, 6, edge_rows, LANES), F32)] * 4,
                *[pltpu.VMEM((chunks, 4, edge_rows, LANES), F32)] * 2,
                *[pltpu.VMEM((chunks, 2, edge_rows, LANES), F32)] * 3,
                pltpu.VMEM((1, WIDTH), jnp.int32),
                *[pltpu.VMEM((chunks, 2, ROWS, LANES), F32)] * 3,
                *[pltpu.VMEM((chunks, 8, LANES), F32)] * 2,
                *[pltpu.VMEM((7, ROWS, LANES), F32)] * 2,
                pltpu.VMEM((7, 80, PADDED), F32),
                *[pltpu.VMEM((4, ROWS, LANES), F32)] * 2,
                pltpu.VMEM((4, 80, PADDED), F32),
                dma((chunks, 4)), dma((2, chunks)), dma((2, chunks)), dma((4, chunks)), dma((4, chunks)), dma((5,)), dma((5,)), dma((12,)), dma((12,)),
            ],
            compiler_params=pltpu.CompilerParams(collective_id=0, has_side_effects=True, vmem_limit_bytes=52 << 20),
            name="ocean_step",
        )(table, wet_levels, col_depth, surf_eta, trans_x, trans_y, *(x.reshape(-1, WIDTH) for x in (vel_x, vel_y, pot_temp, salinity)))

        small = jax.ShapeDtypeStruct((2, ROWS, WIDTH), F32)
        return pl.pallas_call(
            functools.partial(finish_kernel, K, size),
            out_shape=(small,) * 3 + (full,) * 4,
            in_specs=[smem] + [vmem] * 9,
            out_specs=(vmem,) * 3 + (hbm,) * 4,
            scratch_shapes=[
                pltpu.VMEM((8, 80, PADDED), F32),
                pltpu.VMEM((6, ROWS, PADDED), F32),
                *[pltpu.VMEM((K, 2, ROWS, WIDTH), F32)] * 2,
                dma((2, 1 + chunks)),
            ],
            compiler_params=pltpu.CompilerParams(vmem_limit_bytes=20 << 20),
            name="ocean_finish",
        )(avg_weights, *outs)

    spec_3d = P(None, None, "row", "col")
    spec_2d = P(None, "row", "col")
    spec_map = P("row", "col")
    return jax.shard_map(local_step, mesh=mesh, in_specs=(spec_3d,) * 4 + (spec_2d,) * 3 + (spec_map,) * 2 + (P(),), out_specs=(spec_2d,) * 3 + (spec_3d,) * 4, check_vma=False)
```

```python
import functools
import numpy as np
import jax
import jax.numpy as jnp
from jax import lax
from jax.experimental import pallas as pl
from jax.experimental.pallas import tpu as pltpu
from jax.sharding import PartitionSpec as P

WAVE_COURANT = 0.4
THERM_EXP = 0.2
HALINE_CON = 0.15
PRESS_SCALE = 0.5
VISC_NUMBER = 1.0
DIFF_NUMBER = 0.5
SUBCYCLES = 30
HALO = 32
PAIR = (0, 1)
QUAD = (0, 1, 2, 3)
ZERO, HALF = 0.0, 0.5
UNROLL = 5
ROWS, WIDTH, PADDED, LANES = 16, 192, 256, 128
LAST, KEEP = LANES - 1, slice(0, WIDTH)
MESH = pl.DeviceIdType.MESH
F32 = jnp.float32


def solve_tables(level_count):
    rows = []
    for strength in (VISC_NUMBER, DIFF_NUMBER):
        inner, last = np.zeros(level_count), np.zeros(level_count)
        inner[0], last[0] = 1.0 + strength, 1.0
        for k in range(1, level_count):
            inner[k] = 1.0 + 2.0 * strength - strength * strength / inner[k - 1]
            last[k] = 1.0 + strength - strength * strength / inner[k - 1]
        rows += [1.0 / inner, 1.0 / last, strength / inner]
    return np.concatenate(rows).astype(np.float32)


def level_chunk(level_count):
    return next(size for size in (15, 5) if level_count % size == 0)


def step_kernel(
    row_count, col_count, level_count,
    table_hbm, kmt_hbm, depth_hbm, eta_hbm, tx_hbm, ty_hbm, u_hbm, v_hbm, t_hbm, s_hbm,
    pu, pv, pt, ps, mean, faces, coef, force, state,
    table, kmt_in, depth_in, eta_in, tx_in, ty_in, raw_u, raw_v, raw_t, raw_s, ua, va, ta, sa, ub, vb, tb, sb, rows_n, rows_s, send_n, send_s, tail_n, tail_s, north_w, south_e, north_h, kmt_n, pack, col_e, col_w, corner_se, corner_nw,
    edge_e, edge_w, wide, fedge_e, fedge_w, wide_f,
    small_sem, load_sem, row_send, row_recv, col_send, col_recv, misc_send, misc_recv, wide_send, wide_recv,
):
    K = level_count
    open_scope = []

    def mark(name):
        if open_scope:
            open_scope.pop().__exit__(None, None, None)
        if name:
            open_scope.append(jax.named_scope(name))
            open_scope[-1].__enter__()

    size = level_chunk(K)
    chunks = K // size
    r = lax.axis_index("row")
    c = lax.axis_index("col")
    east = lax.rem(c + 1, col_count)
    west = lax.rem(c + col_count - 1, col_count)
    has_n, has_s = r < row_count - 1, r > 0
    has_nn, has_ss = r < row_count - 2, r > 1
    raw, first, second = (raw_u, raw_v, raw_t, raw_s), (ua, va, ta, sa), (ub, vb, tb, sb)

    def one(flag):
        return flag.astype(jnp.int32)

    mark("init")
    def block(k, m):
        return pl.ds(pl.multiple_of((2 * k + m) * ROWS, ROWS), ROWS)

    small = ((kmt_hbm, kmt_in), (depth_hbm, depth_in), (eta_hbm, eta_in), (tx_hbm, tx_in), (ty_hbm, ty_in), (table_hbm, table))
    small_loads = [pltpu.make_async_copy(src, dst, small_sem.at[i]) for i, (src, dst) in enumerate(small)]
    for copy in small_loads:
        copy.start()
    loads = []
    for i in range(chunks):
        levels = pl.ds(i * size * 2 * ROWS, size * 2 * ROWS)
        group = []
        for f, src in enumerate((u_hbm, v_hbm, t_hbm, s_hbm)):
            group.append(pltpu.make_async_copy(src.at[levels], raw[f].at[levels], load_sem.at[i, f]))
        loads.append(group)
    for group in loads:
        for copy in group:
            copy.start()

    wide[...] = jnp.zeros_like(wide)
    wide_f[...] = jnp.zeros_like(wide_f)

    @pl.when(jnp.logical_not(has_n))
    def _():
        rows_n[...] = jnp.zeros_like(rows_n)
        kmt_n[...] = jnp.zeros_like(kmt_n)
        corner_nw[...] = jnp.zeros_like(corner_nw)

    @pl.when(jnp.logical_not(has_s))
    def _():
        rows_s[...] = jnp.zeros_like(rows_s)
        corner_se[...] = jnp.zeros_like(corner_se)

    barrier = pltpu.get_barrier_semaphore()

    def signal(**where):
        pl.semaphore_signal(barrier, inc=1, device_id=where, device_id_type=MESH)

    signal(col=east)
    signal(col=west)

    @pl.when(has_n)
    def _():
        signal(row=r + 1)
        signal(row=r + 1, col=west)

    @pl.when(has_s)
    def _():
        signal(row=r - 1)
        signal(row=r - 1, col=east)

    @pl.when(has_nn)
    def _():
        signal(row=r + 2)

    @pl.when(has_ss)
    def _():
        signal(row=r - 2)

    def remote(src, dst, ssem, rsem, **where):
        return pltpu.make_async_remote_copy(src_ref=src, dst_ref=dst, send_sem=ssem, recv_sem=rsem, device_id=where, device_id_type=MESH)

    lane = lax.broadcasted_iota(jnp.int32, (ROWS, LANES), 1)
    lane8, lane1 = lane[0:8], lane[0:1]
    sub = lax.broadcasted_iota(jnp.int32, (8, LANES), 0)
    sub2 = lax.broadcasted_iota(jnp.int32, (8, PADDED), 0)

    def padded(x):
        return jnp.concatenate([x, jnp.zeros((x.shape[0], PADDED - WIDTH), x.dtype)], axis=1)

    def overlapped(x):
        a, b = x[:, 0:LANES], x[:, LANES:PADDED]
        return jnp.concatenate([a, jnp.where(lane < 64, b, a)], axis=1)

    def linear(x):
        a, b = x[:, 0:LANES], x[:, LANES:PADDED]
        return jnp.concatenate([jnp.where(lane < 96, a, b), b], axis=1)

    for copy in small_loads:
        copy.wait()
    kmt = padded(kmt_in[...]).astype(F32)
    own = pl.ds(HALO, ROWS)
    wide[0, own, :] = jnp.where(kmt > 0.5, padded(depth_in[...]), ZERO)
    for m in PAIR:
        wide[1 + m, own, :] = padded(eta_in[m])
        wide[3 + m, own, :] = padded(tx_in[m])
        wide[5 + m, own, :] = padded(ty_in[m])

    kmt_copy = remote(kmt_in.at[0:1, :], kmt_n, misc_send.at[0], misc_recv.at[0], row=r - 1)

    def south_copy(i):
        return remote(send_s.at[i], rows_n.at[i], row_send.at[0, i], row_recv.at[0, i], row=r - 1)

    def north_copy(i):
        return remote(send_n.at[i], rows_s.at[i], row_send.at[1, i], row_recv.at[1, i], row=r + 1)

    def west_copy(i):
        return remote(pack.at[i], col_e.at[i], col_send.at[0, i], col_recv.at[0, i], col=west)

    def east_copy(i):
        return remote(pack.at[i], col_w.at[i], col_send.at[1, i], col_recv.at[1, i], col=east)

    def corner_v(i):
        return remote(pack.at[i, 0, 8:16, :], corner_se.at[i], col_send.at[2, i], col_recv.at[2, i], row=r + 1, col=west)

    def corner_u(i):
        return remote(pack.at[i, 0, 0:8, :], corner_nw.at[i], col_send.at[3, i], col_recv.at[3, i], row=r - 1, col=east)

    groups = [*range(0, size - 3, 4)] + [size - 4] * (size % 4 > 0)

    def pack_chunk(i):
        for copy in loads[i]:
            copy.wait()

        def collect(j, acc):
            out = []
            here = (lane == j) | (lane == j + 63)
            for f in QUAD:
                for m in PAIR:
                    at = block(i * size + j, m)
                    x = raw[f][at, 0:LANES]
                    first[f][at, :] = x
                    y = jnp.where(lane < 64, padded(raw[f][at, LANES:WIDTH]), x)
                    second[f][at, :] = y
                    out.append(jnp.where(here, pltpu.roll(jnp.where(lane == 0, x, y), j, 1), acc[len(out)]))
            return tuple(out)

        acc = lax.fori_loop(0, size, collect, (jnp.zeros((ROWS, LANES), F32),) * 8, unroll=UNROLL)
        for g in PAIR:
            merged = pltpu.roll(kmt[:, 0:LANES], LAST, 1)
            for n in QUAD:
                low = size * n
                here = (lane >= low) & (lane < low + size) | (lane >= low + 63) & (lane < low + 63 + size)
                merged = jnp.where(here, pltpu.roll(acc[4 * g + n], low, 1), merged)
            pack[i, g] = merged
        for row, dest in ((0, send_s), (15, send_n)):
            for j in groups:
                at, spot = pl.ds((i * size + j) * 2 * ROWS + row, 8, stride=ROWS), pl.ds(2 * j, 8)
                tails = []
                for f in QUAD:
                    dest[i, f, spot, :] = first[f][at, :]
                    tails.append(second[f][at, :])
                for p in PAIR:
                    dest[i, 4 + p, spot, :] = jnp.where(lane8 < 64, tails[2 * p], pltpu.roll(tails[2 * p + 1], 64, 1))

    def start_chunk(i):
        west_copy(i).start()
        east_copy(i).start()

        @pl.when(has_s)
        def _():
            corner_u(i).start()
            south_copy(i).start()

        @pl.when(has_n)
        def _():
            corner_v(i).start()
            north_copy(i).start()

    mark("pack_early")
    def edge_pair(buf, to_east, to_west, sem):
        return [
            remote(buf.at[:, own, 0:LANES], to_west, misc_send.at[sem], misc_recv.at[sem], col=west),
            remote(buf.at[:, own, LANES:PADDED], to_east, misc_send.at[sem + 1], misc_recv.at[sem + 1], col=east),
        ]

    edge_copies = edge_pair(wide, edge_w, edge_e, 1)
    early = 1
    for i in range(early):
        pack_chunk(i)
    mark("barrier_wait")
    pl.semaphore_wait(barrier, 2 + 2 * one(has_n) + 2 * one(has_s) + one(has_nn) + one(has_ss))

    @pl.when(has_s)
    def _():
        kmt_copy.start()

    for i in range(early):
        start_chunk(i)
    for copy in edge_copies:
        copy.start()
    mark("pack_late")
    for i in range(early, chunks):
        pack_chunk(i)
        start_chunk(i)

    def with_edges(x, from_east, from_west):
        b = jnp.where(lane < 64, x[:, LANES:PADDED], jnp.where(lane < 96, pltpu.roll(from_east, 64, 1), pltpu.roll(from_west, 64, 1)))
        return jnp.concatenate([x[:, 0:LANES], b], axis=1)

    def spread(buf, sem):
        even = lax.rem(r, 2) == 0
        odd = jnp.logical_not(even)

        def part(at, to, out, to_sem, row):
            return remote(buf.at[:, pl.ds(at, ROWS), :], buf.at[:, pl.ds(to, ROWS), :], wide_send.at[sem + out], wide_recv.at[sem + to_sem], row=row)

        direct = (
            (has_n, has_s, part(HALO, ROWS, 0, 0, r + 1)),
            (has_s, has_n, part(HALO, 48, 1, 1, r - 1)),
            (has_nn & even, has_ss, part(HALO, 0, 2, 2, r + 2)),
            (has_ss & odd, has_nn, part(HALO, 64, 3, 3, r - 2)),
        )
        relayed = ((has_s & even, part(ROWS, 0, 4, 2, r + 1)), (has_n & odd, part(48, 64, 5, 3, r - 1)))
        return direct, relayed

    def start_spread(copies):
        for there, _, copy in copies[0]:
            @pl.when(there)
            def _():
                copy.start()

    def relay_spread(copies):
        for (_, here, copy), (there, again) in zip(copies[0], copies[1]):
            @pl.when(here)
            def _():
                copy.wait_recv()

            @pl.when(there)
            def _():
                again.start()

    def finish_spread(copies):
        for n, (there, here, copy) in enumerate(copies[0]):
            @pl.when(there)
            def _():
                copy.wait_send()

            if n > 1:
                @pl.when(here)
                def _():
                    copy.wait_recv()

        for there, again in copies[1]:
            @pl.when(there)
            def _():
                again.wait_send()


    def roll_e(x):
        return jnp.concatenate([pltpu.roll(x[:, 0:LANES], LAST, 1), pltpu.roll(x[:, LANES:PADDED], LAST, 1)], axis=1)

    def roll_w(x):
        return jnp.concatenate([pltpu.roll(x[:, 0:LANES], 1, 1), pltpu.roll(x[:, LANES:PADDED], 1, 1)], axis=1)

    def from_north(x, edge):
        low, high = pltpu.roll(x[0:8], 7, 0), pltpu.roll(x[8:16], 7, 0)
        return jnp.concatenate([jnp.where(sub2 == 7, high, low), jnp.where(sub2 == 7, edge, high)], axis=0)

    def from_south(x, edge):
        low, high = pltpu.roll(x[0:8], 1, 0), pltpu.roll(x[8:16], 1, 0)
        return jnp.concatenate([jnp.where(sub2 == 0, edge, low), jnp.where(sub2 == 0, low, high)], axis=0)

    def wait_columns(i):
        west_copy(i).wait_recv()
        east_copy(i).wait_recv()

    def insert_columns(i):
        columns = [jnp.where(lane < 62, col_e[i, g], col_w[i, g]) for g in PAIR]

        def level(j, _):
            k = i * size + j
            for f in QUAD:
                for m in PAIR:
                    place = size * (2 * (f % 2) + m) + j
                    turned = pltpu.roll(columns[f // 2], lax.rem(LANES + 64 - place, LANES), 1)
                    pltpu.store(first[f].at[block(k, m)], turned, mask=lane == LAST)
                    pltpu.store(second[f].at[block(k, m)], turned, mask=lane == 64)
            return 0

        lax.fori_loop(0, size, level, 0, unroll=UNROLL)

    edge_lane = lax.broadcasted_iota(jnp.int32, rows_n.shape[2:], 1)

    def unpack_rows(i):
        for rows, tails in ((rows_n, tail_n), (rows_s, tail_s)):
            for f in QUAD:
                packed = rows[i, 4 + f // 2]
                tails[i, f] = jnp.where(edge_lane < 64, packed if f % 2 == 0 else pltpu.roll(packed, 64, 1), rows[i, f])
        for h, (u, v, t, s) in enumerate(((rows_n.at[i, 0], rows_s.at[i, 1], rows_n.at[i, 2], rows_n.at[i, 3]), (tail_n.at[i, 0], tail_s.at[i, 1], tail_n.at[i, 2], tail_n.at[i, 3]))):
            u, v = u[...], v[...]
            north_w[i, h] = u + pltpu.roll(u, 1, 1)
            south_e[i, h] = v + pltpu.roll(v, LAST, 1)
            north_h[i, h] = (half_scale * HALINE_CON) * s[...] - (half_scale * THERM_EXP) * t[...]

    half_scale = HALF * PRESS_SCALE / K

    def both(tiles, k, m, f):
        return jnp.concatenate([tiles[0][f][block(k, m), :], tiles[1][f][block(k, m), :]], axis=1)

    def edge(rows, tails, f, i, at):
        return jnp.concatenate([rows[i, f, at, :], tails[i, f, at, :]], axis=1)

    mark("column_wait")
    wait_columns(0)

    @pl.when(has_n)
    def _():
        kmt_copy.wait_recv()

    @pl.when(has_s)
    def _():
        kmt_copy.wait_send()

    mark("masks")
    kmt2 = overlapped(kmt)
    kmt_edge = jnp.where(lane == 64, pltpu.roll(col_e[0, 0], 65, 1), kmt2[:, LANES:PADDED])
    kmt_row = padded(kmt_n[...]).astype(F32)
    kmt_north = jnp.concatenate([kmt_row[:, 0:LANES], jnp.where(lane1 < 64, kmt_row[:, LANES:PADDED], kmt_row[:, 0:LANES])], axis=1)
    mu = jnp.minimum(kmt2, roll_e(jnp.concatenate([kmt2[:, 0:LANES], kmt_edge], axis=1)))
    mv = jnp.minimum(kmt2, from_north(kmt2, kmt_north))
    faces[0] = linear(mu)
    faces[1] = linear(mv)

    def solve_factor(depth, k, first):
        inner, last = table[first * K + k], table[(first + 1) * K + k]
        kf = k.astype(F32)
        return jnp.where(depth > kf + 1.0, inner, jnp.where(depth > kf, last, ZERO))

    def momentum(i):
        def level(j, members):
            k = i * size + j
            kf = k.astype(F32)
            out = []
            for m in PAIR:
                total, total_n, gu_sum, gv_sum = members[m]
                at = pl.ds(2 * j + m, 1)
                u, v, t, s = (both((first, second), k, m, f) for f in QUAD)
                step = (half_scale * HALINE_CON) * s - (half_scale * THERM_EXP) * t
                pressure = total + step
                step_n = jnp.concatenate([north_h[i, 0, at, :], north_h[i, 1, at, :]], axis=1)
                pressure_n = total_n + step_n
                corner_n = pltpu.roll(corner_nw[i], 65 - (size * m + j), 1)[0:1]
                corner_s = pltpu.roll(corner_se[i], lax.rem(LANES + 63 - (size * (2 + m) + j), LANES), 1)[7:8]
                u_edge, v_edge = edge(rows_n, tail_n, 0, i, at), edge(rows_s, tail_s, 1, i, at)
                u_pair_n = jnp.concatenate([jnp.where(lane1 == 0, u_edge[:, 0:LANES] + corner_n, north_w[i, 0, at, :]), north_w[i, 1, at, :]], axis=1)
                v_pair_s = jnp.concatenate([south_e[i, 0, at, :], jnp.where(lane1 == 63, v_edge[:, LANES:PADDED] + corner_s, south_e[i, 1, at, :])], axis=1)
                v_e, v_w, u_e, u_w = roll_e(v), roll_w(v), roll_e(u), roll_w(u)
                v_pair, u_pair = v + v_e, u + u_w
                vu = 0.125 * (v_pair + from_south(v_pair, v_pair_s))
                uv = 0.125 * (u_pair + from_north(u_pair, u_pair_n))
                u_n, u_s = from_north(u, u_edge), from_south(u, edge(rows_s, tail_s, 0, i, at))
                v_n, v_s = from_north(v, edge(rows_n, tail_n, 1, i, at)), from_south(v, v_edge)
                p_n = from_north(pressure, pressure_n)
                gu = pressure - roll_e(pressure) - HALF * u * (u_e - u_w) - vu * (u_n - u_s)
                gv = pressure - p_n - uv * (v_e - v_w) - HALF * v * (v_n - v_s)
                gu = jnp.where(mu > kf, gu, ZERO)
                gv = jnp.where(mv > kf, gv, ZERO)
                pu[k, m] = linear(u + gu)[:, KEEP]
                pv[k, m] = linear(v + gv)[:, KEEP]
                out.append((pressure + step, pressure_n + step_n, gu_sum + gu, gv_sum + gv))
            return tuple(out)

        return level

    zero = jnp.zeros((ROWS, PADDED), F32)
    zero_row = jnp.zeros((1, PADDED), F32)
    members = ((zero, zero_row, zero, zero),) * 2
    for i in range(chunks):
        if i > 0:
            wait_columns(i)
        mark("insert")
        insert_columns(i)

        mark("row_wait")
        @pl.when(has_n)
        def _():
            south_copy(i).wait_recv()
            corner_u(i).wait_recv()

        @pl.when(has_s)
        def _():
            north_copy(i).wait_recv()
            corner_v(i).wait_recv()

        mark("momentum")
        unpack_rows(i)
        members = lax.fori_loop(0, size, momentum(i), members, unroll=UNROLL)

        mark("next")
        if i == 0:
            for copy in edge_copies:
                copy.wait()
            for p in range(7):
                wide[p, own, :] = with_edges(wide[p, own, :], edge_e[p], edge_w[p])
            static_copies = spread(wide, 0)
            start_spread(static_copies)

    mark("force")
    relay_spread(static_copies)
    count_u = linear(jnp.maximum(mu, 1.0))
    count_v = linear(jnp.maximum(mv, 1.0))
    for m in PAIR:
        wide_f[m, own, :] = linear(members[m][2]) / count_u
        wide_f[2 + m, own, :] = linear(members[m][3]) / count_v
    force_edges = edge_pair(wide_f, fedge_w, fedge_e, 3)
    for copy in force_edges:
        copy.start()

    def tracers(i, carry):
        def level(j, carry):
            k = i * size + j
            factor = solve_factor(kmt2, k, 3)
            out = []
            for m in PAIR:
                at = pl.ds(2 * j + m, 1)
                u, v = (HALF * both((first, second), k, m, f) for f in PAIR)
                u_w = roll_w(u)
                v_edge = HALF * edge(rows_s, tail_s, 1, i, at)
                for f, dest in ((2, pt), (3, ps)):
                    t = both((first, second), k, m, f)
                    flux_x = u * (t + roll_e(t)) - u_w * (t + roll_w(t))
                    flux_y = v * (t + from_north(t, edge(rows_n, tail_n, f, i, at)))
                    flux_s = v_edge * (edge(rows_s, tail_s, f, i, at) + t[0:1])
                    moved = t - (flux_x + flux_y - from_south(flux_y, flux_s))
                    side = (moved + DIFF_NUMBER * carry[len(out)]) * factor
                    dest[k, m] = linear(side)[:, KEEP]
                    out.append(side)
            return tuple(out)

        return lax.fori_loop(0, size, level, carry, unroll=UNROLL)

    mark("tracer_1")
    tail = (zero,) * 4
    split = (3 * chunks + 4) // 5
    tail = lax.fori_loop(0, split, tracers, tail)

    mark("forward_uv")
    depth_u, depth_v = faces[0][:, KEEP], faces[1][:, KEEP]

    def forward(k, carry):
        out = []
        for field, depth in ((pu, depth_u), (pv, depth_v)):
            factor = solve_factor(depth, k, 0)
            for m in PAIR:
                x = (field[k, m] + VISC_NUMBER * carry[len(out)]) * factor
                field[k, m] = x
                out.append(x)
        return tuple(out)

    sides = lax.fori_loop(0, K, forward, (zero[:, KEEP],) * 4, unroll=UNROLL)

    mark("force_edge_wait")
    for copy in force_edges:
        copy.wait()
    mark("force_spread")
    for p in QUAD:
        wide_f[p, own, :] = with_edges(wide_f[p, own, :], fedge_e[p], fedge_w[p])
    force_copies = spread(wide_f, 6)
    start_spread(force_copies)

    mark("tracer_2")
    tail = lax.fori_loop(split, chunks, tracers, tail)

    def back_tracers(j, carry):
        k = K - 2 - j
        ratio = table[5 * K + k]
        out = []
        for m in PAIR:
            for dest in (pt, ps):
                x = dest[k, m] + ratio * carry[len(out)]
                dest[k, m] = x
                out.append(x)
        return tuple(out)

    mark("back_tracers")
    lax.fori_loop(0, K - 1, back_tracers, tuple(linear(x)[:, KEEP] for x in tail), unroll=2)

    def back(j, carry):
        k = K - 2 - j
        ratio = table[2 * K + k]
        out = []
        for m in PAIR:
            xu, xv, su, sv = carry[m]
            xu = pu[k, m] + ratio * xu
            xv = pv[k, m] + ratio * xv
            pu[k, m] = xu
            pv[k, m] = xv
            out.append((xu, xv, su + xu, sv + xv))
        return tuple(out)

    mark("back_uv")
    start = tuple((sides[m], sides[2 + m], sides[m], sides[2 + m]) for m in PAIR)
    ends = lax.fori_loop(0, K - 1, back, start)

    mark("relay")
    relay_spread(force_copies)
    mark("static_wait")
    finish_spread(static_copies)
    mark("force_wait")
    finish_spread(force_copies)

    mark("coef")
    depth = wide[0]
    depth_e = pltpu.roll(depth, PADDED - 1, 1)
    depth_n = pltpu.roll(depth, 79, 0)
    hu = jnp.where((depth > ZERO) & (depth_e > ZERO), HALF * (depth + depth_e), ZERO)
    hv = jnp.where((depth > ZERO) & (depth_n > ZERO), HALF * (depth + depth_n), ZERO)
    coef[0] = WAVE_COURANT * WAVE_COURANT * hu
    coef[1] = WAVE_COURANT * WAVE_COURANT * hv
    for m in PAIR:
        force[m] = hu * wide_f[m] * (WAVE_COURANT / SUBCYCLES)
        force[2 + m] = hv * wide_f[2 + m] * (WAVE_COURANT / SUBCYCLES)
        state[m] = wide[1 + m]
        state[2 + m] = WAVE_COURANT * wide[3 + m]
        state[4 + m] = WAVE_COURANT * wide[5 + m]
        state[6 + m] = pltpu.roll(wide[1 + m], PADDED - 1, 1)
    mine = slice(HALO, HALO + ROWS)
    for p, (h, count) in enumerate(((hu[mine], count_u), (hv[mine], count_v))):
        faces[2 + p] = 1.0 / (WAVE_COURANT * jnp.where(h > ZERO, h, 1.0))
        for m in PAIR:
            mean[2 * p + m] = padded(ends[m][2 + p]) / count

    mark("send_wait")
    for i in range(chunks):
        west_copy(i).wait_send()
        east_copy(i).wait_send()

    @pl.when(has_s)
    def _():
        for i in range(chunks):
            south_copy(i).wait_send()
            corner_u(i).wait_send()

    @pl.when(has_n)
    def _():
        for i in range(chunks):
            north_copy(i).wait_send()
            corner_v(i).wait_send()
    mark("")


def finish_kernel(
    K, size,
    weights, pu, pv, pt, ps, mean, faces, coef, force, first_state,
    eta_o, tx_o, ty_o, u_o, v_o, t_o, s_o,
    state, avg, small, out_u, out_v, sems,
):
    chunks = K // size
    through = [pltpu.make_async_copy(src, dst, sems.at[i, 0]) for i, (src, dst) in enumerate(((pt, t_o), (ps, s_o)))]
    for copy in through:
        copy.start()
    state[...] = first_state[...]
    avg[...] = jnp.zeros_like(avg)

    def subcycles(first, last, margin):
        height = ROWS + 2 * margin
        rows = pl.ds(HALO - margin, height)
        mine = slice(margin, margin + ROWS)

        def to_e(x):
            return pltpu.roll(x, PADDED - 1, 1)

        def subcycle(n, _):
            weight = weights[n]
            for m in PAIR:
                tx, ty = state[2 + m, rows], state[4 + m, rows]
                tx_e, ty_e = to_e(tx), to_e(ty)
                eta = state[m, rows] - (tx - pltpu.roll(tx, 1, 1) + ty - pltpu.roll(ty, 1, 0))
                eta_e = state[6 + m, rows] - (tx_e - tx + ty_e - pltpu.roll(ty_e, 1, 0))
                tx = tx + force[m, rows] - coef[0, rows] * (eta_e - eta)
                ty = ty + force[2 + m, rows] - coef[1, rows] * (pltpu.roll(eta, height - 1, 0) - eta)
                for p, x in enumerate((eta, tx, ty)):
                    state[2 * p + m, rows] = x
                    avg[2 * p + m] = avg[2 * p + m] + weight * x[mine]
                state[6 + m, rows] = eta_e
            return 0

        lax.fori_loop(first, last, subcycle, 0)

    done = 0
    for margin in (HALO, 24, ROWS, 8):
        last = SUBCYCLES - (margin - 8)
        subcycles(done, last, margin)
        done = last

    corr = []
    for m in PAIR:
        small[0, m] = avg[m][:, KEEP]
        for p in PAIR:
            transport = avg[2 + 2 * p + m]
            small[1 + p, m] = (transport * (1.0 / WAVE_COURANT))[:, KEEP]
            corr.append((transport * faces[2 + p] - mean[2 * p + m])[:, KEEP])
    for p, dest in enumerate((eta_o, tx_o, ty_o)):
        through.append(pltpu.make_async_copy(small.at[p], dest, sems.at[2, p]))
        through[-1].start()
    depth_u, depth_v = faces[0][:, KEEP], faces[1][:, KEEP]

    def out_copies(i):
        levels = pl.ds(i * size, size)
        return [pltpu.make_async_copy(src.at[levels], dst.at[levels], sems.at[p, 1 + i]) for p, (src, dst) in enumerate(((out_u, u_o), (out_v, v_o)))]

    for i in range(chunks):
        def level(j, _):
            k = i * size + j
            kf = k.astype(F32)
            for m in PAIR:
                out_u[k, m] = jnp.where(depth_u > kf, pu[k, m] + corr[2 * m], ZERO)
                out_v[k, m] = jnp.where(depth_v > kf, pv[k, m] + corr[2 * m + 1], ZERO)
            return 0

        lax.fori_loop(0, size, level, 0, unroll=UNROLL)
        for copy in out_copies(i):
            copy.start()

    for copy in through + [copy for i in range(chunks) for copy in out_copies(i)]:
        copy.wait()


def solution(mesh):
    col_count, row_count = mesh.shape["col"], mesh.shape["row"]

    def local_step(vel_x, vel_y, pot_temp, salinity, surf_eta, trans_x, trans_y, col_depth, wet_levels, avg_weights):
        K = vel_x.shape[0]
        size = level_chunk(K)
        chunks = K // size
        edge_rows = (2 * size + 7) // 8 * 8
        table = jnp.asarray(solve_tables(K))
        smem = pl.BlockSpec(memory_space=pltpu.SMEM)
        vmem = pl.BlockSpec(memory_space=pltpu.VMEM)
        hbm = pl.BlockSpec(memory_space=pl.ANY)
        full = jax.ShapeDtypeStruct((K, 2, ROWS, WIDTH), F32)
        held = pltpu.VMEM((K, 2, ROWS, WIDTH), F32)
        dma = pltpu.SemaphoreType.DMA
        outs = pl.pallas_call(
            functools.partial(step_kernel, row_count, col_count, K),
            out_shape=(held,) * 4 + tuple(pltpu.VMEM((n, ROWS, PADDED), F32) for n in (4, 4)) + tuple(pltpu.VMEM((n, 80, PADDED), F32) for n in (2, 4, 8)),
            in_specs=[hbm] * 10,
            out_specs=(vmem,) * 9,
            scratch_shapes=[
                pltpu.SMEM(table.shape, F32),
                pltpu.VMEM((ROWS, WIDTH), jnp.int32),
                pltpu.VMEM((ROWS, WIDTH), F32),
                *[pltpu.VMEM((2, ROWS, WIDTH), F32)] * 3,
                *[pltpu.VMEM((K * 2 * ROWS, WIDTH), F32)] * 4,
                *[pltpu.VMEM((K * 2 * ROWS, LANES), F32)] * 8,
                *[pltpu.VMEM((chunks, 6, edge_rows, LANES), F32)] * 4,
                *[pltpu.VMEM((chunks, 4, edge_rows, LANES), F32)] * 2,
                *[pltpu.VMEM((chunks, 2, edge_rows, LANES), F32)] * 3,
                pltpu.VMEM((1, WIDTH), jnp.int32),
                *[pltpu.VMEM((chunks, 2, ROWS, LANES), F32)] * 3,
                *[pltpu.VMEM((chunks, 8, LANES), F32)] * 2,
                *[pltpu.VMEM((7, ROWS, LANES), F32)] * 2,
                pltpu.VMEM((7, 80, PADDED), F32),
                *[pltpu.VMEM((4, ROWS, LANES), F32)] * 2,
                pltpu.VMEM((4, 80, PADDED), F32),
                dma((6,)), dma((chunks, 4)), dma((2, chunks)), dma((2, chunks)), dma((4, chunks)), dma((4, chunks)), dma((5,)), dma((5,)), dma((12,)), dma((12,)),
            ],
            compiler_params=pltpu.CompilerParams(collective_id=0, has_side_effects=True, vmem_limit_bytes=52 << 20),
            name="ocean_step",
        )(table, wet_levels, col_depth, surf_eta, trans_x, trans_y, *(x.reshape(-1, WIDTH) for x in (vel_x, vel_y, pot_temp, salinity)))

        small = jax.ShapeDtypeStruct((2, ROWS, WIDTH), F32)
        return pl.pallas_call(
            functools.partial(finish_kernel, K, size),
            out_shape=(small,) * 3 + (full,) * 4,
            in_specs=[smem] + [vmem] * 9,
            out_specs=(hbm,) * 7,
            scratch_shapes=[
                pltpu.VMEM((8, 80, PADDED), F32),
                pltpu.VMEM((6, ROWS, PADDED), F32),
                pltpu.VMEM((3, 2, ROWS, WIDTH), F32),
                *[pltpu.VMEM((K, 2, ROWS, WIDTH), F32)] * 2,
                dma((3, 2 + chunks)),
            ],
            compiler_params=pltpu.CompilerParams(vmem_limit_bytes=20 << 20),
            name="ocean_finish",
        )(avg_weights, *outs)

    spec_3d = P(None, None, "row", "col")
    spec_2d = P(None, "row", "col")
    spec_map = P("row", "col")
    return jax.shard_map(local_step, mesh=mesh, in_specs=(spec_3d,) * 4 + (spec_2d,) * 3 + (spec_map,) * 2 + (P(),), out_specs=(spec_2d,) * 3 + (spec_3d,) * 4, check_vma=False)
```

```python
import functools
import numpy as np
import jax
import jax.numpy as jnp
from jax import lax
from jax.experimental import pallas as pl
from jax.experimental.pallas import tpu as pltpu
from jax.sharding import PartitionSpec as P

WAVE_COURANT = 0.4
THERM_EXP = 0.2
HALINE_CON = 0.15
PRESS_SCALE = 0.5
VISC_NUMBER = 1.0
DIFF_NUMBER = 0.5
SUBCYCLES = 30
HALO = 32
PAIR = (0, 1)
QUAD = (0, 1, 2, 3)
ZERO, HALF = 0.0, 0.5
UNROLL = 5
ROWS, WIDTH, PADDED, LANES = 16, 192, 256, 128
LAST, KEEP = LANES - 1, slice(0, WIDTH)
MESH = pl.DeviceIdType.MESH
F32 = jnp.float32


def solve_tables(level_count):
    rows = []
    for strength in (VISC_NUMBER, DIFF_NUMBER):
        inner, last = np.zeros(level_count), np.zeros(level_count)
        inner[0], last[0] = 1.0 + strength, 1.0
        for k in range(1, level_count):
            inner[k] = 1.0 + 2.0 * strength - strength * strength / inner[k - 1]
            last[k] = 1.0 + strength - strength * strength / inner[k - 1]
        rows += [1.0 / inner, 1.0 / last, strength / inner]
    return np.concatenate(rows).astype(np.float32)


def level_chunk(level_count):
    return next(size for size in (15, 5) if level_count % size == 0)


def step_kernel(
    row_count, col_count, level_count,
    table, kmt_in, depth_in, eta_in, tx_in, ty_in, u_hbm, v_hbm, t_hbm, s_hbm,
    pu, pv, pt, ps, mean, faces, coef, force, state,
    raw_u, raw_v, raw_t, raw_s, ua, va, ta, sa, ub, vb, tb, sb, rows_n, rows_s, send_n, send_s, tail_n, tail_s, north_w, south_e, north_h, kmt_n, pack, col_e, col_w, corner_se, corner_nw,
    edge_e, edge_w, wide, fedge_e, fedge_w, wide_f,
    load_sem, row_send, row_recv, col_send, col_recv, misc_send, misc_recv, wide_send, wide_recv,
):
    K = level_count
    open_scope = []

    def mark(name):
        if open_scope:
            open_scope.pop().__exit__(None, None, None)
        if name:
            open_scope.append(jax.named_scope(name))
            open_scope[-1].__enter__()

    size = level_chunk(K)
    chunks = K // size
    r = lax.axis_index("row")
    c = lax.axis_index("col")
    east = lax.rem(c + 1, col_count)
    west = lax.rem(c + col_count - 1, col_count)
    has_n, has_s = r < row_count - 1, r > 0
    has_nn, has_ss = r < row_count - 2, r > 1
    raw, first, second = (raw_u, raw_v, raw_t, raw_s), (ua, va, ta, sa), (ub, vb, tb, sb)

    def one(flag):
        return flag.astype(jnp.int32)

    mark("init")
    def block(k, m):
        return pl.ds(pl.multiple_of((2 * k + m) * ROWS, ROWS), ROWS)

    loads = []
    for i in range(chunks):
        levels = pl.ds(i * size * 2 * ROWS, size * 2 * ROWS)
        group = []
        for f, src in enumerate((u_hbm, v_hbm, t_hbm, s_hbm)):
            group.append(pltpu.make_async_copy(src.at[levels], raw[f].at[levels], load_sem.at[i, f]))
        loads.append(group)
    for group in loads:
        for copy in group:
            copy.start()

    wide[...] = jnp.zeros_like(wide)
    wide_f[...] = jnp.zeros_like(wide_f)

    @pl.when(jnp.logical_not(has_n))
    def _():
        rows_n[...] = jnp.zeros_like(rows_n)
        kmt_n[...] = jnp.zeros_like(kmt_n)
        corner_nw[...] = jnp.zeros_like(corner_nw)

    @pl.when(jnp.logical_not(has_s))
    def _():
        rows_s[...] = jnp.zeros_like(rows_s)
        corner_se[...] = jnp.zeros_like(corner_se)

    barrier = pltpu.get_barrier_semaphore()

    def signal(**where):
        pl.semaphore_signal(barrier, inc=1, device_id=where, device_id_type=MESH)

    signal(col=east)
    signal(col=west)

    @pl.when(has_n)
    def _():
        signal(row=r + 1)
        signal(row=r + 1, col=west)

    @pl.when(has_s)
    def _():
        signal(row=r - 1)
        signal(row=r - 1, col=east)

    @pl.when(has_nn)
    def _():
        signal(row=r + 2)

    @pl.when(has_ss)
    def _():
        signal(row=r - 2)

    def remote(src, dst, ssem, rsem, **where):
        return pltpu.make_async_remote_copy(src_ref=src, dst_ref=dst, send_sem=ssem, recv_sem=rsem, device_id=where, device_id_type=MESH)

    lane = lax.broadcasted_iota(jnp.int32, (ROWS, LANES), 1)
    lane8, lane1 = lane[0:8], lane[0:1]
    sub = lax.broadcasted_iota(jnp.int32, (8, LANES), 0)
    sub2 = lax.broadcasted_iota(jnp.int32, (8, PADDED), 0)

    def padded(x):
        return jnp.concatenate([x, jnp.zeros((x.shape[0], PADDED - WIDTH), x.dtype)], axis=1)

    def overlapped(x):
        a, b = x[:, 0:LANES], x[:, LANES:PADDED]
        return jnp.concatenate([a, jnp.where(lane < 64, b, a)], axis=1)

    def linear(x):
        a, b = x[:, 0:LANES], x[:, LANES:PADDED]
        return jnp.concatenate([jnp.where(lane < 96, a, b), b], axis=1)

    kmt = padded(kmt_in[...]).astype(F32)
    own = pl.ds(HALO, ROWS)
    wide[0, own, :] = jnp.where(kmt > 0.5, padded(depth_in[...]), ZERO)
    for m in PAIR:
        wide[1 + m, own, :] = padded(eta_in[m])
        wide[3 + m, own, :] = padded(tx_in[m])
        wide[5 + m, own, :] = padded(ty_in[m])

    kmt_copy = remote(kmt_in.at[0:1, :], kmt_n, misc_send.at[0], misc_recv.at[0], row=r - 1)

    def south_copy(i):
        return remote(send_s.at[i], rows_n.at[i], row_send.at[0, i], row_recv.at[0, i], row=r - 1)

    def north_copy(i):
        return remote(send_n.at[i], rows_s.at[i], row_send.at[1, i], row_recv.at[1, i], row=r + 1)

    def west_copy(i):
        return remote(pack.at[i], col_e.at[i], col_send.at[0, i], col_recv.at[0, i], col=west)

    def east_copy(i):
        return remote(pack.at[i], col_w.at[i], col_send.at[1, i], col_recv.at[1, i], col=east)

    def corner_v(i):
        return remote(pack.at[i, 0, 8:16, :], corner_se.at[i], col_send.at[2, i], col_recv.at[2, i], row=r + 1, col=west)

    def corner_u(i):
        return remote(pack.at[i, 0, 0:8, :], corner_nw.at[i], col_send.at[3, i], col_recv.at[3, i], row=r - 1, col=east)

    groups = [*range(0, size - 3, 4)] + [size - 4] * (size % 4 > 0)

    def pack_chunk(i):
        for copy in loads[i]:
            copy.wait()

        def collect(j, acc):
            out = []
            here = (lane == j) | (lane == j + 63)
            for f in QUAD:
                for m in PAIR:
                    at = block(i * size + j, m)
                    x = raw[f][at, 0:LANES]
                    first[f][at, :] = x
                    y = jnp.where(lane < 64, padded(raw[f][at, LANES:WIDTH]), x)
                    second[f][at, :] = y
                    out.append(jnp.where(here, pltpu.roll(jnp.where(lane == 0, x, y), j, 1), acc[len(out)]))
            return tuple(out)

        acc = lax.fori_loop(0, size, collect, (jnp.zeros((ROWS, LANES), F32),) * 8, unroll=UNROLL)
        for g in PAIR:
            merged = pltpu.roll(kmt[:, 0:LANES], LAST, 1)
            for n in QUAD:
                low = size * n
                here = (lane >= low) & (lane < low + size) | (lane >= low + 63) & (lane < low + 63 + size)
                merged = jnp.where(here, pltpu.roll(acc[4 * g + n], low, 1), merged)
            pack[i, g] = merged
        for row, dest in ((0, send_s), (15, send_n)):
            for j in groups:
                at, spot = pl.ds((i * size + j) * 2 * ROWS + row, 8, stride=ROWS), pl.ds(2 * j, 8)
                tails = []
                for f in QUAD:
                    dest[i, f, spot, :] = first[f][at, :]
                    tails.append(second[f][at, :])
                for p in PAIR:
                    dest[i, 4 + p, spot, :] = jnp.where(lane8 < 64, tails[2 * p], pltpu.roll(tails[2 * p + 1], 64, 1))

    def start_chunk(i):
        west_copy(i).start()
        east_copy(i).start()

        @pl.when(has_s)
        def _():
            corner_u(i).start()
            south_copy(i).start()

        @pl.when(has_n)
        def _():
            corner_v(i).start()
            north_copy(i).start()

    mark("pack_early")
    def edge_pair(buf, to_east, to_west, sem):
        return [
            remote(buf.at[:, own, 0:LANES], to_west, misc_send.at[sem], misc_recv.at[sem], col=west),
            remote(buf.at[:, own, LANES:PADDED], to_east, misc_send.at[sem + 1], misc_recv.at[sem + 1], col=east),
        ]

    edge_copies = edge_pair(wide, edge_w, edge_e, 1)
    early = 1
    for i in range(early):
        pack_chunk(i)
    mark("barrier_wait")
    pl.semaphore_wait(barrier, 2 + 2 * one(has_n) + 2 * one(has_s) + one(has_nn) + one(has_ss))

    @pl.when(has_s)
    def _():
        kmt_copy.start()

    for i in range(early):
        start_chunk(i)
    for copy in edge_copies:
        copy.start()
    mark("pack_late")
    for i in range(early, chunks):
        pack_chunk(i)
        start_chunk(i)

    def with_edges(x, from_east, from_west):
        b = jnp.where(lane < 64, x[:, LANES:PADDED], jnp.where(lane < 96, pltpu.roll(from_east, 64, 1), pltpu.roll(from_west, 64, 1)))
        return jnp.concatenate([x[:, 0:LANES], b], axis=1)

    def spread(buf, sem):
        even = lax.rem(r, 2) == 0
        odd = jnp.logical_not(even)

        def part(at, to, out, to_sem, row):
            return remote(buf.at[:, pl.ds(at, ROWS), :], buf.at[:, pl.ds(to, ROWS), :], wide_send.at[sem + out], wide_recv.at[sem + to_sem], row=row)

        direct = (
            (has_n, has_s, part(HALO, ROWS, 0, 0, r + 1)),
            (has_s, has_n, part(HALO, 48, 1, 1, r - 1)),
            (has_nn & even, has_ss, part(HALO, 0, 2, 2, r + 2)),
            (has_ss & odd, has_nn, part(HALO, 64, 3, 3, r - 2)),
        )
        relayed = ((has_s & even, part(ROWS, 0, 4, 2, r + 1)), (has_n & odd, part(48, 64, 5, 3, r - 1)))
        return direct, relayed

    def start_spread(copies):
        for there, _, copy in copies[0]:
            @pl.when(there)
            def _():
                copy.start()

    def relay_spread(copies):
        for (_, here, copy), (there, again) in zip(copies[0], copies[1]):
            @pl.when(here)
            def _():
                copy.wait_recv()

            @pl.when(there)
            def _():
                again.start()

    def finish_spread(copies):
        for n, (there, here, copy) in enumerate(copies[0]):
            @pl.when(there)
            def _():
                copy.wait_send()

            if n > 1:
                @pl.when(here)
                def _():
                    copy.wait_recv()

        for there, again in copies[1]:
            @pl.when(there)
            def _():
                again.wait_send()


    def roll_e(x):
        return jnp.concatenate([pltpu.roll(x[:, 0:LANES], LAST, 1), pltpu.roll(x[:, LANES:PADDED], LAST, 1)], axis=1)

    def roll_w(x):
        return jnp.concatenate([pltpu.roll(x[:, 0:LANES], 1, 1), pltpu.roll(x[:, LANES:PADDED], 1, 1)], axis=1)

    def from_north(x, edge):
        low, high = pltpu.roll(x[0:8], 7, 0), pltpu.roll(x[8:16], 7, 0)
        return jnp.concatenate([jnp.where(sub2 == 7, high, low), jnp.where(sub2 == 7, edge, high)], axis=0)

    def from_south(x, edge):
        low, high = pltpu.roll(x[0:8], 1, 0), pltpu.roll(x[8:16], 1, 0)
        return jnp.concatenate([jnp.where(sub2 == 0, edge, low), jnp.where(sub2 == 0, low, high)], axis=0)

    def wait_columns(i):
        west_copy(i).wait_recv()
        east_copy(i).wait_recv()

    def insert_columns(i):
        columns = [jnp.where(lane < 62, col_e[i, g], col_w[i, g]) for g in PAIR]

        def level(j, _):
            k = i * size + j
            for f in QUAD:
                for m in PAIR:
                    place = size * (2 * (f % 2) + m) + j
                    turned = pltpu.roll(columns[f // 2], lax.rem(LANES + 64 - place, LANES), 1)
                    pltpu.store(first[f].at[block(k, m)], turned, mask=lane == LAST)
                    pltpu.store(second[f].at[block(k, m)], turned, mask=lane == 64)
            return 0

        lax.fori_loop(0, size, level, 0, unroll=UNROLL)

    edge_lane = lax.broadcasted_iota(jnp.int32, rows_n.shape[2:], 1)

    def unpack_rows(i):
        for rows, tails in ((rows_n, tail_n), (rows_s, tail_s)):
            for f in QUAD:
                packed = rows[i, 4 + f // 2]
                tails[i, f] = jnp.where(edge_lane < 64, packed if f % 2 == 0 else pltpu.roll(packed, 64, 1), rows[i, f])
        for h, (u, v, t, s) in enumerate(((rows_n.at[i, 0], rows_s.at[i, 1], rows_n.at[i, 2], rows_n.at[i, 3]), (tail_n.at[i, 0], tail_s.at[i, 1], tail_n.at[i, 2], tail_n.at[i, 3]))):
            u, v = u[...], v[...]
            north_w[i, h] = u + pltpu.roll(u, 1, 1)
            south_e[i, h] = v + pltpu.roll(v, LAST, 1)
            north_h[i, h] = (half_scale * HALINE_CON) * s[...] - (half_scale * THERM_EXP) * t[...]

    half_scale = HALF * PRESS_SCALE / K

    def both(tiles, k, m, f):
        return jnp.concatenate([tiles[0][f][block(k, m), :], tiles[1][f][block(k, m), :]], axis=1)

    def edge(rows, tails, f, i, at):
        return jnp.concatenate([rows[i, f, at, :], tails[i, f, at, :]], axis=1)

    mark("column_wait")
    wait_columns(0)

    @pl.when(has_n)
    def _():
        kmt_copy.wait_recv()

    @pl.when(has_s)
    def _():
        kmt_copy.wait_send()

    mark("masks")
    kmt2 = overlapped(kmt)
    kmt_edge = jnp.where(lane == 64, pltpu.roll(col_e[0, 0], 65, 1), kmt2[:, LANES:PADDED])
    kmt_row = padded(kmt_n[...]).astype(F32)
    kmt_north = jnp.concatenate([kmt_row[:, 0:LANES], jnp.where(lane1 < 64, kmt_row[:, LANES:PADDED], kmt_row[:, 0:LANES])], axis=1)
    mu = jnp.minimum(kmt2, roll_e(jnp.concatenate([kmt2[:, 0:LANES], kmt_edge], axis=1)))
    mv = jnp.minimum(kmt2, from_north(kmt2, kmt_north))
    faces[0] = linear(mu)
    faces[1] = linear(mv)

    def solve_factor(depth, k, first):
        inner, last = table[first * K + k], table[(first + 1) * K + k]
        kf = k.astype(F32)
        return jnp.where(depth > kf + 1.0, inner, jnp.where(depth > kf, last, ZERO))

    def momentum(i):
        def level(j, members):
            k = i * size + j
            kf = k.astype(F32)
            factor_u, factor_v = solve_factor(mu, k, 0), solve_factor(mv, k, 0)
            out = []
            for m in PAIR:
                total, total_n, gu_sum, gv_sum, side_u, side_v = members[m]
                at = pl.ds(2 * j + m, 1)
                u, v, t, s = (both((first, second), k, m, f) for f in QUAD)
                step = (half_scale * HALINE_CON) * s - (half_scale * THERM_EXP) * t
                pressure = total + step
                step_n = jnp.concatenate([north_h[i, 0, at, :], north_h[i, 1, at, :]], axis=1)
                pressure_n = total_n + step_n
                corner_n = pltpu.roll(corner_nw[i], 65 - (size * m + j), 1)[0:1]
                corner_s = pltpu.roll(corner_se[i], lax.rem(LANES + 63 - (size * (2 + m) + j), LANES), 1)[7:8]
                u_edge, v_edge = edge(rows_n, tail_n, 0, i, at), edge(rows_s, tail_s, 1, i, at)
                u_pair_n = jnp.concatenate([jnp.where(lane1 == 0, u_edge[:, 0:LANES] + corner_n, north_w[i, 0, at, :]), north_w[i, 1, at, :]], axis=1)
                v_pair_s = jnp.concatenate([south_e[i, 0, at, :], jnp.where(lane1 == 63, v_edge[:, LANES:PADDED] + corner_s, south_e[i, 1, at, :])], axis=1)
                v_e, v_w, u_e, u_w = roll_e(v), roll_w(v), roll_e(u), roll_w(u)
                v_pair, u_pair = v + v_e, u + u_w
                vu = 0.125 * (v_pair + from_south(v_pair, v_pair_s))
                uv = 0.125 * (u_pair + from_north(u_pair, u_pair_n))
                u_n, u_s = from_north(u, u_edge), from_south(u, edge(rows_s, tail_s, 0, i, at))
                v_n, v_s = from_north(v, edge(rows_n, tail_n, 1, i, at)), from_south(v, v_edge)
                p_n = from_north(pressure, pressure_n)
                gu = pressure - roll_e(pressure) - HALF * u * (u_e - u_w) - vu * (u_n - u_s)
                gv = pressure - p_n - uv * (v_e - v_w) - HALF * v * (v_n - v_s)
                gu = jnp.where(mu > kf, gu, ZERO)
                gv = jnp.where(mv > kf, gv, ZERO)
                side_u = (u + gu + VISC_NUMBER * side_u) * factor_u
                side_v = (v + gv + VISC_NUMBER * side_v) * factor_v
                pu[k, m] = linear(side_u)[:, KEEP]
                pv[k, m] = linear(side_v)[:, KEEP]
                out.append((pressure + step, pressure_n + step_n, gu_sum + gu, gv_sum + gv, side_u, side_v))
            return tuple(out)

        return level

    zero = jnp.zeros((ROWS, PADDED), F32)
    zero_row = jnp.zeros((1, PADDED), F32)
    members = ((zero, zero_row, zero, zero, zero, zero),) * 2
    for i in range(chunks):
        if i > 0:
            wait_columns(i)
        mark("insert")
        insert_columns(i)

        mark("row_wait")
        @pl.when(has_n)
        def _():
            south_copy(i).wait_recv()
            corner_u(i).wait_recv()

        @pl.when(has_s)
        def _():
            north_copy(i).wait_recv()
            corner_v(i).wait_recv()

        mark("momentum")
        unpack_rows(i)
        members = lax.fori_loop(0, size, momentum(i), members, unroll=UNROLL)

        mark("next")
        if i == 0:
            for copy in edge_copies:
                copy.wait()
            for p in range(7):
                wide[p, own, :] = with_edges(wide[p, own, :], edge_e[p], edge_w[p])
            static_copies = spread(wide, 0)
            start_spread(static_copies)

    mark("force")
    relay_spread(static_copies)
    count_u = linear(jnp.maximum(mu, 1.0))
    count_v = linear(jnp.maximum(mv, 1.0))
    for m in PAIR:
        wide_f[m, own, :] = linear(members[m][2]) / count_u
        wide_f[2 + m, own, :] = linear(members[m][3]) / count_v
    force_edges = edge_pair(wide_f, fedge_w, fedge_e, 3)
    for copy in force_edges:
        copy.start()

    def tracers(i, carry):
        def level(j, carry):
            k = i * size + j
            factor = solve_factor(kmt2, k, 3)
            out = []
            for m in PAIR:
                at = pl.ds(2 * j + m, 1)
                u, v = (HALF * both((first, second), k, m, f) for f in PAIR)
                u_w = roll_w(u)
                v_edge = HALF * edge(rows_s, tail_s, 1, i, at)
                for f, dest in ((2, pt), (3, ps)):
                    t = both((first, second), k, m, f)
                    flux_x = u * (t + roll_e(t)) - u_w * (t + roll_w(t))
                    flux_y = v * (t + from_north(t, edge(rows_n, tail_n, f, i, at)))
                    flux_s = v_edge * (edge(rows_s, tail_s, f, i, at) + t[0:1])
                    moved = t - (flux_x + flux_y - from_south(flux_y, flux_s))
                    side = (moved + DIFF_NUMBER * carry[len(out)]) * factor
                    dest[k, m] = linear(side)[:, KEEP]
                    out.append(side)
            return tuple(out)

        return lax.fori_loop(0, size, level, carry, unroll=UNROLL)

    mark("tracer_1")
    tail = (zero,) * 4
    split = (3 * chunks + 4) // 5
    tail = lax.fori_loop(0, split, tracers, tail)

    mark("force_edge_wait")
    for copy in force_edges:
        copy.wait()
    mark("force_spread")
    for p in QUAD:
        wide_f[p, own, :] = with_edges(wide_f[p, own, :], fedge_e[p], fedge_w[p])
    force_copies = spread(wide_f, 6)
    start_spread(force_copies)

    mark("tracer_2")
    tail = lax.fori_loop(split, chunks, tracers, tail)

    def back_tracers(j, carry):
        k = K - 2 - j
        ratio = table[5 * K + k]
        out = []
        for m in PAIR:
            for dest in (pt, ps):
                x = dest[k, m] + ratio * carry[len(out)]
                dest[k, m] = x
                out.append(x)
        return tuple(out)

    relay_spread(force_copies)
    mark("back_tracers")
    lax.fori_loop(0, K - 1, back_tracers, tuple(linear(x)[:, KEEP] for x in tail), unroll=2)

    def back(j, carry):
        k = K - 2 - j
        ratio = table[2 * K + k]
        out = []
        for m in PAIR:
            xu, xv, su, sv = carry[m]
            xu = pu[k, m] + ratio * xu
            xv = pv[k, m] + ratio * xv
            pu[k, m] = xu
            pv[k, m] = xv
            out.append((xu, xv, su + xu, sv + xv))
        return tuple(out)

    mark("back_uv")
    start = tuple(tuple(linear(members[m][n])[:, KEEP] for n in (4, 5, 4, 5)) for m in PAIR)
    ends = lax.fori_loop(0, K - 1, back, start)

    mark("static_wait")
    finish_spread(static_copies)
    mark("force_wait")
    finish_spread(force_copies)

    mark("coef")
    depth = wide[0]
    depth_e = pltpu.roll(depth, PADDED - 1, 1)
    depth_n = pltpu.roll(depth, 79, 0)
    hu = jnp.where((depth > ZERO) & (depth_e > ZERO), HALF * (depth + depth_e), ZERO)
    hv = jnp.where((depth > ZERO) & (depth_n > ZERO), HALF * (depth + depth_n), ZERO)
    coef[0] = WAVE_COURANT * WAVE_COURANT * hu
    coef[1] = WAVE_COURANT * WAVE_COURANT * hv
    for m in PAIR:
        force[m] = hu * wide_f[m] * (WAVE_COURANT / SUBCYCLES)
        force[2 + m] = hv * wide_f[2 + m] * (WAVE_COURANT / SUBCYCLES)
        state[m] = wide[1 + m]
        state[2 + m] = WAVE_COURANT * wide[3 + m]
        state[4 + m] = WAVE_COURANT * wide[5 + m]
        state[6 + m] = pltpu.roll(wide[1 + m], PADDED - 1, 1)
    mine = slice(HALO, HALO + ROWS)
    for p, (h, count) in enumerate(((hu[mine], count_u), (hv[mine], count_v))):
        faces[2 + p] = 1.0 / (WAVE_COURANT * jnp.where(h > ZERO, h, 1.0))
        for m in PAIR:
            mean[2 * p + m] = padded(ends[m][2 + p]) / count

    mark("send_wait")
    for i in range(chunks):
        west_copy(i).wait_send()
        east_copy(i).wait_send()

    @pl.when(has_s)
    def _():
        for i in range(chunks):
            south_copy(i).wait_send()
            corner_u(i).wait_send()

    @pl.when(has_n)
    def _():
        for i in range(chunks):
            north_copy(i).wait_send()
            corner_v(i).wait_send()
    mark("")


def finish_kernel(
    K, size,
    weights, pu, pv, pt, ps, mean, faces, coef, force, first_state,
    eta_o, tx_o, ty_o, u_o, v_o, t_o, s_o,
    state, avg, small, out_u, out_v, sems,
):
    chunks = K // size
    through = [pltpu.make_async_copy(src, dst, sems.at[i, 0]) for i, (src, dst) in enumerate(((pt, t_o), (ps, s_o)))]
    for copy in through:
        copy.start()
    state[...] = first_state[...]
    avg[...] = jnp.zeros_like(avg)

    def subcycles(first, last, margin):
        height = ROWS + 2 * margin
        rows = pl.ds(HALO - margin, height)
        mine = slice(margin, margin + ROWS)

        def to_e(x):
            return pltpu.roll(x, PADDED - 1, 1)

        def subcycle(n, _):
            weight = weights[n]
            for m in PAIR:
                tx, ty = state[2 + m, rows], state[4 + m, rows]
                tx_e, ty_e = to_e(tx), to_e(ty)
                eta = state[m, rows] - (tx - pltpu.roll(tx, 1, 1) + ty - pltpu.roll(ty, 1, 0))
                eta_e = state[6 + m, rows] - (tx_e - tx + ty_e - pltpu.roll(ty_e, 1, 0))
                tx = tx + force[m, rows] - coef[0, rows] * (eta_e - eta)
                ty = ty + force[2 + m, rows] - coef[1, rows] * (pltpu.roll(eta, height - 1, 0) - eta)
                for p, x in enumerate((eta, tx, ty)):
                    state[2 * p + m, rows] = x
                    avg[2 * p + m] = avg[2 * p + m] + weight * x[mine]
                state[6 + m, rows] = eta_e
            return 0

        lax.fori_loop(first, last, subcycle, 0)

    done = 0
    for margin in (HALO, 24, ROWS, 8):
        last = SUBCYCLES - (margin - 8)
        subcycles(done, last, margin)
        done = last

    corr = []
    for m in PAIR:
        small[0, m] = avg[m][:, KEEP]
        for p in PAIR:
            transport = avg[2 + 2 * p + m]
            small[1 + p, m] = (transport * (1.0 / WAVE_COURANT))[:, KEEP]
            corr.append((transport * faces[2 + p] - mean[2 * p + m])[:, KEEP])
    for p, dest in enumerate((eta_o, tx_o, ty_o)):
        through.append(pltpu.make_async_copy(small.at[p], dest, sems.at[2, p]))
        through[-1].start()
    depth_u, depth_v = faces[0][:, KEEP], faces[1][:, KEEP]

    def out_copies(i):
        levels = pl.ds(i * size, size)
        return [pltpu.make_async_copy(src.at[levels], dst.at[levels], sems.at[p, 1 + i]) for p, (src, dst) in enumerate(((out_u, u_o), (out_v, v_o)))]

    for i in range(chunks):
        def level(j, _):
            k = i * size + j
            kf = k.astype(F32)
            for m in PAIR:
                out_u[k, m] = jnp.where(depth_u > kf, pu[k, m] + corr[2 * m], ZERO)
                out_v[k, m] = jnp.where(depth_v > kf, pv[k, m] + corr[2 * m + 1], ZERO)
            return 0

        lax.fori_loop(0, size, level, 0, unroll=UNROLL)
        for copy in out_copies(i):
            copy.start()

    for copy in through + [copy for i in range(chunks) for copy in out_copies(i)]:
        copy.wait()


def solution(mesh):
    col_count, row_count = mesh.shape["col"], mesh.shape["row"]

    def local_step(vel_x, vel_y, pot_temp, salinity, surf_eta, trans_x, trans_y, col_depth, wet_levels, avg_weights):
        K = vel_x.shape[0]
        size = level_chunk(K)
        chunks = K // size
        edge_rows = (2 * size + 7) // 8 * 8
        table = jnp.asarray(solve_tables(K))
        smem = pl.BlockSpec(memory_space=pltpu.SMEM)
        vmem = pl.BlockSpec(memory_space=pltpu.VMEM)
        hbm = pl.BlockSpec(memory_space=pl.ANY)
        full = jax.ShapeDtypeStruct((K, 2, ROWS, WIDTH), F32)
        held = pltpu.VMEM((K, 2, ROWS, WIDTH), F32)
        dma = pltpu.SemaphoreType.DMA
        outs = pl.pallas_call(
            functools.partial(step_kernel, row_count, col_count, K),
            out_shape=(held,) * 4 + tuple(pltpu.VMEM((n, ROWS, PADDED), F32) for n in (4, 4)) + tuple(pltpu.VMEM((n, 80, PADDED), F32) for n in (2, 4, 8)),
            in_specs=[smem] + [vmem] * 5 + [hbm] * 4,
            out_specs=(vmem,) * 9,
            scratch_shapes=[
                *[pltpu.VMEM((K * 2 * ROWS, WIDTH), F32)] * 4,
                *[pltpu.VMEM((K * 2 * ROWS, LANES), F32)] * 8,
                *[pltpu.VMEM((chunks, 6, edge_rows, LANES), F32)] * 4,
                *[pltpu.VMEM((chunks, 4, edge_rows, LANES), F32)] * 2,
                *[pltpu.VMEM((chunks, 2, edge_rows, LANES), F32)] * 3,
                pltpu.VMEM((1, WIDTH), jnp.int32),
                *[pltpu.VMEM((chunks, 2, ROWS, LANES), F32)] * 3,
                *[pltpu.VMEM((chunks, 8, LANES), F32)] * 2,
                *[pltpu.VMEM((7, ROWS, LANES), F32)] * 2,
                pltpu.VMEM((7, 80, PADDED), F32),
                *[pltpu.VMEM((4, ROWS, LANES), F32)] * 2,
                pltpu.VMEM((4, 80, PADDED), F32),
                dma((chunks, 4)), dma((2, chunks)), dma((2, chunks)), dma((4, chunks)), dma((4, chunks)), dma((5,)), dma((5,)), dma((12,)), dma((12,)),
            ],
            compiler_params=pltpu.CompilerParams(collective_id=0, has_side_effects=True, vmem_limit_bytes=52 << 20),
            name="ocean_step",
        )(table, wet_levels, col_depth, surf_eta, trans_x, trans_y, *(x.reshape(-1, WIDTH) for x in (vel_x, vel_y, pot_temp, salinity)))

        small = jax.ShapeDtypeStruct((2, ROWS, WIDTH), F32)
        return pl.pallas_call(
            functools.partial(finish_kernel, K, size),
            out_shape=(small,) * 3 + (full,) * 4,
            in_specs=[smem] + [vmem] * 9,
            out_specs=(hbm,) * 7,
            scratch_shapes=[
                pltpu.VMEM((8, 80, PADDED), F32),
                pltpu.VMEM((6, ROWS, PADDED), F32),
                pltpu.VMEM((3, 2, ROWS, WIDTH), F32),
                *[pltpu.VMEM((K, 2, ROWS, WIDTH), F32)] * 2,
                dma((3, 2 + chunks)),
            ],
            compiler_params=pltpu.CompilerParams(vmem_limit_bytes=20 << 20),
            name="ocean_finish",
        )(avg_weights, *outs)

    spec_3d = P(None, None, "row", "col")
    spec_2d = P(None, "row", "col")
    spec_map = P("row", "col")
    return jax.shard_map(local_step, mesh=mesh, in_specs=(spec_3d,) * 4 + (spec_2d,) * 3 + (spec_map,) * 2 + (P(),), out_specs=(spec_2d,) * 3 + (spec_3d,) * 4, check_vma=False)
```

```python
import functools
import numpy as np
import jax
import jax.numpy as jnp
from jax import lax
from jax.experimental import pallas as pl
from jax.experimental.pallas import tpu as pltpu
from jax.sharding import PartitionSpec as P

WAVE_COURANT = 0.4
THERM_EXP = 0.2
HALINE_CON = 0.15
PRESS_SCALE = 0.5
VISC_NUMBER = 1.0
DIFF_NUMBER = 0.5
SUBCYCLES = 30
HALO = 32
PAIR = (0, 1)
QUAD = (0, 1, 2, 3)
ZERO, HALF = 0.0, 0.5
UNROLL = 5
ROWS, WIDTH, PADDED, LANES = 16, 192, 256, 128
LAST, KEEP = LANES - 1, slice(0, WIDTH)
MESH = pl.DeviceIdType.MESH
F32 = jnp.float32


def solve_tables(level_count):
    rows = []
    for strength in (VISC_NUMBER, DIFF_NUMBER):
        inner, last = np.zeros(level_count), np.zeros(level_count)
        inner[0], last[0] = 1.0 + strength, 1.0
        for k in range(1, level_count):
            inner[k] = 1.0 + 2.0 * strength - strength * strength / inner[k - 1]
            last[k] = 1.0 + strength - strength * strength / inner[k - 1]
        rows += [1.0 / inner, 1.0 / last, strength / inner]
    return np.concatenate(rows).astype(np.float32)


def level_chunk(level_count):
    return next(size for size in (15, 5) if level_count % size == 0)


def step_kernel(
    row_count, col_count, level_count,
    table, kmt_in, depth_in, eta_in, tx_in, ty_in, u_hbm, v_hbm, t_hbm, s_hbm,
    pu, pv, pt, ps, mean, faces, coef, force, state,
    raw_u, raw_v, raw_t, raw_s, ua, va, ta, sa, ub, vb, tb, sb, rows_n, rows_s, send_n, send_s, tail_n, tail_s, north_w, south_e, north_h, kmt_n, pack, col_e, col_w, corner_se, corner_nw,
    edge_e, edge_w, wide, fedge_e, fedge_w, wide_f,
    load_sem, row_send, row_recv, col_send, col_recv, misc_send, misc_recv, wide_send, wide_recv,
):
    K = level_count
    open_scope = []

    def mark(name):
        if open_scope:
            open_scope.pop().__exit__(None, None, None)
        if name:
            open_scope.append(jax.named_scope(name))
            open_scope[-1].__enter__()

    size = level_chunk(K)
    chunks = K // size
    r = lax.axis_index("row")
    c = lax.axis_index("col")
    east = lax.rem(c + 1, col_count)
    west = lax.rem(c + col_count - 1, col_count)
    has_n, has_s = r < row_count - 1, r > 0
    has_nn, has_ss = r < row_count - 2, r > 1
    raw, first, second = (raw_u, raw_v, raw_t, raw_s), (ua, va, ta, sa), (ub, vb, tb, sb)

    def one(flag):
        return flag.astype(jnp.int32)

    mark("init")
    def block(k, m):
        return pl.ds(pl.multiple_of((2 * k + m) * ROWS, ROWS), ROWS)

    loads = []
    for i in range(chunks):
        levels = pl.ds(i * size * 2 * ROWS, size * 2 * ROWS)
        group = []
        for f, src in enumerate((u_hbm, v_hbm, t_hbm, s_hbm)):
            group.append(pltpu.make_async_copy(src.at[levels], raw[f].at[levels], load_sem.at[i, f]))
        loads.append(group)
    for group in loads:
        for copy in group:
            copy.start()

    wide[...] = jnp.zeros_like(wide)
    wide_f[...] = jnp.zeros_like(wide_f)

    @pl.when(jnp.logical_not(has_n))
    def _():
        rows_n[...] = jnp.zeros_like(rows_n)
        kmt_n[...] = jnp.zeros_like(kmt_n)
        corner_nw[...] = jnp.zeros_like(corner_nw)

    @pl.when(jnp.logical_not(has_s))
    def _():
        rows_s[...] = jnp.zeros_like(rows_s)
        corner_se[...] = jnp.zeros_like(corner_se)

    barrier = pltpu.get_barrier_semaphore()

    def signal(**where):
        pl.semaphore_signal(barrier, inc=1, device_id=where, device_id_type=MESH)

    signal(col=east)
    signal(col=west)

    @pl.when(has_n)
    def _():
        signal(row=r + 1)
        signal(row=r + 1, col=west)

    @pl.when(has_s)
    def _():
        signal(row=r - 1)
        signal(row=r - 1, col=east)

    @pl.when(has_nn)
    def _():
        signal(row=r + 2)

    @pl.when(has_ss)
    def _():
        signal(row=r - 2)

    def remote(src, dst, ssem, rsem, **where):
        return pltpu.make_async_remote_copy(src_ref=src, dst_ref=dst, send_sem=ssem, recv_sem=rsem, device_id=where, device_id_type=MESH)

    lane = lax.broadcasted_iota(jnp.int32, (ROWS, LANES), 1)
    lane8, lane1 = lane[0:8], lane[0:1]
    sub = lax.broadcasted_iota(jnp.int32, (8, LANES), 0)
    sub2 = lax.broadcasted_iota(jnp.int32, (8, PADDED), 0)

    def padded(x):
        return jnp.concatenate([x, jnp.zeros((x.shape[0], PADDED - WIDTH), x.dtype)], axis=1)

    def overlapped(x):
        a, b = x[:, 0:LANES], x[:, LANES:PADDED]
        return jnp.concatenate([a, jnp.where(lane < 64, b, a)], axis=1)

    def linear(x):
        a, b = x[:, 0:LANES], x[:, LANES:PADDED]
        return jnp.concatenate([jnp.where(lane < 96, a, b), b], axis=1)

    kmt = padded(kmt_in[...]).astype(F32)
    own = pl.ds(HALO, ROWS)
    wide[0, own, :] = jnp.where(kmt > 0.5, padded(depth_in[...]), ZERO)
    for m in PAIR:
        wide[1 + m, own, :] = padded(eta_in[m])
        wide[3 + m, own, :] = padded(tx_in[m])
        wide[5 + m, own, :] = padded(ty_in[m])

    kmt_copy = remote(kmt_in.at[0:1, :], kmt_n, misc_send.at[0], misc_recv.at[0], row=r - 1)

    def south_copy(i):
        return remote(send_s.at[i], rows_n.at[i], row_send.at[0, i], row_recv.at[0, i], row=r - 1)

    def north_copy(i):
        return remote(send_n.at[i], rows_s.at[i], row_send.at[1, i], row_recv.at[1, i], row=r + 1)

    def west_copy(i):
        return remote(pack.at[i], col_e.at[i], col_send.at[0, i], col_recv.at[0, i], col=west)

    def east_copy(i):
        return remote(pack.at[i], col_w.at[i], col_send.at[1, i], col_recv.at[1, i], col=east)

    def corner_v(i):
        return remote(pack.at[i, 0, 8:16, :], corner_se.at[i], col_send.at[2, i], col_recv.at[2, i], row=r + 1, col=west)

    def corner_u(i):
        return remote(pack.at[i, 0, 0:8, :], corner_nw.at[i], col_send.at[3, i], col_recv.at[3, i], row=r - 1, col=east)

    groups = [*range(0, size - 3, 4)] + [size - 4] * (size % 4 > 0)

    def pack_chunk(i):
        for copy in loads[i]:
            copy.wait()

        def collect(j, acc):
            out = []
            here = (lane == j) | (lane == j + 63)
            for f in QUAD:
                for m in PAIR:
                    at = block(i * size + j, m)
                    x = raw[f][at, 0:LANES]
                    first[f][at, :] = x
                    y = jnp.where(lane < 64, padded(raw[f][at, LANES:WIDTH]), x)
                    second[f][at, :] = y
                    out.append(jnp.where(here, pltpu.roll(jnp.where(lane == 0, x, y), j, 1), acc[len(out)]))
            return tuple(out)

        acc = lax.fori_loop(0, size, collect, (jnp.zeros((ROWS, LANES), F32),) * 8, unroll=UNROLL)
        for g in PAIR:
            merged = pltpu.roll(kmt[:, 0:LANES], LAST, 1)
            for n in QUAD:
                low = size * n
                here = (lane >= low) & (lane < low + size) | (lane >= low + 63) & (lane < low + 63 + size)
                merged = jnp.where(here, pltpu.roll(acc[4 * g + n], low, 1), merged)
            pack[i, g] = merged
        for row, dest in ((0, send_s), (15, send_n)):
            for j in groups:
                at, spot = pl.ds((i * size + j) * 2 * ROWS + row, 8, stride=ROWS), pl.ds(2 * j, 8)
                tails = []
                for f in QUAD:
                    dest[i, f, spot, :] = first[f][at, :]
                    tails.append(second[f][at, :])
                for p in PAIR:
                    dest[i, 4 + p, spot, :] = jnp.where(lane8 < 64, tails[2 * p], pltpu.roll(tails[2 * p + 1], 64, 1))

    def start_chunk(i):
        west_copy(i).start()
        east_copy(i).start()

        @pl.when(has_s)
        def _():
            corner_u(i).start()
            south_copy(i).start()

        @pl.when(has_n)
        def _():
            corner_v(i).start()
            north_copy(i).start()

    mark("pack_early")
    def edge_pair(buf, to_east, to_west, sem):
        return [
            remote(buf.at[:, own, 0:LANES], to_west, misc_send.at[sem], misc_recv.at[sem], col=west),
            remote(buf.at[:, own, LANES:PADDED], to_east, misc_send.at[sem + 1], misc_recv.at[sem + 1], col=east),
        ]

    edge_copies = edge_pair(wide, edge_w, edge_e, 1)
    early = 1
    for i in range(early):
        pack_chunk(i)
    mark("barrier_wait")
    pl.semaphore_wait(barrier, 2 + 2 * one(has_n) + 2 * one(has_s) + one(has_nn) + one(has_ss))

    @pl.when(has_s)
    def _():
        kmt_copy.start()

    for i in range(early):
        start_chunk(i)
    for copy in edge_copies:
        copy.start()
    mark("pack_late")
    for i in range(early, chunks):
        pack_chunk(i)
        start_chunk(i)

    def with_edges(x, from_east, from_west):
        b = jnp.where(lane < 64, x[:, LANES:PADDED], jnp.where(lane < 96, pltpu.roll(from_east, 64, 1), pltpu.roll(from_west, 64, 1)))
        return jnp.concatenate([x[:, 0:LANES], b], axis=1)

    def spread(buf, sem):
        even = lax.rem(r, 2) == 0
        odd = jnp.logical_not(even)

        def part(at, to, out, to_sem, row):
            return remote(buf.at[:, pl.ds(at, ROWS), :], buf.at[:, pl.ds(to, ROWS), :], wide_send.at[sem + out], wide_recv.at[sem + to_sem], row=row)

        direct = (
            (has_n, has_s, part(HALO, ROWS, 0, 0, r + 1)),
            (has_s, has_n, part(HALO, 48, 1, 1, r - 1)),
            (has_nn & even, has_ss, part(HALO, 0, 2, 2, r + 2)),
            (has_ss & odd, has_nn, part(HALO, 64, 3, 3, r - 2)),
        )
        relayed = ((has_s & even, part(ROWS, 0, 4, 2, r + 1)), (has_n & odd, part(48, 64, 5, 3, r - 1)))
        return direct, relayed

    def start_spread(copies):
        for there, _, copy in copies[0]:
            @pl.when(there)
            def _():
                copy.start()

    def relay_spread(copies):
        for (_, here, copy), (there, again) in zip(copies[0], copies[1]):
            @pl.when(here)
            def _():
                copy.wait_recv()

            @pl.when(there)
            def _():
                again.start()

    def finish_spread(copies):
        for n, (there, here, copy) in enumerate(copies[0]):
            @pl.when(there)
            def _():
                copy.wait_send()

            if n > 1:
                @pl.when(here)
                def _():
                    copy.wait_recv()

        for there, again in copies[1]:
            @pl.when(there)
            def _():
                again.wait_send()


    def roll_e(x):
        return jnp.concatenate([pltpu.roll(x[:, 0:LANES], LAST, 1), pltpu.roll(x[:, LANES:PADDED], LAST, 1)], axis=1)

    def roll_w(x):
        return jnp.concatenate([pltpu.roll(x[:, 0:LANES], 1, 1), pltpu.roll(x[:, LANES:PADDED], 1, 1)], axis=1)

    def from_north(x, edge):
        low, high = pltpu.roll(x[0:8], 7, 0), pltpu.roll(x[8:16], 7, 0)
        return jnp.concatenate([jnp.where(sub2 == 7, high, low), jnp.where(sub2 == 7, edge, high)], axis=0)

    def from_south(x, edge):
        low, high = pltpu.roll(x[0:8], 1, 0), pltpu.roll(x[8:16], 1, 0)
        return jnp.concatenate([jnp.where(sub2 == 0, edge, low), jnp.where(sub2 == 0, low, high)], axis=0)

    def wait_columns(i):
        west_copy(i).wait_recv()
        east_copy(i).wait_recv()

    def insert_columns(i):
        columns = [jnp.where(lane < 62, col_e[i, g], col_w[i, g]) for g in PAIR]

        def level(j, _):
            k = i * size + j
            for f in QUAD:
                for m in PAIR:
                    place = size * (2 * (f % 2) + m) + j
                    turned = pltpu.roll(columns[f // 2], lax.rem(LANES + 64 - place, LANES), 1)
                    pltpu.store(first[f].at[block(k, m)], turned, mask=lane == LAST)
                    pltpu.store(second[f].at[block(k, m)], turned, mask=lane == 64)
            return 0

        lax.fori_loop(0, size, level, 0, unroll=UNROLL)

    edge_lane = lax.broadcasted_iota(jnp.int32, rows_n.shape[2:], 1)

    def unpack_rows(i):
        for rows, tails in ((rows_n, tail_n), (rows_s, tail_s)):
            for f in QUAD:
                packed = rows[i, 4 + f // 2]
                tails[i, f] = jnp.where(edge_lane < 64, packed if f % 2 == 0 else pltpu.roll(packed, 64, 1), rows[i, f])
        for h, (u, v, t, s) in enumerate(((rows_n.at[i, 0], rows_s.at[i, 1], rows_n.at[i, 2], rows_n.at[i, 3]), (tail_n.at[i, 0], tail_s.at[i, 1], tail_n.at[i, 2], tail_n.at[i, 3]))):
            u, v = u[...], v[...]
            north_w[i, h] = u + pltpu.roll(u, 1, 1)
            south_e[i, h] = v + pltpu.roll(v, LAST, 1)
            north_h[i, h] = (half_scale * HALINE_CON) * s[...] - (half_scale * THERM_EXP) * t[...]

    half_scale = HALF * PRESS_SCALE / K

    def both(tiles, k, m, f):
        return jnp.concatenate([tiles[0][f][block(k, m), :], tiles[1][f][block(k, m), :]], axis=1)

    def edge(rows, tails, f, i, at):
        return jnp.concatenate([rows[i, f, at, :], tails[i, f, at, :]], axis=1)

    mark("column_wait")
    wait_columns(0)

    @pl.when(has_n)
    def _():
        kmt_copy.wait_recv()

    @pl.when(has_s)
    def _():
        kmt_copy.wait_send()

    mark("masks")
    kmt2 = overlapped(kmt)
    kmt_edge = jnp.where(lane == 64, pltpu.roll(col_e[0, 0], 65, 1), kmt2[:, LANES:PADDED])
    kmt_row = padded(kmt_n[...]).astype(F32)
    kmt_north = jnp.concatenate([kmt_row[:, 0:LANES], jnp.where(lane1 < 64, kmt_row[:, LANES:PADDED], kmt_row[:, 0:LANES])], axis=1)
    mu = jnp.minimum(kmt2, roll_e(jnp.concatenate([kmt2[:, 0:LANES], kmt_edge], axis=1)))
    mv = jnp.minimum(kmt2, from_north(kmt2, kmt_north))
    faces[0] = linear(mu)
    faces[1] = linear(mv)

    def solve_factor(depth, k, first):
        inner, last = table[first * K + k], table[(first + 1) * K + k]
        kf = k.astype(F32)
        return jnp.where(depth > kf + 1.0, inner, jnp.where(depth > kf, last, ZERO))

    def momentum(i):
        def level(j, members):
            k = i * size + j
            kf = k.astype(F32)
            factor_u, factor_v = solve_factor(mu, k, 0), solve_factor(mv, k, 0)
            out = []
            for m in PAIR:
                total, total_n, gu_sum, gv_sum, side_u, side_v = members[m]
                at = pl.ds(2 * j + m, 1)
                u, v, t, s = (both((first, second), k, m, f) for f in QUAD)
                step = (half_scale * HALINE_CON) * s - (half_scale * THERM_EXP) * t
                pressure = total + step
                step_n = jnp.concatenate([north_h[i, 0, at, :], north_h[i, 1, at, :]], axis=1)
                pressure_n = total_n + step_n
                corner_n = pltpu.roll(corner_nw[i], 65 - (size * m + j), 1)[0:1]
                corner_s = pltpu.roll(corner_se[i], lax.rem(LANES + 63 - (size * (2 + m) + j), LANES), 1)[7:8]
                u_edge, v_edge = edge(rows_n, tail_n, 0, i, at), edge(rows_s, tail_s, 1, i, at)
                u_pair_n = jnp.concatenate([jnp.where(lane1 == 0, u_edge[:, 0:LANES] + corner_n, north_w[i, 0, at, :]), north_w[i, 1, at, :]], axis=1)
                v_pair_s = jnp.concatenate([south_e[i, 0, at, :], jnp.where(lane1 == 63, v_edge[:, LANES:PADDED] + corner_s, south_e[i, 1, at, :])], axis=1)
                v_e, v_w, u_e, u_w = roll_e(v), roll_w(v), roll_e(u), roll_w(u)
                v_pair, u_pair = v + v_e, u + u_w
                vu = 0.125 * (v_pair + from_south(v_pair, v_pair_s))
                uv = 0.125 * (u_pair + from_north(u_pair, u_pair_n))
                u_n, u_s = from_north(u, u_edge), from_south(u, edge(rows_s, tail_s, 0, i, at))
                v_n, v_s = from_north(v, edge(rows_n, tail_n, 1, i, at)), from_south(v, v_edge)
                p_n = from_north(pressure, pressure_n)
                gu = pressure - roll_e(pressure) - HALF * u * (u_e - u_w) - vu * (u_n - u_s)
                gv = pressure - p_n - uv * (v_e - v_w) - HALF * v * (v_n - v_s)
                gu = jnp.where(mu > kf, gu, ZERO)
                gv = jnp.where(mv > kf, gv, ZERO)
                side_u = (u + gu + VISC_NUMBER * side_u) * factor_u
                side_v = (v + gv + VISC_NUMBER * side_v) * factor_v
                pu[k, m] = linear(side_u)[:, KEEP]
                pv[k, m] = linear(side_v)[:, KEEP]
                out.append((pressure + step, pressure_n + step_n, gu_sum + gu, gv_sum + gv, side_u, side_v))
            return tuple(out)

        return level

    zero = jnp.zeros((ROWS, PADDED), F32)
    zero_row = jnp.zeros((1, PADDED), F32)
    members = ((zero, zero_row, zero, zero, zero, zero),) * 2
    for i in range(chunks):
        if i > 0:
            wait_columns(i)
        mark("insert")
        insert_columns(i)

        mark("row_wait")
        @pl.when(has_n)
        def _():
            south_copy(i).wait_recv()
            corner_u(i).wait_recv()

        @pl.when(has_s)
        def _():
            north_copy(i).wait_recv()
            corner_v(i).wait_recv()

        mark("momentum")
        unpack_rows(i)
        members = lax.fori_loop(0, size, momentum(i), members, unroll=UNROLL)

        mark("next")
        if i == 0:
            for copy in edge_copies:
                copy.wait()
            for p in range(7):
                wide[p, own, :] = with_edges(wide[p, own, :], edge_e[p], edge_w[p])
            static_copies = spread(wide, 0)
            start_spread(static_copies)

    mark("force")
    count_u = linear(jnp.maximum(mu, 1.0))
    count_v = linear(jnp.maximum(mv, 1.0))
    for m in PAIR:
        wide_f[m, own, :] = linear(members[m][2]) / count_u
        wide_f[2 + m, own, :] = linear(members[m][3]) / count_v
    force_edges = edge_pair(wide_f, fedge_w, fedge_e, 3)
    for copy in force_edges:
        copy.start()

    def tracers(i, carry):
        def level(j, carry):
            k = i * size + j
            factor = solve_factor(kmt2, k, 3)
            out = []
            for m in PAIR:
                at = pl.ds(2 * j + m, 1)
                u, v = (HALF * both((first, second), k, m, f) for f in PAIR)
                u_w = roll_w(u)
                v_edge = HALF * edge(rows_s, tail_s, 1, i, at)
                for f, dest in ((2, pt), (3, ps)):
                    t = both((first, second), k, m, f)
                    flux_x = u * (t + roll_e(t)) - u_w * (t + roll_w(t))
                    flux_y = v * (t + from_north(t, edge(rows_n, tail_n, f, i, at)))
                    flux_s = v_edge * (edge(rows_s, tail_s, f, i, at) + t[0:1])
                    moved = t - (flux_x + flux_y - from_south(flux_y, flux_s))
                    side = (moved + DIFF_NUMBER * carry[len(out)]) * factor
                    dest[k, m] = linear(side)[:, KEEP]
                    out.append(side)
            return tuple(out)

        return lax.fori_loop(0, size, level, carry, unroll=UNROLL)

    mark("tracer_1")
    tail = (zero,) * 4
    split = (3 * chunks + 4) // 5
    tail = lax.fori_loop(0, split, tracers, tail)

    mark("static_relay")
    relay_spread(static_copies)
    mark("force_edge_wait")
    for copy in force_edges:
        copy.wait()
    mark("force_spread")
    for p in QUAD:
        wide_f[p, own, :] = with_edges(wide_f[p, own, :], fedge_e[p], fedge_w[p])
    force_copies = spread(wide_f, 6)
    start_spread(force_copies)

    mark("tracer_2")
    tail = lax.fori_loop(split, chunks, tracers, tail)

    def back_tracers(j, carry):
        k = K - 2 - j
        ratio = table[5 * K + k]
        out = []
        for m in PAIR:
            for dest in (pt, ps):
                x = dest[k, m] + ratio * carry[len(out)]
                dest[k, m] = x
                out.append(x)
        return tuple(out)

    mark("back_tracers")
    lax.fori_loop(0, K - 1, back_tracers, tuple(linear(x)[:, KEEP] for x in tail), unroll=2)

    def back(j, carry):
        k = K - 2 - j
        ratio = table[2 * K + k]
        out = []
        for m in PAIR:
            xu, xv, su, sv = carry[m]
            xu = pu[k, m] + ratio * xu
            xv = pv[k, m] + ratio * xv
            pu[k, m] = xu
            pv[k, m] = xv
            out.append((xu, xv, su + xu, sv + xv))
        return tuple(out)

    mark("relay")
    relay_spread(force_copies)
    mark("back_uv")
    start = tuple(tuple(linear(members[m][n])[:, KEEP] for n in (4, 5, 4, 5)) for m in PAIR)
    ends = lax.fori_loop(0, K - 1, back, start)

    mark("static_wait")
    finish_spread(static_copies)
    mark("force_wait")
    finish_spread(force_copies)

    mark("coef")
    depth = wide[0]
    depth_e = pltpu.roll(depth, PADDED - 1, 1)
    depth_n = pltpu.roll(depth, 79, 0)
    hu = jnp.where((depth > ZERO) & (depth_e > ZERO), HALF * (depth + depth_e), ZERO)
    hv = jnp.where((depth > ZERO) & (depth_n > ZERO), HALF * (depth + depth_n), ZERO)
    coef[0] = WAVE_COURANT * WAVE_COURANT * hu
    coef[1] = WAVE_COURANT * WAVE_COURANT * hv
    for m in PAIR:
        force[m] = hu * wide_f[m] * (WAVE_COURANT / SUBCYCLES)
        force[2 + m] = hv * wide_f[2 + m] * (WAVE_COURANT / SUBCYCLES)
        state[m] = wide[1 + m]
        state[2 + m] = WAVE_COURANT * wide[3 + m]
        state[4 + m] = WAVE_COURANT * wide[5 + m]
        state[6 + m] = pltpu.roll(wide[1 + m], PADDED - 1, 1)
    mine = slice(HALO, HALO + ROWS)
    for p, (h, count) in enumerate(((hu[mine], count_u), (hv[mine], count_v))):
        faces[2 + p] = 1.0 / (WAVE_COURANT * jnp.where(h > ZERO, h, 1.0))
        for m in PAIR:
            mean[2 * p + m] = padded(ends[m][2 + p]) / count

    mark("send_wait")
    for i in range(chunks):
        west_copy(i).wait_send()
        east_copy(i).wait_send()

    @pl.when(has_s)
    def _():
        for i in range(chunks):
            south_copy(i).wait_send()
            corner_u(i).wait_send()

    @pl.when(has_n)
    def _():
        for i in range(chunks):
            north_copy(i).wait_send()
            corner_v(i).wait_send()
    mark("")


def finish_kernel(
    K, size,
    weights, pu, pv, pt, ps, mean, faces, coef, force, first_state,
    eta_o, tx_o, ty_o, u_o, v_o, t_o, s_o,
    state, avg, small, out_u, out_v, sems,
):
    chunks = K // size
    through = [pltpu.make_async_copy(src, dst, sems.at[i, 0]) for i, (src, dst) in enumerate(((pt, t_o), (ps, s_o)))]
    for copy in through:
        copy.start()
    state[...] = first_state[...]
    avg[...] = jnp.zeros_like(avg)

    def subcycles(first, last, margin):
        height = ROWS + 2 * margin
        rows = pl.ds(HALO - margin, height)
        mine = slice(margin, margin + ROWS)

        def to_e(x):
            return pltpu.roll(x, PADDED - 1, 1)

        def subcycle(n, _):
            weight = weights[n]
            for m in PAIR:
                tx, ty = state[2 + m, rows], state[4 + m, rows]
                tx_e, ty_e = to_e(tx), to_e(ty)
                eta = state[m, rows] - (tx - pltpu.roll(tx, 1, 1) + ty - pltpu.roll(ty, 1, 0))
                eta_e = state[6 + m, rows] - (tx_e - tx + ty_e - pltpu.roll(ty_e, 1, 0))
                tx = tx + force[m, rows] - coef[0, rows] * (eta_e - eta)
                ty = ty + force[2 + m, rows] - coef[1, rows] * (pltpu.roll(eta, height - 1, 0) - eta)
                for p, x in enumerate((eta, tx, ty)):
                    state[2 * p + m, rows] = x
                    avg[2 * p + m] = avg[2 * p + m] + weight * x[mine]
                state[6 + m, rows] = eta_e
            return 0

        lax.fori_loop(first, last, subcycle, 0)

    done = 0
    for margin in (HALO, 24, ROWS, 8):
        last = SUBCYCLES - (margin - 8)
        subcycles(done, last, margin)
        done = last

    corr = []
    for m in PAIR:
        small[0, m] = avg[m][:, KEEP]
        for p in PAIR:
            transport = avg[2 + 2 * p + m]
            small[1 + p, m] = (transport * (1.0 / WAVE_COURANT))[:, KEEP]
            corr.append((transport * faces[2 + p] - mean[2 * p + m])[:, KEEP])
    for p, dest in enumerate((eta_o, tx_o, ty_o)):
        through.append(pltpu.make_async_copy(small.at[p], dest, sems.at[2, p]))
        through[-1].start()
    depth_u, depth_v = faces[0][:, KEEP], faces[1][:, KEEP]

    def out_copies(i):
        levels = pl.ds(i * size, size)
        return [pltpu.make_async_copy(src.at[levels], dst.at[levels], sems.at[p, 1 + i]) for p, (src, dst) in enumerate(((out_u, u_o), (out_v, v_o)))]

    for i in range(chunks):
        def level(j, _):
            k = i * size + j
            kf = k.astype(F32)
            for m in PAIR:
                out_u[k, m] = jnp.where(depth_u > kf, pu[k, m] + corr[2 * m], ZERO)
                out_v[k, m] = jnp.where(depth_v > kf, pv[k, m] + corr[2 * m + 1], ZERO)
            return 0

        lax.fori_loop(0, size, level, 0, unroll=UNROLL)
        for copy in out_copies(i):
            copy.start()

    for copy in through + [copy for i in range(chunks) for copy in out_copies(i)]:
        copy.wait()


def solution(mesh):
    col_count, row_count = mesh.shape["col"], mesh.shape["row"]

    def local_step(vel_x, vel_y, pot_temp, salinity, surf_eta, trans_x, trans_y, col_depth, wet_levels, avg_weights):
        K = vel_x.shape[0]
        size = level_chunk(K)
        chunks = K // size
        edge_rows = (2 * size + 7) // 8 * 8
        table = jnp.asarray(solve_tables(K))
        smem = pl.BlockSpec(memory_space=pltpu.SMEM)
        vmem = pl.BlockSpec(memory_space=pltpu.VMEM)
        hbm = pl.BlockSpec(memory_space=pl.ANY)
        full = jax.ShapeDtypeStruct((K, 2, ROWS, WIDTH), F32)
        held = pltpu.VMEM((K, 2, ROWS, WIDTH), F32)
        dma = pltpu.SemaphoreType.DMA
        outs = pl.pallas_call(
            functools.partial(step_kernel, row_count, col_count, K),
            out_shape=(held,) * 4 + tuple(pltpu.VMEM((n, ROWS, PADDED), F32) for n in (4, 4)) + tuple(pltpu.VMEM((n, 80, PADDED), F32) for n in (2, 4, 8)),
            in_specs=[smem] + [vmem] * 5 + [hbm] * 4,
            out_specs=(vmem,) * 9,
            scratch_shapes=[
                *[pltpu.VMEM((K * 2 * ROWS, WIDTH), F32)] * 4,
                *[pltpu.VMEM((K * 2 * ROWS, LANES), F32)] * 8,
                *[pltpu.VMEM((chunks, 6, edge_rows, LANES), F32)] * 4,
                *[pltpu.VMEM((chunks, 4, edge_rows, LANES), F32)] * 2,
                *[pltpu.VMEM((chunks, 2, edge_rows, LANES), F32)] * 3,
                pltpu.VMEM((1, WIDTH), jnp.int32),
                *[pltpu.VMEM((chunks, 2, ROWS, LANES), F32)] * 3,
                *[pltpu.VMEM((chunks, 8, LANES), F32)] * 2,
                *[pltpu.VMEM((7, ROWS, LANES), F32)] * 2,
                pltpu.VMEM((7, 80, PADDED), F32),
                *[pltpu.VMEM((4, ROWS, LANES), F32)] * 2,
                pltpu.VMEM((4, 80, PADDED), F32),
                dma((chunks, 4)), dma((2, chunks)), dma((2, chunks)), dma((4, chunks)), dma((4, chunks)), dma((5,)), dma((5,)), dma((12,)), dma((12,)),
            ],
            compiler_params=pltpu.CompilerParams(collective_id=0, has_side_effects=True, vmem_limit_bytes=52 << 20),
            name="ocean_step",
        )(table, wet_levels, col_depth, surf_eta, trans_x, trans_y, *(x.reshape(-1, WIDTH) for x in (vel_x, vel_y, pot_temp, salinity)))

        small = jax.ShapeDtypeStruct((2, ROWS, WIDTH), F32)
        return pl.pallas_call(
            functools.partial(finish_kernel, K, size),
            out_shape=(small,) * 3 + (full,) * 4,
            in_specs=[smem] + [vmem] * 9,
            out_specs=(hbm,) * 7,
            scratch_shapes=[
                pltpu.VMEM((8, 80, PADDED), F32),
                pltpu.VMEM((6, ROWS, PADDED), F32),
                pltpu.VMEM((3, 2, ROWS, WIDTH), F32),
                *[pltpu.VMEM((K, 2, ROWS, WIDTH), F32)] * 2,
                dma((3, 2 + chunks)),
            ],
            compiler_params=pltpu.CompilerParams(vmem_limit_bytes=20 << 20),
            name="ocean_finish",
        )(avg_weights, *outs)

    spec_3d = P(None, None, "row", "col")
    spec_2d = P(None, "row", "col")
    spec_map = P("row", "col")
    return jax.shard_map(local_step, mesh=mesh, in_specs=(spec_3d,) * 4 + (spec_2d,) * 3 + (spec_map,) * 2 + (P(),), out_specs=(spec_2d,) * 3 + (spec_3d,) * 4, check_vma=False)
```

```python
import functools
import numpy as np
import jax
import jax.numpy as jnp
from jax import lax
from jax.experimental import pallas as pl
from jax.experimental.pallas import tpu as pltpu
from jax.sharding import PartitionSpec as P

WAVE_COURANT = 0.4
THERM_EXP = 0.2
HALINE_CON = 0.15
PRESS_SCALE = 0.5
VISC_NUMBER = 1.0
DIFF_NUMBER = 0.5
SUBCYCLES = 30
HALO = 32
PAIR = (0, 1)
QUAD = (0, 1, 2, 3)
ZERO, HALF = 0.0, 0.5
UNROLL = 5
ROWS, WIDTH, PADDED, LANES = 16, 192, 256, 128
LAST, KEEP = LANES - 1, slice(0, WIDTH)
MESH = pl.DeviceIdType.MESH
F32 = jnp.float32


def solve_tables(level_count):
    rows = []
    for strength in (VISC_NUMBER, DIFF_NUMBER):
        inner, last = np.zeros(level_count), np.zeros(level_count)
        inner[0], last[0] = 1.0 + strength, 1.0
        for k in range(1, level_count):
            inner[k] = 1.0 + 2.0 * strength - strength * strength / inner[k - 1]
            last[k] = 1.0 + strength - strength * strength / inner[k - 1]
        rows += [1.0 / inner, 1.0 / last, strength / inner]
    return np.concatenate(rows).astype(np.float32)


def level_chunk(level_count):
    return next(size for size in (15, 5) if level_count % size == 0)


def step_kernel(
    row_count, col_count, level_count,
    table, kmt_in, depth_in, eta_in, tx_in, ty_in, u_hbm, v_hbm, t_hbm, s_hbm,
    pu, pv, pt, ps, mean, faces, coef, force, state,
    raw_u, raw_v, raw_t, raw_s, ua, va, ta, sa, ub, vb, tb, sb, rows_n, rows_s, send_n, send_s, tail_n, tail_s, north_w, south_e, north_h, kmt_n, pack, col_e, col_w, corner_se, corner_nw,
    edge_e, edge_w, wide, fedge_e, fedge_w, wide_f,
    load_sem, row_send, row_recv, col_send, col_recv, misc_send, misc_recv, wide_send, wide_recv,
):
    K = level_count
    size = level_chunk(K)
    chunks = K // size
    r = lax.axis_index("row")
    c = lax.axis_index("col")
    east = lax.rem(c + 1, col_count)
    west = lax.rem(c + col_count - 1, col_count)
    has_n, has_s = r < row_count - 1, r > 0
    has_nn, has_ss = r < row_count - 2, r > 1
    raw, first, second = (raw_u, raw_v, raw_t, raw_s), (ua, va, ta, sa), (ub, vb, tb, sb)

    def one(flag):
        return flag.astype(jnp.int32)

    def block(k, m):
        return pl.ds(pl.multiple_of((2 * k + m) * ROWS, ROWS), ROWS)

    loads = []
    for i in range(chunks):
        levels = pl.ds(i * size * 2 * ROWS, size * 2 * ROWS)
        group = []
        for f, src in enumerate((u_hbm, v_hbm, t_hbm, s_hbm)):
            group.append(pltpu.make_async_copy(src.at[levels], raw[f].at[levels], load_sem.at[i, f]))
        loads.append(group)
    for group in loads:
        for copy in group:
            copy.start()

    wide[...] = jnp.zeros_like(wide)
    wide_f[...] = jnp.zeros_like(wide_f)

    @pl.when(jnp.logical_not(has_n))
    def _():
        rows_n[...] = jnp.zeros_like(rows_n)
        kmt_n[...] = jnp.zeros_like(kmt_n)
        corner_nw[...] = jnp.zeros_like(corner_nw)

    @pl.when(jnp.logical_not(has_s))
    def _():
        rows_s[...] = jnp.zeros_like(rows_s)
        corner_se[...] = jnp.zeros_like(corner_se)

    barrier = pltpu.get_barrier_semaphore()

    def signal(**where):
        pl.semaphore_signal(barrier, inc=1, device_id=where, device_id_type=MESH)

    signal(col=east)
    signal(col=west)

    @pl.when(has_n)
    def _():
        signal(row=r + 1)
        signal(row=r + 1, col=west)

    @pl.when(has_s)
    def _():
        signal(row=r - 1)
        signal(row=r - 1, col=east)

    @pl.when(has_nn)
    def _():
        signal(row=r + 2)

    @pl.when(has_ss)
    def _():
        signal(row=r - 2)

    def remote(src, dst, ssem, rsem, **where):
        return pltpu.make_async_remote_copy(src_ref=src, dst_ref=dst, send_sem=ssem, recv_sem=rsem, device_id=where, device_id_type=MESH)

    lane = lax.broadcasted_iota(jnp.int32, (ROWS, LANES), 1)
    lane8, lane1 = lane[0:8], lane[0:1]
    sub = lax.broadcasted_iota(jnp.int32, (8, LANES), 0)
    sub2 = lax.broadcasted_iota(jnp.int32, (8, PADDED), 0)

    def padded(x):
        return jnp.concatenate([x, jnp.zeros((x.shape[0], PADDED - WIDTH), x.dtype)], axis=1)

    def overlapped(x):
        a, b = x[:, 0:LANES], x[:, LANES:PADDED]
        return jnp.concatenate([a, jnp.where(lane < 64, b, a)], axis=1)

    def linear(x):
        a, b = x[:, 0:LANES], x[:, LANES:PADDED]
        return jnp.concatenate([jnp.where(lane < 96, a, b), b], axis=1)

    kmt = padded(kmt_in[...]).astype(F32)
    own = pl.ds(HALO, ROWS)
    wide[0, own, :] = jnp.where(kmt > 0.5, padded(depth_in[...]), ZERO)
    for m in PAIR:
        wide[1 + m, own, :] = padded(eta_in[m])
        wide[3 + m, own, :] = padded(tx_in[m])
        wide[5 + m, own, :] = padded(ty_in[m])

    kmt_copy = remote(kmt_in.at[0:1, :], kmt_n, misc_send.at[0], misc_recv.at[0], row=r - 1)

    def south_copy(i):
        return remote(send_s.at[i], rows_n.at[i], row_send.at[0, i], row_recv.at[0, i], row=r - 1)

    def north_copy(i):
        return remote(send_n.at[i], rows_s.at[i], row_send.at[1, i], row_recv.at[1, i], row=r + 1)

    def west_copy(i):
        return remote(pack.at[i], col_e.at[i], col_send.at[0, i], col_recv.at[0, i], col=west)

    def east_copy(i):
        return remote(pack.at[i], col_w.at[i], col_send.at[1, i], col_recv.at[1, i], col=east)

    def corner_v(i):
        return remote(pack.at[i, 0, 8:16, :], corner_se.at[i], col_send.at[2, i], col_recv.at[2, i], row=r + 1, col=west)

    def corner_u(i):
        return remote(pack.at[i, 0, 0:8, :], corner_nw.at[i], col_send.at[3, i], col_recv.at[3, i], row=r - 1, col=east)

    groups = [*range(0, size - 3, 4)] + [size - 4] * (size % 4 > 0)

    def pack_chunk(i):
        for copy in loads[i]:
            copy.wait()

        def collect(j, acc):
            out = []
            here = (lane == j) | (lane == j + 63)
            for f in QUAD:
                for m in PAIR:
                    at = block(i * size + j, m)
                    x = raw[f][at, 0:LANES]
                    first[f][at, :] = x
                    y = jnp.where(lane < 64, padded(raw[f][at, LANES:WIDTH]), x)
                    second[f][at, :] = y
                    out.append(jnp.where(here, pltpu.roll(jnp.where(lane == 0, x, y), j, 1), acc[len(out)]))
            return tuple(out)

        acc = lax.fori_loop(0, size, collect, (jnp.zeros((ROWS, LANES), F32),) * 8, unroll=UNROLL)
        for g in PAIR:
            merged = pltpu.roll(kmt[:, 0:LANES], LAST, 1)
            for n in QUAD:
                low = size * n
                here = (lane >= low) & (lane < low + size) | (lane >= low + 63) & (lane < low + 63 + size)
                merged = jnp.where(here, pltpu.roll(acc[4 * g + n], low, 1), merged)
            pack[i, g] = merged
        for row, dest in ((0, send_s), (15, send_n)):
            for j in groups:
                at, spot = pl.ds((i * size + j) * 2 * ROWS + row, 8, stride=ROWS), pl.ds(2 * j, 8)
                tails = []
                for f in QUAD:
                    dest[i, f, spot, :] = first[f][at, :]
                    tails.append(second[f][at, :])
                for p in PAIR:
                    dest[i, 4 + p, spot, :] = jnp.where(lane8 < 64, tails[2 * p], pltpu.roll(tails[2 * p + 1], 64, 1))

    def start_chunk(i):
        west_copy(i).start()
        east_copy(i).start()

        @pl.when(has_s)
        def _():
            corner_u(i).start()
            south_copy(i).start()

        @pl.when(has_n)
        def _():
            corner_v(i).start()
            north_copy(i).start()

    def edge_pair(buf, to_east, to_west, sem):
        return [
            remote(buf.at[:, own, 0:LANES], to_west, misc_send.at[sem], misc_recv.at[sem], col=west),
            remote(buf.at[:, own, LANES:PADDED], to_east, misc_send.at[sem + 1], misc_recv.at[sem + 1], col=east),
        ]

    edge_copies = edge_pair(wide, edge_w, edge_e, 1)
    early = 1
    for i in range(early):
        pack_chunk(i)
    pl.semaphore_wait(barrier, 2 + 2 * one(has_n) + 2 * one(has_s) + one(has_nn) + one(has_ss))

    @pl.when(has_s)
    def _():
        kmt_copy.start()

    for i in range(early):
        start_chunk(i)
    for copy in edge_copies:
        copy.start()
    for i in range(early, chunks):
        pack_chunk(i)
        start_chunk(i)

    def with_edges(x, from_east, from_west):
        b = jnp.where(lane < 64, x[:, LANES:PADDED], jnp.where(lane < 96, pltpu.roll(from_east, 64, 1), pltpu.roll(from_west, 64, 1)))
        return jnp.concatenate([x[:, 0:LANES], b], axis=1)

    def spread(buf, sem):
        even = lax.rem(r, 2) == 0
        odd = jnp.logical_not(even)

        def part(at, to, out, to_sem, row):
            return remote(buf.at[:, pl.ds(at, ROWS), :], buf.at[:, pl.ds(to, ROWS), :], wide_send.at[sem + out], wide_recv.at[sem + to_sem], row=row)

        direct = (
            (has_n, has_s, part(HALO, ROWS, 0, 0, r + 1)),
            (has_s, has_n, part(HALO, 48, 1, 1, r - 1)),
            (has_nn & even, has_ss, part(HALO, 0, 2, 2, r + 2)),
            (has_ss & odd, has_nn, part(HALO, 64, 3, 3, r - 2)),
        )
        relayed = ((has_s & even, part(ROWS, 0, 4, 2, r + 1)), (has_n & odd, part(48, 64, 5, 3, r - 1)))
        return direct, relayed

    def start_spread(copies):
        for there, _, copy in copies[0]:
            @pl.when(there)
            def _():
                copy.start()

    def relay_spread(copies):
        for (_, here, copy), (there, again) in zip(copies[0], copies[1]):
            @pl.when(here)
            def _():
                copy.wait_recv()

            @pl.when(there)
            def _():
                again.start()

    def finish_spread(copies):
        for n, (there, here, copy) in enumerate(copies[0]):
            @pl.when(there)
            def _():
                copy.wait_send()

            if n > 1:
                @pl.when(here)
                def _():
                    copy.wait_recv()

        for there, again in copies[1]:
            @pl.when(there)
            def _():
                again.wait_send()


    def roll_e(x):
        return jnp.concatenate([pltpu.roll(x[:, 0:LANES], LAST, 1), pltpu.roll(x[:, LANES:PADDED], LAST, 1)], axis=1)

    def roll_w(x):
        return jnp.concatenate([pltpu.roll(x[:, 0:LANES], 1, 1), pltpu.roll(x[:, LANES:PADDED], 1, 1)], axis=1)

    def from_north(x, edge):
        low, high = pltpu.roll(x[0:8], 7, 0), pltpu.roll(x[8:16], 7, 0)
        return jnp.concatenate([jnp.where(sub2 == 7, high, low), jnp.where(sub2 == 7, edge, high)], axis=0)

    def from_south(x, edge):
        low, high = pltpu.roll(x[0:8], 1, 0), pltpu.roll(x[8:16], 1, 0)
        return jnp.concatenate([jnp.where(sub2 == 0, edge, low), jnp.where(sub2 == 0, low, high)], axis=0)

    def wait_columns(i):
        west_copy(i).wait_recv()
        east_copy(i).wait_recv()

    def insert_columns(i):
        columns = [jnp.where(lane < 62, col_e[i, g], col_w[i, g]) for g in PAIR]

        def level(j, _):
            k = i * size + j
            for f in QUAD:
                for m in PAIR:
                    place = size * (2 * (f % 2) + m) + j
                    turned = pltpu.roll(columns[f // 2], lax.rem(LANES + 64 - place, LANES), 1)
                    pltpu.store(first[f].at[block(k, m)], turned, mask=lane == LAST)
                    pltpu.store(second[f].at[block(k, m)], turned, mask=lane == 64)
            return 0

        lax.fori_loop(0, size, level, 0, unroll=UNROLL)

    edge_lane = lax.broadcasted_iota(jnp.int32, rows_n.shape[2:], 1)

    def unpack_rows(i):
        for rows, tails in ((rows_n, tail_n), (rows_s, tail_s)):
            for f in QUAD:
                packed = rows[i, 4 + f // 2]
                tails[i, f] = jnp.where(edge_lane < 64, packed if f % 2 == 0 else pltpu.roll(packed, 64, 1), rows[i, f])
        for h, (u, v, t, s) in enumerate(((rows_n.at[i, 0], rows_s.at[i, 1], rows_n.at[i, 2], rows_n.at[i, 3]), (tail_n.at[i, 0], tail_s.at[i, 1], tail_n.at[i, 2], tail_n.at[i, 3]))):
            u, v = u[...], v[...]
            north_w[i, h] = u + pltpu.roll(u, 1, 1)
            south_e[i, h] = v + pltpu.roll(v, LAST, 1)
            north_h[i, h] = (half_scale * HALINE_CON) * s[...] - (half_scale * THERM_EXP) * t[...]

    half_scale = HALF * PRESS_SCALE / K

    def both(tiles, k, m, f):
        return jnp.concatenate([tiles[0][f][block(k, m), :], tiles[1][f][block(k, m), :]], axis=1)

    def edge(rows, tails, f, i, at):
        return jnp.concatenate([rows[i, f, at, :], tails[i, f, at, :]], axis=1)

    wait_columns(0)

    @pl.when(has_n)
    def _():
        kmt_copy.wait_recv()

    @pl.when(has_s)
    def _():
        kmt_copy.wait_send()

    kmt2 = overlapped(kmt)
    kmt_edge = jnp.where(lane == 64, pltpu.roll(col_e[0, 0], 65, 1), kmt2[:, LANES:PADDED])
    kmt_row = padded(kmt_n[...]).astype(F32)
    kmt_north = jnp.concatenate([kmt_row[:, 0:LANES], jnp.where(lane1 < 64, kmt_row[:, LANES:PADDED], kmt_row[:, 0:LANES])], axis=1)
    mu = jnp.minimum(kmt2, roll_e(jnp.concatenate([kmt2[:, 0:LANES], kmt_edge], axis=1)))
    mv = jnp.minimum(kmt2, from_north(kmt2, kmt_north))
    faces[0] = linear(mu)
    faces[1] = linear(mv)

    def solve_factor(depth, k, first):
        inner, last = table[first * K + k], table[(first + 1) * K + k]
        kf = k.astype(F32)
        return jnp.where(depth > kf + 1.0, inner, jnp.where(depth > kf, last, ZERO))

    def momentum(i):
        def level(j, members):
            k = i * size + j
            kf = k.astype(F32)
            factor_u, factor_v = solve_factor(mu, k, 0), solve_factor(mv, k, 0)
            out = []
            for m in PAIR:
                total, total_n, gu_sum, gv_sum, side_u, side_v = members[m]
                at = pl.ds(2 * j + m, 1)
                u, v, t, s = (both((first, second), k, m, f) for f in QUAD)
                step = (half_scale * HALINE_CON) * s - (half_scale * THERM_EXP) * t
                pressure = total + step
                step_n = jnp.concatenate([north_h[i, 0, at, :], north_h[i, 1, at, :]], axis=1)
                pressure_n = total_n + step_n
                corner_n = pltpu.roll(corner_nw[i], 65 - (size * m + j), 1)[0:1]
                corner_s = pltpu.roll(corner_se[i], lax.rem(LANES + 63 - (size * (2 + m) + j), LANES), 1)[7:8]
                u_edge, v_edge = edge(rows_n, tail_n, 0, i, at), edge(rows_s, tail_s, 1, i, at)
                u_pair_n = jnp.concatenate([jnp.where(lane1 == 0, u_edge[:, 0:LANES] + corner_n, north_w[i, 0, at, :]), north_w[i, 1, at, :]], axis=1)
                v_pair_s = jnp.concatenate([south_e[i, 0, at, :], jnp.where(lane1 == 63, v_edge[:, LANES:PADDED] + corner_s, south_e[i, 1, at, :])], axis=1)
                v_e, v_w, u_e, u_w = roll_e(v), roll_w(v), roll_e(u), roll_w(u)
                v_pair, u_pair = v + v_e, u + u_w
                vu = 0.125 * (v_pair + from_south(v_pair, v_pair_s))
                uv = 0.125 * (u_pair + from_north(u_pair, u_pair_n))
                u_n, u_s = from_north(u, u_edge), from_south(u, edge(rows_s, tail_s, 0, i, at))
                v_n, v_s = from_north(v, edge(rows_n, tail_n, 1, i, at)), from_south(v, v_edge)
                p_n = from_north(pressure, pressure_n)
                gu = pressure - roll_e(pressure) - HALF * u * (u_e - u_w) - vu * (u_n - u_s)
                gv = pressure - p_n - uv * (v_e - v_w) - HALF * v * (v_n - v_s)
                gu = jnp.where(mu > kf, gu, ZERO)
                gv = jnp.where(mv > kf, gv, ZERO)
                side_u = (u + gu + VISC_NUMBER * side_u) * factor_u
                side_v = (v + gv + VISC_NUMBER * side_v) * factor_v
                pu[k, m] = linear(side_u)[:, KEEP]
                pv[k, m] = linear(side_v)[:, KEEP]
                out.append((pressure + step, pressure_n + step_n, gu_sum + gu, gv_sum + gv, side_u, side_v))
            return tuple(out)

        return level

    zero = jnp.zeros((ROWS, PADDED), F32)
    zero_row = jnp.zeros((1, PADDED), F32)
    members = ((zero, zero_row, zero, zero, zero, zero),) * 2
    for i in range(chunks):
        if i > 0:
            wait_columns(i)
        insert_columns(i)

        @pl.when(has_n)
        def _():
            south_copy(i).wait_recv()
            corner_u(i).wait_recv()

        @pl.when(has_s)
        def _():
            north_copy(i).wait_recv()
            corner_v(i).wait_recv()

        unpack_rows(i)
        members = lax.fori_loop(0, size, momentum(i), members, unroll=UNROLL)

        if i == 0:
            for copy in edge_copies:
                copy.wait()
            for p in range(7):
                wide[p, own, :] = with_edges(wide[p, own, :], edge_e[p], edge_w[p])
            static_copies = spread(wide, 0)
            start_spread(static_copies)

    count_u = linear(jnp.maximum(mu, 1.0))
    count_v = linear(jnp.maximum(mv, 1.0))
    for m in PAIR:
        wide_f[m, own, :] = linear(members[m][2]) / count_u
        wide_f[2 + m, own, :] = linear(members[m][3]) / count_v
    force_edges = edge_pair(wide_f, fedge_w, fedge_e, 3)
    for copy in force_edges:
        copy.start()

    def tracers(i, carry):
        def level(j, carry):
            k = i * size + j
            factor = solve_factor(kmt2, k, 3)
            out = []
            for m in PAIR:
                at = pl.ds(2 * j + m, 1)
                u, v = (HALF * both((first, second), k, m, f) for f in PAIR)
                u_w = roll_w(u)
                v_edge = HALF * edge(rows_s, tail_s, 1, i, at)
                for f, dest in ((2, pt), (3, ps)):
                    t = both((first, second), k, m, f)
                    flux_x = u * (t + roll_e(t)) - u_w * (t + roll_w(t))
                    flux_y = v * (t + from_north(t, edge(rows_n, tail_n, f, i, at)))
                    flux_s = v_edge * (edge(rows_s, tail_s, f, i, at) + t[0:1])
                    moved = t - (flux_x + flux_y - from_south(flux_y, flux_s))
                    side = (moved + DIFF_NUMBER * carry[len(out)]) * factor
                    dest[k, m] = linear(side)[:, KEEP]
                    out.append(side)
            return tuple(out)

        return lax.fori_loop(0, size, level, carry, unroll=UNROLL)

    tail = (zero,) * 4
    split = (3 * chunks + 4) // 5
    tail = lax.fori_loop(0, split, tracers, tail)

    relay_spread(static_copies)
    for copy in force_edges:
        copy.wait()
    for p in QUAD:
        wide_f[p, own, :] = with_edges(wide_f[p, own, :], fedge_e[p], fedge_w[p])
    force_copies = spread(wide_f, 6)
    start_spread(force_copies)

    tail = lax.fori_loop(split, chunks, tracers, tail)

    def back_tracers(j, carry):
        k = K - 2 - j
        ratio = table[5 * K + k]
        out = []
        for m in PAIR:
            for dest in (pt, ps):
                x = dest[k, m] + ratio * carry[len(out)]
                dest[k, m] = x
                out.append(x)
        return tuple(out)

    relay_spread(force_copies)
    lax.fori_loop(0, K - 1, back_tracers, tuple(linear(x)[:, KEEP] for x in tail), unroll=2)

    def back(j, carry):
        k = K - 2 - j
        ratio = table[2 * K + k]
        out = []
        for m in PAIR:
            xu, xv, su, sv = carry[m]
            xu = pu[k, m] + ratio * xu
            xv = pv[k, m] + ratio * xv
            pu[k, m] = xu
            pv[k, m] = xv
            out.append((xu, xv, su + xu, sv + xv))
        return tuple(out)

    start = tuple(tuple(linear(members[m][n])[:, KEEP] for n in (4, 5, 4, 5)) for m in PAIR)
    ends = lax.fori_loop(0, K - 1, back, start)

    finish_spread(static_copies)
    finish_spread(force_copies)

    depth = wide[0]
    depth_e = pltpu.roll(depth, PADDED - 1, 1)
    depth_n = pltpu.roll(depth, 79, 0)
    hu = jnp.where((depth > ZERO) & (depth_e > ZERO), HALF * (depth + depth_e), ZERO)
    hv = jnp.where((depth > ZERO) & (depth_n > ZERO), HALF * (depth + depth_n), ZERO)
    coef[0] = WAVE_COURANT * WAVE_COURANT * hu
    coef[1] = WAVE_COURANT * WAVE_COURANT * hv
    for m in PAIR:
        force[m] = hu * wide_f[m] * (WAVE_COURANT / SUBCYCLES)
        force[2 + m] = hv * wide_f[2 + m] * (WAVE_COURANT / SUBCYCLES)
        state[m] = wide[1 + m]
        state[2 + m] = WAVE_COURANT * wide[3 + m]
        state[4 + m] = WAVE_COURANT * wide[5 + m]
        state[6 + m] = pltpu.roll(wide[1 + m], PADDED - 1, 1)
    mine = slice(HALO, HALO + ROWS)
    for p, (h, count) in enumerate(((hu[mine], count_u), (hv[mine], count_v))):
        faces[2 + p] = 1.0 / (WAVE_COURANT * jnp.where(h > ZERO, h, 1.0))
        for m in PAIR:
            mean[2 * p + m] = padded(ends[m][2 + p]) / count

    for i in range(chunks):
        west_copy(i).wait_send()
        east_copy(i).wait_send()

    @pl.when(has_s)
    def _():
        for i in range(chunks):
            south_copy(i).wait_send()
            corner_u(i).wait_send()

    @pl.when(has_n)
    def _():
        for i in range(chunks):
            north_copy(i).wait_send()
            corner_v(i).wait_send()


def finish_kernel(
    K, size,
    weights, pu, pv, pt, ps, mean, faces, coef, force, first_state,
    eta_o, tx_o, ty_o, u_o, v_o, t_o, s_o,
    state, avg, small, out_u, out_v, sems,
):
    chunks = K // size
    through = [pltpu.make_async_copy(src, dst, sems.at[i, 0]) for i, (src, dst) in enumerate(((pt, t_o), (ps, s_o)))]
    for copy in through:
        copy.start()
    state[...] = first_state[...]
    avg[...] = jnp.zeros_like(avg)

    def subcycles(first, last, margin):
        height = ROWS + 2 * margin
        rows = pl.ds(HALO - margin, height)
        mine = slice(margin, margin + ROWS)

        def to_e(x):
            return pltpu.roll(x, PADDED - 1, 1)

        def subcycle(n, _):
            weight = weights[n]
            for m in PAIR:
                tx, ty = state[2 + m, rows], state[4 + m, rows]
                tx_e, ty_e = to_e(tx), to_e(ty)
                eta = state[m, rows] - (tx - pltpu.roll(tx, 1, 1) + ty - pltpu.roll(ty, 1, 0))
                eta_e = state[6 + m, rows] - (tx_e - tx + ty_e - pltpu.roll(ty_e, 1, 0))
                tx = tx + force[m, rows] - coef[0, rows] * (eta_e - eta)
                ty = ty + force[2 + m, rows] - coef[1, rows] * (pltpu.roll(eta, height - 1, 0) - eta)
                for p, x in enumerate((eta, tx, ty)):
                    state[2 * p + m, rows] = x
                    avg[2 * p + m] = avg[2 * p + m] + weight * x[mine]
                state[6 + m, rows] = eta_e
            return 0

        lax.fori_loop(first, last, subcycle, 0)

    done = 0
    for margin in (HALO, 24, ROWS, 8):
        last = SUBCYCLES - (margin - 8)
        subcycles(done, last, margin)
        done = last

    corr = []
    for m in PAIR:
        small[0, m] = avg[m][:, KEEP]
        for p in PAIR:
            transport = avg[2 + 2 * p + m]
            small[1 + p, m] = (transport * (1.0 / WAVE_COURANT))[:, KEEP]
            corr.append((transport * faces[2 + p] - mean[2 * p + m])[:, KEEP])
    for p, dest in enumerate((eta_o, tx_o, ty_o)):
        through.append(pltpu.make_async_copy(small.at[p], dest, sems.at[2, p]))
        through[-1].start()
    depth_u, depth_v = faces[0][:, KEEP], faces[1][:, KEEP]

    def out_copies(i):
        levels = pl.ds(i * size, size)
        return [pltpu.make_async_copy(src.at[levels], dst.at[levels], sems.at[p, 1 + i]) for p, (src, dst) in enumerate(((out_u, u_o), (out_v, v_o)))]

    for i in range(chunks):
        def level(j, _):
            k = i * size + j
            kf = k.astype(F32)
            for m in PAIR:
                out_u[k, m] = jnp.where(depth_u > kf, pu[k, m] + corr[2 * m], ZERO)
                out_v[k, m] = jnp.where(depth_v > kf, pv[k, m] + corr[2 * m + 1], ZERO)
            return 0

        lax.fori_loop(0, size, level, 0, unroll=UNROLL)
        for copy in out_copies(i):
            copy.start()

    for copy in through + [copy for i in range(chunks) for copy in out_copies(i)]:
        copy.wait()


def solution(mesh):
    col_count, row_count = mesh.shape["col"], mesh.shape["row"]

    def local_step(vel_x, vel_y, pot_temp, salinity, surf_eta, trans_x, trans_y, col_depth, wet_levels, avg_weights):
        K = vel_x.shape[0]
        size = level_chunk(K)
        chunks = K // size
        edge_rows = (2 * size + 7) // 8 * 8
        table = jnp.asarray(solve_tables(K))
        smem = pl.BlockSpec(memory_space=pltpu.SMEM)
        vmem = pl.BlockSpec(memory_space=pltpu.VMEM)
        hbm = pl.BlockSpec(memory_space=pl.ANY)
        full = jax.ShapeDtypeStruct((K, 2, ROWS, WIDTH), F32)
        held = pltpu.VMEM((K, 2, ROWS, WIDTH), F32)
        dma = pltpu.SemaphoreType.DMA
        outs = pl.pallas_call(
            functools.partial(step_kernel, row_count, col_count, K),
            out_shape=(held,) * 4 + tuple(pltpu.VMEM((n, ROWS, PADDED), F32) for n in (4, 4)) + tuple(pltpu.VMEM((n, 80, PADDED), F32) for n in (2, 4, 8)),
            in_specs=[smem] + [vmem] * 5 + [hbm] * 4,
            out_specs=(vmem,) * 9,
            scratch_shapes=[
                *[pltpu.VMEM((K * 2 * ROWS, WIDTH), F32)] * 4,
                *[pltpu.VMEM((K * 2 * ROWS, LANES), F32)] * 8,
                *[pltpu.VMEM((chunks, 6, edge_rows, LANES), F32)] * 4,
                *[pltpu.VMEM((chunks, 4, edge_rows, LANES), F32)] * 2,
                *[pltpu.VMEM((chunks, 2, edge_rows, LANES), F32)] * 3,
                pltpu.VMEM((1, WIDTH), jnp.int32),
                *[pltpu.VMEM((chunks, 2, ROWS, LANES), F32)] * 3,
                *[pltpu.VMEM((chunks, 8, LANES), F32)] * 2,
                *[pltpu.VMEM((7, ROWS, LANES), F32)] * 2,
                pltpu.VMEM((7, 80, PADDED), F32),
                *[pltpu.VMEM((4, ROWS, LANES), F32)] * 2,
                pltpu.VMEM((4, 80, PADDED), F32),
                dma((chunks, 4)), dma((2, chunks)), dma((2, chunks)), dma((4, chunks)), dma((4, chunks)), dma((5,)), dma((5,)), dma((12,)), dma((12,)),
            ],
            compiler_params=pltpu.CompilerParams(collective_id=0, has_side_effects=True, vmem_limit_bytes=52 << 20),
            name="ocean_step",
        )(table, wet_levels, col_depth, surf_eta, trans_x, trans_y, *(x.reshape(-1, WIDTH) for x in (vel_x, vel_y, pot_temp, salinity)))

        small = jax.ShapeDtypeStruct((2, ROWS, WIDTH), F32)
        return pl.pallas_call(
            functools.partial(finish_kernel, K, size),
            out_shape=(small,) * 3 + (full,) * 4,
            in_specs=[smem] + [vmem] * 9,
            out_specs=(hbm,) * 7,
            scratch_shapes=[
                pltpu.VMEM((8, 80, PADDED), F32),
                pltpu.VMEM((6, ROWS, PADDED), F32),
                pltpu.VMEM((3, 2, ROWS, WIDTH), F32),
                *[pltpu.VMEM((K, 2, ROWS, WIDTH), F32)] * 2,
                dma((3, 2 + chunks)),
            ],
            compiler_params=pltpu.CompilerParams(vmem_limit_bytes=20 << 20),
            name="ocean_finish",
        )(avg_weights, *outs)

    spec_3d = P(None, None, "row", "col")
    spec_2d = P(None, "row", "col")
    spec_map = P("row", "col")
    return jax.shard_map(local_step, mesh=mesh, in_specs=(spec_3d,) * 4 + (spec_2d,) * 3 + (spec_map,) * 2 + (P(),), out_specs=(spec_2d,) * 3 + (spec_3d,) * 4, check_vma=False)
```
